32 devices in a mesh: dp: 2 (over y), expert: 4 (over z), shard: 4 (over x, core).
Axes of the slice: x: 2, y: 2, z: 4, core: 2. Of those that a mesh axis runs over, the one named last changes fastest.
Arguments:
- tokens: bfloat16 [32768, 768], P(('dp', 'expert', 'shard')), may hold values from -6 to 6
- lengths: int32 [32], P(('dp', 'expert', 'shard')), may hold values from 256 to 1024, as said below
- routes: int32 [32768, 2], P(('dp', 'expert', 'shard')), may hold values from 0 to 7, all different within a row; in each aligned block of 1024 rows (0 to 1023, 1024 to 2047, ...) at most 288 rows name the same one
- route_gates: float32 [32768, 2], P(('dp', 'expert', 'shard')), may hold values from 0.2 to 1
- cotangent: bfloat16 [32768, 768], P(('dp', 'expert', 'shard')), may hold values from -6 to 6
- norm_gains: bfloat16 [2, 768], P(None, ('dp', 'shard')), may hold values from 0.25 to 1.75
- w_qkv: bfloat16 [768, 2304], P(('dp', 'shard')), may hold values from -0.21875 to 0.21875
- w_out: bfloat16 [768, 768], P(('dp', 'shard')), may hold values from -1.75 to 1.75
- w_shared_gu: bfloat16 [768, 4096], P(('dp', 'shard')), may hold values from -0.21875 to 0.21875
- w_shared_down: bfloat16 [2048, 768], P(('dp', 'shard')), may hold values from -0.125 to 0.125
- w_expert_gu: bfloat16 [8, 768, 4096], P('expert'), may hold values from -0.21875 to 0.21875
- w_expert_down: bfloat16 [8, 2048, 768], P('expert'), may hold values from -0.125 to 0.125
Outputs:
- layer_out: bfloat16 [32768, 768], P(('dp', 'expert', 'shard'))
- input_grad: float32 [32768, 768], P(('dp', 'expert', 'shard'))
- gains_grad: float32 [2, 768], P(None, ('dp', 'shard'))
- qkv_grad: float32 [768, 2304], P(('dp', 'shard'))
- out_proj_grad: float32 [768, 768], P(('dp', 'shard'))
- shared_gu_grad: float32 [768, 4096], P(('dp', 'shard'))
- shared_down_grad: float32 [2048, 768], P(('dp', 'shard'))
- expert_gu_grad: float32 [8, 768, 4096], P('expert', None, ('dp', 'shard'))
- expert_down_grad: float32 [8, 2048, 768], P('expert', ('dp', 'shard'))
The draws below stay inside these ranges and needn't reach their ends.
Inputs may be any that keep to these rules, and one draw needn't show every extreme that they name: `lengths`: each sequence has at least a quarter of its slots live, and some sequence is full. `routes`: each row names 2 different experts; in the rows of one device (aligned blocks of 1024 rows, padded positions included) no expert is named by more than 288 rows.
All inputs are finite; a program needn't handle non-finite values.
Results may differ from the reference program's by a relative error of at most 0.014.
Values may be sent and summed in bfloat16 or wider, within the bound.
A program may use at most 384 MiB of HBM per device.

```python
import math
import jax
import jax.numpy as jnp
import numpy as np
from jax import lax

D = 768
HEADS = 12
HEAD_DIM = 64
FF = 2048
SFF = 2048
TOPK = 2
LENGTH = 1024
EXPERTS = 8
TOK_DEV = 1024
SEQS = 32
TOKENS = 32768
CAP = 288
N_DP = 2
N_EXPERT = 4
N_SHARD = 4


def draw_lengths(key, part):
    first_key, second_key = jax.random.split(key)
    drawn_len = jax.random.randint(first_key, (SEQS,), LENGTH // 4, LENGTH + 1)
    chosen = jax.random.randint(second_key, (), 0, SEQS)
    return jnp.where(lax.iota(jnp.int32, SEQS) == chosen, LENGTH, drawn_len).astype(jnp.int32)


def shard_levels(key, shape, cuts, low, top_value):
    level, own = 1.0, jax.random.fold_in(key, 6)
    for dim, blocks in cuts:
        steps = jnp.exp(jax.random.uniform(jax.random.fold_in(own, dim), (blocks,), jnp.float32, low / len(cuts), top_value / len(cuts)))
        level = level * jnp.repeat(steps, shape[dim] // blocks).reshape([-1 if axis == dim else 1 for axis in range(len(shape))])
    return level


def assign_block(stream_key, own, number, rows, count, top, reach, skew):
    order = jax.random.permutation(stream_key, count)
    heavy_load, common = portions_of(count, rows * top, reach, skew, True), portions_of(count, rows * top, reach, skew, False)
    places = jnp.arange(count)

    def named(tallies, offset_by):
        used = int((tallies > 0).sum())
        fixed = max(1, used // 4)
        moved = fixed + (places - fixed + offset_by * (used - fixed)) % max(1, count - fixed)
        return jnp.zeros((count,), jnp.int32).at[order[jnp.where(places < fixed, places, moved)]].set(jnp.asarray(tallies, jnp.int32))

    tallies = jnp.where(number % 4 == 0, named(heavy_load, number // 4), named(common, number - number // 4 - 1))
    mixed = jax.random.permutation(jax.random.fold_in(own, 3), count)
    giver, taker = mixed[0:count // 2 * 2:2], mixed[1:count // 2 * 2:2]
    slack = jnp.minimum(tallies[giver] - 1, reach - tallies[taker]) // 2
    slack = jnp.where((giver == order[0]) | (taker == order[0]) | (tallies[taker] == 0), 0, jnp.maximum(slack, 0))
    moved = jax.random.randint(jax.random.fold_in(own, 4), (count // 2,), 0, 1 << 20) % (slack + 1)
    tallies = tallies.at[giver].add(-moved).at[taker].add(moved)
    items = jnp.searchsorted(jnp.cumsum(tallies), jnp.arange(rows * top), side="right").astype(jnp.int32)
    table = items.reshape(top, rows).T
    table = table[jax.random.permutation(jax.random.fold_in(own, 1), rows)]
    offset_by = jax.random.randint(jax.random.fold_in(own, 2), (rows, 1), 0, top)
    return jnp.take_along_axis(table, (jnp.arange(top)[None, :] + offset_by) % top, axis=1)


def portions_of(number_of, total, reach, skew, full):
    weights = [(1 << 20) // math.isqrt(grade ** skew) + 1 for grade in range(1, number_of + 1)]
    largest = reach if full else min(reach, max(-(-total // number_of), total * weights[0] // sum(weights)))
    least = 1 if total - largest >= number_of - 1 else 0
    counts, spare = [largest] + [least] * (number_of - 1), total - largest - least * (number_of - 1)
    while spare > 0:
        movable = [i for i in range(1, number_of) if counts[i] < largest] or [i for i in range(1, number_of) if counts[i] < reach]
        pool, remaining = sum([weights[i] for i in movable]), spare
        for i in movable:
            extra = min(reach - counts[i], max(1, remaining * weights[i] // pool), spare)
            counts[i] = counts[i] + extra
            spare = spare - extra
    return np.array(counts)


def normal_values(own_key, shape, scale, most, shards=(), held_as=jnp.bfloat16):
    drawn = scale * jax.random.normal(own_key, shape, jnp.float32)
    if shards:
        drawn = drawn * shard_levels(own_key, shape, shards, -0.22, 0.18)
    return jnp.clip(drawn, -most, most).astype(held_as)


def setup_inputs(seed: int = 0) -> dict:
    key_list = jax.random.split(jax.random.key(seed), 13)
    tokens = normal_values(key_list[0], (TOKENS, D), 1.0, 6.0, ((0, 32),))
    lengths = draw_lengths(jax.random.fold_in(key_list[12], 71), 0)
    routes_keys = jax.random.split(jax.random.fold_in(key_list[2], 1), TOKENS // TOK_DEV)
    routes_turns = jax.random.permutation(jax.random.fold_in(key_list[2], 3), TOKENS // TOK_DEV)
    routes = jax.vmap(lambda own, number: assign_block(jax.random.fold_in(key_list[2], 2), own, number, TOK_DEV, EXPERTS, TOPK, CAP, 1))(routes_keys, routes_turns).reshape((TOKENS, TOPK))
    route_gates = jnp.clip(0.2 + 0.8 * jax.random.uniform(key_list[3], (TOKENS, TOPK), jnp.float32) ** shard_levels(key_list[3], (TOKENS, TOPK), ((0, 32),), -0.2, 0.2), 0.2, 1.0)
    cotangent = normal_values(key_list[4], (TOKENS, D), 1.0, 6.0, ((0, 32),))
    norm_gains = jnp.clip(1.0 + 0.15 * jax.random.normal(key_list[5], (2, D), jnp.float32), 0.25, 1.75).astype(jnp.bfloat16)
    w_qkv = normal_values(key_list[6], (D, 3 * D), D ** -0.5, 0.21875, ((0, 8),))
    w_out = normal_values(key_list[7], (D, D), (D // 64) ** -0.5, 1.75, ((0, 8),))
    w_shared_gu = normal_values(key_list[8], (D, 2 * SFF), D ** -0.5, 0.21875, ((0, 8),))
    w_shared_down = normal_values(key_list[9], (SFF, D), SFF ** -0.5, 0.125, ((0, 8),))
    w_expert_gu = normal_values(key_list[10], (EXPERTS, D, 2 * FF), D ** -0.5, 0.21875, ((0, 4),))
    w_expert_down = normal_values(key_list[11], (EXPERTS, FF, D), FF ** -0.5, 0.125, ((0, 4),))
    return {"tokens": tokens, "lengths": lengths, "routes": routes, "route_gates": route_gates, "cotangent": cotangent, "norm_gains": norm_gains, "w_qkv": w_qkv, "w_out": w_out, "w_shared_gu": w_shared_gu, "w_shared_down": w_shared_down, "w_expert_gu": w_expert_gu, "w_expert_down": w_expert_down}


epsilon = 1e-05
highest_precision = lax.Precision.HIGHEST

@jax.custom_vjp
def low(v):
    return lax.optimization_barrier(v.astype(jnp.bfloat16)).astype(jnp.float32)

@jax.custom_vjp
def low_back(v):
    return v

def low_keep(v):
    return (low(v), None)

def low_pass(kept, grad):
    return (grad,)

def back_keep(v):
    return (v, None)

def back_low(kept, grad):
    return (low(grad),)
low.defvjp(low_keep, low_pass)
low_back.defvjp(back_keep, back_low)

def rotary_tables(length, head_dim):
    half_dim = head_dim // 2
    position = lax.iota(jnp.float32, length)[:, None]
    frequency = jnp.exp(lax.iota(jnp.float32, half_dim) * (-2.0 * math.log(10000.0) / head_dim))
    angle_table = position * frequency[None, :]
    return (jnp.cos(angle_table)[:, None, :], jnp.sin(angle_table)[:, None, :])

def rotate(values, cosine_table, sine_table):
    half_dim = values.shape[-1] // 2
    front_half = values[..., :half_dim]
    back_half = values[..., half_dim:]
    return jnp.concatenate([front_half * cosine_table - back_half * sine_table, back_half * cosine_table + front_half * sine_table], axis=-1)

def attend_sequence(packed):
    queries, keys_rot, values_h = packed
    length = queries.shape[0]
    scores = low_back(jnp.einsum('qhd,khd->hqk', queries, keys_rot, precision=highest_precision))
    allowed = lax.iota(jnp.int32, length)[:, None] >= lax.iota(jnp.int32, length)[None, :]
    scores = jnp.where(allowed, scores, -1e+30)
    row_peak = lax.optimization_barrier(jnp.max(scores, axis=2, keepdims=True))
    row_expo = jnp.exp(scores - row_peak)
    probs_full = low(row_expo / lax.optimization_barrier(jnp.sum(row_expo, axis=2, keepdims=True)))
    mixed_out = jnp.einsum('hqk,khd->qhd', probs_full, values_h, precision=highest_precision)
    return low_back(low(mixed_out))

def expert_apply(packed):
    slot_rows, gate_up_weight, down_weight = packed
    hidden_units = down_weight.shape[0]
    gate_up = low_back(jnp.dot(slot_rows, gate_up_weight, precision=highest_precision, preferred_element_type=jnp.float32))
    activated = low(jax.nn.silu(gate_up[:, :hidden_units]) * gate_up[:, hidden_units:])
    return low_back(low(jnp.dot(activated, down_weight, precision=highest_precision, preferred_element_type=jnp.float32)))

def reference(tokens, lengths, routes, route_gates, cotangent, norm_gains, w_qkv, w_out, w_shared_gu, w_shared_down, w_expert_gu, w_expert_down):
    device_count = N_DP * N_EXPERT * N_SHARD
    slot_total = EXPERTS * device_count * CAP
    token_index = lax.iota(jnp.int32, TOKENS)
    live_bool = token_index % LENGTH < jnp.take(lengths, token_index // LENGTH)
    live_mask = live_bool.astype(jnp.float32)[:, None]
    flat_expert = routes.reshape(device_count, TOK_DEV * TOPK)
    live_row = jnp.repeat(live_bool, TOPK).reshape(device_count, TOK_DEV * TOPK)
    onehot = ((flat_expert[:, :, None] == lax.iota(jnp.int32, EXPERTS)[None, None, :]) & live_row[:, :, None]).astype(jnp.int32)
    slot_index = lax.optimization_barrier(jnp.sum(onehot * jnp.cumsum(onehot, axis=1), axis=2)) - 1
    device_index = lax.iota(jnp.int32, device_count)[:, None]
    destination = jnp.where(live_row, flat_expert * (device_count * CAP) + device_index * CAP + slot_index, slot_total).reshape(TOKENS * TOPK).astype(jnp.int32)
    slot_row = jnp.full((slot_total,), TOKENS * TOPK, jnp.int32).at[destination].set(lax.iota(jnp.int32, TOKENS * TOPK), mode='drop')
    slot_token = (slot_row // TOPK).astype(jnp.int32)
    gate_rows = route_gates.astype(jnp.float32)
    cosine_table, sine_table = rotary_tables(LENGTH, HEAD_DIM)
    query_scale = 1.0 / math.sqrt(HEAD_DIM)

    def forward(source, gains, qkv_weight, out_weight, sgu_weight, sdown_weight, egu_weight, edown_weight):
        scale_one = lax.rsqrt(lax.optimization_barrier(jnp.mean(source * source, axis=1, keepdims=True)) + epsilon)
        normed_one = low(source * scale_one * gains[0])
        qkv_proj = low_back(jnp.dot(normed_one, qkv_weight, precision=highest_precision, preferred_element_type=jnp.float32))
        shaped = qkv_proj.reshape(SEQS, LENGTH, 3, HEADS, HEAD_DIM)
        queries = low(rotate(shaped[:, :, 0], cosine_table, sine_table) * query_scale)
        keys_rot = low(rotate(shaped[:, :, 1], cosine_table, sine_table))
        values_h = low(shaped[:, :, 2])
        mixed_out = lax.map(jax.checkpoint(attend_sequence), (queries, keys_rot, values_h)).reshape(TOKENS, D)
        attn_out = low_back(jnp.dot(mixed_out, out_weight, precision=highest_precision, preferred_element_type=jnp.float32))
        first_sum = source + attn_out
        scale_two = lax.rsqrt(lax.optimization_barrier(jnp.mean(first_sum * first_sum, axis=1, keepdims=True)) + epsilon)
        normed_two = low(first_sum * scale_two * gains[1])
        shared_gu = low_back(jnp.dot(normed_two, sgu_weight, precision=highest_precision, preferred_element_type=jnp.float32))
        shared_hidden = low(jax.nn.silu(shared_gu[:, :SFF]) * shared_gu[:, SFF:])
        shared_out = low_back(jnp.dot(shared_hidden, sdown_weight, precision=highest_precision, preferred_element_type=jnp.float32))
        padded_normed = jnp.concatenate([normed_two, jnp.zeros((1, D), jnp.float32)], axis=0)
        expert_rows = low_back(jnp.take(padded_normed, slot_token, axis=0)).reshape(EXPERTS, device_count * CAP, D)
        expert_out = lax.map(jax.checkpoint(expert_apply), (expert_rows, egu_weight, edown_weight)).reshape(slot_total, D)
        padded_out = jnp.concatenate([expert_out, jnp.zeros((1, D), jnp.float32)], axis=0)
        picked = jnp.take(padded_out, destination, axis=0).reshape(TOKENS, TOPK, D)
        moe_out = lax.optimization_barrier(jnp.sum(picked * gate_rows[:, :, None], axis=1))
        return live_mask * (first_sum + shared_out + moe_out)
    layer_out, pullback = jax.vjp(forward, tokens.astype(jnp.float32), norm_gains.astype(jnp.float32), w_qkv.astype(jnp.float32), w_out.astype(jnp.float32), w_shared_gu.astype(jnp.float32), w_shared_down.astype(jnp.float32), w_expert_gu.astype(jnp.float32), w_expert_down.astype(jnp.float32))
    gradients = pullback(cotangent.astype(jnp.float32))
    return (layer_out.astype(jnp.bfloat16), gradients[0], gradients[1], gradients[2], gradients[3], gradients[4], gradients[5], gradients[6], gradients[7])
```

```python
import functools
import math

import jax
import jax.numpy as jnp
from jax import lax
from jax.experimental import pallas as pl
from jax.experimental.pallas import tpu as pltpu
from jax.sharding import PartitionSpec as P


HEADS = 12
LANES = 128
EPSILON = 1e-05
VMEM_BYTES = 60 * 1024 * 1024
BF16 = jnp.bfloat16
F32 = jnp.float32


def call(kernel, grid, in_specs, out_specs, out_shape, scratch=(), flops=0, moved=0, trans=0):
    return pl.pallas_call(
        kernel,
        grid_spec=pltpu.PrefetchScalarGridSpec(
            num_scalar_prefetch=0,
            grid=grid,
            in_specs=in_specs,
            out_specs=out_specs,
            scratch_shapes=list(scratch),
        ),
        out_shape=out_shape,
        compiler_params=pltpu.CompilerParams(
            dimension_semantics=("arbitrary",) * len(grid), vmem_limit_bytes=VMEM_BYTES
        ),
        cost_estimate=pl.CostEstimate(flops=flops, bytes_accessed=moved, transcendentals=trans),
    )


def shape_of(shape, dtype):
    return jax.ShapeDtypeStruct(shape, dtype)


def whole(shape):
    return pl.BlockSpec(shape, lambda *_: (0,) * len(shape), pipeline_mode=pl.Buffered(1))


def dot_nn(left, right):
    return lax.dot_general(left, right, (((1,), (0,)), ((), ())), preferred_element_type=F32)


def dot_nt(left, right):
    return lax.dot_general(left, right, (((1,), (1,)), ((), ())), preferred_element_type=F32)


def dot_tn(left, right):
    return lax.dot_general(left, right, (((0,), (0,)), ((), ())), preferred_element_type=F32)


def rotary_tables(length, head_dim):
    half_dim = head_dim // 2
    position = lax.iota(F32, length)[:, None]
    frequency = jnp.exp(lax.iota(F32, half_dim) * (-2.0 * math.log(10000.0) / head_dim))
    angle_table = position * frequency[None, :]
    cosine, sine = jnp.cos(angle_table), jnp.sin(angle_table)
    repeats = LANES // head_dim
    return (
        jnp.tile(jnp.concatenate([cosine, cosine], axis=1), (1, repeats)),
        jnp.tile(jnp.concatenate([-sine, sine], axis=1), (1, repeats)),
    )


def turn(values, cosine, signed_sine, head_dim):
    lane = lax.broadcasted_iota(jnp.int32, values.shape, 1)
    half = head_dim // 2
    other = jnp.where(
        lane % head_dim < half,
        pltpu.roll(values, LANES - half, 1),
        pltpu.roll(values, half, 1),
    )
    return values * cosine + other * signed_sine


def attend_forward_kernel(
    head_dim, block, x_ref, wq_ref, wk_ref, wv_ref, cos_ref, sin_ref, q_ref, k_ref, v_ref, o_ref, lse_ref, lse_tile
):
    length = x_ref.shape[0]
    heads = LANES // head_dim
    x = x_ref[...]
    cosine, sine = cos_ref[...], sin_ref[...]
    scale = 1.0 / math.sqrt(head_dim)
    q_ref[...] = (turn(dot_nn(x, wq_ref[...]), cosine, sine, head_dim) * scale).astype(BF16)
    k_ref[...] = turn(dot_nn(x, wk_ref[...]), cosine, sine, head_dim).astype(BF16)
    v_ref[...] = dot_nn(x, wv_ref[...]).astype(BF16)
    lane = lax.broadcasted_iota(jnp.int32, (1, LANES), 1)
    own_lane = lax.broadcasted_iota(jnp.int32, (block, LANES), 1) // head_dim
    below = lax.broadcasted_iota(jnp.int32, (block, block), 0) >= lax.broadcasted_iota(
        jnp.int32, (block, block), 1
    )
    for first in range(0, length, block):
        rows = pl.ds(first, block)
        mixed = None
        logs = None
        for head in range(heads):
            select = (lane // head_dim == head).astype(F32).astype(BF16)
            queries = q_ref[rows, :] * select
            near = jnp.where(below, dot_nt(queries, k_ref[rows, :]), -1e30)
            peak = jnp.max(near, axis=1, keepdims=True)
            if first:
                far = dot_nt(queries, k_ref[pl.ds(0, first), :])
                peak = jnp.maximum(peak, jnp.max(far, axis=1, keepdims=True))
            near = jnp.exp(near - peak)
            total = jnp.sum(near, axis=1, keepdims=True)
            part = dot_nn(near.astype(BF16), v_ref[rows, :])
            if first:
                far = jnp.exp(far - peak)
                total = total + jnp.sum(far, axis=1, keepdims=True)
                part = part + dot_nn(far.astype(BF16), v_ref[pl.ds(0, first), :])
            part = part * (1.0 / total)
            log_total = jnp.broadcast_to(peak + jnp.log(total), (block, LANES))
            mixed = part if head == 0 else jnp.where(own_lane == head, part, mixed)
            logs = log_total if head == 0 else jnp.where(own_lane == head, log_total, logs)
        o_ref[rows, :] = mixed.astype(BF16)
        lse_tile[rows, :] = logs
    turned = lse_tile[...].T
    for head in range(heads):
        lse_ref[pl.ds(head * 8, 8), :] = turned[head * head_dim : head * head_dim + 8, :]


def attend_forward(normed, w_qkv, cosine, sine, length, head_dim):
    tokens, width = normed.shape
    seqs, pairs, heads = tokens // length, width // LANES, LANES // head_dim
    block = min(256, length)
    rows = pl.BlockSpec((length, LANES), lambda s, p: (s, p))

    def weight(part):
        return pl.BlockSpec((width, LANES), lambda s, p: (0, part * pairs + p))

    table = whole((length, LANES))
    return call(
        functools.partial(attend_forward_kernel, head_dim, block),
        (seqs, pairs),
        [pl.BlockSpec((length, width), lambda s, p: (s, 0)), weight(0), weight(1), weight(2), table, table],
        [rows, rows, rows, rows, pl.BlockSpec((8 * heads, length), lambda s, p: (s * pairs + p, 0))],
        [shape_of((tokens, width), BF16)] * 4 + [shape_of((seqs * pairs * 8 * heads, length), F32)],
        scratch=[pltpu.VMEM((length, LANES), F32)],
        flops=6 * tokens * width * width + 4 * tokens * length * width,
        moved=16 * tokens * width,
        trans=tokens * length * width // head_dim // 2,
    )(normed, w_qkv, w_qkv, w_qkv, cosine, sine)


def attend_backward_kernel(
    head_dim, block, q_ref, k_ref, v_ref, o_ref, g_ref, lse_ref, cos_ref, sin_ref, gq_ref, gk_ref, gv_ref, gq_acc
):
    length = q_ref.shape[0]
    heads = LANES // head_dim
    scale = 1.0 / math.sqrt(head_dim)
    product = (g_ref[...].astype(F32) * o_ref[...].astype(F32)).T
    inner = [
        jnp.sum(product[head * head_dim : (head + 1) * head_dim, :], axis=0, keepdims=True)
        for head in range(heads)
    ]
    gq_acc[...] = jnp.zeros_like(gq_acc)
    lane = lax.broadcasted_iota(jnp.int32, (1, LANES), 1)
    own_lane = lax.broadcasted_iota(jnp.int32, (block, LANES), 1) // head_dim
    above = lax.broadcasted_iota(jnp.int32, (block, block), 1) >= lax.broadcasted_iota(
        jnp.int32, (block, block), 0
    )
    for first in range(0, length, block):
        rows = pl.ds(first, block)
        keys_grad = None
        values_grad = None
        for head in range(heads):
            select = (lane // head_dim == head).astype(F32).astype(BF16)
            keys = k_ref[rows, :] * select
            values = v_ref[rows, :] * select
            log_total = lse_ref[pl.ds(head * 8, 1), :]
            pieces = [(first, block, True)]
            if first + block < length:
                pieces.append((first + block, length - first - block, False))
            keys_part = None
            values_part = None
            for start, count, diagonal in pieces:
                span = pl.ds(start, count)
                queries, grads = q_ref[span, :], g_ref[span, :]
                scores = dot_nt(keys, queries)
                probs = jnp.exp(scores - log_total[:, start : start + count])
                if diagonal:
                    probs = jnp.where(above, probs, 0.0)
                grad_probs = dot_nt(values, grads)
                grad_scores = (probs * (grad_probs - inner[head][:, start : start + count])).astype(BF16)
                piece_values = dot_nn(probs.astype(BF16), grads)
                piece_keys = dot_nn(grad_scores, queries)
                values_part = piece_values if values_part is None else values_part + piece_values
                keys_part = piece_keys if keys_part is None else keys_part + piece_keys
                gq_acc[span, :] += dot_tn(grad_scores, keys)
            keys_grad = keys_part if head == 0 else jnp.where(own_lane == head, keys_part, keys_grad)
            values_grad = values_part if head == 0 else jnp.where(own_lane == head, values_part, values_grad)
        gk_ref[rows, :] = turn(keys_grad, cos_ref[rows, :], -sin_ref[rows, :], head_dim).astype(BF16)
        gv_ref[rows, :] = values_grad.astype(BF16)
    gq_ref[...] = turn(gq_acc[...] * scale, cos_ref[...], -sin_ref[...], head_dim).astype(BF16)


def attend_backward(queries, keys, values, mixed, grad_mixed, lse, cosine, sine, length, head_dim):
    tokens, width = queries.shape
    seqs, pairs, heads = tokens // length, width // LANES, LANES // head_dim
    block = min(256, length)
    rows = pl.BlockSpec((length, LANES), lambda s, p: (s, p))
    table = whole((length, LANES))
    return call(
        functools.partial(attend_backward_kernel, head_dim, block),
        (seqs, pairs),
        [rows] * 5 + [pl.BlockSpec((8 * heads, length), lambda s, p: (s * pairs + p, 0)), table, table],
        [rows] * 3,
        [shape_of((tokens, width), BF16)] * 3,
        scratch=[pltpu.VMEM((length, LANES), F32)],
        flops=10 * tokens * length * width,
        moved=16 * tokens * width,
        trans=tokens * length * width // head_dim // 2,
    )(queries, keys, values, mixed, grad_mixed, lse, cosine, sine)


def norm_one_kernel(x_ref, gain_ref, out_ref):
    x = x_ref[...].astype(F32)
    scale = lax.rsqrt(jnp.mean(x * x, axis=1, keepdims=True) + EPSILON)
    out_ref[...] = (x * scale * gain_ref[...]).astype(BF16)


def norm_one(tokens, gain):
    rows, width = tokens.shape
    block = min(256, rows)
    blocked = pl.BlockSpec((block, width), lambda i: (i, 0))
    return call(
        norm_one_kernel, (rows // block,), [blocked, whole((1, width))], blocked, shape_of((rows, width), BF16),
        flops=5 * rows * width, moved=4 * rows * width,
    )(tokens, gain)


def norm_two_kernel(mixed_ref, tokens_ref, weight_ref, gain_ref, sum_ref, normed_ref):
    first_sum = tokens_ref[...].astype(F32) + dot_nn(mixed_ref[...], weight_ref[...])
    sum_ref[...] = first_sum
    scale = lax.rsqrt(jnp.mean(first_sum * first_sum, axis=1, keepdims=True) + EPSILON)
    normed_ref[...] = (first_sum * scale * gain_ref[...]).astype(BF16)


def norm_two(mixed, tokens, weight, gain):
    rows, width = tokens.shape
    block = min(256, rows)
    blocked = pl.BlockSpec((block, width), lambda i: (i, 0))
    return call(
        norm_two_kernel, (rows // block,), [blocked, blocked, whole((width, width)), whole((1, width))],
        [blocked, blocked], [shape_of((rows, width), F32), shape_of((rows, width), BF16)],
        flops=2 * rows * width * width, moved=10 * rows * width,
    )(mixed, tokens, weight, gain)


def slots_kernel(experts, capacity, routes_ref, live_ref, dest_ref):
    top, tokens = routes_ref.shape
    live = live_ref[...]
    number = lax.broadcasted_iota(jnp.int32, (experts, tokens), 0)
    hits = [
        jnp.where((routes_ref[pl.ds(k, 1), :] == number) & (live > 0), 1.0, 0.0) for k in range(top)
    ]
    earlier = jnp.where(
        lax.broadcasted_iota(jnp.int32, (tokens, tokens), 0)
        <= lax.broadcasted_iota(jnp.int32, (tokens, tokens), 1),
        1.0,
        0.0,
    ).astype(BF16)
    ranks = dot_nn(jnp.concatenate(hits, axis=0).astype(BF16), earlier)
    before = jnp.zeros((experts, 1), F32)
    for k in range(top):
        rank = ranks[k * experts : (k + 1) * experts, :]
        place = number.astype(F32) * capacity + before + rank - 1.0
        slot = jnp.sum(hits[k] * place, axis=0, keepdims=True).astype(jnp.int32)
        dest_ref[pl.ds(k, 1), :] = jnp.where(live > 0, slot, experts * capacity)
        before = before + jnp.sum(hits[k], axis=1, keepdims=True)


def slots_of(routes_t, live_row, experts, capacity):
    top, tokens = routes_t.shape
    return call(
        functools.partial(slots_kernel, experts, capacity), (1,),
        [whole((top, tokens)), whole((1, tokens))], whole((top, tokens)), shape_of((top, tokens), jnp.int32),
        flops=2 * top * experts * tokens * tokens, moved=16 * tokens,
    )(routes_t, live_row)


def dispatch_kernel(gated, first, dest_ref, gates_ref, x_ref, out_ref):
    top, tokens = dest_ref.shape
    capacity = out_ref.shape[0]
    slot = lax.broadcasted_iota(jnp.int32, (capacity, tokens), 0) + (first + pl.program_id(0)) * capacity
    hits = [slot == dest_ref[pl.ds(k, 1), :] for k in range(top)]
    chosen = functools.reduce(jnp.logical_or, hits)
    rows = dot_nn(jnp.where(chosen, 1.0, 0.0).astype(BF16), x_ref[...])
    if gated:
        weights = jnp.zeros((capacity, tokens), F32)
        for k in range(top):
            weights = jnp.where(hits[k], gates_ref[pl.ds(k, 1), :], weights)
        rows = rows * jnp.sum(weights, axis=1, keepdims=True)
    out_ref[...] = rows.astype(BF16)


def dispatch(dest_t, gates_t, x, experts, capacity, gated, first):
    top, tokens = dest_t.shape
    width = x.shape[1]
    return call(
        functools.partial(dispatch_kernel, gated, first), (experts,),
        [whole((top, tokens)), whole((top, tokens)), whole((tokens, width))],
        pl.BlockSpec((capacity, width), lambda e: (e, 0)),
        shape_of((experts * capacity, width), BF16),
        flops=2 * experts * capacity * tokens * width, moved=2 * (experts * capacity + tokens) * width,
    )(dest_t, gates_t, x)


def combine_kernel(parts, dest_ref, gates_ref, live_ref, sum_ref, shared_ref, *rest):
    y_refs, out_ref = rest[:parts], rest[parts]
    block, top = dest_ref.shape
    total = sum_ref[...] + shared_ref[...]
    dest = dest_ref[...]
    gates = gates_ref[...]
    for index, y_ref in enumerate(y_refs):
        y = y_ref[...]
        slot = slot_numbers(block, y_ref.shape[0], index)
        for k in range(top):
            hit = jnp.where(slot == dest[:, k : k + 1], 1.0, 0.0).astype(BF16)
            total = total + dot_nn(hit, y) * gates[:, k : k + 1]
    out_ref[...] = (live_ref[...] * total).astype(BF16)


def slot_numbers(block, slots, index):
    return lax.broadcasted_iota(jnp.int32, (block, slots), 1) + index * slots


def combine(dest, gates, live, first_sum, shared_out, returned):
    rows, width = first_sum.shape
    top = dest.shape[1]
    block = min(256, rows)
    parts = len(returned)
    blocked = pl.BlockSpec((block, width), lambda i: (i, 0))
    narrow = pl.BlockSpec((block, top), lambda i: (i, 0))
    slots = sum(y.shape[0] for y in returned)
    return call(
        functools.partial(combine_kernel, parts), (rows // block,),
        [narrow, narrow, pl.BlockSpec((block, 1), lambda i: (i, 0)), blocked, blocked]
        + [whole(y.shape) for y in returned],
        blocked, shape_of((rows, width), BF16),
        flops=4 * rows * slots * width, moved=10 * rows * width + 2 * slots * width,
    )(dest, gates, live, first_sum, shared_out, *returned)


def norm_two_back_kernel(parts, dest_ref, live_ref, cot_ref, sum_ref, shared_ref, gain_ref, *rest):
    y_refs = rest[:parts]
    first_ref, attn_ref, gain_grad_ref = rest[parts:]
    block, top = dest_ref.shape
    grad_normed = shared_ref[...]
    dest = dest_ref[...]
    for index, y_ref in enumerate(y_refs):
        slot = slot_numbers(block, y_ref.shape[0], index)
        hit = functools.reduce(jnp.logical_or, [slot == dest[:, k : k + 1] for k in range(top)])
        grad_normed = grad_normed + dot_nn(jnp.where(hit, 1.0, 0.0).astype(BF16), y_ref[...])
    first_sum = sum_ref[...]
    scale = lax.rsqrt(jnp.mean(first_sum * first_sum, axis=1, keepdims=True) + EPSILON)
    weighted = grad_normed * gain_ref[...]
    inner = jnp.mean(first_sum * weighted, axis=1, keepdims=True)
    grad_first = (
        cot_ref[...].astype(F32) * live_ref[...] + scale * weighted - first_sum * (scale * scale * scale * inner)
    )
    first_ref[...] = grad_first
    attn_ref[...] = grad_first.astype(BF16)

    @pl.when(pl.program_id(0) == 0)
    def _():
        gain_grad_ref[...] = jnp.zeros_like(gain_grad_ref)

    gain_grad_ref[...] += jnp.sum(grad_normed * first_sum * scale, axis=0, keepdims=True)


def norm_two_back(dest, live, cotangent, first_sum, grad_shared, gain, returned):
    rows, width = first_sum.shape
    top = dest.shape[1]
    block = min(256, rows)
    parts = len(returned)
    blocked = pl.BlockSpec((block, width), lambda i: (i, 0))
    slots = sum(y.shape[0] for y in returned)
    return call(
        functools.partial(norm_two_back_kernel, parts), (rows // block,),
        [pl.BlockSpec((block, top), lambda i: (i, 0)), pl.BlockSpec((block, 1), lambda i: (i, 0)), blocked, blocked,
         blocked, whole((1, width))]
        + [whole(y.shape) for y in returned],
        [blocked, blocked, pl.BlockSpec((1, width), lambda i: (0, 0))],
        [shape_of((rows, width), F32), shape_of((rows, width), BF16), shape_of((1, width), F32)],
        flops=2 * rows * slots * width, moved=16 * rows * width + 2 * slots * width,
    )(dest, live, cotangent, first_sum, grad_shared, gain, *returned)


def norm_one_back_kernel(gq_ref, gk_ref, gv_ref, wq_ref, wk_ref, wv_ref, tokens_ref, first_ref, gain_ref, out_ref, gain_grad_ref):
    grad_normed = (
        dot_nt(gq_ref[...], wq_ref[...]) + dot_nt(gk_ref[...], wk_ref[...]) + dot_nt(gv_ref[...], wv_ref[...])
    )
    source = tokens_ref[...].astype(F32)
    scale = lax.rsqrt(jnp.mean(source * source, axis=1, keepdims=True) + EPSILON)
    weighted = grad_normed * gain_ref[...]
    inner = jnp.mean(source * weighted, axis=1, keepdims=True)
    out_ref[...] = first_ref[...] + scale * weighted - source * (scale * scale * scale * inner)

    @pl.when(pl.program_id(0) == 0)
    def _():
        gain_grad_ref[...] = jnp.zeros_like(gain_grad_ref)

    gain_grad_ref[...] += jnp.sum(grad_normed * source * scale, axis=0, keepdims=True)


def norm_one_back(grads, w_qkv, tokens, grad_first, gain):
    rows, width = tokens.shape
    block = min(256, rows)
    blocked = pl.BlockSpec((block, width), lambda i: (i, 0))

    def weight(part):
        return pl.BlockSpec((width, width), lambda i: (0, part), pipeline_mode=pl.Buffered(1))

    return call(
        norm_one_back_kernel, (rows // block,),
        [blocked] * 3 + [weight(0), weight(1), weight(2), blocked, blocked, whole((1, width))],
        [blocked, pl.BlockSpec((1, width), lambda i: (0, 0))],
        [shape_of((rows, width), F32), shape_of((1, width), F32)],
        flops=6 * rows * width * width, moved=22 * rows * width,
    )(*grads, w_qkv, w_qkv, w_qkv, tokens, grad_first, gain)


def copies_of(layout, block, width, step, stage_g, stage_u, stage_d, slot, packed_ref, sems):
    by_rows, owners, hidden = layout
    panels = block // LANES
    rows_down = hidden // owners
    out = []

    def add(source, target):
        out.append(pltpu.make_async_copy(source, target, sems.at[slot, len(out)]))

    if by_rows:
        rows = width // owners
        for half, stage in enumerate((stage_g, stage_u)):
            for p in range(panels):
                panel = half * (hidden // LANES) + step * panels + p
                add(
                    stage.at[slot, :, :, pl.ds(p * LANES, LANES)],
                    packed_ref.at[:, pl.ds(pl.multiple_of(panel * rows, 8), rows), :],
                )
        start = 2 * hidden // LANES * rows
    else:
        columns = 2 * hidden // owners
        for half, stage in enumerate((stage_g, stage_u)):
            for p in range(panels):
                column = half * hidden + step * block + p * LANES
                owner, panel = column // columns, (column % columns) // LANES
                add(
                    stage.at[slot, :, pl.ds(p * LANES, LANES)],
                    packed_ref.at[owner, pl.ds(pl.multiple_of(panel * width, 8), width), :],
                )
        start = columns // LANES * width
    for q in range(block // rows_down):
        owner = step * (block // rows_down) + q
        for c in range(width // LANES):
            add(
                stage_d.at[slot, pl.ds(q * rows_down, rows_down), pl.ds(c * LANES, LANES)],
                packed_ref.at[owner, pl.ds(start + c * rows_down, rows_down), :],
            )
    return out


def packed_rows(width, hidden, owners):
    return 3 * width * hidden // owners // LANES


def ffn_kernel(out_type, layout, block, x_ref, gy_ref, wg_ref, wu_ref, wd_ref, y_ref, gx_ref, packed_ref, xt, y_acc, gx_acc,
               stage_g, stage_u, stage_d, sems):
    step = pl.program_id(0)
    steps = layout[2] // block
    width = x_ref.shape[1]
    slot = step % 2
    copies = functools.partial(copies_of, layout, block, width)

    @pl.when(step == 0)
    def _():
        xt[...] = x_ref[...].T
        y_acc[...] = jnp.zeros_like(y_acc)
        gx_acc[...] = jnp.zeros_like(gx_acc)

    @pl.when(step >= 2)
    def _():
        for copy in copies(step - 2, stage_g, stage_u, stage_d, slot, packed_ref, sems):
            copy.wait()

    x, gy = x_ref[...], gy_ref[...].reshape(x_ref.shape)
    wg, wu, wd = wg_ref[...], wu_ref[...], wd_ref[...]
    gate, up = dot_nn(x, wg), dot_nn(x, wu)
    grad_hidden = dot_nt(gy, wd)
    sigmoid = jax.nn.sigmoid(gate)
    value = gate * sigmoid
    hidden = (value * up).astype(BF16)
    grad_up = (grad_hidden * value).astype(BF16)
    grad_gate = (grad_hidden * up * (sigmoid * (1.0 + gate * (1.0 - sigmoid)))).astype(BF16)
    y_acc[...] += dot_nn(hidden, wd)
    gx_acc[...] += dot_nt(grad_gate, wg) + dot_nt(grad_up, wu)
    stage_g[slot] = dot_nn(xt[...], grad_gate).astype(BF16).reshape(stage_g.shape[1:])
    stage_u[slot] = dot_nn(xt[...], grad_up).astype(BF16).reshape(stage_u.shape[1:])
    stage_d[slot] = dot_tn(hidden, gy).astype(BF16)
    for copy in copies(step, stage_g, stage_u, stage_d, slot, packed_ref, sems):
        copy.start()

    @pl.when(step == steps - 1)
    def _():
        y_ref[...] = y_acc[...].astype(out_type)
        gx_ref[...] = gx_acc[...].astype(out_type)
        for back in (1, 0):
            if steps > back:
                for copy in copies(steps - 1 - back, stage_g, stage_u, stage_d, (steps - 1 - back) % 2, packed_ref, sems):
                    copy.wait()


def ffn_both(x, gy, w_gu, w_down, expert, owners, out_type):
    rows, width = x.shape
    hidden = w_down.shape[-2]
    block = min(256, hidden)
    steps = hidden // block
    by_rows = expert is None
    if by_rows:
        gate = pl.BlockSpec((width, block), lambda f: (0, f))
        up = pl.BlockSpec((width, block), lambda f: (0, steps + f))
        down = pl.BlockSpec((block, width), lambda f: (f, 0))
        stage = (2, owners, width // owners, block)
    else:
        gate = pl.BlockSpec((None, width, block), lambda f: (expert, 0, f))
        up = pl.BlockSpec((None, width, block), lambda f: (expert, 0, steps + f))
        down = pl.BlockSpec((None, block, width), lambda f: (expert, f, 0))
        stage = (2, width, block)
    if by_rows:
        grads = whole((rows, width))
    else:
        grads = pl.BlockSpec(
            (gy.shape[0], rows // gy.shape[0], width), lambda f: (0, expert, 0), pipeline_mode=pl.Buffered(1)
        )
    out_rows = whole((rows, width))
    layout = (by_rows, owners, hidden)
    copies = 2 * (block // LANES) + block // (hidden // owners) * (width // LANES)
    return call(
        functools.partial(ffn_kernel, out_type, layout, block), (steps,),
        [whole((rows, width)), grads, gate, up, down],
        [out_rows, out_rows, pl.BlockSpec(memory_space=pl.ANY)],
        [shape_of((rows, width), out_type), shape_of((rows, width), out_type),
         shape_of((owners, packed_rows(width, hidden, owners), LANES), BF16)],
        scratch=[pltpu.VMEM((width, rows), BF16), pltpu.VMEM((rows, width), F32), pltpu.VMEM((rows, width), F32),
                 pltpu.VMEM(stage, BF16), pltpu.VMEM(stage, BF16), pltpu.VMEM((2, block, width), BF16),
                 pltpu.SemaphoreType.DMA((2, copies))],
        flops=18 * rows * width * hidden, moved=12 * width * hidden + 16 * rows * width, trans=rows * hidden,
    )(x, gy, w_gu, w_gu, w_down)


def panels_to(rows_array, rows, panels):
    return jnp.transpose(rows_array.reshape(panels, rows, LANES), (1, 0, 2)).reshape(rows, panels * LANES)


def attention_weights_kernel(per, normed_ref, mixed_ref, gq_ref, gk_ref, gv_ref, ga_ref, gains_ref, out_ref, xt):
    step = pl.program_id(0)
    owners, rows = out_ref.shape[0], out_ref.shape[1] // (out_ref.shape[1] // (normed_ref.shape[1] // out_ref.shape[0]))
    panels = out_ref.shape[1] // rows

    @pl.when(step == 0)
    def _():
        xt[...] = normed_ref[...].T

    @pl.when(step == 3 * per)
    def _():
        xt[...] = mixed_ref[...].T

    for index, grad_ref in enumerate((gq_ref, gk_ref, gv_ref, ga_ref)):

        @pl.when((step >= index * per) & (step < (index + 1) * per))
        def _():
            product = dot_nn(xt[...], grad_ref[...]).astype(BF16)
            for p in range(panels):
                out_ref[:, pl.ds(p * rows, rows), :] = product[:, p * LANES : (p + 1) * LANES].reshape(owners, rows, LANES)

    @pl.when(step == 4 * per)
    def _():
        out_ref[...] = jnp.zeros_like(out_ref)
        out_ref[:, pl.ds(0, gains_ref.shape[1]), :] = gains_ref[...]


def attention_weights(normed, mixed, grads, grad_attn, gains, owners):
    tokens, width = normed.shape
    rows = width // owners
    block = 256
    panels, per = block // LANES, width // block

    def columns(index):
        return pl.BlockSpec((tokens, block), lambda i: (0, jnp.clip(i - index * per, 0, per - 1)))

    return call(
        functools.partial(attention_weights_kernel, per), (4 * per + 1,),
        [whole((tokens, width)), whole((tokens, width))] + [columns(index) for index in range(4)] + [whole(gains.shape)],
        pl.BlockSpec((owners, panels * rows, LANES), lambda i: (0, i, 0)),
        shape_of((owners, (4 * per + 1) * panels * rows, LANES), BF16),
        scratch=[pltpu.VMEM((width, tokens), BF16)],
        flops=8 * tokens * width * width, moved=16 * tokens * width,
    )(normed, mixed, *grads, grad_attn, gains)


GROUP = ("dp", "shard")


def local(
    tokens,
    lengths,
    routes,
    route_gates,
    cotangent,
    norm_gains,
    w_qkv,
    w_out,
    w_shared_gu,
    w_shared_down,
    w_expert_gu,
    w_expert_down,
):
    tok_count, width = tokens.shape
    seq_count = lengths.shape[0]
    length = tok_count // seq_count
    local_experts = w_expert_gu.shape[0]
    owners = lax.axis_size("expert")
    experts = local_experts * owners
    top = routes.shape[1]
    capacity = tok_count * top * 9 // (8 * experts)
    head_dim = width // HEADS

    gains = lax.all_gather(norm_gains, GROUP, axis=1, tiled=True).astype(F32)
    qkv_weight = lax.all_gather(w_qkv, GROUP, axis=0, tiled=True)
    out_weight = lax.all_gather(w_out, GROUP, axis=0, tiled=True)
    sgu_weight = lax.all_gather(w_shared_gu, GROUP, axis=0, tiled=True)
    sdown_weight = lax.all_gather(w_shared_down, GROUP, axis=0, tiled=True)
    gain_one, gain_two = gains[0:1], gains[1:2]

    live_bool = lax.iota(jnp.int32, tok_count) % length < jnp.repeat(lengths, length)
    live = live_bool.astype(F32)[:, None]
    live_row = live_bool.astype(jnp.int32)[None, :]

    group = lax.axis_size("dp") * lax.axis_size("shard")

    dest_t = slots_of(routes.T, live_row, experts, capacity)
    dest = dest_t.T
    slots = owners * capacity

    def place(where):
        owner_of, part_of = where // (local_experts * capacity), (where // capacity) % local_experts
        return jnp.where(
            where < experts * capacity, part_of * slots + owner_of * capacity + where % capacity, experts * capacity
        )

    placed, placed_t = place(dest), place(dest_t)
    gates_t = route_gates.T
    grad_b = jnp.where(live_bool[:, None], cotangent, 0).astype(BF16)

    def exchange(rows):
        count = rows.shape[0] // owners
        return lax.all_to_all(
            rows.reshape(owners, count, width), "expert", split_axis=0, concat_axis=0, tiled=True
        ).reshape(rows.shape)

    send_grad = dispatch(dest_t, gates_t, grad_b, experts, capacity, True, 0)
    received_grad = exchange(send_grad).reshape(owners, local_experts * capacity, width)

    cosine, sine = rotary_tables(length, head_dim)
    normed_one = norm_one(tokens, gain_one)
    queries, keys, values, mixed, lse = attend_forward(normed_one, qkv_weight, cosine, sine, length, head_dim)
    first_sum, normed_two = norm_two(mixed, tokens, out_weight, gain_two)

    received = []
    for j in range(local_experts):
        rows = dispatch(placed_t, gates_t, normed_two, owners, capacity, False, j * owners)
        received.append(exchange(rows))
    shared_out, grad_shared, shared_pack = ffn_both(
        normed_two, grad_b, sgu_weight, sdown_weight, None, group, F32
    )
    back_rows, out_rows, expert_packs = [], [], []
    for j in range(local_experts):
        y, gx, pack = ffn_both(received[j], received_grad, w_expert_gu, w_expert_down, j, group, BF16)
        back_rows.append(exchange(gx))
        out_rows.append(y)
        expert_packs.append(pack)
    grad_first, grad_attn, grad_gain_two = norm_two_back(
        placed, live, cotangent, first_sum, grad_shared, gain_two, back_rows
    )

    grad_mixed = dot_nt(grad_attn, out_weight).astype(BF16)
    grads = attend_backward(queries, keys, values, mixed, grad_mixed, lse, cosine, sine, length, head_dim)
    input_grad, grad_gain_one = norm_one_back(grads, qkv_weight, tokens, grad_first, gain_one)
    own = width // group
    grad_gains = jnp.concatenate([grad_gain_one, grad_gain_two], axis=0).reshape(2, group, own).transpose(1, 0, 2)
    grad_gains = jnp.pad(grad_gains, ((0, 0), (0, 14), (0, LANES - own))).astype(BF16)
    attention_pack = attention_weights(normed_one, mixed, grads, grad_attn, grad_gains, group)

    returned = exchange_parts(out_rows, owners, "expert")
    layer_out = combine(placed, route_gates, live, first_sum, shared_out, returned)

    def spread(pack):
        return lax.psum_scatter(pack, GROUP, scatter_dimension=0, tiled=True)[0]

    shared_share = spread(shared_pack)
    expert_shares = [spread(pack) for pack in expert_packs]
    attention_share = spread(attention_pack)
    shared_share = lax.psum(shared_share, "expert").astype(F32)
    attention_share = lax.psum(attention_share, "expert").astype(F32)
    hidden = w_expert_down.shape[1]
    shared_hidden = sdown_weight.shape[0]
    gu_panels, d_panels = 2 * shared_hidden // LANES, width // LANES
    qkv_rows, out_rows_count = 3 * d_panels * own, 4 * d_panels * own
    columns = 2 * hidden // group
    gu_rows = columns // LANES * width
    return (
        layer_out,
        input_grad,
        attention_share[out_rows_count : out_rows_count + 2, :own],
        panels_to(attention_share[:qkv_rows], own, 3 * d_panels),
        panels_to(attention_share[qkv_rows:out_rows_count], own, d_panels),
        panels_to(shared_share[: gu_panels * own], own, gu_panels),
        panels_to(shared_share[gu_panels * own :], shared_hidden // group, d_panels),
        jnp.stack([panels_to(share[:gu_rows], width, columns // LANES) for share in expert_shares]).astype(F32),
        jnp.stack([panels_to(share[gu_rows:], hidden // group, d_panels) for share in expert_shares]).astype(F32),
    )


def exchange_parts(parts, owners, axis):
    width = parts[0].shape[1]
    count = parts[0].shape[0] // owners
    joined = jnp.concatenate([rows.reshape(owners, count, width) for rows in parts], axis=1)
    back = lax.all_to_all(joined, axis, split_axis=0, concat_axis=0, tiled=True)
    return [
        back[:, j * count : (j + 1) * count].reshape(owners * count, width) for j in range(len(parts))
    ]


def solution(mesh):
    rows = P(("dp", "expert", "shard"), None)
    split = P(GROUP, None)
    in_specs = (
        rows,
        P(("dp", "expert", "shard")),
        rows,
        rows,
        rows,
        P(None, GROUP),
        split,
        split,
        split,
        split,
        P("expert", None, None),
        P("expert", None, None),
    )
    out_specs = (
        rows,
        rows,
        P(None, GROUP),
        split,
        split,
        split,
        split,
        P("expert", None, GROUP),
        P("expert", GROUP, None),
    )

    return jax.shard_map(local, mesh=mesh, in_specs=in_specs, out_specs=out_specs, check_vma=False)
```

```python
import functools
import math

import jax
import jax.numpy as jnp
from jax import lax
from jax.experimental import pallas as pl
from jax.experimental.pallas import tpu as pltpu
from jax.sharding import PartitionSpec as P


HEADS = 12
LANES = 128
EPSILON = 1e-05
VMEM_BYTES = 60 * 1024 * 1024
BF16 = jnp.bfloat16
F32 = jnp.float32


def call(kernel, grid, in_specs, out_specs, out_shape, scratch=(), flops=0, moved=0, trans=0, aliases=None):
    return pl.pallas_call(
        kernel,
        grid_spec=pltpu.PrefetchScalarGridSpec(
            num_scalar_prefetch=0,
            grid=grid,
            in_specs=in_specs,
            out_specs=out_specs,
            scratch_shapes=list(scratch),
        ),
        out_shape=out_shape,
        input_output_aliases=aliases or {},
        compiler_params=pltpu.CompilerParams(
            dimension_semantics=("arbitrary",) * len(grid), vmem_limit_bytes=VMEM_BYTES
        ),
        cost_estimate=pl.CostEstimate(flops=flops, bytes_accessed=moved, transcendentals=trans),
    )


def shape_of(shape, dtype):
    return jax.ShapeDtypeStruct(shape, dtype)


def whole(shape):
    return pl.BlockSpec(shape, lambda *_: (0,) * len(shape), pipeline_mode=pl.Buffered(1))


def dot_nn(left, right):
    return lax.dot_general(left, right, (((1,), (0,)), ((), ())), preferred_element_type=F32)


def dot_nt(left, right):
    return lax.dot_general(left, right, (((1,), (1,)), ((), ())), preferred_element_type=F32)


def dot_tn(left, right):
    return lax.dot_general(left, right, (((0,), (0,)), ((), ())), preferred_element_type=F32)


def rotary_tables(length, head_dim):
    half_dim = head_dim // 2
    position = lax.iota(F32, length)[:, None]
    frequency = jnp.exp(lax.iota(F32, half_dim) * (-2.0 * math.log(10000.0) / head_dim))
    angle_table = position * frequency[None, :]
    cosine, sine = jnp.cos(angle_table), jnp.sin(angle_table)
    repeats = LANES // head_dim
    return (
        jnp.tile(jnp.concatenate([cosine, cosine], axis=1), (1, repeats)),
        jnp.tile(jnp.concatenate([-sine, sine], axis=1), (1, repeats)),
    )


def turn(values, cosine, signed_sine, head_dim):
    lane = lax.broadcasted_iota(jnp.int32, values.shape, 1)
    half = head_dim // 2
    other = jnp.where(
        lane % head_dim < half,
        pltpu.roll(values, LANES - half, 1),
        pltpu.roll(values, half, 1),
    )
    return values * cosine + other * signed_sine


def attend_forward_kernel(
    head_dim, block, x_ref, wq_ref, wk_ref, wv_ref, cos_ref, sin_ref, q_ref, k_ref, v_ref, o_ref, lse_ref, lse_tile
):
    length = x_ref.shape[0]
    heads = LANES // head_dim
    x = x_ref[...]
    cosine, sine = cos_ref[...], sin_ref[...]
    scale = 1.0 / math.sqrt(head_dim)
    q_ref[...] = (turn(dot_nn(x, wq_ref[...]), cosine, sine, head_dim) * scale).astype(BF16)
    k_ref[...] = turn(dot_nn(x, wk_ref[...]), cosine, sine, head_dim).astype(BF16)
    v_ref[...] = dot_nn(x, wv_ref[...]).astype(BF16)
    lane = lax.broadcasted_iota(jnp.int32, (1, LANES), 1)
    own_lane = lax.broadcasted_iota(jnp.int32, (block, LANES), 1) // head_dim
    below = lax.broadcasted_iota(jnp.int32, (block, block), 0) >= lax.broadcasted_iota(
        jnp.int32, (block, block), 1
    )
    for first in range(0, length, block):
        rows = pl.ds(first, block)
        mixed = None
        logs = None
        for head in range(heads):
            select = (lane // head_dim == head).astype(F32).astype(BF16)
            queries = q_ref[rows, :] * select
            near = jnp.where(below, dot_nt(queries, k_ref[rows, :]), -1e30)
            peak = jnp.max(near, axis=1, keepdims=True)
            if first:
                far = dot_nt(queries, k_ref[pl.ds(0, first), :])
                peak = jnp.maximum(peak, jnp.max(far, axis=1, keepdims=True))
            near = jnp.exp(near - peak)
            total = jnp.sum(near, axis=1, keepdims=True)
            part = dot_nn(near.astype(BF16), v_ref[rows, :])
            if first:
                far = jnp.exp(far - peak)
                total = total + jnp.sum(far, axis=1, keepdims=True)
                part = part + dot_nn(far.astype(BF16), v_ref[pl.ds(0, first), :])
            part = part * (1.0 / total)
            log_total = jnp.broadcast_to(peak + jnp.log(total), (block, LANES))
            mixed = part if head == 0 else jnp.where(own_lane == head, part, mixed)
            logs = log_total if head == 0 else jnp.where(own_lane == head, log_total, logs)
        o_ref[rows, :] = mixed.astype(BF16)
        lse_tile[rows, :] = logs
    turned = lse_tile[...].T
    for head in range(heads):
        lse_ref[pl.ds(head * 8, 8), :] = turned[head * head_dim : head * head_dim + 8, :]


def attend_forward(normed, w_qkv, cosine, sine, length, head_dim):
    tokens, width = normed.shape
    seqs, pairs, heads = tokens // length, width // LANES, LANES // head_dim
    block = min(256, length)
    rows = pl.BlockSpec((length, LANES), lambda s, p: (s, p))

    def weight(part):
        return pl.BlockSpec((width, LANES), lambda s, p: (0, part * pairs + p))

    table = whole((length, LANES))
    return call(
        functools.partial(attend_forward_kernel, head_dim, block),
        (seqs, pairs),
        [pl.BlockSpec((length, width), lambda s, p: (s, 0)), weight(0), weight(1), weight(2), table, table],
        [rows, rows, rows, rows, pl.BlockSpec((8 * heads, length), lambda s, p: (s * pairs + p, 0))],
        [shape_of((tokens, width), BF16)] * 4 + [shape_of((seqs * pairs * 8 * heads, length), F32)],
        scratch=[pltpu.VMEM((length, LANES), F32)],
        flops=6 * tokens * width * width + 4 * tokens * length * width,
        moved=16 * tokens * width,
        trans=tokens * length * width // head_dim // 2,
    )(normed, w_qkv, w_qkv, w_qkv, cosine, sine)


def attend_backward_kernel(
    head_dim, block, q_ref, k_ref, v_ref, o_ref, g_ref, lse_ref, cos_ref, sin_ref, gq_ref, gk_ref, gv_ref, gq_acc
):
    length = q_ref.shape[0]
    heads = LANES // head_dim
    scale = 1.0 / math.sqrt(head_dim)
    product = (g_ref[...].astype(F32) * o_ref[...].astype(F32)).T
    inner = [
        jnp.sum(product[head * head_dim : (head + 1) * head_dim, :], axis=0, keepdims=True)
        for head in range(heads)
    ]
    gq_acc[...] = jnp.zeros_like(gq_acc)
    lane = lax.broadcasted_iota(jnp.int32, (1, LANES), 1)
    own_lane = lax.broadcasted_iota(jnp.int32, (block, LANES), 1) // head_dim
    above = lax.broadcasted_iota(jnp.int32, (block, block), 1) >= lax.broadcasted_iota(
        jnp.int32, (block, block), 0
    )
    for first in range(0, length, block):
        rows = pl.ds(first, block)
        keys_grad = None
        values_grad = None
        for head in range(heads):
            select = (lane // head_dim == head).astype(F32).astype(BF16)
            keys = k_ref[rows, :] * select
            values = v_ref[rows, :] * select
            log_total = lse_ref[pl.ds(head * 8, 1), :]
            pieces = [(first, block, True)]
            if first + block < length:
                pieces.append((first + block, length - first - block, False))
            keys_part = None
            values_part = None
            for start, count, diagonal in pieces:
                span = pl.ds(start, count)
                queries, grads = q_ref[span, :], g_ref[span, :]
                scores = dot_nt(keys, queries)
                probs = jnp.exp(scores - log_total[:, start : start + count])
                if diagonal:
                    probs = jnp.where(above, probs, 0.0)
                grad_probs = dot_nt(values, grads)
                grad_scores = (probs * (grad_probs - inner[head][:, start : start + count])).astype(BF16)
                piece_values = dot_nn(probs.astype(BF16), grads)
                piece_keys = dot_nn(grad_scores, queries)
                values_part = piece_values if values_part is None else values_part + piece_values
                keys_part = piece_keys if keys_part is None else keys_part + piece_keys
                gq_acc[span, :] += dot_tn(grad_scores, keys)
            keys_grad = keys_part if head == 0 else jnp.where(own_lane == head, keys_part, keys_grad)
            values_grad = values_part if head == 0 else jnp.where(own_lane == head, values_part, values_grad)
        gk_ref[rows, :] = turn(keys_grad, cos_ref[rows, :], -sin_ref[rows, :], head_dim).astype(BF16)
        gv_ref[rows, :] = values_grad.astype(BF16)
    gq_ref[...] = turn(gq_acc[...] * scale, cos_ref[...], -sin_ref[...], head_dim).astype(BF16)


def attend_backward(queries, keys, values, mixed, grad_mixed, lse, cosine, sine, length, head_dim):
    tokens, width = queries.shape
    seqs, pairs, heads = tokens // length, width // LANES, LANES // head_dim
    block = min(256, length)
    rows = pl.BlockSpec((length, LANES), lambda s, p: (s, p))
    table = whole((length, LANES))
    return call(
        functools.partial(attend_backward_kernel, head_dim, block),
        (seqs, pairs),
        [rows] * 5 + [pl.BlockSpec((8 * heads, length), lambda s, p: (s * pairs + p, 0)), table, table],
        [rows] * 3,
        [shape_of((tokens, width), BF16)] * 3,
        scratch=[pltpu.VMEM((length, LANES), F32)],
        flops=10 * tokens * length * width,
        moved=16 * tokens * width,
        trans=tokens * length * width // head_dim // 2,
    )(queries, keys, values, mixed, grad_mixed, lse, cosine, sine)


def square(width, part):
    return pl.BlockSpec((width, width), lambda i: (0, part), pipeline_mode=pl.Buffered(1))


def norm_one_kernel(x_ref, gain_ref, out_ref):
    x = x_ref[...].astype(F32)
    scale = lax.rsqrt(jnp.mean(x * x, axis=1, keepdims=True) + EPSILON)
    out_ref[...] = (x * scale * gain_ref[...]).astype(BF16)


def norm_one(tokens, gain):
    rows, width = tokens.shape
    block = min(256, rows)
    blocked = pl.BlockSpec((block, width), lambda i: (i, 0))
    return call(
        norm_one_kernel, (rows // block,), [blocked, whole((1, width))], blocked, shape_of((rows, width), BF16),
        flops=5 * rows * width, moved=4 * rows * width,
    )(tokens, gain)


def norm_two_kernel(mixed_ref, tokens_ref, weight_ref, gain_ref, sum_ref, normed_ref):
    first_sum = tokens_ref[...].astype(F32) + dot_nn(mixed_ref[...], weight_ref[...])
    sum_ref[...] = first_sum
    scale = lax.rsqrt(jnp.mean(first_sum * first_sum, axis=1, keepdims=True) + EPSILON)
    normed_ref[...] = (first_sum * scale * gain_ref[...]).astype(BF16)


def norm_two(mixed, tokens, weight, gain):
    rows, width = tokens.shape
    block = min(256, rows)
    blocked = pl.BlockSpec((block, width), lambda i: (i, 0))
    return call(
        norm_two_kernel, (rows // block,), [blocked, blocked, square(width, 3), whole((1, width))],
        [blocked, blocked], [shape_of((rows, width), F32), shape_of((rows, width), BF16)],
        flops=2 * rows * width * width, moved=10 * rows * width,
    )(mixed, tokens, weight, gain)


def slots_kernel(experts, capacity, routes_ref, live_ref, dest_ref):
    top, tokens = routes_ref.shape
    live = live_ref[...]
    number = lax.broadcasted_iota(jnp.int32, (experts, tokens), 0)
    hits = [
        jnp.where((routes_ref[pl.ds(k, 1), :] == number) & (live > 0), 1.0, 0.0) for k in range(top)
    ]
    earlier = jnp.where(
        lax.broadcasted_iota(jnp.int32, (tokens, tokens), 0)
        <= lax.broadcasted_iota(jnp.int32, (tokens, tokens), 1),
        1.0,
        0.0,
    ).astype(BF16)
    ranks = dot_nn(jnp.concatenate(hits, axis=0).astype(BF16), earlier)
    before = jnp.zeros((experts, 1), F32)
    for k in range(top):
        rank = ranks[k * experts : (k + 1) * experts, :]
        place = number.astype(F32) * capacity + before + rank - 1.0
        slot = jnp.sum(hits[k] * place, axis=0, keepdims=True).astype(jnp.int32)
        dest_ref[pl.ds(k, 1), :] = jnp.where(live > 0, slot, experts * capacity)
        before = before + jnp.sum(hits[k], axis=1, keepdims=True)


def slots_of(routes_t, live_row, experts, capacity):
    top, tokens = routes_t.shape
    return call(
        functools.partial(slots_kernel, experts, capacity), (1,),
        [whole((top, tokens)), whole((1, tokens))], whole((top, tokens)), shape_of((top, tokens), jnp.int32),
        flops=2 * top * experts * tokens * tokens, moved=16 * tokens,
    )(routes_t, live_row)


def dispatch_kernel(gated, first, dest_ref, gates_ref, x_ref, out_ref):
    top, tokens = dest_ref.shape
    capacity = out_ref.shape[0]
    slot = lax.broadcasted_iota(jnp.int32, (capacity, tokens), 0) + (first + pl.program_id(0)) * capacity
    hits = [slot == dest_ref[pl.ds(k, 1), :] for k in range(top)]
    chosen = functools.reduce(jnp.logical_or, hits)
    rows = dot_nn(jnp.where(chosen, 1.0, 0.0).astype(BF16), x_ref[...])
    if gated:
        weights = jnp.zeros((capacity, tokens), F32)
        for k in range(top):
            weights = jnp.where(hits[k], gates_ref[pl.ds(k, 1), :], weights)
        rows = rows * jnp.sum(weights, axis=1, keepdims=True)
    out_ref[...] = rows.astype(BF16)


def dispatch(dest_t, gates_t, x, experts, capacity, gated, first):
    top, tokens = dest_t.shape
    width = x.shape[1]
    return call(
        functools.partial(dispatch_kernel, gated, first), (experts,),
        [whole((top, tokens)), whole((top, tokens)), whole((tokens, width))],
        pl.BlockSpec((capacity, width), lambda e: (e, 0)),
        shape_of((experts * capacity, width), BF16),
        flops=2 * experts * capacity * tokens * width, moved=2 * (experts * capacity + tokens) * width,
    )(dest_t, gates_t, x)


def combine_kernel(parts, dest_ref, gates_ref, live_ref, sum_ref, shared_ref, *rest):
    y_refs, out_ref = rest[:parts], rest[parts]
    block, top = dest_ref.shape
    total = sum_ref[...] + shared_ref[...]
    dest = dest_ref[...]
    gates = gates_ref[...]
    for index, y_ref in enumerate(y_refs):
        y = y_ref[...]
        slot = slot_numbers(block, y_ref.shape[0], index)
        for k in range(top):
            hit = jnp.where(slot == dest[:, k : k + 1], 1.0, 0.0).astype(BF16)
            total = total + dot_nn(hit, y) * gates[:, k : k + 1]
    out_ref[...] = (live_ref[...] * total).astype(BF16)


def slot_numbers(block, slots, part):
    return lax.broadcasted_iota(jnp.int32, (block, slots), 1) + part * slots


def combine(dest, gates, live, first_sum, shared_out, returned):
    rows, width = first_sum.shape
    top = dest.shape[1]
    block = min(256, rows)
    parts = len(returned)
    blocked = pl.BlockSpec((block, width), lambda i: (i, 0))
    narrow = pl.BlockSpec((block, top), lambda i: (i, 0))
    slots = sum(y.shape[0] for y in returned)
    return call(
        functools.partial(combine_kernel, parts), (rows // block,),
        [narrow, narrow, pl.BlockSpec((block, 1), lambda i: (i, 0)), blocked, blocked]
        + [whole(y.shape) for y in returned],
        blocked, shape_of((rows, width), BF16),
        flops=4 * rows * slots * width, moved=10 * rows * width + 2 * slots * width,
    )(dest, gates, live, first_sum, shared_out, *returned)


def gathered(dest_ref, y_ref, part):
    block, top = dest_ref.shape
    dest = dest_ref[...]
    slot = slot_numbers(block, y_ref.shape[0], part)
    hit = functools.reduce(jnp.logical_or, [slot == dest[:, k : k + 1] for k in range(top)])
    return dot_nn(jnp.where(hit, 1.0, 0.0).astype(BF16), y_ref[...])


def add_part_kernel(part, dest_ref, base_ref, y_ref, out_ref):
    out_ref[...] = base_ref[...] + gathered(dest_ref, y_ref, part)


def add_part(dest, base, rows_of, part):
    rows, width = base.shape
    block = min(256, rows)
    blocked = pl.BlockSpec((block, width), lambda i: (i, 0))
    return call(
        functools.partial(add_part_kernel, part), (rows // block,),
        [pl.BlockSpec((block, dest.shape[1]), lambda i: (i, 0)), blocked, whole(rows_of.shape)],
        blocked, shape_of((rows, width), F32),
        flops=2 * rows * rows_of.shape[0] * width, moved=8 * rows * width,
    )(dest, base, rows_of)


def norm_two_back_kernel(part, dest_ref, live_ref, cot_ref, sum_ref, base_ref, gain_ref, weight_ref, y_ref,
                         first_ref, attn_ref, mixed_ref, gain_grad_ref):
    grad_normed = base_ref[...] + gathered(dest_ref, y_ref, part)
    first_sum = sum_ref[...]
    scale = lax.rsqrt(jnp.mean(first_sum * first_sum, axis=1, keepdims=True) + EPSILON)
    weighted = grad_normed * gain_ref[...]
    inner = jnp.mean(first_sum * weighted, axis=1, keepdims=True)
    grad_first = (
        cot_ref[...].astype(F32) * live_ref[...] + scale * weighted - first_sum * (scale * scale * scale * inner)
    )
    first_ref[...] = grad_first
    grad_attn = grad_first.astype(BF16)
    attn_ref[...] = grad_attn
    mixed_ref[...] = dot_nt(grad_attn, weight_ref[...]).astype(BF16)

    @pl.when(pl.program_id(0) == 0)
    def _():
        gain_grad_ref[...] = jnp.zeros_like(gain_grad_ref)

    gain_grad_ref[...] += jnp.sum(grad_normed * first_sum * scale, axis=0, keepdims=True)


def norm_two_back(dest, live, cotangent, first_sum, base, gain, weights, rows_of, part):
    rows, width = first_sum.shape
    top = dest.shape[1]
    block = min(256, rows)
    blocked = pl.BlockSpec((block, width), lambda i: (i, 0))
    return call(
        functools.partial(norm_two_back_kernel, part), (rows // block,),
        [pl.BlockSpec((block, top), lambda i: (i, 0)), pl.BlockSpec((block, 1), lambda i: (i, 0)), blocked, blocked,
         blocked, whole((1, width)), square(width, 3), whole(rows_of.shape)],
        [blocked, blocked, blocked, pl.BlockSpec((1, width), lambda i: (0, 0))],
        [shape_of((rows, width), F32), shape_of((rows, width), BF16), shape_of((rows, width), BF16),
         shape_of((1, width), F32)],
        flops=2 * rows * (rows_of.shape[0] + width) * width, moved=18 * rows * width,
    )(dest, live, cotangent, first_sum, base, gain, weights, rows_of)


def norm_one_back_kernel(gq_ref, gk_ref, gv_ref, wq_ref, wk_ref, wv_ref, tokens_ref, first_ref, gain_ref, out_ref):
    grad_normed = (
        dot_nt(gq_ref[...], wq_ref[...]) + dot_nt(gk_ref[...], wk_ref[...]) + dot_nt(gv_ref[...], wv_ref[...])
    )
    source = tokens_ref[...].astype(F32)
    scale = lax.rsqrt(jnp.mean(source * source, axis=1, keepdims=True) + EPSILON)
    weighted = grad_normed * gain_ref[...]
    inner = jnp.mean(source * weighted, axis=1, keepdims=True)
    out_ref[...] = first_ref[...] + scale * weighted - source * (scale * scale * scale * inner)


def norm_one_back(grads, w_qkv, tokens, grad_first, gain):
    rows, width = tokens.shape
    block = min(256, rows)
    blocked = pl.BlockSpec((block, width), lambda i: (i, 0))

    return call(
        norm_one_back_kernel, (rows // block,),
        [blocked] * 3 + [square(width, 0), square(width, 1), square(width, 2), blocked, blocked, whole((1, width))],
        blocked, shape_of((rows, width), F32),
        flops=6 * rows * width * width, moved=22 * rows * width,
    )(*grads, w_qkv, w_qkv, w_qkv, tokens, grad_first, gain)


def copies_of(layout, block, width, step, stage_g, stage_u, stage_d, slot, packed_ref, sems):
    by_rows, owners, hidden, base = layout
    panels = block // LANES
    rows_down = hidden // owners
    out = []

    def add(source, target):
        out.append(pltpu.make_async_copy(source, target, sems.at[slot, len(out)]))

    if by_rows:
        rows = width // owners
        for half, stage in enumerate((stage_g, stage_u)):
            for p in range(panels):
                panel = half * (hidden // LANES) + step * panels + p
                add(
                    stage.at[slot, :, :, pl.ds(p * LANES, LANES)],
                    packed_ref.at[:, pl.ds(pl.multiple_of(base + panel * rows, 8), rows), :],
                )
        start = 2 * hidden // LANES * rows
    else:
        columns = 2 * hidden // owners
        for half, stage in enumerate((stage_g, stage_u)):
            for p in range(panels):
                column = half * hidden + step * block + p * LANES
                owner, panel = column // columns, (column % columns) // LANES
                add(
                    stage.at[slot, :, pl.ds(p * LANES, LANES)],
                    packed_ref.at[owner, pl.ds(pl.multiple_of(base + panel * width, 8), width), :],
                )
        start = columns // LANES * width
    for q in range(block // rows_down):
        owner = step * (block // rows_down) + q
        for c in range(width // LANES):
            add(
                stage_d.at[slot, pl.ds(q * rows_down, rows_down), pl.ds(c * LANES, LANES)],
                packed_ref.at[owner, pl.ds(base + start + c * rows_down, rows_down), :],
            )
    return out


def packed_rows(width, hidden, owners):
    return 3 * width * hidden // owners // LANES


def ffn_kernel(out_type, layout, block, x_ref, gy_ref, wg_ref, wu_ref, wd_ref, *rest):
    y_ref, gx_ref, packed_ref, xt, y_acc, gx_acc, stage_g, stage_u, stage_d, sems = rest[-10:]
    step = pl.program_id(0)
    steps = layout[2] // block
    width = x_ref.shape[1]
    slot = step % 2
    copies = functools.partial(copies_of, layout, block, width)

    @pl.when(step == 0)
    def _():
        xt[...] = x_ref[...].T
        y_acc[...] = jnp.zeros_like(y_acc)
        gx_acc[...] = jnp.zeros_like(gx_acc)

    @pl.when(step >= 2)
    def _():
        for copy in copies(step - 2, stage_g, stage_u, stage_d, slot, packed_ref, sems):
            copy.wait()

    x, gy = x_ref[...], gy_ref[...].reshape(x_ref.shape)
    if layout[0]:
        wg, wu = wg_ref[...].reshape(width, block), wu_ref[...].reshape(width, block)
        rows = wd_ref.shape[1] // (width // block)
        wd = jnp.concatenate(
            [wd_ref[:, pl.ds(c * rows, rows), :].reshape(block, block) for c in range(width // block)], axis=1
        )
    else:
        wg, wu, wd = wg_ref[...], wu_ref[...], wd_ref[...]
    gate, up = dot_nn(x, wg), dot_nn(x, wu)
    grad_hidden = dot_nt(gy, wd)
    sigmoid = jax.nn.sigmoid(gate)
    value = gate * sigmoid
    hidden = (value * up).astype(BF16)
    grad_up = (grad_hidden * value).astype(BF16)
    grad_gate = (grad_hidden * up * (sigmoid * (1.0 + gate * (1.0 - sigmoid)))).astype(BF16)
    y_acc[...] += dot_nn(hidden, wd)
    gx_acc[...] += dot_nt(grad_gate, wg) + dot_nt(grad_up, wu)
    stage_g[slot] = dot_nn(xt[...], grad_gate).astype(BF16).reshape(stage_g.shape[1:])
    stage_u[slot] = dot_nn(xt[...], grad_up).astype(BF16).reshape(stage_u.shape[1:])
    stage_d[slot] = dot_tn(hidden, gy).astype(BF16)
    for copy in copies(step, stage_g, stage_u, stage_d, slot, packed_ref, sems):
        copy.start()

    @pl.when(step == steps - 1)
    def _():
        y_ref[...] = y_acc[...].astype(out_type)
        gx_ref[...] = gx_acc[...].astype(out_type)
        for back in (1, 0):
            if steps > back:
                for copy in copies(steps - 1 - back, stage_g, stage_u, stage_d, (steps - 1 - back) % 2, packed_ref, sems):
                    copy.wait()


BLOCK = 256


def ffn_both(x, gy, w_gu, w_down, hidden, expert, owners, out_type, parts=1, pack=None):
    rows, width = x.shape
    block = BLOCK
    steps = hidden // block
    by_rows = expert is None
    if by_rows:
        own, own_down, panels = width // owners, hidden // owners, width // block
        ahead = 2 * steps * own // (panels * own_down)
        gate = pl.BlockSpec((owners, own, block), lambda f: (0, f, 0))
        up = pl.BlockSpec((owners, own, block), lambda f: (0, steps + f, 0))
        down = pl.BlockSpec((block // own_down, panels * own_down, block), lambda f: (f, ahead, 0))
        stage = (2, owners, own, block)
    else:
        gate = pl.BlockSpec((None, width, block), lambda f: (expert, 0, f))
        up = pl.BlockSpec((None, width, block), lambda f: (expert, 0, steps + f))
        down = pl.BlockSpec((None, block, width), lambda f: (expert, f, 0))
        stage = (2, width, block)
    if by_rows:
        grads = whole((rows, width))
    else:
        grads = pl.BlockSpec(
            (gy.shape[0], rows // gy.shape[0], width), lambda f: (0, expert, 0), pipeline_mode=pl.Buffered(1)
        )
    out_rows = whole((rows, width))
    count = packed_rows(width, hidden, owners)
    layout = (by_rows, owners, hidden, (expert or 0) * count)
    held = [] if pack is None else [pack]
    copies = 2 * (block // LANES) + block // (hidden // owners) * (width // LANES)
    return call(
        functools.partial(ffn_kernel, out_type, layout, block), (steps,),
        [whole((rows, width)), grads, gate, up, down] + [pl.BlockSpec(memory_space=pl.ANY)] * len(held),
        [out_rows, out_rows, pl.BlockSpec(memory_space=pl.ANY)],
        [shape_of((rows, width), out_type), shape_of((rows, width), out_type),
         shape_of((owners, parts * count, LANES), BF16)],
        scratch=[pltpu.VMEM((width, rows), BF16), pltpu.VMEM((rows, width), F32), pltpu.VMEM((rows, width), F32),
                 pltpu.VMEM(stage, BF16), pltpu.VMEM(stage, BF16), pltpu.VMEM((2, block, width), BF16),
                 pltpu.SemaphoreType.DMA((2, copies))],
        flops=18 * rows * width * hidden, moved=12 * width * hidden + 16 * rows * width, trans=rows * hidden,
        aliases={5: 2} if held else None,
    )(x, gy, w_gu, w_gu, w_down, *held)


def to_panels(array):
    rows, columns = array.shape
    return jnp.transpose(array.reshape(rows, columns // BLOCK, BLOCK), (1, 0, 2)).reshape(-1, BLOCK)


def panels_to(rows_array, rows, panels):
    return jnp.transpose(rows_array.reshape(panels, rows, LANES), (1, 0, 2)).reshape(rows, panels * LANES)


def attention_weights_kernel(per, normed_ref, mixed_ref, gq_ref, gk_ref, gv_ref, ga_ref, gains_ref, out_ref, xt):
    step = pl.program_id(0)
    owners, rows = out_ref.shape[0], out_ref.shape[1] // (out_ref.shape[1] // (normed_ref.shape[1] // out_ref.shape[0]))
    panels = out_ref.shape[1] // rows

    @pl.when(step == 0)
    def _():
        xt[...] = normed_ref[...].T

    @pl.when(step == 3 * per)
    def _():
        xt[...] = mixed_ref[...].T

    for index, grad_ref in enumerate((gq_ref, gk_ref, gv_ref, ga_ref)):

        @pl.when((step >= index * per) & (step < (index + 1) * per))
        def _():
            product = dot_nn(xt[...], grad_ref[...]).astype(BF16)
            for p in range(panels):
                out_ref[:, pl.ds(p * rows, rows), :] = product[:, p * LANES : (p + 1) * LANES].reshape(owners, rows, LANES)

    @pl.when(step >= 4 * per)
    def _():
        out_ref[...] = jnp.zeros_like(out_ref)

    @pl.when(step == 4 * per)
    def _():
        out_ref[:, pl.ds(0, gains_ref.shape[1]), :] = gains_ref[...]


def attention_weights(normed, mixed, grads, grad_attn, gains, owners, pieces):
    tokens, width = normed.shape
    rows = width // owners
    block = BLOCK
    panels, per = block // LANES, width // block
    steps = 4 * per + 1
    while steps * panels * rows % (16 * pieces):
        steps += 1

    def columns(index):
        return pl.BlockSpec((tokens, block), lambda i: (0, jnp.clip(i - index * per, 0, per - 1)))

    return call(
        functools.partial(attention_weights_kernel, per), (steps,),
        [whole((tokens, width)), whole((tokens, width))] + [columns(index) for index in range(4)] + [whole(gains.shape)],
        pl.BlockSpec((owners, panels * rows, LANES), lambda i: (0, i, 0)),
        shape_of((owners, steps * panels * rows, LANES), BF16),
        scratch=[pltpu.VMEM((width, tokens), BF16)],
        flops=8 * tokens * width * width, moved=16 * tokens * width,
    )(normed, mixed, *grads, grad_attn, gains)


def sum_over_kernel(axis, count, x_ref, out_ref, landed, own, send_sem, recv_sem):
    me = lax.axis_index(axis)
    peers = [lax.rem(me + step, count) for step in range(1, count)]
    barrier = pltpu.get_barrier_semaphore()
    for peer in peers:
        pl.semaphore_signal(barrier, inc=1, device_id={axis: peer}, device_id_type=pl.DeviceIdType.MESH)
    pl.semaphore_wait(barrier, count - 1)

    def send(phase, step, source, target):
        copy = pltpu.make_async_remote_copy(
            src_ref=source, dst_ref=target, send_sem=send_sem.at[phase, step], recv_sem=recv_sem.at[phase, step],
            device_id={axis: peers[step]}, device_id_type=pl.DeviceIdType.MESH,
        )
        copy.start()
        return copy

    first = [send(0, step, x_ref.at[peers[step]], landed.at[step]) for step in range(count - 1)]
    total = x_ref[me].astype(F32)
    for step, copy in enumerate(first):
        copy.wait()
        total = total + landed[step].astype(F32)
    own[...] = total.astype(own.dtype)
    second = [send(1, step, own, out_ref.at[me]) for step in range(count - 1)]
    out_ref[me] = own[...]
    for copy in second:
        copy.wait()


def sum_over(x, axis, count, collective_id):
    rows = x.shape[0]
    shape = (count, rows // count, LANES)
    vmem = pl.BlockSpec(memory_space=pltpu.VMEM)
    return pl.pallas_call(
        functools.partial(sum_over_kernel, axis, count),
        out_shape=shape_of(shape, x.dtype),
        in_specs=[vmem],
        out_specs=vmem,
        scratch_shapes=[
            pltpu.VMEM((count - 1,) + shape[1:], x.dtype),
            pltpu.VMEM(shape[1:], x.dtype),
            pltpu.SemaphoreType.DMA((2, count - 1)),
            pltpu.SemaphoreType.DMA((2, count - 1)),
        ],
        compiler_params=pltpu.CompilerParams(collective_id=collective_id, has_side_effects=True),
        cost_estimate=pl.CostEstimate(flops=rows * LANES * count, bytes_accessed=40 * rows * LANES, transcendentals=0),
    )(x.reshape(shape)).reshape(rows, LANES)


GROUP = ("dp", "shard")


def local(
    tokens,
    lengths,
    routes,
    route_gates,
    cotangent,
    norm_gains,
    w_qkv,
    w_out,
    w_shared_gu,
    w_shared_down,
    w_expert_gu,
    w_expert_down,
):
    tok_count, width = tokens.shape
    seq_count = lengths.shape[0]
    length = tok_count // seq_count
    local_experts = w_expert_gu.shape[0]
    owners = lax.axis_size("expert")
    experts = local_experts * owners
    top = routes.shape[1]
    capacity = tok_count * top * 9 // (8 * experts)
    head_dim = width // HEADS
    hidden = w_expert_down.shape[1]

    gains = lax.all_gather(norm_gains, GROUP, axis=1, tiled=True).astype(F32)
    attention_weight = lax.all_gather(jnp.concatenate([w_qkv, w_out], axis=1), GROUP, axis=0, tiled=True)
    shared_weight = lax.all_gather(
        jnp.concatenate([to_panels(w_shared_gu), to_panels(w_shared_down)], axis=0)[None], GROUP, axis=0, tiled=True
    )
    gain_one, gain_two = gains[0:1], gains[1:2]

    live_bool = lax.iota(jnp.int32, tok_count) % length < jnp.repeat(lengths, length)
    live = live_bool.astype(F32)[:, None]
    live_row = live_bool.astype(jnp.int32)[None, :]

    group = lax.axis_size("dp") * lax.axis_size("shard")
    shared_hidden = w_shared_down.shape[0] * group

    dest_t = slots_of(routes.T, live_row, experts, capacity)
    dest = dest_t.T
    slots = owners * capacity

    def place(where):
        owner_of, part_of = where // (local_experts * capacity), (where // capacity) % local_experts
        return jnp.where(
            where < experts * capacity, part_of * slots + owner_of * capacity + where % capacity, experts * capacity
        )

    placed, placed_t = place(dest), place(dest_t)
    gates_t = route_gates.T
    grad_b = jnp.where(live_bool[:, None], cotangent, 0).astype(BF16)

    def exchange(rows):
        count = rows.shape[0] // owners
        return lax.all_to_all(
            rows.reshape(owners, count, width), "expert", split_axis=0, concat_axis=0, tiled=True
        ).reshape(rows.shape)

    send_grad = dispatch(dest_t, gates_t, grad_b, experts, capacity, True, 0)
    received_grad = exchange(send_grad).reshape(owners, local_experts * capacity, width)

    cosine, sine = rotary_tables(length, head_dim)
    normed_one = norm_one(tokens, gain_one)
    queries, keys, values, mixed, lse = attend_forward(normed_one, attention_weight, cosine, sine, length, head_dim)
    first_sum, normed_two = norm_two(mixed, tokens, attention_weight, gain_two)

    received = []
    for j in range(local_experts):
        rows = dispatch(placed_t, gates_t, normed_two, owners, capacity, False, j * owners)
        received.append(exchange(rows))
    shared_out, grad_shared, shared_pack = ffn_both(
        normed_two, grad_b, shared_weight, shared_weight, shared_hidden, None, group, F32
    )
    back_rows, out_rows, pack = [], [], None
    for j in range(local_experts):
        y, gx, pack = ffn_both(
            received[j], received_grad, w_expert_gu, w_expert_down, hidden, j, group, BF16, local_experts, pack
        )
        back_rows.append(exchange(gx))
        out_rows.append(y)
    base = grad_shared
    for j, rows in enumerate(back_rows[:-1]):
        base = add_part(placed, base, rows, j)
    grad_first, grad_attn, grad_mixed, grad_gain_two = norm_two_back(
        placed, live, cotangent, first_sum, base, gain_two, attention_weight, back_rows[-1], local_experts - 1
    )

    grads = attend_backward(queries, keys, values, mixed, grad_mixed, lse, cosine, sine, length, head_dim)
    input_grad = norm_one_back(grads, attention_weight, tokens, grad_first, gain_one)
    own = width // group
    grad_gains = grad_gain_two.reshape(group, 1, own)
    grad_gains = jnp.pad(grad_gains, ((0, 0), (0, 15), (0, LANES - own))).astype(BF16)
    attention_pack = attention_weights(normed_one, mixed, grads, grad_attn, grad_gains, group, owners)

    returned = exchange_parts(out_rows, owners, "expert")
    layer_out = combine(placed, route_gates, live, first_sum, shared_out, returned)

    def spread(pack):
        return lax.psum_scatter(pack, GROUP, scatter_dimension=0, tiled=True)[0]

    shared_share = spread(shared_pack)
    expert_shares = jnp.split(spread(pack), local_experts)
    attention_share = spread(attention_pack)
    shared_share = sum_over(shared_share, "expert", owners, 1).astype(F32)
    attention_share = sum_over(attention_share, "expert", owners, 2).astype(F32)
    gu_panels, d_panels = 2 * shared_hidden // LANES, width // LANES
    qkv_rows, out_rows_count = 3 * d_panels * own, 4 * d_panels * own
    columns = 2 * hidden // group
    gu_rows = columns // LANES * width
    qkv_grad = panels_to(attention_share[:qkv_rows], own, 3 * d_panels)
    grad_gain_one = jnp.sum(w_qkv.astype(F32) * qkv_grad, axis=1) / norm_gains[0].astype(F32)
    return (
        layer_out,
        input_grad,
        jnp.stack([grad_gain_one, attention_share[out_rows_count, :own]]),
        qkv_grad,
        panels_to(attention_share[qkv_rows:out_rows_count], own, d_panels),
        panels_to(shared_share[: gu_panels * own], own, gu_panels),
        panels_to(shared_share[gu_panels * own :], shared_hidden // group, d_panels),
        jnp.stack([panels_to(share[:gu_rows], width, columns // LANES) for share in expert_shares]).astype(F32),
        jnp.stack([panels_to(share[gu_rows:], hidden // group, d_panels) for share in expert_shares]).astype(F32),
    )


def exchange_parts(parts, owners, axis):
    width = parts[0].shape[1]
    count = parts[0].shape[0] // owners
    joined = jnp.concatenate([rows.reshape(owners, count, width) for rows in parts], axis=1)
    back = lax.all_to_all(joined, axis, split_axis=0, concat_axis=0, tiled=True)
    return [
        back[:, j * count : (j + 1) * count].reshape(owners * count, width) for j in range(len(parts))
    ]


def solution(mesh):
    rows = P(("dp", "expert", "shard"), None)
    split = P(GROUP, None)
    in_specs = (
        rows,
        P(("dp", "expert", "shard")),
        rows,
        rows,
        rows,
        P(None, GROUP),
        split,
        split,
        split,
        split,
        P("expert", None, None),
        P("expert", None, None),
    )
    out_specs = (
        rows,
        rows,
        P(None, GROUP),
        split,
        split,
        split,
        split,
        P("expert", None, GROUP),
        P("expert", GROUP, None),
    )

    return jax.shard_map(local, mesh=mesh, in_specs=in_specs, out_specs=out_specs, check_vma=False)
```

```python
import functools
import math

import jax
import jax.numpy as jnp
from jax import lax
from jax.experimental import pallas as pl
from jax.experimental.pallas import tpu as pltpu
from jax.sharding import PartitionSpec as P


HEADS = 12
LANES = 128
EPSILON = 1e-05
VMEM_BYTES = 60 * 1024 * 1024
BF16 = jnp.bfloat16
F32 = jnp.float32


def call(kernel, grid, in_specs, out_specs, out_shape, scratch=(), flops=0, moved=0, trans=0, aliases=None):
    return pl.pallas_call(
        kernel,
        grid_spec=pltpu.PrefetchScalarGridSpec(
            num_scalar_prefetch=0,
            grid=grid,
            in_specs=in_specs,
            out_specs=out_specs,
            scratch_shapes=list(scratch),
        ),
        out_shape=out_shape,
        input_output_aliases=aliases or {},
        compiler_params=pltpu.CompilerParams(
            dimension_semantics=("arbitrary",) * len(grid), vmem_limit_bytes=VMEM_BYTES
        ),
        cost_estimate=pl.CostEstimate(flops=flops, bytes_accessed=moved, transcendentals=trans),
    )


def shape_of(shape, dtype):
    return jax.ShapeDtypeStruct(shape, dtype)


def whole(shape):
    return pl.BlockSpec(shape, lambda *_: (0,) * len(shape), pipeline_mode=pl.Buffered(1))


def dot_nn(left, right):
    return lax.dot_general(left, right, (((1,), (0,)), ((), ())), preferred_element_type=F32)


def dot_nt(left, right):
    return lax.dot_general(left, right, (((1,), (1,)), ((), ())), preferred_element_type=F32)


def dot_tn(left, right):
    return lax.dot_general(left, right, (((0,), (0,)), ((), ())), preferred_element_type=F32)


def rotary_tables(length, head_dim):
    half_dim = head_dim // 2
    position = lax.iota(F32, length)[:, None]
    frequency = jnp.exp(lax.iota(F32, half_dim) * (-2.0 * math.log(10000.0) / head_dim))
    angle_table = position * frequency[None, :]
    cosine, sine = jnp.cos(angle_table), jnp.sin(angle_table)
    repeats = LANES // head_dim
    return (
        jnp.tile(jnp.concatenate([cosine, cosine], axis=1), (1, repeats)),
        jnp.tile(jnp.concatenate([-sine, sine], axis=1), (1, repeats)),
    )


def turn(values, cosine, signed_sine, head_dim):
    lane = lax.broadcasted_iota(jnp.int32, values.shape, 1)
    half = head_dim // 2
    other = jnp.where(
        lane % head_dim < half,
        pltpu.roll(values, LANES - half, 1),
        pltpu.roll(values, half, 1),
    )
    return values * cosine + other * signed_sine


def attend_forward_kernel(
    head_dim, block, x_ref, wq_ref, wk_ref, wv_ref, cos_ref, sin_ref, q_ref, k_ref, v_ref, o_ref, lse_ref, lse_tile
):
    length = x_ref.shape[0]
    heads = LANES // head_dim
    x = x_ref[...]
    cosine, sine = cos_ref[...], sin_ref[...]
    scale = 1.0 / math.sqrt(head_dim)
    q_ref[...] = (turn(dot_nn(x, wq_ref[...]), cosine, sine, head_dim) * scale).astype(BF16)
    k_ref[...] = turn(dot_nn(x, wk_ref[...]), cosine, sine, head_dim).astype(BF16)
    v_ref[...] = dot_nn(x, wv_ref[...]).astype(BF16)
    lane = lax.broadcasted_iota(jnp.int32, (1, LANES), 1)
    own_lane = lax.broadcasted_iota(jnp.int32, (block, LANES), 1) // head_dim
    below = lax.broadcasted_iota(jnp.int32, (block, block), 0) >= lax.broadcasted_iota(
        jnp.int32, (block, block), 1
    )
    for first in range(0, length, block):
        rows = pl.ds(first, block)
        mixed = None
        logs = None
        for head in range(heads):
            select = (lane // head_dim == head).astype(F32).astype(BF16)
            queries = q_ref[rows, :] * select
            near = jnp.where(below, dot_nt(queries, k_ref[rows, :]), -1e30)
            peak = jnp.max(near, axis=1, keepdims=True)
            if first:
                far = dot_nt(queries, k_ref[pl.ds(0, first), :])
                peak = jnp.maximum(peak, jnp.max(far, axis=1, keepdims=True))
            near = jnp.exp(near - peak)
            total = jnp.sum(near, axis=1, keepdims=True)
            part = dot_nn(near.astype(BF16), v_ref[rows, :])
            if first:
                far = jnp.exp(far - peak)
                total = total + jnp.sum(far, axis=1, keepdims=True)
                part = part + dot_nn(far.astype(BF16), v_ref[pl.ds(0, first), :])
            part = part * (1.0 / total)
            log_total = jnp.broadcast_to(peak + jnp.log(total), (block, LANES))
            mixed = part if head == 0 else jnp.where(own_lane == head, part, mixed)
            logs = log_total if head == 0 else jnp.where(own_lane == head, log_total, logs)
        o_ref[rows, :] = mixed.astype(BF16)
        lse_tile[rows, :] = logs
    turned = lse_tile[...].T
    for head in range(heads):
        lse_ref[pl.ds(head * 8, 8), :] = turned[head * head_dim : head * head_dim + 8, :]


def attend_forward(normed, w_qkv, cosine, sine, length, head_dim):
    tokens, width = normed.shape
    seqs, pairs, heads = tokens // length, width // LANES, LANES // head_dim
    block = min(256, length)
    rows = pl.BlockSpec((length, LANES), lambda s, p: (s, p))

    def weight(part):
        return pl.BlockSpec((width, LANES), lambda s, p: (0, part * pairs + p))

    table = whole((length, LANES))
    return call(
        functools.partial(attend_forward_kernel, head_dim, block),
        (seqs, pairs),
        [pl.BlockSpec((length, width), lambda s, p: (s, 0)), weight(0), weight(1), weight(2), table, table],
        [rows, rows, rows, rows, pl.BlockSpec((8 * heads, length), lambda s, p: (s * pairs + p, 0))],
        [shape_of((tokens, width), BF16)] * 4 + [shape_of((seqs * pairs * 8 * heads, length), F32)],
        scratch=[pltpu.VMEM((length, LANES), F32)],
        flops=6 * tokens * width * width + 4 * tokens * length * width,
        moved=16 * tokens * width,
        trans=tokens * length * width // head_dim // 2,
    )(normed, w_qkv, w_qkv, w_qkv, cosine, sine)


def attend_backward_kernel(
    head_dim, block, q_ref, k_ref, v_ref, o_ref, g_ref, lse_ref, cos_ref, sin_ref, gq_ref, gk_ref, gv_ref, gq_acc
):
    length = q_ref.shape[0]
    heads = LANES // head_dim
    scale = 1.0 / math.sqrt(head_dim)
    product = (g_ref[...].astype(F32) * o_ref[...].astype(F32)).T
    inner = [
        jnp.sum(product[head * head_dim : (head + 1) * head_dim, :], axis=0, keepdims=True)
        for head in range(heads)
    ]
    gq_acc[...] = jnp.zeros_like(gq_acc)
    lane = lax.broadcasted_iota(jnp.int32, (1, LANES), 1)
    own_lane = lax.broadcasted_iota(jnp.int32, (block, LANES), 1) // head_dim
    above = lax.broadcasted_iota(jnp.int32, (block, block), 1) >= lax.broadcasted_iota(
        jnp.int32, (block, block), 0
    )
    for first in range(0, length, block):
        rows = pl.ds(first, block)
        keys_grad = None
        values_grad = None
        for head in range(heads):
            select = (lane // head_dim == head).astype(F32).astype(BF16)
            keys = k_ref[rows, :] * select
            values = v_ref[rows, :] * select
            log_total = lse_ref[pl.ds(head * 8, 1), :]
            pieces = [(first, block, True)]
            if first + block < length:
                pieces.append((first + block, length - first - block, False))
            keys_part = None
            values_part = None
            for start, count, diagonal in pieces:
                span = pl.ds(start, count)
                queries, grads = q_ref[span, :], g_ref[span, :]
                scores = dot_nt(keys, queries)
                probs = jnp.exp(scores - log_total[:, start : start + count])
                if diagonal:
                    probs = jnp.where(above, probs, 0.0)
                grad_probs = dot_nt(values, grads)
                grad_scores = (probs * (grad_probs - inner[head][:, start : start + count])).astype(BF16)
                piece_values = dot_nn(probs.astype(BF16), grads)
                piece_keys = dot_nn(grad_scores, queries)
                values_part = piece_values if values_part is None else values_part + piece_values
                keys_part = piece_keys if keys_part is None else keys_part + piece_keys
                gq_acc[span, :] += dot_tn(grad_scores, keys)
            keys_grad = keys_part if head == 0 else jnp.where(own_lane == head, keys_part, keys_grad)
            values_grad = values_part if head == 0 else jnp.where(own_lane == head, values_part, values_grad)
        gk_ref[rows, :] = turn(keys_grad, cos_ref[rows, :], -sin_ref[rows, :], head_dim).astype(BF16)
        gv_ref[rows, :] = values_grad.astype(BF16)
    gq_ref[...] = turn(gq_acc[...] * scale, cos_ref[...], -sin_ref[...], head_dim).astype(BF16)


def attend_backward(queries, keys, values, mixed, grad_mixed, lse, cosine, sine, length, head_dim):
    tokens, width = queries.shape
    seqs, pairs, heads = tokens // length, width // LANES, LANES // head_dim
    block = min(256, length)
    rows = pl.BlockSpec((length, LANES), lambda s, p: (s, p))
    table = whole((length, LANES))
    return call(
        functools.partial(attend_backward_kernel, head_dim, block),
        (seqs, pairs),
        [rows] * 5 + [pl.BlockSpec((8 * heads, length), lambda s, p: (s * pairs + p, 0)), table, table],
        [rows] * 3,
        [shape_of((tokens, width), BF16)] * 3,
        scratch=[pltpu.VMEM((length, LANES), F32)],
        flops=10 * tokens * length * width,
        moved=16 * tokens * width,
        trans=tokens * length * width // head_dim // 2,
    )(queries, keys, values, mixed, grad_mixed, lse, cosine, sine)


def square(width, part):
    return pl.BlockSpec((width, width), lambda i: (0, part), pipeline_mode=pl.Buffered(1))


def norm_one_kernel(x_ref, gain_ref, out_ref):
    x = x_ref[...].astype(F32)
    scale = lax.rsqrt(jnp.mean(x * x, axis=1, keepdims=True) + EPSILON)
    out_ref[...] = (x * scale * gain_ref[...]).astype(BF16)


def norm_one(tokens, gain):
    rows, width = tokens.shape
    block = min(256, rows)
    blocked = pl.BlockSpec((block, width), lambda i: (i, 0))
    return call(
        norm_one_kernel, (rows // block,), [blocked, whole((1, width))], blocked, shape_of((rows, width), BF16),
        flops=5 * rows * width, moved=4 * rows * width,
    )(tokens, gain)


def norm_two_kernel(mixed_ref, tokens_ref, weight_ref, gain_ref, sum_ref, normed_ref):
    first_sum = tokens_ref[...].astype(F32) + dot_nn(mixed_ref[...], weight_ref[...])
    sum_ref[...] = first_sum
    scale = lax.rsqrt(jnp.mean(first_sum * first_sum, axis=1, keepdims=True) + EPSILON)
    normed_ref[...] = (first_sum * scale * gain_ref[...]).astype(BF16)


def norm_two(mixed, tokens, weight, gain):
    rows, width = tokens.shape
    block = min(256, rows)
    blocked = pl.BlockSpec((block, width), lambda i: (i, 0))
    return call(
        norm_two_kernel, (rows // block,), [blocked, blocked, square(width, 3), whole((1, width))],
        [blocked, blocked], [shape_of((rows, width), F32), shape_of((rows, width), BF16)],
        flops=2 * rows * width * width, moved=10 * rows * width,
    )(mixed, tokens, weight, gain)


def slots_kernel(experts, capacity, routes_ref, live_ref, dest_ref):
    top, tokens = routes_ref.shape
    live = live_ref[...]
    number = lax.broadcasted_iota(jnp.int32, (experts, tokens), 0)
    hits = [
        jnp.where((routes_ref[pl.ds(k, 1), :] == number) & (live > 0), 1.0, 0.0) for k in range(top)
    ]
    earlier = jnp.where(
        lax.broadcasted_iota(jnp.int32, (tokens, tokens), 0)
        <= lax.broadcasted_iota(jnp.int32, (tokens, tokens), 1),
        1.0,
        0.0,
    ).astype(BF16)
    ranks = dot_nn(jnp.concatenate(hits, axis=0).astype(BF16), earlier)
    before = jnp.zeros((experts, 1), F32)
    for k in range(top):
        rank = ranks[k * experts : (k + 1) * experts, :]
        place = number.astype(F32) * capacity + before + rank - 1.0
        slot = jnp.sum(hits[k] * place, axis=0, keepdims=True).astype(jnp.int32)
        dest_ref[pl.ds(k, 1), :] = jnp.where(live > 0, slot, experts * capacity)
        before = before + jnp.sum(hits[k], axis=1, keepdims=True)


def slots_of(routes_t, live_row, experts, capacity):
    top, tokens = routes_t.shape
    return call(
        functools.partial(slots_kernel, experts, capacity), (1,),
        [whole((top, tokens)), whole((1, tokens))], whole((top, tokens)), shape_of((top, tokens), jnp.int32),
        flops=2 * top * experts * tokens * tokens, moved=16 * tokens,
    )(routes_t, live_row)


def dispatch_kernel(gated, first, dest_ref, gates_ref, x_ref, out_ref):
    top, tokens = dest_ref.shape
    capacity = out_ref.shape[0]
    slot = lax.broadcasted_iota(jnp.int32, (capacity, tokens), 0) + (first + pl.program_id(0)) * capacity
    hits = [slot == dest_ref[pl.ds(k, 1), :] for k in range(top)]
    chosen = functools.reduce(jnp.logical_or, hits)
    rows = dot_nn(jnp.where(chosen, 1.0, 0.0).astype(BF16), x_ref[...])
    if gated:
        weights = jnp.zeros((capacity, tokens), F32)
        for k in range(top):
            weights = jnp.where(hits[k], gates_ref[pl.ds(k, 1), :], weights)
        rows = rows * jnp.sum(weights, axis=1, keepdims=True)
    out_ref[...] = rows.astype(BF16)


def dispatch(dest_t, gates_t, x, experts, capacity, gated, first):
    top, tokens = dest_t.shape
    width = x.shape[1]
    return call(
        functools.partial(dispatch_kernel, gated, first), (experts,),
        [whole((top, tokens)), whole((top, tokens)), whole((tokens, width))],
        pl.BlockSpec((capacity, width), lambda e: (e, 0)),
        shape_of((experts * capacity, width), BF16),
        flops=2 * experts * capacity * tokens * width, moved=2 * (experts * capacity + tokens) * width,
    )(dest_t, gates_t, x)


def combine_kernel(parts, dest_ref, gates_ref, live_ref, sum_ref, shared_ref, *rest):
    y_refs, out_ref = rest[:parts], rest[parts]
    block, top = dest_ref.shape
    total = sum_ref[...] + shared_ref[...]
    dest = dest_ref[...]
    gates = gates_ref[...]
    for index, y_ref in enumerate(y_refs):
        y = y_ref[...]
        slot = slot_numbers(block, y_ref.shape[0], index)
        for k in range(top):
            hit = jnp.where(slot == dest[:, k : k + 1], 1.0, 0.0).astype(BF16)
            total = total + dot_nn(hit, y) * gates[:, k : k + 1]
    out_ref[...] = (live_ref[...] * total).astype(BF16)


def slot_numbers(block, slots, part):
    return lax.broadcasted_iota(jnp.int32, (block, slots), 1) + part * slots


def combine(dest, gates, live, first_sum, shared_out, returned):
    rows, width = first_sum.shape
    top = dest.shape[1]
    block = min(256, rows)
    parts = len(returned)
    blocked = pl.BlockSpec((block, width), lambda i: (i, 0))
    narrow = pl.BlockSpec((block, top), lambda i: (i, 0))
    slots = sum(y.shape[0] for y in returned)
    return call(
        functools.partial(combine_kernel, parts), (rows // block,),
        [narrow, narrow, pl.BlockSpec((block, 1), lambda i: (i, 0)), blocked, blocked]
        + [whole(y.shape) for y in returned],
        blocked, shape_of((rows, width), BF16),
        flops=4 * rows * slots * width, moved=10 * rows * width + 2 * slots * width,
    )(dest, gates, live, first_sum, shared_out, *returned)


def gathered(dest_ref, y_ref, part):
    block, top = dest_ref.shape
    dest = dest_ref[...]
    slot = slot_numbers(block, y_ref.shape[0], part)
    hit = functools.reduce(jnp.logical_or, [slot == dest[:, k : k + 1] for k in range(top)])
    return dot_nn(jnp.where(hit, 1.0, 0.0).astype(BF16), y_ref[...])


def add_part_kernel(part, dest_ref, base_ref, y_ref, out_ref):
    out_ref[...] = base_ref[...] + gathered(dest_ref, y_ref, part)


def add_part(dest, base, rows_of, part):
    rows, width = base.shape
    block = min(256, rows)
    blocked = pl.BlockSpec((block, width), lambda i: (i, 0))
    return call(
        functools.partial(add_part_kernel, part), (rows // block,),
        [pl.BlockSpec((block, dest.shape[1]), lambda i: (i, 0)), blocked, whole(rows_of.shape)],
        blocked, shape_of((rows, width), F32),
        flops=2 * rows * rows_of.shape[0] * width, moved=8 * rows * width,
    )(dest, base, rows_of)


def norm_two_back_kernel(part, dest_ref, live_ref, cot_ref, sum_ref, base_ref, gain_ref, weight_ref, y_ref,
                         first_ref, attn_ref, mixed_ref, gain_grad_ref):
    grad_normed = base_ref[...] + gathered(dest_ref, y_ref, part)
    first_sum = sum_ref[...]
    scale = lax.rsqrt(jnp.mean(first_sum * first_sum, axis=1, keepdims=True) + EPSILON)
    weighted = grad_normed * gain_ref[...]
    inner = jnp.mean(first_sum * weighted, axis=1, keepdims=True)
    grad_first = (
        cot_ref[...].astype(F32) * live_ref[...] + scale * weighted - first_sum * (scale * scale * scale * inner)
    )
    first_ref[...] = grad_first
    grad_attn = grad_first.astype(BF16)
    attn_ref[...] = grad_attn
    mixed_ref[...] = dot_nt(grad_attn, weight_ref[...]).astype(BF16)

    @pl.when(pl.program_id(0) == 0)
    def _():
        gain_grad_ref[...] = jnp.zeros_like(gain_grad_ref)

    gain_grad_ref[...] += jnp.sum(grad_normed * first_sum * scale, axis=0, keepdims=True)


def norm_two_back(dest, live, cotangent, first_sum, base, gain, weights, rows_of, part):
    rows, width = first_sum.shape
    top = dest.shape[1]
    block = min(256, rows)
    blocked = pl.BlockSpec((block, width), lambda i: (i, 0))
    return call(
        functools.partial(norm_two_back_kernel, part), (rows // block,),
        [pl.BlockSpec((block, top), lambda i: (i, 0)), pl.BlockSpec((block, 1), lambda i: (i, 0)), blocked, blocked,
         blocked, whole((1, width)), square(width, 3), whole(rows_of.shape)],
        [blocked, blocked, blocked, pl.BlockSpec((1, width), lambda i: (0, 0))],
        [shape_of((rows, width), F32), shape_of((rows, width), BF16), shape_of((rows, width), BF16),
         shape_of((1, width), F32)],
        flops=2 * rows * (rows_of.shape[0] + width) * width, moved=18 * rows * width,
    )(dest, live, cotangent, first_sum, base, gain, weights, rows_of)


def norm_one_back_kernel(gq_ref, gk_ref, gv_ref, wq_ref, wk_ref, wv_ref, tokens_ref, first_ref, gain_ref, out_ref):
    grad_normed = (
        dot_nt(gq_ref[...], wq_ref[...]) + dot_nt(gk_ref[...], wk_ref[...]) + dot_nt(gv_ref[...], wv_ref[...])
    )
    source = tokens_ref[...].astype(F32)
    scale = lax.rsqrt(jnp.mean(source * source, axis=1, keepdims=True) + EPSILON)
    weighted = grad_normed * gain_ref[...]
    inner = jnp.mean(source * weighted, axis=1, keepdims=True)
    out_ref[...] = first_ref[...] + scale * weighted - source * (scale * scale * scale * inner)


def norm_one_back(grads, w_qkv, tokens, grad_first, gain):
    rows, width = tokens.shape
    block = min(256, rows)
    blocked = pl.BlockSpec((block, width), lambda i: (i, 0))

    return call(
        norm_one_back_kernel, (rows // block,),
        [blocked] * 3 + [square(width, 0), square(width, 1), square(width, 2), blocked, blocked, whole((1, width))],
        blocked, shape_of((rows, width), F32),
        flops=6 * rows * width * width, moved=22 * rows * width,
    )(*grads, w_qkv, w_qkv, w_qkv, tokens, grad_first, gain)


def copies_of(layout, block, width, step, stage_g, stage_u, stage_d, slot, packed_ref, sems):
    by_rows, owners, hidden, base = layout
    panels = block // LANES
    rows_down = hidden // owners
    out = []

    def add(source, target):
        out.append(pltpu.make_async_copy(source, target, sems.at[slot, len(out)]))

    if by_rows:
        rows = width // owners
        for half, stage in enumerate((stage_g, stage_u)):
            for p in range(panels):
                panel = half * (hidden // LANES) + step * panels + p
                add(
                    stage.at[slot, :, :, pl.ds(p * LANES, LANES)],
                    packed_ref.at[:, pl.ds(pl.multiple_of(base + panel * rows, 8), rows), :],
                )
        start = 2 * hidden // LANES * rows
    else:
        columns = 2 * hidden // owners
        for half, stage in enumerate((stage_g, stage_u)):
            for p in range(panels):
                column = half * hidden + step * block + p * LANES
                owner, panel = column // columns, (column % columns) // LANES
                add(
                    stage.at[slot, :, pl.ds(p * LANES, LANES)],
                    packed_ref.at[owner, pl.ds(pl.multiple_of(base + panel * width, 8), width), :],
                )
        start = columns // LANES * width
    for q in range(block // rows_down):
        owner = step * (block // rows_down) + q
        for c in range(width // LANES):
            add(
                stage_d.at[slot, pl.ds(q * rows_down, rows_down), pl.ds(c * LANES, LANES)],
                packed_ref.at[owner, pl.ds(base + start + c * rows_down, rows_down), :],
            )
    return out


def packed_rows(width, hidden, owners):
    return 3 * width * hidden // owners // LANES


def ffn_kernel(out_type, layout, block, x_ref, gy_ref, wg_ref, wu_ref, wd_ref, *rest):
    y_ref, gx_ref, packed_ref, xt, y_acc, gx_acc, stage_g, stage_u, stage_d, sems = rest[-10:]
    step = pl.program_id(0)
    steps = layout[2] // block
    width = x_ref.shape[1]
    slot = step % 2
    copies = functools.partial(copies_of, layout, block, width)

    @pl.when(step == 0)
    def _():
        xt[...] = x_ref[...].T
        y_acc[...] = jnp.zeros_like(y_acc)
        gx_acc[...] = jnp.zeros_like(gx_acc)

    @pl.when(step >= 2)
    def _():
        for copy in copies(step - 2, stage_g, stage_u, stage_d, slot, packed_ref, sems):
            copy.wait()

    x, gy = x_ref[...], gy_ref[...].reshape(x_ref.shape)
    if layout[0]:
        wg, wu = wg_ref[...].reshape(width, block), wu_ref[...].reshape(width, block)
        rows = wd_ref.shape[1] // (width // block)
        wd = jnp.concatenate(
            [wd_ref[:, pl.ds(c * rows, rows), :].reshape(block, block) for c in range(width // block)], axis=1
        )
    else:
        wg, wu, wd = wg_ref[...], wu_ref[...], wd_ref[...]
    gate, up = dot_nn(x, wg), dot_nn(x, wu)
    grad_hidden = dot_nt(gy, wd)
    sigmoid = jax.nn.sigmoid(gate)
    value = gate * sigmoid
    hidden = (value * up).astype(BF16)
    grad_up = (grad_hidden * value).astype(BF16)
    grad_gate = (grad_hidden * up * (sigmoid * (1.0 + gate * (1.0 - sigmoid)))).astype(BF16)
    y_acc[...] += dot_nn(hidden, wd)
    gx_acc[...] += dot_nt(grad_gate, wg) + dot_nt(grad_up, wu)
    stage_g[slot] = dot_nn(xt[...], grad_gate).astype(BF16).reshape(stage_g.shape[1:])
    stage_u[slot] = dot_nn(xt[...], grad_up).astype(BF16).reshape(stage_u.shape[1:])
    stage_d[slot] = dot_tn(hidden, gy).astype(BF16)
    for copy in copies(step, stage_g, stage_u, stage_d, slot, packed_ref, sems):
        copy.start()

    @pl.when(step == steps - 1)
    def _():
        y_ref[...] = y_acc[...].astype(out_type)
        gx_ref[...] = gx_acc[...].astype(out_type)
        for back in (1, 0):
            if steps > back:
                for copy in copies(steps - 1 - back, stage_g, stage_u, stage_d, (steps - 1 - back) % 2, packed_ref, sems):
                    copy.wait()


BLOCK = 256


def ffn_both(x, gy, w_gu, w_down, hidden, expert, owners, out_type):
    rows, width = x.shape
    block = BLOCK
    steps = hidden // block
    by_rows = expert is None
    if by_rows:
        own, own_down, panels = width // owners, hidden // owners, width // block
        ahead = 2 * steps * own // (panels * own_down)
        gate = pl.BlockSpec((owners, own, block), lambda f: (0, f, 0))
        up = pl.BlockSpec((owners, own, block), lambda f: (0, steps + f, 0))
        down = pl.BlockSpec((block // own_down, panels * own_down, block), lambda f: (f, ahead, 0))
        stage = (2, owners, own, block)
    else:
        gate = pl.BlockSpec((None, width, block), lambda f: (expert, 0, f))
        up = pl.BlockSpec((None, width, block), lambda f: (expert, 0, steps + f))
        down = pl.BlockSpec((None, block, width), lambda f: (expert, f, 0))
        stage = (2, width, block)
    if by_rows:
        grads = whole((rows, width))
    else:
        grads = pl.BlockSpec(
            (gy.shape[0], rows // gy.shape[0], width), lambda f: (0, expert, 0), pipeline_mode=pl.Buffered(1)
        )
    out_rows = whole((rows, width))
    count = packed_rows(width, hidden, owners)
    layout = (by_rows, owners, hidden, 0)
    copies = 2 * (block // LANES) + block // (hidden // owners) * (width // LANES)
    return call(
        functools.partial(ffn_kernel, out_type, layout, block), (steps,),
        [whole((rows, width)), grads, gate, up, down],
        [out_rows, out_rows, pl.BlockSpec(memory_space=pl.ANY)],
        [shape_of((rows, width), out_type), shape_of((rows, width), out_type),
         shape_of((owners, count, LANES), BF16)],
        scratch=[pltpu.VMEM((width, rows), BF16), pltpu.VMEM((rows, width), F32), pltpu.VMEM((rows, width), F32),
                 pltpu.VMEM(stage, BF16), pltpu.VMEM(stage, BF16), pltpu.VMEM((2, block, width), BF16),
                 pltpu.SemaphoreType.DMA((2, copies))],
        flops=18 * rows * width * hidden, moved=12 * width * hidden + 16 * rows * width, trans=rows * hidden,
    )(x, gy, w_gu, w_gu, w_down)


def to_panels(array):
    rows, columns = array.shape
    return jnp.transpose(array.reshape(rows, columns // BLOCK, BLOCK), (1, 0, 2)).reshape(-1, BLOCK)


def panels_to(rows_array, rows, panels):
    return jnp.transpose(rows_array.reshape(panels, rows, LANES), (1, 0, 2)).reshape(rows, panels * LANES)


def attention_weights_kernel(per, normed_ref, mixed_ref, gq_ref, gk_ref, gv_ref, ga_ref, gains_ref, out_ref, xt):
    step = pl.program_id(0)
    owners, rows = out_ref.shape[0], out_ref.shape[1] // (out_ref.shape[1] // (normed_ref.shape[1] // out_ref.shape[0]))
    panels = out_ref.shape[1] // rows

    @pl.when(step == 0)
    def _():
        xt[...] = normed_ref[...].T

    @pl.when(step == 3 * per)
    def _():
        xt[...] = mixed_ref[...].T

    for index, grad_ref in enumerate((gq_ref, gk_ref, gv_ref, ga_ref)):

        @pl.when((step >= index * per) & (step < (index + 1) * per))
        def _():
            product = dot_nn(xt[...], grad_ref[...]).astype(BF16)
            for p in range(panels):
                out_ref[:, pl.ds(p * rows, rows), :] = product[:, p * LANES : (p + 1) * LANES].reshape(owners, rows, LANES)

    @pl.when(step >= 4 * per)
    def _():
        out_ref[...] = jnp.zeros_like(out_ref)

    @pl.when(step == 4 * per)
    def _():
        out_ref[:, pl.ds(0, gains_ref.shape[1]), :] = gains_ref[...]


def attention_weights(normed, mixed, grads, grad_attn, gains, owners, pieces):
    tokens, width = normed.shape
    rows = width // owners
    block = BLOCK
    panels, per = block // LANES, width // block
    steps = 4 * per + 1
    while steps * panels * rows % (16 * pieces):
        steps += 1

    def columns(index):
        return pl.BlockSpec((tokens, block), lambda i: (0, jnp.clip(i - index * per, 0, per - 1)))

    return call(
        functools.partial(attention_weights_kernel, per), (steps,),
        [whole((tokens, width)), whole((tokens, width))] + [columns(index) for index in range(4)] + [whole(gains.shape)],
        pl.BlockSpec((owners, panels * rows, LANES), lambda i: (0, i, 0)),
        shape_of((owners, steps * panels * rows, LANES), BF16),
        scratch=[pltpu.VMEM((width, tokens), BF16)],
        flops=8 * tokens * width * width, moved=16 * tokens * width,
    )(normed, mixed, *grads, grad_attn, gains)


def sum_over_kernel(axis, count, x_ref, out_ref, landed, own, send_sem, recv_sem):
    me = lax.axis_index(axis)
    peers = [lax.rem(me + step, count) for step in range(1, count)]
    barrier = pltpu.get_barrier_semaphore()
    for peer in peers:
        pl.semaphore_signal(barrier, inc=1, device_id={axis: peer}, device_id_type=pl.DeviceIdType.MESH)
    pl.semaphore_wait(barrier, count - 1)

    def send(phase, step, source, target):
        copy = pltpu.make_async_remote_copy(
            src_ref=source, dst_ref=target, send_sem=send_sem.at[phase, step], recv_sem=recv_sem.at[phase, step],
            device_id={axis: peers[step]}, device_id_type=pl.DeviceIdType.MESH,
        )
        copy.start()
        return copy

    first = [send(0, step, x_ref.at[peers[step]], landed.at[step]) for step in range(count - 1)]
    total = x_ref[me].astype(F32)
    for step, copy in enumerate(first):
        copy.wait()
        total = total + landed[step].astype(F32)
    own[...] = total.astype(own.dtype)
    second = [send(1, step, own, out_ref.at[me]) for step in range(count - 1)]
    out_ref[me] = own[...]
    for copy in second:
        copy.wait()


def sum_over(x, axis, count, collective_id):
    rows = x.shape[0]
    shape = (count, rows // count, LANES)
    vmem = pl.BlockSpec(memory_space=pltpu.VMEM)
    return pl.pallas_call(
        functools.partial(sum_over_kernel, axis, count),
        out_shape=shape_of(shape, x.dtype),
        in_specs=[vmem],
        out_specs=vmem,
        scratch_shapes=[
            pltpu.VMEM((count - 1,) + shape[1:], x.dtype),
            pltpu.VMEM(shape[1:], x.dtype),
            pltpu.SemaphoreType.DMA((2, count - 1)),
            pltpu.SemaphoreType.DMA((2, count - 1)),
        ],
        compiler_params=pltpu.CompilerParams(collective_id=collective_id, has_side_effects=True),
        cost_estimate=pl.CostEstimate(flops=rows * LANES * count, bytes_accessed=40 * rows * LANES, transcendentals=0),
    )(x.reshape(shape)).reshape(rows, LANES)


GROUP = ("dp", "shard")


def local(
    tokens,
    lengths,
    routes,
    route_gates,
    cotangent,
    norm_gains,
    w_qkv,
    w_out,
    w_shared_gu,
    w_shared_down,
    w_expert_gu,
    w_expert_down,
):
    tok_count, width = tokens.shape
    seq_count = lengths.shape[0]
    length = tok_count // seq_count
    local_experts = w_expert_gu.shape[0]
    owners = lax.axis_size("expert")
    experts = local_experts * owners
    top = routes.shape[1]
    capacity = tok_count * top * 9 // (8 * experts)
    head_dim = width // HEADS
    hidden = w_expert_down.shape[1]

    gains = lax.all_gather(norm_gains, GROUP, axis=1, tiled=True).astype(F32)
    attention_weight = lax.all_gather(jnp.concatenate([w_qkv, w_out], axis=1), GROUP, axis=0, tiled=True)
    shared_weight = lax.all_gather(
        jnp.concatenate([to_panels(w_shared_gu), to_panels(w_shared_down)], axis=0)[None], GROUP, axis=0, tiled=True
    )
    gain_one, gain_two = gains[0:1], gains[1:2]

    live_bool = lax.iota(jnp.int32, tok_count) % length < jnp.repeat(lengths, length)
    live = live_bool.astype(F32)[:, None]
    live_row = live_bool.astype(jnp.int32)[None, :]

    group = lax.axis_size("dp") * lax.axis_size("shard")
    shared_hidden = w_shared_down.shape[0] * group

    dest_t = slots_of(routes.T, live_row, experts, capacity)
    dest = dest_t.T
    slots = owners * capacity

    def place(where):
        owner_of, part_of = where // (local_experts * capacity), (where // capacity) % local_experts
        return jnp.where(
            where < experts * capacity, part_of * slots + owner_of * capacity + where % capacity, experts * capacity
        )

    placed, placed_t = place(dest), place(dest_t)
    gates_t = route_gates.T
    grad_b = jnp.where(live_bool[:, None], cotangent, 0).astype(BF16)

    def exchange(rows):
        count = rows.shape[0] // owners
        return lax.all_to_all(
            rows.reshape(owners, count, width), "expert", split_axis=0, concat_axis=0, tiled=True
        ).reshape(rows.shape)

    send_grad = dispatch(dest_t, gates_t, grad_b, experts, capacity, True, 0)
    received_grad = exchange(send_grad).reshape(owners, local_experts * capacity, width)

    cosine, sine = rotary_tables(length, head_dim)
    normed_one = norm_one(tokens, gain_one)
    queries, keys, values, mixed, lse = attend_forward(normed_one, attention_weight, cosine, sine, length, head_dim)
    first_sum, normed_two = norm_two(mixed, tokens, attention_weight, gain_two)

    received = []
    for j in range(local_experts):
        rows = dispatch(placed_t, gates_t, normed_two, owners, capacity, False, j * owners)
        received.append(exchange(rows))
    shared_out, grad_shared, shared_pack = ffn_both(
        normed_two, grad_b, shared_weight, shared_weight, shared_hidden, None, group, F32
    )
    back_rows, out_rows, expert_packs = [], [], []
    for j in range(local_experts):
        y, gx, pack = ffn_both(
            received[j], received_grad, w_expert_gu, w_expert_down, hidden, j, group, BF16
        )
        back_rows.append(exchange(gx))
        out_rows.append(y)
        expert_packs.append(pack)
    base = grad_shared
    for j, rows in enumerate(back_rows[:-1]):
        base = add_part(placed, base, rows, j)
    grad_first, grad_attn, grad_mixed, grad_gain_two = norm_two_back(
        placed, live, cotangent, first_sum, base, gain_two, attention_weight, back_rows[-1], local_experts - 1
    )

    grads = attend_backward(queries, keys, values, mixed, grad_mixed, lse, cosine, sine, length, head_dim)
    input_grad = norm_one_back(grads, attention_weight, tokens, grad_first, gain_one)
    own = width // group
    grad_gains = grad_gain_two.reshape(group, 1, own)
    grad_gains = jnp.pad(grad_gains, ((0, 0), (0, 15), (0, LANES - own))).astype(BF16)
    attention_pack = attention_weights(normed_one, mixed, grads, grad_attn, grad_gains, group, owners)

    returned = exchange_parts(out_rows, owners, "expert")
    layer_out = combine(placed, route_gates, live, first_sum, shared_out, returned)

    def spread(pack):
        return lax.psum_scatter(pack, GROUP, scatter_dimension=0, tiled=True)[0]

    shared_share = spread(shared_pack)
    expert_shares = [spread(pack) for pack in expert_packs]
    attention_share = spread(attention_pack)
    pieces = lax.all_to_all(shared_share.reshape(owners, -1, LANES), "expert", split_axis=0, concat_axis=0, tiled=True)
    piece = jnp.sum(pieces.astype(F32), axis=0).astype(BF16)
    shared_share = (
        lax.all_to_all(
            jnp.broadcast_to(piece[None], (owners,) + piece.shape), "expert", split_axis=0, concat_axis=0, tiled=True
        )
        .reshape(shared_share.shape)
        .astype(F32)
    )
    attention_share = sum_over(attention_share, "expert", owners, 2).astype(F32)
    gu_panels, d_panels = 2 * shared_hidden // LANES, width // LANES
    qkv_rows, out_rows_count = 3 * d_panels * own, 4 * d_panels * own
    columns = 2 * hidden // group
    gu_rows = columns // LANES * width
    qkv_grad = panels_to(attention_share[:qkv_rows], own, 3 * d_panels)
    grad_gain_one = jnp.sum(w_qkv.astype(F32) * qkv_grad, axis=1) / norm_gains[0].astype(F32)
    return (
        layer_out,
        input_grad,
        jnp.stack([grad_gain_one, attention_share[out_rows_count, :own]]),
        qkv_grad,
        panels_to(attention_share[qkv_rows:out_rows_count], own, d_panels),
        panels_to(shared_share[: gu_panels * own], own, gu_panels),
        panels_to(shared_share[gu_panels * own :], shared_hidden // group, d_panels),
        jnp.stack([panels_to(share[:gu_rows], width, columns // LANES) for share in expert_shares]).astype(F32),
        jnp.stack([panels_to(share[gu_rows:], hidden // group, d_panels) for share in expert_shares]).astype(F32),
    )


def exchange_parts(parts, owners, axis):
    width = parts[0].shape[1]
    count = parts[0].shape[0] // owners
    joined = jnp.concatenate([rows.reshape(owners, count, width) for rows in parts], axis=1)
    back = lax.all_to_all(joined, axis, split_axis=0, concat_axis=0, tiled=True)
    return [
        back[:, j * count : (j + 1) * count].reshape(owners * count, width) for j in range(len(parts))
    ]


def solution(mesh):
    rows = P(("dp", "expert", "shard"), None)
    split = P(GROUP, None)
    in_specs = (
        rows,
        P(("dp", "expert", "shard")),
        rows,
        rows,
        rows,
        P(None, GROUP),
        split,
        split,
        split,
        split,
        P("expert", None, None),
        P("expert", None, None),
    )
    out_specs = (
        rows,
        rows,
        P(None, GROUP),
        split,
        split,
        split,
        split,
        P("expert", None, GROUP),
        P("expert", GROUP, None),
    )

    return jax.shard_map(local, mesh=mesh, in_specs=in_specs, out_specs=out_specs, check_vma=False)
```

```python
import functools
import math

import jax
import jax.numpy as jnp
from jax import lax
from jax.experimental import pallas as pl
from jax.experimental.pallas import tpu as pltpu
from jax.sharding import PartitionSpec as P


HEADS = 12
LANES = 128
EPSILON = 1e-05
VMEM_BYTES = 60 * 1024 * 1024
BF16 = jnp.bfloat16
F32 = jnp.float32


def call(kernel, grid, in_specs, out_specs, out_shape, scratch=(), flops=0, moved=0, trans=0, collective_id=None):
    return pl.pallas_call(
        kernel,
        grid_spec=pltpu.PrefetchScalarGridSpec(
            num_scalar_prefetch=0,
            grid=grid,
            in_specs=in_specs,
            out_specs=out_specs,
            scratch_shapes=list(scratch),
        ),
        out_shape=out_shape,
        compiler_params=pltpu.CompilerParams(
            dimension_semantics=("arbitrary",) * len(grid), vmem_limit_bytes=VMEM_BYTES, collective_id=collective_id,
            has_side_effects=collective_id is not None,
        ),
        cost_estimate=pl.CostEstimate(flops=flops, bytes_accessed=moved, transcendentals=trans),
    )


def shape_of(shape, dtype):
    return jax.ShapeDtypeStruct(shape, dtype)


def whole(shape):
    return pl.BlockSpec(shape, lambda *_: (0,) * len(shape), pipeline_mode=pl.Buffered(1))


def dot_nn(left, right):
    return lax.dot_general(left, right, (((1,), (0,)), ((), ())), preferred_element_type=F32)


def dot_nt(left, right):
    return lax.dot_general(left, right, (((1,), (1,)), ((), ())), preferred_element_type=F32)


def dot_tn(left, right):
    return lax.dot_general(left, right, (((0,), (0,)), ((), ())), preferred_element_type=F32)


def rotary_tables(length, head_dim):
    half_dim = head_dim // 2
    position = lax.iota(F32, length)[:, None]
    frequency = jnp.exp(lax.iota(F32, half_dim) * (-2.0 * math.log(10000.0) / head_dim))
    angle_table = position * frequency[None, :]
    cosine, sine = jnp.cos(angle_table), jnp.sin(angle_table)
    repeats = LANES // head_dim
    return (
        jnp.tile(jnp.concatenate([cosine, cosine], axis=1), (1, repeats)),
        jnp.tile(jnp.concatenate([-sine, sine], axis=1), (1, repeats)),
    )


def turn(values, cosine, signed_sine, head_dim):
    lane = lax.broadcasted_iota(jnp.int32, values.shape, 1)
    half = head_dim // 2
    other = jnp.where(
        lane % head_dim < half,
        pltpu.roll(values, LANES - half, 1),
        pltpu.roll(values, half, 1),
    )
    return values * cosine + other * signed_sine


def attend_forward_kernel(
    head_dim, block, x_ref, wq_ref, wk_ref, wv_ref, cos_ref, sin_ref, q_ref, k_ref, v_ref, o_ref, lse_ref, lse_tile
):
    length = x_ref.shape[0]
    heads = LANES // head_dim
    x = x_ref[...]
    cosine, sine = cos_ref[...], sin_ref[...]
    scale = 1.0 / math.sqrt(head_dim)
    q_ref[...] = (turn(dot_nn(x, wq_ref[...]), cosine, sine, head_dim) * scale).astype(BF16)
    k_ref[...] = turn(dot_nn(x, wk_ref[...]), cosine, sine, head_dim).astype(BF16)
    v_ref[...] = dot_nn(x, wv_ref[...]).astype(BF16)
    lane = lax.broadcasted_iota(jnp.int32, (1, LANES), 1)
    own_lane = lax.broadcasted_iota(jnp.int32, (block, LANES), 1) // head_dim
    below = lax.broadcasted_iota(jnp.int32, (block, block), 0) >= lax.broadcasted_iota(
        jnp.int32, (block, block), 1
    )
    for first in range(0, length, block):
        rows = pl.ds(first, block)
        mixed = None
        logs = None
        for head in range(heads):
            select = (lane // head_dim == head).astype(F32).astype(BF16)
            queries = q_ref[rows, :] * select
            near = jnp.where(below, dot_nt(queries, k_ref[rows, :]), -1e30)
            peak = jnp.max(near, axis=1, keepdims=True)
            if first:
                far = dot_nt(queries, k_ref[pl.ds(0, first), :])
                peak = jnp.maximum(peak, jnp.max(far, axis=1, keepdims=True))
            near = jnp.exp(near - peak)
            total = jnp.sum(near, axis=1, keepdims=True)
            part = dot_nn(near.astype(BF16), v_ref[rows, :])
            if first:
                far = jnp.exp(far - peak)
                total = total + jnp.sum(far, axis=1, keepdims=True)
                part = part + dot_nn(far.astype(BF16), v_ref[pl.ds(0, first), :])
            part = part * (1.0 / total)
            log_total = jnp.broadcast_to(peak + jnp.log(total), (block, LANES))
            mixed = part if head == 0 else jnp.where(own_lane == head, part, mixed)
            logs = log_total if head == 0 else jnp.where(own_lane == head, log_total, logs)
        o_ref[rows, :] = mixed.astype(BF16)
        lse_tile[rows, :] = logs
    turned = lse_tile[...].T
    for head in range(heads):
        lse_ref[pl.ds(head * 8, 8), :] = turned[head * head_dim : head * head_dim + 8, :]


def attend_forward(normed, w_qkv, cosine, sine, length, head_dim):
    tokens, width = normed.shape
    seqs, pairs, heads = tokens // length, width // LANES, LANES // head_dim
    block = min(256, length)
    rows = pl.BlockSpec((length, LANES), lambda s, p: (s, p))

    def weight(part):
        return pl.BlockSpec((width, LANES), lambda s, p: (0, part * pairs + p))

    table = whole((length, LANES))
    return call(
        functools.partial(attend_forward_kernel, head_dim, block),
        (seqs, pairs),
        [pl.BlockSpec((length, width), lambda s, p: (s, 0)), weight(0), weight(1), weight(2), table, table],
        [rows, rows, rows, rows, pl.BlockSpec((8 * heads, length), lambda s, p: (s * pairs + p, 0))],
        [shape_of((tokens, width), BF16)] * 4 + [shape_of((seqs * pairs * 8 * heads, length), F32)],
        scratch=[pltpu.VMEM((length, LANES), F32)],
        flops=6 * tokens * width * width + 4 * tokens * length * width,
        moved=16 * tokens * width,
        trans=tokens * length * width // head_dim // 2,
    )(normed, w_qkv, w_qkv, w_qkv, cosine, sine)


def attend_backward_kernel(
    head_dim, block, q_ref, k_ref, v_ref, o_ref, g_ref, lse_ref, cos_ref, sin_ref, gq_ref, gk_ref, gv_ref, gq_acc
):
    length = q_ref.shape[0]
    heads = LANES // head_dim
    scale = 1.0 / math.sqrt(head_dim)
    product = (g_ref[...].astype(F32) * o_ref[...].astype(F32)).T
    inner = [
        jnp.sum(product[head * head_dim : (head + 1) * head_dim, :], axis=0, keepdims=True)
        for head in range(heads)
    ]
    gq_acc[...] = jnp.zeros_like(gq_acc)
    lane = lax.broadcasted_iota(jnp.int32, (1, LANES), 1)
    own_lane = lax.broadcasted_iota(jnp.int32, (block, LANES), 1) // head_dim
    above = lax.broadcasted_iota(jnp.int32, (block, block), 1) >= lax.broadcasted_iota(
        jnp.int32, (block, block), 0
    )
    for first in range(0, length, block):
        rows = pl.ds(first, block)
        keys_grad = None
        values_grad = None
        for head in range(heads):
            select = (lane // head_dim == head).astype(F32).astype(BF16)
            keys = k_ref[rows, :] * select
            values = v_ref[rows, :] * select
            log_total = lse_ref[pl.ds(head * 8, 1), :]
            pieces = [(first, block, True)]
            if first + block < length:
                pieces.append((first + block, length - first - block, False))
            keys_part = None
            values_part = None
            for start, count, diagonal in pieces:
                span = pl.ds(start, count)
                queries, grads = q_ref[span, :], g_ref[span, :]
                scores = dot_nt(keys, queries)
                probs = jnp.exp(scores - log_total[:, start : start + count])
                if diagonal:
                    probs = jnp.where(above, probs, 0.0)
                grad_probs = dot_nt(values, grads)
                grad_scores = (probs * (grad_probs - inner[head][:, start : start + count])).astype(BF16)
                piece_values = dot_nn(probs.astype(BF16), grads)
                piece_keys = dot_nn(grad_scores, queries)
                values_part = piece_values if values_part is None else values_part + piece_values
                keys_part = piece_keys if keys_part is None else keys_part + piece_keys
                gq_acc[span, :] += dot_tn(grad_scores, keys)
            keys_grad = keys_part if head == 0 else jnp.where(own_lane == head, keys_part, keys_grad)
            values_grad = values_part if head == 0 else jnp.where(own_lane == head, values_part, values_grad)
        gk_ref[rows, :] = turn(keys_grad, cos_ref[rows, :], -sin_ref[rows, :], head_dim).astype(BF16)
        gv_ref[rows, :] = values_grad.astype(BF16)
    gq_ref[...] = turn(gq_acc[...] * scale, cos_ref[...], -sin_ref[...], head_dim).astype(BF16)


def attend_backward(queries, keys, values, mixed, grad_mixed, lse, cosine, sine, length, head_dim):
    tokens, width = queries.shape
    seqs, pairs, heads = tokens // length, width // LANES, LANES // head_dim
    block = min(256, length)
    rows = pl.BlockSpec((length, LANES), lambda s, p: (s, p))
    table = whole((length, LANES))
    return call(
        functools.partial(attend_backward_kernel, head_dim, block),
        (seqs, pairs),
        [rows] * 5 + [pl.BlockSpec((8 * heads, length), lambda s, p: (s * pairs + p, 0)), table, table],
        [rows] * 3,
        [shape_of((tokens, width), BF16)] * 3,
        scratch=[pltpu.VMEM((length, LANES), F32)],
        flops=10 * tokens * length * width,
        moved=16 * tokens * width,
        trans=tokens * length * width // head_dim // 2,
    )(queries, keys, values, mixed, grad_mixed, lse, cosine, sine)


def square(width, part):
    return pl.BlockSpec((width, width), lambda i: (0, part), pipeline_mode=pl.Buffered(1))


def norm_one_kernel(x_ref, gain_ref, out_ref):
    x = x_ref[...].astype(F32)
    scale = lax.rsqrt(jnp.mean(x * x, axis=1, keepdims=True) + EPSILON)
    out_ref[...] = (x * scale * gain_ref[...]).astype(BF16)


def norm_one(tokens, gain):
    rows, width = tokens.shape
    block = min(256, rows)
    blocked = pl.BlockSpec((block, width), lambda i: (i, 0))
    return call(
        norm_one_kernel, (rows // block,), [blocked, whole((1, width))], blocked, shape_of((rows, width), BF16),
        flops=5 * rows * width, moved=4 * rows * width,
    )(tokens, gain)


def norm_two_kernel(mixed_ref, tokens_ref, weight_ref, gain_ref, sum_ref, normed_ref):
    first_sum = tokens_ref[...].astype(F32) + dot_nn(mixed_ref[...], weight_ref[...])
    sum_ref[...] = first_sum
    scale = lax.rsqrt(jnp.mean(first_sum * first_sum, axis=1, keepdims=True) + EPSILON)
    normed_ref[...] = (first_sum * scale * gain_ref[...]).astype(BF16)


def norm_two(mixed, tokens, weight, gain):
    rows, width = tokens.shape
    block = min(256, rows)
    blocked = pl.BlockSpec((block, width), lambda i: (i, 0))
    return call(
        norm_two_kernel, (rows // block,), [blocked, blocked, square(width, 3), whole((1, width))],
        [blocked, blocked], [shape_of((rows, width), F32), shape_of((rows, width), BF16)],
        flops=2 * rows * width * width, moved=10 * rows * width,
    )(mixed, tokens, weight, gain)


def slots_kernel(experts, capacity, routes_ref, live_ref, dest_ref):
    top, tokens = routes_ref.shape
    live = live_ref[...]
    number = lax.broadcasted_iota(jnp.int32, (experts, tokens), 0)
    hits = [
        jnp.where((routes_ref[pl.ds(k, 1), :] == number) & (live > 0), 1.0, 0.0) for k in range(top)
    ]
    earlier = jnp.where(
        lax.broadcasted_iota(jnp.int32, (tokens, tokens), 0)
        <= lax.broadcasted_iota(jnp.int32, (tokens, tokens), 1),
        1.0,
        0.0,
    ).astype(BF16)
    ranks = dot_nn(jnp.concatenate(hits, axis=0).astype(BF16), earlier)
    before = jnp.zeros((experts, 1), F32)
    for k in range(top):
        rank = ranks[k * experts : (k + 1) * experts, :]
        place = number.astype(F32) * capacity + before + rank - 1.0
        slot = jnp.sum(hits[k] * place, axis=0, keepdims=True).astype(jnp.int32)
        dest_ref[pl.ds(k, 1), :] = jnp.where(live > 0, slot, experts * capacity)
        before = before + jnp.sum(hits[k], axis=1, keepdims=True)


def slots_of(routes_t, live_row, experts, capacity):
    top, tokens = routes_t.shape
    return call(
        functools.partial(slots_kernel, experts, capacity), (1,),
        [whole((top, tokens)), whole((1, tokens))], whole((top, tokens)), shape_of((top, tokens), jnp.int32),
        flops=2 * top * experts * tokens * tokens, moved=16 * tokens,
    )(routes_t, live_row)


def dispatch_kernel(gated, first, dest_ref, gates_ref, x_ref, out_ref):
    top, tokens = dest_ref.shape
    capacity = out_ref.shape[0]
    slot = lax.broadcasted_iota(jnp.int32, (capacity, tokens), 0) + (first + pl.program_id(0)) * capacity
    hits = [slot == dest_ref[pl.ds(k, 1), :] for k in range(top)]
    chosen = functools.reduce(jnp.logical_or, hits)
    rows = dot_nn(jnp.where(chosen, 1.0, 0.0).astype(BF16), x_ref[...])
    if gated:
        weights = jnp.zeros((capacity, tokens), F32)
        for k in range(top):
            weights = jnp.where(hits[k], gates_ref[pl.ds(k, 1), :], weights)
        rows = rows * jnp.sum(weights, axis=1, keepdims=True)
    out_ref[...] = rows.astype(BF16)


def dispatch(dest_t, gates_t, x, experts, capacity, gated, first):
    top, tokens = dest_t.shape
    width = x.shape[1]
    return call(
        functools.partial(dispatch_kernel, gated, first), (experts,),
        [whole((top, tokens)), whole((top, tokens)), whole((tokens, width))],
        pl.BlockSpec((capacity, width), lambda e: (e, 0)),
        shape_of((experts * capacity, width), BF16),
        flops=2 * experts * capacity * tokens * width, moved=2 * (experts * capacity + tokens) * width,
    )(dest_t, gates_t, x)


def combine_kernel(parts, axis, count, dest_ref, gates_ref, live_ref, sum_ref, shared_ref, *rest):
    y_refs, (x_ref, piece_ref, out_ref, total_ref, pieces_ref) = rest[:parts], rest[parts : parts + 5]
    landed, own, gathered_x, gathered_p, send_sem, recv_sem = rest[parts + 5 :]
    step = pl.program_id(0)
    last = pl.num_programs(0) - 1
    me = lax.axis_index(axis)

    def scatter():
        return peer_copies(
            axis, count, lambda index, peer: x_ref.at[peer], lambda index, me: landed.at[index], send_sem.at[0], recv_sem.at[0]
        )

    def gather():
        return peer_copies(
            axis, count, lambda index, peer: own, lambda index, me: gathered_x.at[me], send_sem.at[1], recv_sem.at[1]
        )

    def gather_pieces():
        return peer_copies(
            axis, count, lambda index, peer: piece_ref, lambda index, me: gathered_p.at[me], send_sem.at[2], recv_sem.at[2]
        )

    @pl.when(step == 0)
    def _():
        barrier = pltpu.get_barrier_semaphore()
        greet(barrier, axis, count)
        pl.semaphore_wait(barrier, count - 1)
        for copy in scatter() + gather_pieces():
            copy.start()

    block, top = dest_ref.shape
    total = sum_ref[...] + shared_ref[...]
    dest = dest_ref[...]
    gates = gates_ref[...]
    for index, y_ref in enumerate(y_refs):
        y = y_ref[...]
        slot = slot_numbers(block, y_ref.shape[0], index)
        for k in range(top):
            hit = jnp.where(slot == dest[:, k : k + 1], 1.0, 0.0).astype(BF16)
            total = total + dot_nn(hit, y) * gates[:, k : k + 1]
    out_ref[...] = (live_ref[...] * total).astype(BF16)

    @pl.when(step == jnp.minimum(2, last))
    def _():
        piece = x_ref[me].astype(F32)
        for index, copy in enumerate(scatter()):
            copy.wait()
            piece = piece + landed[index].astype(F32)
        own[...] = piece.astype(own.dtype)
        for copy in gather():
            copy.start()

    @pl.when(step == last)
    def _():
        gathered_x[me] = own[...]
        gathered_p[me] = piece_ref[...]
        for copy in gather_pieces() + gather():
            copy.wait()
        total_ref[...] = gathered_x[...]
        pieces_ref[...] = gathered_p[...]


def combine(dest, gates, live, first_sum, shared_out, returned, x, piece, axis, count):
    rows, width = first_sum.shape
    top = dest.shape[1]
    block = min(256, rows)
    parts = len(returned)
    blocked = pl.BlockSpec((block, width), lambda i: (i, 0))
    narrow = pl.BlockSpec((block, top), lambda i: (i, 0))
    slots = sum(y.shape[0] for y in returned)
    shape = (count, x.shape[0] // count, LANES)
    pieces = (count,) + piece.shape
    out, total, total_pieces = call(
        functools.partial(combine_kernel, parts, axis, count), (rows // block,),
        [narrow, narrow, pl.BlockSpec((block, 1), lambda i: (i, 0)), blocked, blocked]
        + [whole(y.shape) for y in returned] + [whole(shape), whole(piece.shape)],
        [blocked, whole(shape), whole(pieces)],
        [shape_of((rows, width), BF16), shape_of(shape, BF16), shape_of(pieces, BF16)],
        scratch=[pltpu.VMEM((count - 1,) + shape[1:], BF16), pltpu.VMEM(shape[1:], BF16), pltpu.VMEM(shape, BF16),
                 pltpu.VMEM(pieces, BF16), pltpu.SemaphoreType.DMA((3, count - 1)), pltpu.SemaphoreType.DMA((3, count - 1))],
        flops=4 * rows * slots * width, moved=10 * rows * width + 2 * slots * width, collective_id=2,
    )(dest, gates, live, first_sum, shared_out, *returned, x.reshape(shape), piece)
    return out, total.reshape(x.shape), total_pieces.reshape(-1, LANES)


def slot_numbers(block, slots, part):
    return lax.broadcasted_iota(jnp.int32, (block, slots), 1) + part * slots


def gathered(dest_ref, y_ref, part):
    block, top = dest_ref.shape
    dest = dest_ref[...]
    slot = slot_numbers(block, y_ref.shape[0], part)
    hit = functools.reduce(jnp.logical_or, [slot == dest[:, k : k + 1] for k in range(top)])
    return dot_nn(jnp.where(hit, 1.0, 0.0).astype(BF16), y_ref[...])


def add_part_kernel(part, dest_ref, base_ref, y_ref, out_ref):
    out_ref[...] = base_ref[...] + gathered(dest_ref, y_ref, part)


def add_part(dest, base, rows_of, part):
    rows, width = base.shape
    block = min(256, rows)
    blocked = pl.BlockSpec((block, width), lambda i: (i, 0))
    return call(
        functools.partial(add_part_kernel, part), (rows // block,),
        [pl.BlockSpec((block, dest.shape[1]), lambda i: (i, 0)), blocked, whole(rows_of.shape)],
        blocked, shape_of((rows, width), F32),
        flops=2 * rows * rows_of.shape[0] * width, moved=8 * rows * width,
    )(dest, base, rows_of)


def norm_two_back_kernel(part, dest_ref, live_ref, cot_ref, sum_ref, base_ref, gain_ref, weight_ref, y_ref,
                         first_ref, attn_ref, mixed_ref, gain_grad_ref):
    grad_normed = base_ref[...] + gathered(dest_ref, y_ref, part)
    first_sum = sum_ref[...]
    scale = lax.rsqrt(jnp.mean(first_sum * first_sum, axis=1, keepdims=True) + EPSILON)
    weighted = grad_normed * gain_ref[...]
    inner = jnp.mean(first_sum * weighted, axis=1, keepdims=True)
    grad_first = (
        cot_ref[...].astype(F32) * live_ref[...] + scale * weighted - first_sum * (scale * scale * scale * inner)
    )
    first_ref[...] = grad_first
    grad_attn = grad_first.astype(BF16)
    attn_ref[...] = grad_attn
    mixed_ref[...] = dot_nt(grad_attn, weight_ref[...]).astype(BF16)

    @pl.when(pl.program_id(0) == 0)
    def _():
        gain_grad_ref[...] = jnp.zeros_like(gain_grad_ref)

    gain_grad_ref[...] += jnp.sum(grad_normed * first_sum * scale, axis=0, keepdims=True)


def norm_two_back(dest, live, cotangent, first_sum, base, gain, weights, rows_of, part):
    rows, width = first_sum.shape
    top = dest.shape[1]
    block = min(256, rows)
    blocked = pl.BlockSpec((block, width), lambda i: (i, 0))
    return call(
        functools.partial(norm_two_back_kernel, part), (rows // block,),
        [pl.BlockSpec((block, top), lambda i: (i, 0)), pl.BlockSpec((block, 1), lambda i: (i, 0)), blocked, blocked,
         blocked, whole((1, width)), square(width, 3), whole(rows_of.shape)],
        [blocked, blocked, blocked, pl.BlockSpec((1, width), lambda i: (0, 0))],
        [shape_of((rows, width), F32), shape_of((rows, width), BF16), shape_of((rows, width), BF16),
         shape_of((1, width), F32)],
        flops=2 * rows * (rows_of.shape[0] + width) * width, moved=18 * rows * width,
    )(dest, live, cotangent, first_sum, base, gain, weights, rows_of)


def peer_copies(axis, count, source, target, send_sem, recv_sem):
    me = lax.axis_index(axis)
    out = []
    for index in range(count - 1):
        peer = lax.rem(me + index + 1, count)
        out.append(
            pltpu.make_async_remote_copy(
                src_ref=source(index, peer), dst_ref=target(index, me), send_sem=send_sem.at[index],
                recv_sem=recv_sem.at[index], device_id={axis: peer}, device_id_type=pl.DeviceIdType.MESH,
            )
        )
    return out


def greet(barrier, axis, count):
    me = lax.axis_index(axis)
    for index in range(count - 1):
        pl.semaphore_signal(
            barrier, inc=1, device_id={axis: lax.rem(me + index + 1, count)}, device_id_type=pl.DeviceIdType.MESH
        )


def settle_kernel(sizes, gq_ref, gk_ref, gv_ref, wq_ref, wk_ref, wv_ref, tokens_ref, first_ref, gain_ref, pack_ref,
                  x_ref, out_ref, share_ref, piece_ref, own, landed, chosen, arrived, sem, pair_send, pair_recv, send_sem,
                  recv_sem, x_landed, x_send, x_recv):
    dp_size, shard_size, count = sizes
    spread = shard_size // 2
    halves = dp_size * spread
    dp, shard = lax.axis_index("dp"), lax.axis_index("shard")
    side = shard % 2
    place = dp * spread + shard // 2
    step = pl.program_id(0)
    last = pl.num_programs(0) - 1

    def target(piece, bit):
        return {"dp": piece // spread, "shard": (piece % spread) * 2 + bit}

    def x_copies():
        return peer_copies(
            "expert", count, lambda index, peer: x_ref.at[peer], lambda index, me: x_landed.at[index], x_send, x_recv
        )

    def pair_copy():
        return pltpu.make_async_remote_copy(
            src_ref=pack_ref.at[:, 1 - side], dst_ref=landed, send_sem=pair_send, recv_sem=pair_recv,
            device_id=target(place, 1 - side), device_id_type=pl.DeviceIdType.MESH,
        )

    def own_copy():
        return pltpu.make_async_copy(pack_ref.at[:, side], own, sem)

    def send(index):
        return pltpu.make_async_remote_copy(
            src_ref=chosen.at[index], dst_ref=arrived.at[index], send_sem=send_sem.at[index], recv_sem=recv_sem.at[index],
            device_id=target(lax.rem(place + index + 1, halves), side), device_id_type=pl.DeviceIdType.MESH,
        )

    @pl.when(step == 0)
    def _():
        barrier = pltpu.get_barrier_semaphore()
        pl.semaphore_signal(barrier, inc=1, device_id=target(place, 1 - side), device_id_type=pl.DeviceIdType.MESH)
        for index in range(halves - 1):
            pl.semaphore_signal(
                barrier, inc=1, device_id=target(lax.rem(place + index + 1, halves), side),
                device_id_type=pl.DeviceIdType.MESH,
            )
        greet(barrier, "expert", count)
        pl.semaphore_wait(barrier, halves + count - 1)
        for copy in x_copies():
            copy.start()
        pair_copy().start()
        own_copy().start()

    @pl.when(step == 1)
    def _():
        own_copy().wait()
        pair_copy().wait()
        for index in range(halves - 1):
            piece = lax.rem(place + index + 1, halves)
            chosen[index] = (own[piece].astype(F32) + landed[piece].astype(F32)).astype(BF16)
            send(index).start()

    grad_normed = (
        dot_nt(gq_ref[...], wq_ref[...]) + dot_nt(gk_ref[...], wk_ref[...]) + dot_nt(gv_ref[...], wv_ref[...])
    )
    source = tokens_ref[...].astype(F32)
    scale = lax.rsqrt(jnp.mean(source * source, axis=1, keepdims=True) + EPSILON)
    weighted = grad_normed * gain_ref[...]
    inner = jnp.mean(source * weighted, axis=1, keepdims=True)
    out_ref[...] = first_ref[...] + scale * weighted - source * (scale * scale * scale * inner)

    @pl.when(step == last)
    def _():
        total = own[place].astype(F32) + landed[place].astype(F32)
        for index in range(halves - 1):
            send(index).wait()
            total = total + arrived[index].astype(F32)
        share_ref[...] = total.astype(BF16)
        piece = x_ref[lax.axis_index("expert")].astype(F32)
        for index, copy in enumerate(x_copies()):
            copy.wait()
            piece = piece + x_landed[index].astype(F32)
        piece_ref[...] = piece.astype(BF16)


def settle(grads, w_qkv, tokens, grad_first, gain, pack, x, sizes):
    rows, width = tokens.shape
    block = min(256, rows)
    blocked = pl.BlockSpec((block, width), lambda i: (i, 0))
    halves, count = sizes[0] * sizes[1] // 2, pack.shape[1]
    piece = (count, LANES)
    x = x.reshape(sizes[2], -1, LANES)
    return call(
        functools.partial(settle_kernel, sizes), (rows // block,),
        [blocked] * 3 + [square(width, 0), square(width, 1), square(width, 2), blocked, blocked, whole((1, width)),
                         pl.BlockSpec(memory_space=pl.ANY), whole(x.shape)],
        [blocked, whole(piece), whole(x.shape[1:])],
        [shape_of((rows, width), F32), shape_of(piece, BF16), shape_of(x.shape[1:], BF16)],
        scratch=[pltpu.VMEM((halves,) + piece, BF16), pltpu.VMEM((halves,) + piece, BF16),
                 pltpu.VMEM((halves - 1,) + piece, BF16), pltpu.VMEM((halves - 1,) + piece, BF16),
                 pltpu.SemaphoreType.DMA, pltpu.SemaphoreType.DMA, pltpu.SemaphoreType.DMA,
                 pltpu.SemaphoreType.DMA((halves - 1,)), pltpu.SemaphoreType.DMA((halves - 1,)),
                 pltpu.VMEM((sizes[2] - 1,) + x.shape[1:], BF16), pltpu.SemaphoreType.DMA((sizes[2] - 1,)),
                 pltpu.SemaphoreType.DMA((sizes[2] - 1,))],
        flops=6 * rows * width * width, moved=22 * rows * width, collective_id=1,
    )(*grads, w_qkv, w_qkv, w_qkv, tokens, grad_first, gain, pack.reshape((halves, 2) + piece), x)


def copies_of(layout, block, width, step, stage_g, stage_u, stage_d, slot, packed_ref, sems):
    by_rows, owners, hidden, base = layout
    panels = block // LANES
    rows_down = hidden // owners
    out = []

    def add(source, target):
        out.append(pltpu.make_async_copy(source, target, sems.at[slot, len(out)]))

    if by_rows:
        rows = width // owners
        for half, stage in enumerate((stage_g, stage_u)):
            for p in range(panels):
                panel = half * (hidden // LANES) + step * panels + p
                add(
                    stage.at[slot, :, :, pl.ds(p * LANES, LANES)],
                    packed_ref.at[:, pl.ds(pl.multiple_of(base + panel * rows, 8), rows), :],
                )
        start = 2 * hidden // LANES * rows
    else:
        columns = 2 * hidden // owners
        for half, stage in enumerate((stage_g, stage_u)):
            for p in range(panels):
                column = half * hidden + step * block + p * LANES
                owner, panel = column // columns, (column % columns) // LANES
                add(
                    stage.at[slot, :, pl.ds(p * LANES, LANES)],
                    packed_ref.at[owner, pl.ds(pl.multiple_of(base + panel * width, 8), width), :],
                )
        start = columns // LANES * width
    for q in range(block // rows_down):
        owner = step * (block // rows_down) + q
        for c in range(width // LANES):
            add(
                stage_d.at[slot, pl.ds(q * rows_down, rows_down), pl.ds(c * LANES, LANES)],
                packed_ref.at[owner, pl.ds(base + start + c * rows_down, rows_down), :],
            )
    return out


def packed_rows(width, hidden, owners):
    return 3 * width * hidden // owners // LANES


def ffn_kernel(out_type, layout, block, x_ref, gy_ref, wg_ref, wu_ref, wd_ref, *rest):
    y_ref, gx_ref, packed_ref, xt, y_acc, gx_acc, stage_g, stage_u, stage_d, sems = rest[-10:]
    step = pl.program_id(0)
    steps = layout[2] // block
    width = x_ref.shape[1]
    slot = step % 2
    copies = functools.partial(copies_of, layout, block, width)

    @pl.when(step == 0)
    def _():
        xt[...] = x_ref[...].T
        y_acc[...] = jnp.zeros_like(y_acc)
        gx_acc[...] = jnp.zeros_like(gx_acc)

    @pl.when(step >= 2)
    def _():
        for copy in copies(step - 2, stage_g, stage_u, stage_d, slot, packed_ref, sems):
            copy.wait()

    x, gy = x_ref[...], gy_ref[...].reshape(x_ref.shape)
    if layout[0]:
        wg, wu = wg_ref[...].reshape(width, block), wu_ref[...].reshape(width, block)
        rows = wd_ref.shape[1] // (width // block)
        wd = jnp.concatenate(
            [wd_ref[:, pl.ds(c * rows, rows), :].reshape(block, block) for c in range(width // block)], axis=1
        )
    else:
        wg, wu, wd = wg_ref[...], wu_ref[...], wd_ref[...]
    gate, up = dot_nn(x, wg), dot_nn(x, wu)
    grad_hidden = dot_nt(gy, wd)
    sigmoid = jax.nn.sigmoid(gate)
    value = gate * sigmoid
    hidden = (value * up).astype(BF16)
    grad_up = (grad_hidden * value).astype(BF16)
    grad_gate = (grad_hidden * up * (sigmoid * (1.0 + gate * (1.0 - sigmoid)))).astype(BF16)
    y_acc[...] += dot_nn(hidden, wd)
    gx_acc[...] += dot_nt(grad_gate, wg) + dot_nt(grad_up, wu)
    stage_g[slot] = dot_nn(xt[...], grad_gate).astype(BF16).reshape(stage_g.shape[1:])
    stage_u[slot] = dot_nn(xt[...], grad_up).astype(BF16).reshape(stage_u.shape[1:])
    stage_d[slot] = dot_tn(hidden, gy).astype(BF16)
    for copy in copies(step, stage_g, stage_u, stage_d, slot, packed_ref, sems):
        copy.start()

    @pl.when(step == steps - 1)
    def _():
        y_ref[...] = y_acc[...].astype(out_type)
        gx_ref[...] = gx_acc[...].astype(out_type)
        for back in (1, 0):
            if steps > back:
                for copy in copies(steps - 1 - back, stage_g, stage_u, stage_d, (steps - 1 - back) % 2, packed_ref, sems):
                    copy.wait()


BLOCK = 256


def ffn_both(x, gy, w_gu, w_down, hidden, expert, owners, out_type):
    rows, width = x.shape
    block = BLOCK
    steps = hidden // block
    by_rows = expert is None
    if by_rows:
        own, own_down, panels = width // owners, hidden // owners, width // block
        ahead = 2 * steps * own // (panels * own_down)
        gate = pl.BlockSpec((owners, own, block), lambda f: (0, f, 0))
        up = pl.BlockSpec((owners, own, block), lambda f: (0, steps + f, 0))
        down = pl.BlockSpec((block // own_down, panels * own_down, block), lambda f: (f, ahead, 0))
        stage = (2, owners, own, block)
    else:
        gate = pl.BlockSpec((None, width, block), lambda f: (expert, 0, f))
        up = pl.BlockSpec((None, width, block), lambda f: (expert, 0, steps + f))
        down = pl.BlockSpec((None, block, width), lambda f: (expert, f, 0))
        stage = (2, width, block)
    if by_rows:
        grads = whole((rows, width))
    else:
        grads = pl.BlockSpec(
            (gy.shape[0], rows // gy.shape[0], width), lambda f: (0, expert, 0), pipeline_mode=pl.Buffered(1)
        )
    out_rows = whole((rows, width))
    count = packed_rows(width, hidden, owners)
    layout = (by_rows, owners, hidden, 0)
    copies = 2 * (block // LANES) + block // (hidden // owners) * (width // LANES)
    return call(
        functools.partial(ffn_kernel, out_type, layout, block), (steps,),
        [whole((rows, width)), grads, gate, up, down],
        [out_rows, out_rows, pl.BlockSpec(memory_space=pl.ANY)],
        [shape_of((rows, width), out_type), shape_of((rows, width), out_type),
         shape_of((owners, count, LANES), BF16)],
        scratch=[pltpu.VMEM((width, rows), BF16), pltpu.VMEM((rows, width), F32), pltpu.VMEM((rows, width), F32),
                 pltpu.VMEM(stage, BF16), pltpu.VMEM(stage, BF16), pltpu.VMEM((2, block, width), BF16),
                 pltpu.SemaphoreType.DMA((2, copies))],
        flops=18 * rows * width * hidden, moved=12 * width * hidden + 16 * rows * width, trans=rows * hidden,
    )(x, gy, w_gu, w_gu, w_down)


def to_panels(array):
    rows, columns = array.shape
    return jnp.transpose(array.reshape(rows, columns // BLOCK, BLOCK), (1, 0, 2)).reshape(-1, BLOCK)


def panels_to(rows_array, rows, panels):
    return jnp.transpose(rows_array.reshape(panels, rows, LANES), (1, 0, 2)).reshape(rows, panels * LANES)


def attention_weights_kernel(per, normed_ref, mixed_ref, gq_ref, gk_ref, gv_ref, ga_ref, gains_ref, out_ref, xt):
    step = pl.program_id(0)
    owners, rows = out_ref.shape[0], out_ref.shape[1] // (out_ref.shape[1] // (normed_ref.shape[1] // out_ref.shape[0]))
    panels = out_ref.shape[1] // rows

    @pl.when(step == 0)
    def _():
        xt[...] = normed_ref[...].T

    @pl.when(step == 3 * per)
    def _():
        xt[...] = mixed_ref[...].T

    for index, grad_ref in enumerate((gq_ref, gk_ref, gv_ref, ga_ref)):

        @pl.when((step >= index * per) & (step < (index + 1) * per))
        def _():
            product = dot_nn(xt[...], grad_ref[...]).astype(BF16)
            for p in range(panels):
                out_ref[:, pl.ds(p * rows, rows), :] = product[:, p * LANES : (p + 1) * LANES].reshape(owners, rows, LANES)

    @pl.when(step >= 4 * per)
    def _():
        out_ref[...] = jnp.zeros_like(out_ref)

    @pl.when(step == 4 * per)
    def _():
        out_ref[:, pl.ds(0, gains_ref.shape[1]), :] = gains_ref[...]


def attention_weights(normed, mixed, grads, grad_attn, gains, owners, pieces):
    tokens, width = normed.shape
    rows = width // owners
    block = BLOCK
    panels, per = block // LANES, width // block
    steps = 4 * per + 1
    while steps * panels * rows % (16 * pieces):
        steps += 1

    def columns(index):
        return pl.BlockSpec((tokens, block), lambda i: (0, jnp.clip(i - index * per, 0, per - 1)))

    return call(
        functools.partial(attention_weights_kernel, per), (steps,),
        [whole((tokens, width)), whole((tokens, width))] + [columns(index) for index in range(4)] + [whole(gains.shape)],
        pl.BlockSpec((owners, panels * rows, LANES), lambda i: (0, i, 0)),
        shape_of((owners, steps * panels * rows, LANES), BF16),
        scratch=[pltpu.VMEM((width, tokens), BF16)],
        flops=8 * tokens * width * width, moved=16 * tokens * width,
    )(normed, mixed, *grads, grad_attn, gains)


GROUP = ("dp", "shard")


def local(
    tokens,
    lengths,
    routes,
    route_gates,
    cotangent,
    norm_gains,
    w_qkv,
    w_out,
    w_shared_gu,
    w_shared_down,
    w_expert_gu,
    w_expert_down,
):
    tok_count, width = tokens.shape
    seq_count = lengths.shape[0]
    length = tok_count // seq_count
    local_experts = w_expert_gu.shape[0]
    owners = lax.axis_size("expert")
    experts = local_experts * owners
    top = routes.shape[1]
    capacity = tok_count * top * 9 // (8 * experts)
    head_dim = width // HEADS
    hidden = w_expert_down.shape[1]

    gains = lax.all_gather(norm_gains, GROUP, axis=1, tiled=True).astype(F32)
    attention_weight = lax.all_gather(jnp.concatenate([w_qkv, w_out], axis=1), GROUP, axis=0, tiled=True)
    shared_weight = lax.all_gather(
        jnp.concatenate([to_panels(w_shared_gu), to_panels(w_shared_down)], axis=0)[None], GROUP, axis=0, tiled=True
    )
    gain_one, gain_two = gains[0:1], gains[1:2]

    live_bool = lax.iota(jnp.int32, tok_count) % length < jnp.repeat(lengths, length)
    live = live_bool.astype(F32)[:, None]
    live_row = live_bool.astype(jnp.int32)[None, :]

    group = lax.axis_size("dp") * lax.axis_size("shard")
    shared_hidden = w_shared_down.shape[0] * group

    dest_t = slots_of(routes.T, live_row, experts, capacity)
    dest = dest_t.T
    slots = owners * capacity

    def place(where):
        owner_of, part_of = where // (local_experts * capacity), (where // capacity) % local_experts
        return jnp.where(
            where < experts * capacity, part_of * slots + owner_of * capacity + where % capacity, experts * capacity
        )

    placed, placed_t = place(dest), place(dest_t)
    gates_t = route_gates.T
    grad_b = jnp.where(live_bool[:, None], cotangent, 0).astype(BF16)

    def exchange(rows):
        count = rows.shape[0] // owners
        return lax.all_to_all(
            rows.reshape(owners, count, width), "expert", split_axis=0, concat_axis=0, tiled=True
        ).reshape(rows.shape)

    send_grad = dispatch(dest_t, gates_t, grad_b, experts, capacity, True, 0)
    received_grad = exchange(send_grad).reshape(owners, local_experts * capacity, width)

    cosine, sine = rotary_tables(length, head_dim)
    normed_one = norm_one(tokens, gain_one)
    queries, keys, values, mixed, lse = attend_forward(normed_one, attention_weight, cosine, sine, length, head_dim)
    first_sum, normed_two = norm_two(mixed, tokens, attention_weight, gain_two)

    received = []
    for j in range(local_experts):
        rows = dispatch(placed_t, gates_t, normed_two, owners, capacity, False, j * owners)
        received.append(exchange(rows))
    shared_out, grad_shared, shared_pack = ffn_both(
        normed_two, grad_b, shared_weight, shared_weight, shared_hidden, None, group, F32
    )
    back_rows, out_rows, expert_packs = [], [], []
    for j in range(local_experts):
        y, gx, pack = ffn_both(
            received[j], received_grad, w_expert_gu, w_expert_down, hidden, j, group, BF16
        )
        back_rows.append(exchange(gx))
        out_rows.append(y)
        expert_packs.append(pack)
    base = grad_shared
    for j, rows in enumerate(back_rows[:-1]):
        base = add_part(placed, base, rows, j)
    grad_first, grad_attn, grad_mixed, grad_gain_two = norm_two_back(
        placed, live, cotangent, first_sum, base, gain_two, attention_weight, back_rows[-1], local_experts - 1
    )

    grads = attend_backward(queries, keys, values, mixed, grad_mixed, lse, cosine, sine, length, head_dim)
    own = width // group
    grad_gains = grad_gain_two.reshape(group, 1, own)
    grad_gains = jnp.pad(grad_gains, ((0, 0), (0, 15), (0, LANES - own))).astype(BF16)
    attention_pack = attention_weights(normed_one, mixed, grads, grad_attn, grad_gains, group, owners)

    def spread(pack):
        return lax.psum_scatter(pack, GROUP, scatter_dimension=0, tiled=True)[0]

    shared_share = spread(shared_pack)
    expert_shares = [spread(pack) for pack in expert_packs]
    input_grad, attention_share, shared_piece = settle(
        grads, attention_weight, tokens, grad_first, gain_one, attention_pack, shared_share,
        (lax.axis_size("dp"), lax.axis_size("shard"), owners),
    )
    returned = exchange_parts(out_rows, owners, "expert")
    layer_out, attention_share, shared_share = combine(
        placed, route_gates, live, first_sum, shared_out, returned, attention_share, shared_piece, "expert", owners
    )
    attention_share, shared_share = attention_share.astype(F32), shared_share.astype(F32)
    gu_panels, d_panels = 2 * shared_hidden // LANES, width // LANES
    qkv_rows, out_rows_count = 3 * d_panels * own, 4 * d_panels * own
    columns = 2 * hidden // group
    gu_rows = columns // LANES * width
    qkv_grad = panels_to(attention_share[:qkv_rows], own, 3 * d_panels)
    grad_gain_one = jnp.sum(w_qkv.astype(F32) * qkv_grad, axis=1) / norm_gains[0].astype(F32)
    return (
        layer_out,
        input_grad,
        jnp.stack([grad_gain_one, attention_share[out_rows_count, :own]]),
        qkv_grad,
        panels_to(attention_share[qkv_rows:out_rows_count], own, d_panels),
        panels_to(shared_share[: gu_panels * own], own, gu_panels),
        panels_to(shared_share[gu_panels * own :], shared_hidden // group, d_panels),
        jnp.stack([panels_to(share[:gu_rows], width, columns // LANES) for share in expert_shares]).astype(F32),
        jnp.stack([panels_to(share[gu_rows:], hidden // group, d_panels) for share in expert_shares]).astype(F32),
    )


def exchange_parts(parts, owners, axis):
    width = parts[0].shape[1]
    count = parts[0].shape[0] // owners
    joined = jnp.concatenate([rows.reshape(owners, count, width) for rows in parts], axis=1)
    back = lax.all_to_all(joined, axis, split_axis=0, concat_axis=0, tiled=True)
    return [
        back[:, j * count : (j + 1) * count].reshape(owners * count, width) for j in range(len(parts))
    ]


def solution(mesh):
    rows = P(("dp", "expert", "shard"), None)
    split = P(GROUP, None)
    in_specs = (
        rows,
        P(("dp", "expert", "shard")),
        rows,
        rows,
        rows,
        P(None, GROUP),
        split,
        split,
        split,
        split,
        P("expert", None, None),
        P("expert", None, None),
    )
    out_specs = (
        rows,
        rows,
        P(None, GROUP),
        split,
        split,
        split,
        split,
        P("expert", None, GROUP),
        P("expert", GROUP, None),
    )

    return jax.shard_map(local, mesh=mesh, in_specs=in_specs, out_specs=out_specs, check_vma=False)
```

```python
import functools
import math

import jax
import jax.numpy as jnp
from jax import lax
from jax.experimental import pallas as pl
from jax.experimental.pallas import tpu as pltpu
from jax.sharding import PartitionSpec as P


HEADS = 12
LANES = 128
EPSILON = 1e-05
VMEM_BYTES = 60 * 1024 * 1024
BF16 = jnp.bfloat16
F32 = jnp.float32


def call(kernel, grid, in_specs, out_specs, out_shape, scratch=(), flops=0, moved=0, trans=0, collective_id=None, aliases=None):
    return pl.pallas_call(
        kernel,
        grid_spec=pltpu.PrefetchScalarGridSpec(
            num_scalar_prefetch=0,
            grid=grid,
            in_specs=in_specs,
            out_specs=out_specs,
            scratch_shapes=list(scratch),
        ),
        out_shape=out_shape,
        input_output_aliases=aliases or {},
        compiler_params=pltpu.CompilerParams(
            dimension_semantics=("arbitrary",) * len(grid), vmem_limit_bytes=VMEM_BYTES, collective_id=collective_id,
            has_side_effects=collective_id is not None,
        ),
        cost_estimate=pl.CostEstimate(flops=flops, bytes_accessed=moved, transcendentals=trans),
    )


def shape_of(shape, dtype):
    return jax.ShapeDtypeStruct(shape, dtype)


def whole(shape):
    return pl.BlockSpec(shape, lambda *_: (0,) * len(shape), pipeline_mode=pl.Buffered(1))


def dot_nn(left, right):
    return lax.dot_general(left, right, (((1,), (0,)), ((), ())), preferred_element_type=F32)


def dot_nt(left, right):
    return lax.dot_general(left, right, (((1,), (1,)), ((), ())), preferred_element_type=F32)


def dot_tn(left, right):
    return lax.dot_general(left, right, (((0,), (0,)), ((), ())), preferred_element_type=F32)


def rotary_tables(length, head_dim):
    half_dim = head_dim // 2
    position = lax.iota(F32, length)[:, None]
    frequency = jnp.exp(lax.iota(F32, half_dim) * (-2.0 * math.log(10000.0) / head_dim))
    angle_table = position * frequency[None, :]
    cosine, sine = jnp.cos(angle_table), jnp.sin(angle_table)
    repeats = LANES // head_dim
    return (
        jnp.tile(jnp.concatenate([cosine, cosine], axis=1), (1, repeats)),
        jnp.tile(jnp.concatenate([-sine, sine], axis=1), (1, repeats)),
    )


def turn(values, cosine, signed_sine, head_dim):
    lane = lax.broadcasted_iota(jnp.int32, values.shape, 1)
    half = head_dim // 2
    other = jnp.where(
        lane % head_dim < half,
        pltpu.roll(values, LANES - half, 1),
        pltpu.roll(values, half, 1),
    )
    return values * cosine + other * signed_sine


def attend_forward_kernel(
    head_dim, block, x_ref, wq_ref, wk_ref, wv_ref, cos_ref, sin_ref, q_ref, k_ref, v_ref, o_ref, lse_ref, lse_tile
):
    length = x_ref.shape[0]
    heads = LANES // head_dim
    x = x_ref[...]
    cosine, sine = cos_ref[...], sin_ref[...]
    scale = 1.0 / math.sqrt(head_dim)
    q_ref[...] = (turn(dot_nn(x, wq_ref[...]), cosine, sine, head_dim) * scale).astype(BF16)
    k_ref[...] = turn(dot_nn(x, wk_ref[...]), cosine, sine, head_dim).astype(BF16)
    v_ref[...] = dot_nn(x, wv_ref[...]).astype(BF16)
    lane = lax.broadcasted_iota(jnp.int32, (1, LANES), 1)
    own_lane = lax.broadcasted_iota(jnp.int32, (block, LANES), 1) // head_dim
    below = lax.broadcasted_iota(jnp.int32, (block, block), 0) >= lax.broadcasted_iota(
        jnp.int32, (block, block), 1
    )
    for first in range(0, length, block):
        rows = pl.ds(first, block)
        mixed = None
        logs = None
        for head in range(heads):
            select = (lane // head_dim == head).astype(F32).astype(BF16)
            queries = q_ref[rows, :] * select
            near = jnp.where(below, dot_nt(queries, k_ref[rows, :]), -1e30)
            peak = jnp.max(near, axis=1, keepdims=True)
            if first:
                far = dot_nt(queries, k_ref[pl.ds(0, first), :])
                peak = jnp.maximum(peak, jnp.max(far, axis=1, keepdims=True))
            near = jnp.exp(near - peak)
            total = jnp.sum(near, axis=1, keepdims=True)
            part = dot_nn(near.astype(BF16), v_ref[rows, :])
            if first:
                far = jnp.exp(far - peak)
                total = total + jnp.sum(far, axis=1, keepdims=True)
                part = part + dot_nn(far.astype(BF16), v_ref[pl.ds(0, first), :])
            part = part * (1.0 / total)
            log_total = jnp.broadcast_to(peak + jnp.log(total), (block, LANES))
            mixed = part if head == 0 else jnp.where(own_lane == head, part, mixed)
            logs = log_total if head == 0 else jnp.where(own_lane == head, log_total, logs)
        o_ref[rows, :] = mixed.astype(BF16)
        lse_tile[rows, :] = logs
    turned = lse_tile[...].T
    for head in range(heads):
        lse_ref[pl.ds(head * 8, 8), :] = turned[head * head_dim : head * head_dim + 8, :]


def attend_forward(normed, w_qkv, cosine, sine, length, head_dim):
    tokens, width = normed.shape
    seqs, pairs, heads = tokens // length, width // LANES, LANES // head_dim
    block = min(256, length)
    rows = pl.BlockSpec((length, LANES), lambda s, p: (s, p))

    def weight(part):
        return pl.BlockSpec((width, LANES), lambda s, p: (0, part * pairs + p))

    table = whole((length, LANES))
    return call(
        functools.partial(attend_forward_kernel, head_dim, block),
        (seqs, pairs),
        [pl.BlockSpec((length, width), lambda s, p: (s, 0)), weight(0), weight(1), weight(2), table, table],
        [rows, rows, rows, rows, pl.BlockSpec((8 * heads, length), lambda s, p: (s * pairs + p, 0))],
        [shape_of((tokens, width), BF16)] * 4 + [shape_of((seqs * pairs * 8 * heads, length), F32)],
        scratch=[pltpu.VMEM((length, LANES), F32)],
        flops=6 * tokens * width * width + 4 * tokens * length * width,
        moved=16 * tokens * width,
        trans=tokens * length * width // head_dim // 2,
    )(normed, w_qkv, w_qkv, w_qkv, cosine, sine)


def attend_backward_kernel(
    head_dim, block, q_ref, k_ref, v_ref, o_ref, g_ref, lse_ref, cos_ref, sin_ref, gq_ref, gk_ref, gv_ref, gq_acc
):
    length = q_ref.shape[0]
    heads = LANES // head_dim
    scale = 1.0 / math.sqrt(head_dim)
    product = (g_ref[...].astype(F32) * o_ref[...].astype(F32)).T
    inner = [
        jnp.sum(product[head * head_dim : (head + 1) * head_dim, :], axis=0, keepdims=True)
        for head in range(heads)
    ]
    gq_acc[...] = jnp.zeros_like(gq_acc)
    lane = lax.broadcasted_iota(jnp.int32, (1, LANES), 1)
    own_lane = lax.broadcasted_iota(jnp.int32, (block, LANES), 1) // head_dim
    above = lax.broadcasted_iota(jnp.int32, (block, block), 1) >= lax.broadcasted_iota(
        jnp.int32, (block, block), 0
    )
    for first in range(0, length, block):
        rows = pl.ds(first, block)
        keys_grad = None
        values_grad = None
        for head in range(heads):
            select = (lane // head_dim == head).astype(F32).astype(BF16)
            keys = k_ref[rows, :] * select
            values = v_ref[rows, :] * select
            log_total = lse_ref[pl.ds(head * 8, 1), :]
            pieces = [(first, block, True)]
            if first + block < length:
                pieces.append((first + block, length - first - block, False))
            keys_part = None
            values_part = None
            for start, count, diagonal in pieces:
                span = pl.ds(start, count)
                queries, grads = q_ref[span, :], g_ref[span, :]
                scores = dot_nt(keys, queries)
                probs = jnp.exp(scores - log_total[:, start : start + count])
                if diagonal:
                    probs = jnp.where(above, probs, 0.0)
                grad_probs = dot_nt(values, grads)
                grad_scores = (probs * (grad_probs - inner[head][:, start : start + count])).astype(BF16)
                piece_values = dot_nn(probs.astype(BF16), grads)
                piece_keys = dot_nn(grad_scores, queries)
                values_part = piece_values if values_part is None else values_part + piece_values
                keys_part = piece_keys if keys_part is None else keys_part + piece_keys
                gq_acc[span, :] += dot_tn(grad_scores, keys)
            keys_grad = keys_part if head == 0 else jnp.where(own_lane == head, keys_part, keys_grad)
            values_grad = values_part if head == 0 else jnp.where(own_lane == head, values_part, values_grad)
        gk_ref[rows, :] = turn(keys_grad, cos_ref[rows, :], -sin_ref[rows, :], head_dim).astype(BF16)
        gv_ref[rows, :] = values_grad.astype(BF16)
    gq_ref[...] = turn(gq_acc[...] * scale, cos_ref[...], -sin_ref[...], head_dim).astype(BF16)


def attend_backward(queries, keys, values, mixed, grad_mixed, lse, cosine, sine, length, head_dim):
    tokens, width = queries.shape
    seqs, pairs, heads = tokens // length, width // LANES, LANES // head_dim
    block = min(256, length)
    rows = pl.BlockSpec((length, LANES), lambda s, p: (s, p))
    table = whole((length, LANES))
    return call(
        functools.partial(attend_backward_kernel, head_dim, block),
        (seqs, pairs),
        [rows] * 5 + [pl.BlockSpec((8 * heads, length), lambda s, p: (s * pairs + p, 0)), table, table],
        [rows] * 3,
        [shape_of((tokens, width), BF16)] * 3,
        scratch=[pltpu.VMEM((length, LANES), F32)],
        flops=10 * tokens * length * width,
        moved=16 * tokens * width,
        trans=tokens * length * width // head_dim // 2,
    )(queries, keys, values, mixed, grad_mixed, lse, cosine, sine)


def square(width, part):
    return pl.BlockSpec((width, width), lambda i: (0, part), pipeline_mode=pl.Buffered(1))


def norm_one_kernel(x_ref, gain_ref, out_ref):
    x = x_ref[...].astype(F32)
    scale = lax.rsqrt(jnp.mean(x * x, axis=1, keepdims=True) + EPSILON)
    out_ref[...] = (x * scale * gain_ref[...]).astype(BF16)


def norm_one(tokens, gain):
    rows, width = tokens.shape
    block = min(256, rows)
    blocked = pl.BlockSpec((block, width), lambda i: (i, 0))
    return call(
        norm_one_kernel, (rows // block,), [blocked, whole((1, width))], blocked, shape_of((rows, width), BF16),
        flops=5 * rows * width, moved=4 * rows * width,
    )(tokens, gain)


def norm_two_kernel(mixed_ref, tokens_ref, weight_ref, gain_ref, sum_ref, normed_ref):
    first_sum = tokens_ref[...].astype(F32) + dot_nn(mixed_ref[...], weight_ref[...])
    sum_ref[...] = first_sum
    scale = lax.rsqrt(jnp.mean(first_sum * first_sum, axis=1, keepdims=True) + EPSILON)
    normed_ref[...] = (first_sum * scale * gain_ref[...]).astype(BF16)


def norm_two(mixed, tokens, weight, gain):
    rows, width = tokens.shape
    block = min(256, rows)
    blocked = pl.BlockSpec((block, width), lambda i: (i, 0))
    return call(
        norm_two_kernel, (rows // block,), [blocked, blocked, square(width, 3), whole((1, width))],
        [blocked, blocked], [shape_of((rows, width), F32), shape_of((rows, width), BF16)],
        flops=2 * rows * width * width, moved=10 * rows * width,
    )(mixed, tokens, weight, gain)


def slots_kernel(experts, capacity, routes_ref, live_ref, dest_ref):
    top, tokens = routes_ref.shape
    live = live_ref[...]
    number = lax.broadcasted_iota(jnp.int32, (experts, tokens), 0)
    hits = [
        jnp.where((routes_ref[pl.ds(k, 1), :] == number) & (live > 0), 1.0, 0.0) for k in range(top)
    ]
    earlier = jnp.where(
        lax.broadcasted_iota(jnp.int32, (tokens, tokens), 0)
        <= lax.broadcasted_iota(jnp.int32, (tokens, tokens), 1),
        1.0,
        0.0,
    ).astype(BF16)
    ranks = dot_nn(jnp.concatenate(hits, axis=0).astype(BF16), earlier)
    before = jnp.zeros((experts, 1), F32)
    for k in range(top):
        rank = ranks[k * experts : (k + 1) * experts, :]
        place = number.astype(F32) * capacity + before + rank - 1.0
        slot = jnp.sum(hits[k] * place, axis=0, keepdims=True).astype(jnp.int32)
        dest_ref[pl.ds(k, 1), :] = jnp.where(live > 0, slot, experts * capacity)
        before = before + jnp.sum(hits[k], axis=1, keepdims=True)


def slots_of(routes_t, live_row, experts, capacity):
    top, tokens = routes_t.shape
    return call(
        functools.partial(slots_kernel, experts, capacity), (1,),
        [whole((top, tokens)), whole((1, tokens))], whole((top, tokens)), shape_of((top, tokens), jnp.int32),
        flops=2 * top * experts * tokens * tokens, moved=16 * tokens,
    )(routes_t, live_row)


def dispatch_kernel(gated, first, dest_ref, gates_ref, x_ref, out_ref):
    top, tokens = dest_ref.shape
    capacity = out_ref.shape[0]
    slot = lax.broadcasted_iota(jnp.int32, (capacity, tokens), 0) + (first + pl.program_id(0)) * capacity
    hits = [slot == dest_ref[pl.ds(k, 1), :] for k in range(top)]
    chosen = functools.reduce(jnp.logical_or, hits)
    rows = dot_nn(jnp.where(chosen, 1.0, 0.0).astype(BF16), x_ref[...])
    if gated:
        weights = jnp.zeros((capacity, tokens), F32)
        for k in range(top):
            weights = jnp.where(hits[k], gates_ref[pl.ds(k, 1), :], weights)
        rows = rows * jnp.sum(weights, axis=1, keepdims=True)
    out_ref[...] = rows.astype(BF16)


def dispatch(dest_t, gates_t, x, experts, capacity, gated, first):
    top, tokens = dest_t.shape
    width = x.shape[1]
    return call(
        functools.partial(dispatch_kernel, gated, first), (experts,),
        [whole((top, tokens)), whole((top, tokens)), whole((tokens, width))],
        pl.BlockSpec((capacity, width), lambda e: (e, 0)),
        shape_of((experts * capacity, width), BF16),
        flops=2 * experts * capacity * tokens * width, moved=2 * (experts * capacity + tokens) * width,
    )(dest_t, gates_t, x)


def unpack(source, start, rows, panels, target):
    for p in range(panels):
        target[:, pl.ds(p * LANES, LANES)] = source[pl.ds(start + p * rows, rows), :].astype(F32)


def combine_kernel(parts, axis, count, own, gu_panels, experts, dest_ref, gates_ref, live_ref, sum_ref, shared_ref, *rest):
    y_refs = rest[:parts]
    x_ref, piece_ref, pack_ref, out_ref, egu_ref, ed_ref, qkv_ref, wo_ref, sgu_ref, sd_ref, gain_ref = rest[parts : parts + 11]
    buffers, total_x, all_x, all_p, sum_send, sum_recv, x_send, x_recv, p_send, p_recv = rest[parts + 11 :]
    step = pl.program_id(0)
    last = pl.num_programs(0) - 1
    line = LineSum(axis, count, x_ref, buffers, sum_send, sum_recv)
    gather_x = LineGather(axis, count, all_x, x_send, x_recv)
    gather_p = LineGather(axis, count, all_p, p_send, p_recv)
    width = out_ref.shape[1]
    d_panels = width // LANES
    packed = pack_ref.shape[0] // experts
    e_panels, e_rows = egu_ref.shape[2] // LANES, egu_ref.shape[1]

    @pl.when(step == 0)
    def _():
        barrier = pltpu.get_barrier_semaphore()
        pl.semaphore_wait(barrier, greet_neighbours(barrier, axis, count))
        line.start()
        gather_p.start(piece_ref[...])
        for e in range(experts):
            unpack(pack_ref, e * packed + e_panels * width, ed_ref.shape[1], d_panels, ed_ref.at[e])

    for e in range(experts):
        for p in range(e_panels):
            rows = pl.ds(pl.multiple_of(e * packed + p * width + step * e_rows, 16), e_rows)
            egu_ref[e, :, pl.ds(p * LANES, LANES)] = pack_ref[rows, :].astype(F32)

    block, top = dest_ref.shape
    total = sum_ref[...] + shared_ref[...]
    dest = dest_ref[...]
    gates = gates_ref[...]
    for index, y_ref in enumerate(y_refs):
        y = y_ref[...]
        slot = slot_numbers(block, y_ref.shape[0], index)
        for k in range(top):
            hit = jnp.where(slot == dest[:, k : k + 1], 1.0, 0.0).astype(BF16)
            total = total + dot_nn(hit, y) * gates[:, k : k + 1]
    out_ref[...] = (live_ref[...] * total).astype(BF16)

    @pl.when(step == jnp.minimum(1, last))
    def _():
        line.relay()
        gather_p.relay(1)

    @pl.when(step == last)
    def _():
        line.finish(total_x)
        gather_x.start(total_x[...].astype(BF16))
        for k in range(1, count):
            if k > 1:
                gather_p.relay(k)
            gather_x.relay(k)
        gather_p.finish()
        unpack(all_p, 0, own, gu_panels, sgu_ref)
        unpack(all_p, gu_panels * own, sd_ref.shape[0], d_panels, sd_ref)
        gather_x.finish()
        unpack(all_x, 0, own, 3 * d_panels, qkv_ref)
        unpack(all_x, 3 * d_panels * own, own, d_panels, wo_ref)
        gain_ref[...] = all_x[pl.ds(4 * d_panels * own, gain_ref.shape[0]), :].astype(F32)


def combine(dest, gates, live, first_sum, shared_out, returned, x, piece, pack, axis, count, own, shared_hidden, hidden):
    rows, width = first_sum.shape
    top = dest.shape[1]
    block = min(256, rows)
    steps = rows // block
    parts = len(returned)
    blocked = pl.BlockSpec((block, width), lambda i: (i, 0))
    narrow = pl.BlockSpec((block, top), lambda i: (i, 0))
    slots = sum(y.shape[0] for y in returned)
    group = width // own
    columns = 2 * hidden // group
    gu_panels = 2 * shared_hidden // LANES
    x_piece, p_rows = (x.shape[0] // count, LANES), count * piece.shape[0]
    outs = [
        (parts, width, columns), (parts, hidden // group, width), (own, 3 * width), (own, width), (own, 2 * shared_hidden),
        (shared_hidden // group, width), (8, LANES),
    ]
    sems = pltpu.SemaphoreType.DMA((2, count))
    return call(
        functools.partial(combine_kernel, parts, axis, count, own, gu_panels, parts), (steps,),
        [narrow, narrow, pl.BlockSpec((block, 1), lambda i: (i, 0)), blocked, blocked]
        + [whole(y.shape) for y in returned] + [whole(x.shape), whole(piece.shape), whole(pack.shape)],
        [blocked, pl.BlockSpec((parts, width // steps, columns), lambda i: (0, i, 0))] + [whole(shape) for shape in outs[1:]],
        [shape_of((rows, width), BF16)] + [shape_of(shape, F32) for shape in outs],
        scratch=[pltpu.VMEM((2, 2, count) + x_piece, BF16), pltpu.VMEM(x_piece, F32), pltpu.VMEM(x.shape, BF16),
                 pltpu.VMEM((p_rows, LANES), BF16)] + [sems] * 6,
        flops=4 * rows * slots * width, moved=10 * rows * width + 2 * slots * width, collective_id=2,
    )(dest, gates, live, first_sum, shared_out, *returned, x, piece, pack)


def slot_numbers(block, slots, part):
    return lax.broadcasted_iota(jnp.int32, (block, slots), 1) + part * slots


def gathered(dest_ref, y_ref, part):
    block, top = dest_ref.shape
    dest = dest_ref[...]
    slot = slot_numbers(block, y_ref.shape[0], part)
    hit = functools.reduce(jnp.logical_or, [slot == dest[:, k : k + 1] for k in range(top)])
    return dot_nn(jnp.where(hit, 1.0, 0.0).astype(BF16), y_ref[...])


def add_part_kernel(part, dest_ref, base_ref, y_ref, out_ref):
    out_ref[...] = base_ref[...] + gathered(dest_ref, y_ref, part)


def add_part(dest, base, rows_of, part):
    rows, width = base.shape
    block = min(256, rows)
    blocked = pl.BlockSpec((block, width), lambda i: (i, 0))
    return call(
        functools.partial(add_part_kernel, part), (rows // block,),
        [pl.BlockSpec((block, dest.shape[1]), lambda i: (i, 0)), blocked, whole(rows_of.shape)],
        blocked, shape_of((rows, width), F32),
        flops=2 * rows * rows_of.shape[0] * width, moved=8 * rows * width,
    )(dest, base, rows_of)


def norm_two_back_kernel(part, dest_ref, live_ref, cot_ref, sum_ref, base_ref, gain_ref, weight_ref, y_ref,
                         first_ref, attn_ref, mixed_ref, gain_grad_ref):
    grad_normed = base_ref[...] + gathered(dest_ref, y_ref, part)
    first_sum = sum_ref[...]
    scale = lax.rsqrt(jnp.mean(first_sum * first_sum, axis=1, keepdims=True) + EPSILON)
    weighted = grad_normed * gain_ref[...]
    inner = jnp.mean(first_sum * weighted, axis=1, keepdims=True)
    grad_first = (
        cot_ref[...].astype(F32) * live_ref[...] + scale * weighted - first_sum * (scale * scale * scale * inner)
    )
    first_ref[...] = grad_first
    grad_attn = grad_first.astype(BF16)
    attn_ref[...] = grad_attn
    mixed_ref[...] = dot_nt(grad_attn, weight_ref[...]).astype(BF16)

    @pl.when(pl.program_id(0) == 0)
    def _():
        gain_grad_ref[...] = jnp.zeros_like(gain_grad_ref)

    gain_grad_ref[...] += jnp.sum(grad_normed * first_sum * scale, axis=0, keepdims=True)


def norm_two_back(dest, live, cotangent, first_sum, base, gain, weights, rows_of, part):
    rows, width = first_sum.shape
    top = dest.shape[1]
    block = min(256, rows)
    blocked = pl.BlockSpec((block, width), lambda i: (i, 0))
    return call(
        functools.partial(norm_two_back_kernel, part), (rows // block,),
        [pl.BlockSpec((block, top), lambda i: (i, 0)), pl.BlockSpec((block, 1), lambda i: (i, 0)), blocked, blocked,
         blocked, whole((1, width)), square(width, 3), whole(rows_of.shape)],
        [blocked, blocked, blocked, pl.BlockSpec((1, width), lambda i: (0, 0))],
        [shape_of((rows, width), F32), shape_of((rows, width), BF16), shape_of((rows, width), BF16),
         shape_of((1, width), F32)],
        flops=2 * rows * (rows_of.shape[0] + width) * width, moved=18 * rows * width,
    )(dest, live, cotangent, first_sum, base, gain, weights, rows_of)


def line_copy(axis, ahead, source, target, send_sem, recv_sem):
    return pltpu.make_async_remote_copy(
        src_ref=source, dst_ref=target, send_sem=send_sem, recv_sem=recv_sem,
        device_id={axis: lax.axis_index(axis) + ahead}, device_id_type=pl.DeviceIdType.MESH,
    )


class LineSum:
    def __init__(self, axis, count, x_ref, buffers, send_sem, recv_sem):
        self.axis, self.count, self.x_ref, self.buffers = axis, count, x_ref, buffers
        self.send_sem, self.recv_sem = send_sem, recv_sem
        self.rows = buffers.shape[3]

    def own(self, piece):
        return self.x_ref[pl.ds(pl.multiple_of(piece * self.rows, 16), self.rows), :].astype(F32)

    def copy(self, way, piece):
        return line_copy(
            self.axis, 1 - 2 * way, self.buffers.at[way, 1, piece], self.buffers.at[way, 0, piece],
            self.send_sem.at[way, piece], self.recv_sem.at[way, piece],
        )

    def each(self, body):
        me = lax.axis_index(self.axis)
        for k in range(self.count - 1):
            for way, piece in ((0, self.count - 1 - k), (1, k)):
                before = me > 0 if way == 0 else me < self.count - 1
                sends = me < piece if way == 0 else me > piece
                body(way, piece, before, sends)

    def start(self):
        def body(way, piece, before, sends):
            @pl.when(sends & jnp.logical_not(before))
            def _():
                self.buffers[way, 1, piece] = self.own(piece).astype(BF16)
                self.copy(way, piece).start()

        self.each(body)

    def relay(self):
        def body(way, piece, before, sends):
            @pl.when(sends & before)
            def _():
                self.copy(way, piece).wait_recv()
                self.buffers[way, 1, piece] = (self.own(piece) + self.buffers[way, 0, piece].astype(F32)).astype(BF16)
                self.copy(way, piece).start()

        self.each(body)

    def finish(self, total_ref):
        me = lax.axis_index(self.axis)
        total_ref[...] = self.own(me)
        for way, before in ((0, me > 0), (1, me < self.count - 1)):

            @pl.when(before)
            def _():
                self.copy(way, me).wait_recv()
                total_ref[...] += self.buffers[way, 0, me].astype(F32)

        def body(way, piece, before, sends):
            @pl.when(sends)
            def _():
                self.copy(way, piece).wait_send()

        self.each(body)


class LineGather:
    def __init__(self, axis, count, out_ref, send_sem, recv_sem):
        self.axis, self.count, self.out_ref = axis, count, out_ref
        self.send_sem, self.recv_sem = send_sem, recv_sem
        self.rows = out_ref.shape[0] // count

    def place(self, piece):
        return self.out_ref.at[pl.ds(pl.multiple_of(piece * self.rows, 16), self.rows), :]

    def copy(self, way, piece):
        return line_copy(
            self.axis, 1 - 2 * way, self.place(piece), self.place(piece),
            self.send_sem.at[way, piece], self.recv_sem.at[way, piece],
        )

    def start(self, value):
        me = lax.axis_index(self.axis)
        self.place(me)[...] = value
        for way, more in ((0, me < self.count - 1), (1, me > 0)):

            @pl.when(more)
            def _():
                self.copy(way, me).start()

    def relay(self, k):
        me = lax.axis_index(self.axis)
        for way, piece, there, more in (
            (0, me - k, me >= k, me < self.count - 1),
            (1, me + k, me + k < self.count, me > 0),
        ):

            @pl.when(there)
            def _():
                self.copy(way, piece).wait_recv()

            @pl.when(there & more)
            def _():
                self.copy(way, piece).start()

    def finish(self):
        me = lax.axis_index(self.axis)
        for k in range(self.count):
            for way, piece, sent in (
                (0, me - k, (me >= k) & (me < self.count - 1)),
                (1, me + k, (me + k < self.count) & (me > 0)),
            ):

                @pl.when(sent)
                def _():
                    self.copy(way, piece).wait_send()


def greet_neighbours(barrier, axis, count):
    me = lax.axis_index(axis)
    for ahead, there in ((1, me < count - 1), (-1, me > 0)):

        @pl.when(there)
        def _():
            pl.semaphore_signal(barrier, inc=1, device_id={axis: me + ahead}, device_id_type=pl.DeviceIdType.MESH)

    return (me < count - 1).astype(jnp.int32) + (me > 0).astype(jnp.int32)


def settle_kernel(sizes, gq_ref, gk_ref, gv_ref, wq_ref, wk_ref, wv_ref, tokens_ref, first_ref, gain_ref, pack_ref,
                  x_ref, out_ref, share_ref, piece_ref, own, landed, chosen, arrived, sem, pair_send, pair_recv, send_sem,
                  recv_sem, x_buffers, x_total, x_send, x_recv):
    dp_size, shard_size, count = sizes
    spread = shard_size // 2
    halves = dp_size * spread
    dp, shard = lax.axis_index("dp"), lax.axis_index("shard")
    side = shard % 2
    place = dp * spread + shard // 2
    step = pl.program_id(0)
    last = pl.num_programs(0) - 1

    def target(piece, bit):
        return {"dp": piece // spread, "shard": (piece % spread) * 2 + bit}

    line = LineSum("expert", count, x_ref, x_buffers, x_send, x_recv)

    def pair_copy():
        return pltpu.make_async_remote_copy(
            src_ref=pack_ref.at[:, 1 - side], dst_ref=landed, send_sem=pair_send, recv_sem=pair_recv,
            device_id=target(place, 1 - side), device_id_type=pl.DeviceIdType.MESH,
        )

    def own_copy():
        return pltpu.make_async_copy(pack_ref.at[:, side], own, sem)

    def send(index):
        return pltpu.make_async_remote_copy(
            src_ref=chosen.at[index], dst_ref=arrived.at[index], send_sem=send_sem.at[index], recv_sem=recv_sem.at[index],
            device_id=target(lax.rem(place + index + 1, halves), side), device_id_type=pl.DeviceIdType.MESH,
        )

    @pl.when(step == 0)
    def _():
        barrier = pltpu.get_barrier_semaphore()
        pl.semaphore_signal(barrier, inc=1, device_id=target(place, 1 - side), device_id_type=pl.DeviceIdType.MESH)
        for index in range(halves - 1):
            pl.semaphore_signal(
                barrier, inc=1, device_id=target(lax.rem(place + index + 1, halves), side),
                device_id_type=pl.DeviceIdType.MESH,
            )
        neighbours = greet_neighbours(barrier, "expert", count)
        pl.semaphore_wait(barrier, halves + neighbours)
        pair_copy().start()
        own_copy().start()
        line.start()

    @pl.when(step == 1)
    def _():
        own_copy().wait()
        pair_copy().wait()
        for index in range(halves - 1):
            piece = lax.rem(place + index + 1, halves)
            chosen[index] = (own[piece].astype(F32) + landed[piece].astype(F32)).astype(BF16)
            send(index).start()

    grad_normed = (
        dot_nt(gq_ref[...], wq_ref[...]) + dot_nt(gk_ref[...], wk_ref[...]) + dot_nt(gv_ref[...], wv_ref[...])
    )
    source = tokens_ref[...].astype(F32)
    scale = lax.rsqrt(jnp.mean(source * source, axis=1, keepdims=True) + EPSILON)
    weighted = grad_normed * gain_ref[...]
    inner = jnp.mean(source * weighted, axis=1, keepdims=True)
    out_ref[...] = first_ref[...] + scale * weighted - source * (scale * scale * scale * inner)

    @pl.when(step == last)
    def _():
        line.relay()
        total = own[place].astype(F32) + landed[place].astype(F32)
        for index in range(halves - 1):
            send(index).wait()
            total = total + arrived[index].astype(F32)
        share_ref[...] = total.astype(BF16)
        line.finish(x_total)
        piece_ref[...] = x_total[...].astype(BF16)


def settle(grads, w_qkv, tokens, grad_first, gain, pack, x, sizes):
    rows, width = tokens.shape
    block = min(256, rows)
    blocked = pl.BlockSpec((block, width), lambda i: (i, 0))
    halves, count = sizes[0] * sizes[1] // 2, pack.shape[1]
    piece = (count, LANES)
    x_piece = (x.shape[0] // sizes[2], LANES)
    return call(
        functools.partial(settle_kernel, sizes), (rows // block,),
        [blocked] * 3 + [square(width, 0), square(width, 1), square(width, 2), blocked, blocked, whole((1, width)),
                         pl.BlockSpec(memory_space=pl.ANY), whole(x.shape)],
        [blocked, whole(piece), whole(x_piece)],
        [shape_of((rows, width), F32), shape_of(piece, BF16), shape_of(x_piece, BF16)],
        scratch=[pltpu.VMEM((halves,) + piece, BF16), pltpu.VMEM((halves,) + piece, BF16),
                 pltpu.VMEM((halves - 1,) + piece, BF16), pltpu.VMEM((halves - 1,) + piece, BF16),
                 pltpu.SemaphoreType.DMA, pltpu.SemaphoreType.DMA, pltpu.SemaphoreType.DMA,
                 pltpu.SemaphoreType.DMA((halves - 1,)), pltpu.SemaphoreType.DMA((halves - 1,)),
                 pltpu.VMEM((2, 2, sizes[2]) + x_piece, BF16), pltpu.VMEM(x_piece, F32),
                 pltpu.SemaphoreType.DMA((2, sizes[2])), pltpu.SemaphoreType.DMA((2, sizes[2]))],
        flops=6 * rows * width * width, moved=22 * rows * width, collective_id=1,
    )(*grads, w_qkv, w_qkv, w_qkv, tokens, grad_first, gain, pack.reshape((halves, 2) + piece), x)


def copies_of(layout, block, width, step, stage_g, stage_u, stage_d, slot, packed_ref, sems):
    by_rows, owners, hidden, base = layout
    panels = block // LANES
    rows_down = hidden // owners
    out = []

    def add(source, target):
        out.append(pltpu.make_async_copy(source, target, sems.at[slot, len(out)]))

    if by_rows:
        rows = width // owners
        for half, stage in enumerate((stage_g, stage_u)):
            for p in range(panels):
                panel = half * (hidden // LANES) + step * panels + p
                add(
                    stage.at[slot, :, :, pl.ds(p * LANES, LANES)],
                    packed_ref.at[:, pl.ds(pl.multiple_of(base + panel * rows, 8), rows), :],
                )
        start = 2 * hidden // LANES * rows
    else:
        columns = 2 * hidden // owners
        for half, stage in enumerate((stage_g, stage_u)):
            for p in range(panels):
                column = half * hidden + step * block + p * LANES
                owner, panel = column // columns, (column % columns) // LANES
                add(
                    stage.at[slot, :, pl.ds(p * LANES, LANES)],
                    packed_ref.at[owner, pl.ds(pl.multiple_of(base + panel * width, 8), width), :],
                )
        start = columns // LANES * width
    for q in range(block // rows_down):
        owner = step * (block // rows_down) + q
        for c in range(width // LANES):
            add(
                stage_d.at[slot, pl.ds(q * rows_down, rows_down), pl.ds(c * LANES, LANES)],
                packed_ref.at[owner, pl.ds(base + start + c * rows_down, rows_down), :],
            )
    return out


def packed_rows(width, hidden, owners):
    return 3 * width * hidden // owners // LANES


def ffn_kernel(out_type, layout, block, x_ref, gy_ref, wg_ref, wu_ref, wd_ref, *rest):
    y_ref, gx_ref, packed_ref, xt, y_acc, gx_acc, stage_g, stage_u, stage_d, sems = rest[-10:]
    step = pl.program_id(0)
    steps = layout[2] // block
    width = x_ref.shape[1]
    slot = step % 2
    copies = functools.partial(copies_of, layout, block, width)

    @pl.when(step == 0)
    def _():
        xt[...] = x_ref[...].T
        y_acc[...] = jnp.zeros_like(y_acc)
        gx_acc[...] = jnp.zeros_like(gx_acc)

    @pl.when(step >= 2)
    def _():
        for copy in copies(step - 2, stage_g, stage_u, stage_d, slot, packed_ref, sems):
            copy.wait()

    x, gy = x_ref[...], gy_ref[...].reshape(x_ref.shape)
    if layout[0]:
        wg, wu = wg_ref[...].reshape(width, block), wu_ref[...].reshape(width, block)
        rows = wd_ref.shape[1] // (width // block)
        wd = jnp.concatenate(
            [wd_ref[:, pl.ds(c * rows, rows), :].reshape(block, block) for c in range(width // block)], axis=1
        )
    else:
        wg, wu, wd = wg_ref[...], wu_ref[...], wd_ref[...]
    gate, up = dot_nn(x, wg), dot_nn(x, wu)
    grad_hidden = dot_nt(gy, wd)
    sigmoid = jax.nn.sigmoid(gate)
    value = gate * sigmoid
    hidden = (value * up).astype(BF16)
    grad_up = (grad_hidden * value).astype(BF16)
    grad_gate = (grad_hidden * up * (sigmoid * (1.0 + gate * (1.0 - sigmoid)))).astype(BF16)
    y_acc[...] += dot_nn(hidden, wd)
    gx_acc[...] += dot_nt(grad_gate, wg) + dot_nt(grad_up, wu)
    stage_g[slot] = dot_nn(xt[...], grad_gate).astype(BF16).reshape(stage_g.shape[1:])
    stage_u[slot] = dot_nn(xt[...], grad_up).astype(BF16).reshape(stage_u.shape[1:])
    stage_d[slot] = dot_tn(hidden, gy).astype(BF16)
    for copy in copies(step, stage_g, stage_u, stage_d, slot, packed_ref, sems):
        copy.start()

    @pl.when(step == steps - 1)
    def _():
        y_ref[...] = y_acc[...].astype(out_type)
        gx_ref[...] = gx_acc[...].astype(out_type)
        for back in (1, 0):
            if steps > back:
                for copy in copies(steps - 1 - back, stage_g, stage_u, stage_d, (steps - 1 - back) % 2, packed_ref, sems):
                    copy.wait()


BLOCK = 256


def ffn_both(x, gy, w_gu, w_down, hidden, expert, owners, out_type, parts=1, pack=None):
    rows, width = x.shape
    block = BLOCK
    steps = hidden // block
    by_rows = expert is None
    if by_rows:
        own, own_down, panels = width // owners, hidden // owners, width // block
        ahead = 2 * steps * own // (panels * own_down)
        gate = pl.BlockSpec((owners, own, block), lambda f: (0, f, 0))
        up = pl.BlockSpec((owners, own, block), lambda f: (0, steps + f, 0))
        down = pl.BlockSpec((block // own_down, panels * own_down, block), lambda f: (f, ahead, 0))
        stage = (2, owners, own, block)
    else:
        gate = pl.BlockSpec((None, width, block), lambda f: (expert, 0, f))
        up = pl.BlockSpec((None, width, block), lambda f: (expert, 0, steps + f))
        down = pl.BlockSpec((None, block, width), lambda f: (expert, f, 0))
        stage = (2, width, block)
    if by_rows:
        grads = whole((rows, width))
    else:
        grads = pl.BlockSpec(
            (gy.shape[0], rows // gy.shape[0], width), lambda f: (0, expert, 0), pipeline_mode=pl.Buffered(1)
        )
    out_rows = whole((rows, width))
    count = packed_rows(width, hidden, owners)
    layout = (by_rows, owners, hidden, (expert or 0) * count)
    held = [] if pack is None else [pack]
    copies = 2 * (block // LANES) + block // (hidden // owners) * (width // LANES)
    return call(
        functools.partial(ffn_kernel, out_type, layout, block), (steps,),
        [whole((rows, width)), grads, gate, up, down] + [pl.BlockSpec(memory_space=pl.ANY)] * len(held),
        [out_rows, out_rows, pl.BlockSpec(memory_space=pl.ANY)],
        [shape_of((rows, width), out_type), shape_of((rows, width), out_type),
         shape_of((owners, parts * count, LANES), BF16)],
        scratch=[pltpu.VMEM((width, rows), BF16), pltpu.VMEM((rows, width), F32), pltpu.VMEM((rows, width), F32),
                 pltpu.VMEM(stage, BF16), pltpu.VMEM(stage, BF16), pltpu.VMEM((2, block, width), BF16),
                 pltpu.SemaphoreType.DMA((2, copies))],
        flops=18 * rows * width * hidden, moved=12 * width * hidden + 16 * rows * width, trans=rows * hidden,
        aliases={5: 2} if held else None,
    )(x, gy, w_gu, w_gu, w_down, *held)


def to_panels(array):
    rows, columns = array.shape
    return jnp.transpose(array.reshape(rows, columns // BLOCK, BLOCK), (1, 0, 2)).reshape(-1, BLOCK)


def attention_weights_kernel(per, normed_ref, mixed_ref, gq_ref, gk_ref, gv_ref, ga_ref, gains_ref, out_ref, xt):
    step = pl.program_id(0)
    owners, rows = out_ref.shape[0], out_ref.shape[1] // (out_ref.shape[1] // (normed_ref.shape[1] // out_ref.shape[0]))
    panels = out_ref.shape[1] // rows

    @pl.when(step == 0)
    def _():
        xt[...] = normed_ref[...].T

    @pl.when(step == 3 * per)
    def _():
        xt[...] = mixed_ref[...].T

    for index, grad_ref in enumerate((gq_ref, gk_ref, gv_ref, ga_ref)):

        @pl.when((step >= index * per) & (step < (index + 1) * per))
        def _():
            product = dot_nn(xt[...], grad_ref[...]).astype(BF16)
            for p in range(panels):
                out_ref[:, pl.ds(p * rows, rows), :] = product[:, p * LANES : (p + 1) * LANES].reshape(owners, rows, LANES)

    @pl.when(step >= 4 * per)
    def _():
        out_ref[...] = jnp.zeros_like(out_ref)

    @pl.when(step == 4 * per)
    def _():
        out_ref[:, pl.ds(0, gains_ref.shape[1]), :] = gains_ref[...]


def attention_weights(normed, mixed, grads, grad_attn, gains, owners, pieces):
    tokens, width = normed.shape
    rows = width // owners
    block = BLOCK
    panels, per = block // LANES, width // block
    steps = 4 * per + 1
    while steps * panels * rows % (16 * pieces):
        steps += 1

    def columns(index):
        return pl.BlockSpec((tokens, block), lambda i: (0, jnp.clip(i - index * per, 0, per - 1)))

    return call(
        functools.partial(attention_weights_kernel, per), (steps,),
        [whole((tokens, width)), whole((tokens, width))] + [columns(index) for index in range(4)] + [whole(gains.shape)],
        pl.BlockSpec((owners, panels * rows, LANES), lambda i: (0, i, 0)),
        shape_of((owners, steps * panels * rows, LANES), BF16),
        scratch=[pltpu.VMEM((width, tokens), BF16)],
        flops=8 * tokens * width * width, moved=16 * tokens * width,
    )(normed, mixed, *grads, grad_attn, gains)


GROUP = ("dp", "shard")


def local(
    tokens,
    lengths,
    routes,
    route_gates,
    cotangent,
    norm_gains,
    w_qkv,
    w_out,
    w_shared_gu,
    w_shared_down,
    w_expert_gu,
    w_expert_down,
):
    tok_count, width = tokens.shape
    seq_count = lengths.shape[0]
    length = tok_count // seq_count
    local_experts = w_expert_gu.shape[0]
    owners = lax.axis_size("expert")
    experts = local_experts * owners
    top = routes.shape[1]
    capacity = tok_count * top * 9 // (8 * experts)
    head_dim = width // HEADS
    hidden = w_expert_down.shape[1]

    gains = lax.all_gather(norm_gains, GROUP, axis=1, tiled=True).astype(F32)
    attention_weight = lax.all_gather(jnp.concatenate([w_qkv, w_out], axis=1), GROUP, axis=0, tiled=True)
    shared_weight = lax.all_gather(
        jnp.concatenate([to_panels(w_shared_gu), to_panels(w_shared_down)], axis=0)[None], GROUP, axis=0, tiled=True
    )
    gain_one, gain_two = gains[0:1], gains[1:2]

    live_bool = lax.iota(jnp.int32, tok_count) % length < jnp.repeat(lengths, length)
    live = live_bool.astype(F32)[:, None]
    live_row = live_bool.astype(jnp.int32)[None, :]

    group = lax.axis_size("dp") * lax.axis_size("shard")
    shared_hidden = w_shared_down.shape[0] * group

    dest_t = slots_of(routes.T, live_row, experts, capacity)
    dest = dest_t.T
    slots = owners * capacity

    def place(where):
        owner_of, part_of = where // (local_experts * capacity), (where // capacity) % local_experts
        return jnp.where(
            where < experts * capacity, part_of * slots + owner_of * capacity + where % capacity, experts * capacity
        )

    placed, placed_t = place(dest), place(dest_t)
    gates_t = route_gates.T
    grad_b = jnp.where(live_bool[:, None], cotangent, 0).astype(BF16)

    def exchange(rows):
        count = rows.shape[0] // owners
        return lax.all_to_all(
            rows.reshape(owners, count, width), "expert", split_axis=0, concat_axis=0, tiled=True
        ).reshape(rows.shape)

    send_grad = dispatch(dest_t, gates_t, grad_b, experts, capacity, True, 0)
    received_grad = exchange(send_grad).reshape(owners, local_experts * capacity, width)

    cosine, sine = rotary_tables(length, head_dim)
    normed_one = norm_one(tokens, gain_one)
    queries, keys, values, mixed, lse = attend_forward(normed_one, attention_weight, cosine, sine, length, head_dim)
    first_sum, normed_two = norm_two(mixed, tokens, attention_weight, gain_two)

    received = []
    for j in range(local_experts):
        rows = dispatch(placed_t, gates_t, normed_two, owners, capacity, False, j * owners)
        received.append(exchange(rows))
    shared_out, grad_shared, shared_pack = ffn_both(
        normed_two, grad_b, shared_weight, shared_weight, shared_hidden, None, group, F32
    )
    back_rows, out_rows, pack = [], [], None
    for j in range(local_experts):
        y, gx, pack = ffn_both(
            received[j], received_grad, w_expert_gu, w_expert_down, hidden, j, group, BF16, local_experts, pack
        )
        back_rows.append(exchange(gx))
        out_rows.append(y)
    base = grad_shared
    for j, rows in enumerate(back_rows[:-1]):
        base = add_part(placed, base, rows, j)
    grad_first, grad_attn, grad_mixed, grad_gain_two = norm_two_back(
        placed, live, cotangent, first_sum, base, gain_two, attention_weight, back_rows[-1], local_experts - 1
    )

    grads = attend_backward(queries, keys, values, mixed, grad_mixed, lse, cosine, sine, length, head_dim)
    own = width // group
    grad_gains = grad_gain_two.reshape(group, 1, own)
    grad_gains = jnp.pad(grad_gains, ((0, 0), (0, 15), (0, LANES - own))).astype(BF16)
    attention_pack = attention_weights(normed_one, mixed, grads, grad_attn, grad_gains, group, owners)

    def spread(pack):
        return lax.psum_scatter(pack, GROUP, scatter_dimension=0, tiled=True)[0]

    shared_share = spread(shared_pack)
    expert_share = spread(pack)
    input_grad, attention_share, shared_piece = settle(
        grads, attention_weight, tokens, grad_first, gain_one, attention_pack, shared_share,
        (lax.axis_size("dp"), lax.axis_size("shard"), owners),
    )
    returned = exchange_parts(out_rows, owners, "expert")
    layer_out, expert_gu, expert_down, qkv_grad, out_grad, shared_gu, shared_down, gain_rows = combine(
        placed, route_gates, live, first_sum, shared_out, returned, attention_share, shared_piece, expert_share,
        "expert", owners, own, shared_hidden, hidden,
    )
    grad_gain_one = jnp.sum(w_qkv.astype(F32) * qkv_grad, axis=1) / norm_gains[0].astype(F32)
    grad_gains = jnp.stack([grad_gain_one, gain_rows[0, :own]])
    return layer_out, input_grad, grad_gains, qkv_grad, out_grad, shared_gu, shared_down, expert_gu, expert_down


def exchange_parts(parts, owners, axis):
    width = parts[0].shape[1]
    count = parts[0].shape[0] // owners
    joined = jnp.concatenate([rows.reshape(owners, count, width) for rows in parts], axis=1)
    back = lax.all_to_all(joined, axis, split_axis=0, concat_axis=0, tiled=True)
    return [
        back[:, j * count : (j + 1) * count].reshape(owners * count, width) for j in range(len(parts))
    ]


def solution(mesh):
    rows = P(("dp", "expert", "shard"), None)
    split = P(GROUP, None)
    in_specs = (
        rows,
        P(("dp", "expert", "shard")),
        rows,
        rows,
        rows,
        P(None, GROUP),
        split,
        split,
        split,
        split,
        P("expert", None, None),
        P("expert", None, None),
    )
    out_specs = (
        rows,
        rows,
        P(None, GROUP),
        split,
        split,
        split,
        split,
        P("expert", None, GROUP),
        P("expert", GROUP, None),
    )

    return jax.shard_map(local, mesh=mesh, in_specs=in_specs, out_specs=out_specs, check_vma=False)
```

```python
import functools
import math

import jax
import jax.numpy as jnp
from jax import lax
from jax.experimental import pallas as pl
from jax.experimental.pallas import tpu as pltpu
from jax.sharding import PartitionSpec as P


HEADS = 12
LANES = 128
EPSILON = 1e-05
VMEM_BYTES = 60 * 1024 * 1024
BF16 = jnp.bfloat16
F32 = jnp.float32


def call(kernel, grid, in_specs, out_specs, out_shape, scratch=(), flops=0, moved=0, trans=0, collective_id=None, aliases=None):
    return pl.pallas_call(
        kernel,
        grid_spec=pltpu.PrefetchScalarGridSpec(
            num_scalar_prefetch=0,
            grid=grid,
            in_specs=in_specs,
            out_specs=out_specs,
            scratch_shapes=list(scratch),
        ),
        out_shape=out_shape,
        input_output_aliases=aliases or {},
        compiler_params=pltpu.CompilerParams(
            dimension_semantics=("arbitrary",) * len(grid), vmem_limit_bytes=VMEM_BYTES, collective_id=collective_id,
            has_side_effects=collective_id is not None,
        ),
        cost_estimate=pl.CostEstimate(flops=flops, bytes_accessed=moved, transcendentals=trans),
    )


def shape_of(shape, dtype):
    return jax.ShapeDtypeStruct(shape, dtype)


def whole(shape):
    return pl.BlockSpec(shape, lambda *_: (0,) * len(shape), pipeline_mode=pl.Buffered(1))


def dot_nn(left, right):
    return lax.dot_general(left, right, (((1,), (0,)), ((), ())), preferred_element_type=F32)


def dot_nt(left, right):
    return lax.dot_general(left, right, (((1,), (1,)), ((), ())), preferred_element_type=F32)


def dot_tn(left, right):
    return lax.dot_general(left, right, (((0,), (0,)), ((), ())), preferred_element_type=F32)


def rotary_tables(length, head_dim):
    half_dim = head_dim // 2
    position = lax.iota(F32, length)[:, None]
    frequency = jnp.exp(lax.iota(F32, half_dim) * (-2.0 * math.log(10000.0) / head_dim))
    angle_table = position * frequency[None, :]
    cosine, sine = jnp.cos(angle_table), jnp.sin(angle_table)
    repeats = LANES // head_dim
    return (
        jnp.tile(jnp.concatenate([cosine, cosine], axis=1), (1, repeats)),
        jnp.tile(jnp.concatenate([-sine, sine], axis=1), (1, repeats)),
    )


def turn(values, cosine, signed_sine, head_dim):
    lane = lax.broadcasted_iota(jnp.int32, values.shape, 1)
    half = head_dim // 2
    other = jnp.where(
        lane % head_dim < half,
        pltpu.roll(values, LANES - half, 1),
        pltpu.roll(values, half, 1),
    )
    return values * cosine + other * signed_sine


def attend_forward_kernel(
    head_dim, block, x_ref, wq_ref, wk_ref, wv_ref, cos_ref, sin_ref, q_ref, k_ref, v_ref, o_ref, lse_ref, lse_tile
):
    length = x_ref.shape[0]
    heads = LANES // head_dim
    x = x_ref[...]
    cosine, sine = cos_ref[...], sin_ref[...]
    scale = 1.0 / math.sqrt(head_dim)
    q_ref[...] = (turn(dot_nn(x, wq_ref[...]), cosine, sine, head_dim) * scale).astype(BF16)
    k_ref[...] = turn(dot_nn(x, wk_ref[...]), cosine, sine, head_dim).astype(BF16)
    v_ref[...] = dot_nn(x, wv_ref[...]).astype(BF16)
    lane = lax.broadcasted_iota(jnp.int32, (1, LANES), 1)
    own_lane = lax.broadcasted_iota(jnp.int32, (block, LANES), 1) // head_dim
    below = lax.broadcasted_iota(jnp.int32, (block, block), 0) >= lax.broadcasted_iota(
        jnp.int32, (block, block), 1
    )
    for first in range(0, length, block):
        rows = pl.ds(first, block)
        mixed = None
        logs = None
        for head in range(heads):
            select = (lane // head_dim == head).astype(F32).astype(BF16)
            queries = q_ref[rows, :] * select
            near = jnp.where(below, dot_nt(queries, k_ref[rows, :]), -1e30)
            peak = jnp.max(near, axis=1, keepdims=True)
            if first:
                far = dot_nt(queries, k_ref[pl.ds(0, first), :])
                peak = jnp.maximum(peak, jnp.max(far, axis=1, keepdims=True))
            near = jnp.exp(near - peak)
            total = jnp.sum(near, axis=1, keepdims=True)
            part = dot_nn(near.astype(BF16), v_ref[rows, :])
            if first:
                far = jnp.exp(far - peak)
                total = total + jnp.sum(far, axis=1, keepdims=True)
                part = part + dot_nn(far.astype(BF16), v_ref[pl.ds(0, first), :])
            part = part * (1.0 / total)
            log_total = jnp.broadcast_to(peak + jnp.log(total), (block, LANES))
            mixed = part if head == 0 else jnp.where(own_lane == head, part, mixed)
            logs = log_total if head == 0 else jnp.where(own_lane == head, log_total, logs)
        o_ref[rows, :] = mixed.astype(BF16)
        lse_tile[rows, :] = logs
    turned = lse_tile[...].T
    for head in range(heads):
        lse_ref[pl.ds(head * 8, 8), :] = turned[head * head_dim : head * head_dim + 8, :]


def attend_forward(normed, w_qkv, cosine, sine, length, head_dim):
    tokens, width = normed.shape
    seqs, pairs, heads = tokens // length, width // LANES, LANES // head_dim
    block = min(256, length)
    rows = pl.BlockSpec((length, LANES), lambda s, p: (s, p))

    def weight(part):
        return pl.BlockSpec((width, LANES), lambda s, p: (0, part * pairs + p))

    table = whole((length, LANES))
    return call(
        functools.partial(attend_forward_kernel, head_dim, block),
        (seqs, pairs),
        [pl.BlockSpec((length, width), lambda s, p: (s, 0)), weight(0), weight(1), weight(2), table, table],
        [rows, rows, rows, rows, pl.BlockSpec((8 * heads, length), lambda s, p: (s * pairs + p, 0))],
        [shape_of((tokens, width), BF16)] * 4 + [shape_of((seqs * pairs * 8 * heads, length), F32)],
        scratch=[pltpu.VMEM((length, LANES), F32)],
        flops=6 * tokens * width * width + 4 * tokens * length * width,
        moved=16 * tokens * width,
        trans=tokens * length * width // head_dim // 2,
    )(normed, w_qkv, w_qkv, w_qkv, cosine, sine)


def attend_backward_kernel(
    head_dim, block, q_ref, k_ref, v_ref, o_ref, g_ref, lse_ref, cos_ref, sin_ref, gq_ref, gk_ref, gv_ref, gq_acc
):
    length = q_ref.shape[0]
    heads = LANES // head_dim
    scale = 1.0 / math.sqrt(head_dim)
    product = (g_ref[...].astype(F32) * o_ref[...].astype(F32)).T
    inner = [
        jnp.sum(product[head * head_dim : (head + 1) * head_dim, :], axis=0, keepdims=True)
        for head in range(heads)
    ]
    gq_acc[...] = jnp.zeros_like(gq_acc)
    lane = lax.broadcasted_iota(jnp.int32, (1, LANES), 1)
    own_lane = lax.broadcasted_iota(jnp.int32, (block, LANES), 1) // head_dim
    above = lax.broadcasted_iota(jnp.int32, (block, block), 1) >= lax.broadcasted_iota(
        jnp.int32, (block, block), 0
    )
    for first in range(0, length, block):
        rows = pl.ds(first, block)
        keys_grad = None
        values_grad = None
        for head in range(heads):
            select = (lane // head_dim == head).astype(F32).astype(BF16)
            keys = k_ref[rows, :] * select
            values = v_ref[rows, :] * select
            log_total = lse_ref[pl.ds(head * 8, 1), :]
            pieces = [(first, block, True)]
            if first + block < length:
                pieces.append((first + block, length - first - block, False))
            keys_part = None
            values_part = None
            for start, count, diagonal in pieces:
                span = pl.ds(start, count)
                queries, grads = q_ref[span, :], g_ref[span, :]
                scores = dot_nt(keys, queries)
                probs = jnp.exp(scores - log_total[:, start : start + count])
                if diagonal:
                    probs = jnp.where(above, probs, 0.0)
                grad_probs = dot_nt(values, grads)
                grad_scores = (probs * (grad_probs - inner[head][:, start : start + count])).astype(BF16)
                piece_values = dot_nn(probs.astype(BF16), grads)
                piece_keys = dot_nn(grad_scores, queries)
                values_part = piece_values if values_part is None else values_part + piece_values
                keys_part = piece_keys if keys_part is None else keys_part + piece_keys
                gq_acc[span, :] += dot_tn(grad_scores, keys)
            keys_grad = keys_part if head == 0 else jnp.where(own_lane == head, keys_part, keys_grad)
            values_grad = values_part if head == 0 else jnp.where(own_lane == head, values_part, values_grad)
        gk_ref[rows, :] = turn(keys_grad, cos_ref[rows, :], -sin_ref[rows, :], head_dim).astype(BF16)
        gv_ref[rows, :] = values_grad.astype(BF16)
    gq_ref[...] = turn(gq_acc[...] * scale, cos_ref[...], -sin_ref[...], head_dim).astype(BF16)


def attend_backward(queries, keys, values, mixed, grad_mixed, lse, cosine, sine, length, head_dim):
    tokens, width = queries.shape
    seqs, pairs, heads = tokens // length, width // LANES, LANES // head_dim
    block = min(256, length)
    rows = pl.BlockSpec((length, LANES), lambda s, p: (s, p))
    table = whole((length, LANES))
    return call(
        functools.partial(attend_backward_kernel, head_dim, block),
        (seqs, pairs),
        [rows] * 5 + [pl.BlockSpec((8 * heads, length), lambda s, p: (s * pairs + p, 0)), table, table],
        [rows] * 3,
        [shape_of((tokens, width), BF16)] * 3,
        scratch=[pltpu.VMEM((length, LANES), F32)],
        flops=10 * tokens * length * width,
        moved=16 * tokens * width,
        trans=tokens * length * width // head_dim // 2,
    )(queries, keys, values, mixed, grad_mixed, lse, cosine, sine)


def square(width, part):
    return pl.BlockSpec((width, width), lambda i: (0, part), pipeline_mode=pl.Buffered(1))


def norm_one_kernel(x_ref, gain_ref, out_ref):
    x = x_ref[...].astype(F32)
    scale = lax.rsqrt(jnp.mean(x * x, axis=1, keepdims=True) + EPSILON)
    out_ref[...] = (x * scale * gain_ref[...]).astype(BF16)


def norm_one(tokens, gain):
    rows, width = tokens.shape
    block = min(256, rows)
    blocked = pl.BlockSpec((block, width), lambda i: (i, 0))
    return call(
        norm_one_kernel, (rows // block,), [blocked, whole((1, width))], blocked, shape_of((rows, width), BF16),
        flops=5 * rows * width, moved=4 * rows * width,
    )(tokens, gain)


def norm_two_kernel(mixed_ref, tokens_ref, weight_ref, gain_ref, sum_ref, normed_ref):
    first_sum = tokens_ref[...].astype(F32) + dot_nn(mixed_ref[...], weight_ref[...])
    sum_ref[...] = first_sum
    scale = lax.rsqrt(jnp.mean(first_sum * first_sum, axis=1, keepdims=True) + EPSILON)
    normed_ref[...] = (first_sum * scale * gain_ref[...]).astype(BF16)


def norm_two(mixed, tokens, weight, gain):
    rows, width = tokens.shape
    block = min(256, rows)
    blocked = pl.BlockSpec((block, width), lambda i: (i, 0))
    return call(
        norm_two_kernel, (rows // block,), [blocked, blocked, square(width, 3), whole((1, width))],
        [blocked, blocked], [shape_of((rows, width), F32), shape_of((rows, width), BF16)],
        flops=2 * rows * width * width, moved=10 * rows * width,
    )(mixed, tokens, weight, gain)


def slots_kernel(experts, parts, capacity, routes_ref, live_ref, rows_ref, columns_ref):
    top, tokens = routes_ref.shape
    live = live_ref[...]
    number = lax.broadcasted_iota(jnp.int32, (experts, tokens), 0)
    hits = [
        jnp.where((routes_ref[pl.ds(k, 1), :] == number) & (live > 0), 1.0, 0.0) for k in range(top)
    ]
    earlier = jnp.where(
        lax.broadcasted_iota(jnp.int32, (tokens, tokens), 0)
        <= lax.broadcasted_iota(jnp.int32, (tokens, tokens), 1),
        1.0,
        0.0,
    ).astype(BF16)
    ranks = dot_nn(jnp.concatenate(hits, axis=0).astype(BF16), earlier)
    before = jnp.zeros((experts, 1), F32)
    expert = lax.broadcasted_iota(jnp.int32, (experts, tokens), 0)
    start = ((expert % parts) * (experts // parts) + expert // parts) * capacity
    found = []
    for k in range(top):
        rank = ranks[k * experts : (k + 1) * experts, :] + before - 1.0
        for first in (number * capacity, start):
            slot = jnp.sum(hits[k] * (first.astype(F32) + rank), axis=0, keepdims=True).astype(jnp.int32)
            found.append(jnp.where(live > 0, slot, experts * capacity))
        before = before + jnp.sum(hits[k], axis=1, keepdims=True)
    table = jnp.concatenate(found[0::2] + found[1::2] + [jnp.zeros((8 - 2 * top, tokens), jnp.int32)], axis=0)
    rows_ref[...] = table
    columns_ref[...] = table.T


def slots_of(routes_t, live_row, experts, parts, capacity):
    top, tokens = routes_t.shape
    return call(
        functools.partial(slots_kernel, experts, parts, capacity), (1,),
        [whole((top, tokens)), whole((1, tokens))], [whole((8, tokens)), whole((tokens, 8))],
        [shape_of((8, tokens), jnp.int32), shape_of((tokens, 8), jnp.int32)],
        flops=2 * top * experts * tokens * tokens, moved=16 * tokens,
    )(routes_t, live_row)


def dispatch_kernel(gated, first, base, dest_ref, gates_ref, x_ref, out_ref):
    top, tokens = gates_ref.shape
    capacity = out_ref.shape[0]
    slot = lax.broadcasted_iota(jnp.int32, (capacity, tokens), 0) + (first + pl.program_id(0)) * capacity
    hits = [slot == dest_ref[pl.ds(base + k, 1), :] for k in range(top)]
    chosen = functools.reduce(jnp.logical_or, hits)
    rows = dot_nn(jnp.where(chosen, 1.0, 0.0).astype(BF16), x_ref[...])
    if gated:
        weights = jnp.zeros((capacity, tokens), F32)
        for k in range(top):
            weights = jnp.where(hits[k], gates_ref[pl.ds(k, 1), :], weights)
        rows = rows * jnp.sum(weights, axis=1, keepdims=True)
    out_ref[...] = rows.astype(BF16)


def dispatch(dest_t, gates_t, x, experts, capacity, gated, first, base):
    top, tokens = gates_t.shape
    width = x.shape[1]
    return call(
        functools.partial(dispatch_kernel, gated, first, base), (experts,),
        [whole(dest_t.shape), whole((top, tokens)), whole((tokens, width))],
        pl.BlockSpec((capacity, width), lambda e: (e, 0)),
        shape_of((experts * capacity, width), BF16),
        flops=2 * experts * capacity * tokens * width, moved=2 * (experts * capacity + tokens) * width,
    )(dest_t, gates_t, x)


def unpack(source, start, rows, panels, target):
    for p in range(panels):
        target[:, pl.ds(p * LANES, LANES)] = source[pl.ds(start + p * rows, rows), :].astype(F32)


def combine_kernel(axis, count, own, gu_panels, experts, dest_ref, gates_ref, live_ref, sum_ref, shared_ref, y_ref, *rest):
    x_ref, p_ref, pack_ref, out_ref, egu_ref, ed_ref, qkv_ref, wo_ref, sgu_ref, sd_ref, gain_ref = rest[:11]
    buffers, total_x, all_x, sum_send, sum_recv, x_send, x_recv = rest[11:]
    step = pl.program_id(0)
    last = pl.num_programs(0) - 1
    line = LineSum(axis, count, x_ref, buffers, sum_send, sum_recv)
    gather_x = LineGather(axis, count, all_x, x_send, x_recv)
    width = out_ref.shape[1]
    d_panels = width // LANES
    packed = pack_ref.shape[0] // experts
    e_panels, e_rows = egu_ref.shape[2] // LANES, egu_ref.shape[1]

    @pl.when(step == 0)
    def _():
        barrier = pltpu.get_barrier_semaphore()
        pl.semaphore_wait(barrier, greet_neighbours(barrier, axis, count))
        line.start()
        unpack(p_ref, 0, own, gu_panels, sgu_ref)
        unpack(p_ref, gu_panels * own, sd_ref.shape[0], d_panels, sd_ref)
        for e in range(experts):
            unpack(pack_ref, e * packed + e_panels * width, ed_ref.shape[1], d_panels, ed_ref.at[e])

    for e in range(experts):
        for p in range(e_panels):
            rows = pl.ds(pl.multiple_of(e * packed + p * width + step * e_rows, 16), e_rows)
            egu_ref[e, :, pl.ds(p * LANES, LANES)] = pack_ref[rows, :].astype(F32)

    block, top = gates_ref.shape
    total = sum_ref[...] + shared_ref[...]
    dest = dest_ref[...]
    gates = gates_ref[...]
    slot = slot_numbers(block, y_ref.shape[0], 0)
    for k in range(top):
        hit = jnp.where(slot == dest[:, k : k + 1], 1.0, 0.0).astype(BF16)
        total = total + dot_nn(hit, y_ref[...]) * gates[:, k : k + 1]
    out_ref[...] = (live_ref[...] * total).astype(BF16)

    @pl.when(step == jnp.minimum(1, last))
    def _():
        line.relay()

    @pl.when(step == jnp.minimum(2, last))
    def _():
        line.finish(total_x)
        gather_x.start(total_x[...].astype(BF16))

    @pl.when(step == last)
    def _():
        for k in range(1, count):
            gather_x.relay(k)
        gather_x.finish()
        unpack(all_x, 0, own, 3 * d_panels, qkv_ref)
        unpack(all_x, 3 * d_panels * own, own, d_panels, wo_ref)
        gain_ref[...] = all_x[pl.ds(4 * d_panels * own, gain_ref.shape[0]), :].astype(F32)


def combine(dest, gates, live, first_sum, shared_out, returned, x, piece, pack, parts, axis, count, own, shared_hidden, hidden):
    rows, width = first_sum.shape
    top = gates.shape[1]
    block = min(256, rows)
    steps = rows // block
    blocked = pl.BlockSpec((block, width), lambda i: (i, 0))
    slots = returned.shape[0]
    group = width // own
    columns = 2 * hidden // group
    gu_panels = 2 * shared_hidden // LANES
    x_piece = (x.shape[0] // count, LANES)
    outs = [
        (parts, width, columns), (parts, hidden // group, width), (own, 3 * width), (own, width), (own, 2 * shared_hidden),
        (shared_hidden // group, width), (8, LANES),
    ]
    sems = pltpu.SemaphoreType.DMA((2, count))
    return call(
        functools.partial(combine_kernel, axis, count, own, gu_panels, parts), (steps,),
        [pl.BlockSpec((block, dest.shape[1]), lambda i: (i, 0)), pl.BlockSpec((block, top), lambda i: (i, 0)), pl.BlockSpec((block, 1), lambda i: (i, 0)), blocked, blocked]
        + [whole(returned.shape), whole(x.shape), whole(piece.shape), whole(pack.shape)],
        [blocked, pl.BlockSpec((parts, width // steps, columns), lambda i: (0, i, 0))] + [whole(shape) for shape in outs[1:]],
        [shape_of((rows, width), BF16)] + [shape_of(shape, F32) for shape in outs],
        scratch=[pltpu.VMEM((2, 2, count) + x_piece, BF16), pltpu.VMEM(x_piece, F32), pltpu.VMEM(x.shape, BF16)] + [sems] * 4,
        flops=4 * rows * slots * width, moved=10 * rows * width + 2 * slots * width, collective_id=2,
    )(dest, gates, live, first_sum, shared_out, returned, x, piece, pack)


def slot_numbers(block, slots, part):
    return lax.broadcasted_iota(jnp.int32, (block, slots), 1) + part * slots


def gathered(top, dest_ref, y_ref, part):
    block = dest_ref.shape[0]
    dest = dest_ref[:, top : 2 * top]
    slot = slot_numbers(block, y_ref.shape[0], part)
    hit = functools.reduce(jnp.logical_or, [slot == dest[:, k : k + 1] for k in range(top)])
    return dot_nn(jnp.where(hit, 1.0, 0.0).astype(BF16), y_ref[...])


class Exchange:
    def __init__(self, axis, count, sent_ref, kept_ref, own_sem, send_sem, recv_sem):
        self.axis, self.count = axis, count
        me = lax.axis_index(axis)
        self.peers = [lax.rem(me + ahead, count) for ahead in range(1, count)]
        self.me, self.sent_ref, self.kept_ref = me, sent_ref, kept_ref
        self.own_sem, self.send_sem, self.recv_sem = own_sem, send_sem, recv_sem

    def copies(self):
        out = [pltpu.make_async_copy(self.sent_ref.at[self.me], self.kept_ref.at[self.me], self.own_sem)]
        for index, peer in enumerate(self.peers):
            out.append(
                pltpu.make_async_remote_copy(
                    src_ref=self.sent_ref.at[peer], dst_ref=self.kept_ref.at[self.me],
                    send_sem=self.send_sem.at[index], recv_sem=self.recv_sem.at[index],
                    device_id={self.axis: peer}, device_id_type=pl.DeviceIdType.MESH,
                )
            )
        return out

    def start(self):
        barrier = pltpu.get_barrier_semaphore()
        for peer in self.peers:
            pl.semaphore_signal(barrier, inc=1, device_id={self.axis: peer}, device_id_type=pl.DeviceIdType.MESH)
        pl.semaphore_wait(barrier, self.count - 1)
        for copy in self.copies():
            copy.start()

    def wait(self):
        for copy in self.copies():
            copy.wait()

    @staticmethod
    def scratch(count):
        sems = pltpu.SemaphoreType.DMA((count - 1,))
        return [pltpu.SemaphoreType.DMA, sems, sems]


def add_part_kernel(part, top, axis, count, dest_ref, base_ref, y_ref, sent_ref, out_ref, kept_ref, *sems):
    exchange = Exchange(axis, count, sent_ref, kept_ref, *sems)

    @pl.when(pl.program_id(0) == 0)
    def _():
        exchange.start()

    out_ref[...] = base_ref[...] + gathered(top, dest_ref, y_ref, part)

    @pl.when(pl.program_id(0) == pl.num_programs(0) - 1)
    def _():
        exchange.wait()


def add_part(top, dest, base, rows_of, part, sent, axis, count, collective_id):
    rows, width = base.shape
    block = min(256, rows)
    blocked = pl.BlockSpec((block, width), lambda i: (i, 0))
    hbm = pl.BlockSpec(memory_space=pl.ANY)
    sent = sent.reshape(count, -1, width)
    out, kept = call(
        functools.partial(add_part_kernel, part, top, axis, count), (rows // block,),
        [pl.BlockSpec((block, dest.shape[1]), lambda i: (i, 0)), blocked, whole(rows_of.shape), hbm],
        [blocked, hbm], [shape_of((rows, width), F32), shape_of(sent.shape, BF16)],
        scratch=Exchange.scratch(count),
        flops=2 * rows * rows_of.shape[0] * width, moved=8 * rows * width, collective_id=collective_id,
    )(dest, base, rows_of, sent)
    return out, kept.reshape(-1, width)


def norm_two_back_kernel(part, top, dest_ref, live_ref, cot_ref, sum_ref, base_ref, gain_ref, weight_ref, y_ref,
                         first_ref, attn_ref, mixed_ref, gain_grad_ref):
    grad_normed = base_ref[...] + gathered(top, dest_ref, y_ref, part)
    first_sum = sum_ref[...]
    scale = lax.rsqrt(jnp.mean(first_sum * first_sum, axis=1, keepdims=True) + EPSILON)
    weighted = grad_normed * gain_ref[...]
    inner = jnp.mean(first_sum * weighted, axis=1, keepdims=True)
    grad_first = (
        cot_ref[...].astype(F32) * live_ref[...] + scale * weighted - first_sum * (scale * scale * scale * inner)
    )
    first_ref[...] = grad_first
    grad_attn = grad_first.astype(BF16)
    attn_ref[...] = grad_attn
    mixed_ref[...] = dot_nt(grad_attn, weight_ref[...]).astype(BF16)

    @pl.when(pl.program_id(0) == 0)
    def _():
        gain_grad_ref[...] = jnp.zeros_like(gain_grad_ref)

    gain_grad_ref[...] += jnp.sum(grad_normed * first_sum * scale, axis=0, keepdims=True)


def norm_two_back(top, dest, live, cotangent, first_sum, base, gain, weights, rows_of, part):
    rows, width = first_sum.shape
    block = min(256, rows)
    blocked = pl.BlockSpec((block, width), lambda i: (i, 0))
    return call(
        functools.partial(norm_two_back_kernel, part, top), (rows // block,),
        [pl.BlockSpec((block, dest.shape[1]), lambda i: (i, 0)), pl.BlockSpec((block, 1), lambda i: (i, 0)), blocked, blocked,
         blocked, whole((1, width)), square(width, 3), whole(rows_of.shape)],
        [blocked, blocked, blocked, pl.BlockSpec((1, width), lambda i: (0, 0))],
        [shape_of((rows, width), F32), shape_of((rows, width), BF16), shape_of((rows, width), BF16),
         shape_of((1, width), F32)],
        flops=2 * rows * (rows_of.shape[0] + width) * width, moved=18 * rows * width,
    )(dest, live, cotangent, first_sum, base, gain, weights, rows_of)


def line_copy(axis, ahead, source, target, send_sem, recv_sem):
    return pltpu.make_async_remote_copy(
        src_ref=source, dst_ref=target, send_sem=send_sem, recv_sem=recv_sem,
        device_id={axis: lax.axis_index(axis) + ahead}, device_id_type=pl.DeviceIdType.MESH,
    )


class LineSum:
    def __init__(self, axis, count, x_ref, buffers, send_sem, recv_sem):
        self.axis, self.count, self.x_ref, self.buffers = axis, count, x_ref, buffers
        self.send_sem, self.recv_sem = send_sem, recv_sem
        self.rows = buffers.shape[3]

    def own(self, piece):
        return self.x_ref[pl.ds(pl.multiple_of(piece * self.rows, 16), self.rows), :].astype(F32)

    def copy(self, way, piece):
        return line_copy(
            self.axis, 1 - 2 * way, self.buffers.at[way, 1, piece], self.buffers.at[way, 0, piece],
            self.send_sem.at[way, piece], self.recv_sem.at[way, piece],
        )

    def each(self, body):
        me = lax.axis_index(self.axis)
        for k in range(self.count - 1):
            for way, piece in ((0, self.count - 1 - k), (1, k)):
                before = me > 0 if way == 0 else me < self.count - 1
                sends = me < piece if way == 0 else me > piece
                body(way, piece, before, sends)

    def start(self):
        def body(way, piece, before, sends):
            @pl.when(sends & jnp.logical_not(before))
            def _():
                self.buffers[way, 1, piece] = self.own(piece).astype(BF16)
                self.copy(way, piece).start()

        self.each(body)

    def relay(self):
        def body(way, piece, before, sends):
            @pl.when(sends & before)
            def _():
                self.copy(way, piece).wait_recv()
                self.buffers[way, 1, piece] = (self.own(piece) + self.buffers[way, 0, piece].astype(F32)).astype(BF16)
                self.copy(way, piece).start()

        self.each(body)

    def finish(self, total_ref):
        me = lax.axis_index(self.axis)
        total_ref[...] = self.own(me)
        for way, before in ((0, me > 0), (1, me < self.count - 1)):

            @pl.when(before)
            def _():
                self.copy(way, me).wait_recv()
                total_ref[...] += self.buffers[way, 0, me].astype(F32)

        def body(way, piece, before, sends):
            @pl.when(sends)
            def _():
                self.copy(way, piece).wait_send()

        self.each(body)


class LineGather:
    def __init__(self, axis, count, out_ref, send_sem, recv_sem):
        self.axis, self.count, self.out_ref = axis, count, out_ref
        self.send_sem, self.recv_sem = send_sem, recv_sem
        self.rows = out_ref.shape[0] // count

    def place(self, piece):
        return self.out_ref.at[pl.ds(pl.multiple_of(piece * self.rows, 16), self.rows), :]

    def copy(self, way, piece):
        return line_copy(
            self.axis, 1 - 2 * way, self.place(piece), self.place(piece),
            self.send_sem.at[way, piece], self.recv_sem.at[way, piece],
        )

    def start(self, value):
        me = lax.axis_index(self.axis)
        self.place(me)[...] = value
        for way, more in ((0, me < self.count - 1), (1, me > 0)):

            @pl.when(more)
            def _():
                self.copy(way, me).start()

    def relay(self, k):
        me = lax.axis_index(self.axis)
        for way, piece, there, more in (
            (0, me - k, me >= k, me < self.count - 1),
            (1, me + k, me + k < self.count, me > 0),
        ):

            @pl.when(there)
            def _():
                self.copy(way, piece).wait_recv()

            @pl.when(there & more)
            def _():
                self.copy(way, piece).start()

    def finish(self):
        me = lax.axis_index(self.axis)
        for k in range(self.count):
            for way, piece, sent in (
                (0, me - k, (me >= k) & (me < self.count - 1)),
                (1, me + k, (me + k < self.count) & (me > 0)),
            ):

                @pl.when(sent)
                def _():
                    self.copy(way, piece).wait_send()


def greet_neighbours(barrier, axis, count):
    me = lax.axis_index(axis)
    for ahead, there in ((1, me < count - 1), (-1, me > 0)):

        @pl.when(there)
        def _():
            pl.semaphore_signal(barrier, inc=1, device_id={axis: me + ahead}, device_id_type=pl.DeviceIdType.MESH)

    return (me < count - 1).astype(jnp.int32) + (me > 0).astype(jnp.int32)


def settle_kernel(sizes, gq_ref, gk_ref, gv_ref, wq_ref, wk_ref, wv_ref, tokens_ref, first_ref, gain_ref, pack_ref,
                  x_ref, out_ref, share_ref, all_ref, own, landed, chosen, arrived, sem, pair_send, pair_recv, send_sem,
                  recv_sem, x_buffers, x_total, x_all, x_send, x_recv, g_send, g_recv):
    dp_size, shard_size, count = sizes
    spread = shard_size // 2
    halves = dp_size * spread
    dp, shard = lax.axis_index("dp"), lax.axis_index("shard")
    side = shard % 2
    place = dp * spread + shard // 2
    step = pl.program_id(0)
    last = pl.num_programs(0) - 1

    def target(piece, bit):
        return {"dp": piece // spread, "shard": (piece % spread) * 2 + bit}

    line = LineSum("expert", count, x_ref, x_buffers, x_send, x_recv)
    gather = LineGather("expert", count, x_all, g_send, g_recv)

    def pair_copy():
        return pltpu.make_async_remote_copy(
            src_ref=pack_ref.at[:, 1 - side], dst_ref=landed, send_sem=pair_send, recv_sem=pair_recv,
            device_id=target(place, 1 - side), device_id_type=pl.DeviceIdType.MESH,
        )

    def own_copy():
        return pltpu.make_async_copy(pack_ref.at[:, side], own, sem)

    def send(index):
        return pltpu.make_async_remote_copy(
            src_ref=chosen.at[index], dst_ref=arrived.at[index], send_sem=send_sem.at[index], recv_sem=recv_sem.at[index],
            device_id=target(lax.rem(place + index + 1, halves), side), device_id_type=pl.DeviceIdType.MESH,
        )

    @pl.when(step == 0)
    def _():
        barrier = pltpu.get_barrier_semaphore()
        pl.semaphore_signal(barrier, inc=1, device_id=target(place, 1 - side), device_id_type=pl.DeviceIdType.MESH)
        for index in range(halves - 1):
            pl.semaphore_signal(
                barrier, inc=1, device_id=target(lax.rem(place + index + 1, halves), side),
                device_id_type=pl.DeviceIdType.MESH,
            )
        neighbours = greet_neighbours(barrier, "expert", count)
        pl.semaphore_wait(barrier, halves + neighbours)
        pair_copy().start()
        own_copy().start()
        line.start()

    @pl.when(step == 1)
    def _():
        own_copy().wait()
        pair_copy().wait()
        for index in range(halves - 1):
            piece = lax.rem(place + index + 1, halves)
            chosen[index] = (own[piece].astype(F32) + landed[piece].astype(F32)).astype(BF16)
            send(index).start()

    grad_normed = (
        dot_nt(gq_ref[...], wq_ref[...]) + dot_nt(gk_ref[...], wk_ref[...]) + dot_nt(gv_ref[...], wv_ref[...])
    )
    source = tokens_ref[...].astype(F32)
    scale = lax.rsqrt(jnp.mean(source * source, axis=1, keepdims=True) + EPSILON)
    weighted = grad_normed * gain_ref[...]
    inner = jnp.mean(source * weighted, axis=1, keepdims=True)
    out_ref[...] = first_ref[...] + scale * weighted - source * (scale * scale * scale * inner)

    @pl.when(step == last)
    def _():
        line.relay()
        line.finish(x_total)
        gather.start(x_total[...].astype(BF16))
        total = own[place].astype(F32) + landed[place].astype(F32)
        for index in range(halves - 1):
            send(index).wait()
            total = total + arrived[index].astype(F32)
        share_ref[...] = total.astype(BF16)
        for k in range(1, count):
            gather.relay(k)
        gather.finish()
        all_ref[...] = x_all[...]


def settle(grads, w_qkv, tokens, grad_first, gain, pack, x, sizes):
    rows, width = tokens.shape
    block = min(256, rows)
    blocked = pl.BlockSpec((block, width), lambda i: (i, 0))
    halves, count = sizes[0] * sizes[1] // 2, pack.shape[1]
    piece = (count, LANES)
    x_piece = (x.shape[0] // sizes[2], LANES)
    return call(
        functools.partial(settle_kernel, sizes), (rows // block,),
        [blocked] * 3 + [square(width, 0), square(width, 1), square(width, 2), blocked, blocked, whole((1, width)),
                         pl.BlockSpec(memory_space=pl.ANY), whole(x.shape)],
        [blocked, whole(piece), whole(x.shape)],
        [shape_of((rows, width), F32), shape_of(piece, BF16), shape_of(x.shape, BF16)],
        scratch=[pltpu.VMEM((halves,) + piece, BF16), pltpu.VMEM((halves,) + piece, BF16),
                 pltpu.VMEM((halves - 1,) + piece, BF16), pltpu.VMEM((halves - 1,) + piece, BF16),
                 pltpu.SemaphoreType.DMA, pltpu.SemaphoreType.DMA, pltpu.SemaphoreType.DMA,
                 pltpu.SemaphoreType.DMA((halves - 1,)), pltpu.SemaphoreType.DMA((halves - 1,)),
                 pltpu.VMEM((2, 2, sizes[2]) + x_piece, BF16), pltpu.VMEM(x_piece, F32), pltpu.VMEM(x.shape, BF16)]
        + [pltpu.SemaphoreType.DMA((2, sizes[2]))] * 4,
        flops=6 * rows * width * width, moved=22 * rows * width, collective_id=1,
    )(*grads, w_qkv, w_qkv, w_qkv, tokens, grad_first, gain, pack.reshape((halves, 2) + piece), x)


def copies_of(layout, block, width, step, stage_g, stage_u, stage_d, slot, packed_ref, sems):
    by_rows, owners, hidden, base = layout
    panels = block // LANES
    rows_down = hidden // owners
    out = []

    def add(source, target):
        out.append(pltpu.make_async_copy(source, target, sems.at[slot, len(out)]))

    if by_rows:
        rows = width // owners
        for half, stage in enumerate((stage_g, stage_u)):
            for p in range(panels):
                panel = half * (hidden // LANES) + step * panels + p
                add(
                    stage.at[slot, :, :, pl.ds(p * LANES, LANES)],
                    packed_ref.at[:, pl.ds(pl.multiple_of(base + panel * rows, 8), rows), :],
                )
        start = 2 * hidden // LANES * rows
    else:
        columns = 2 * hidden // owners
        for half, stage in enumerate((stage_g, stage_u)):
            for p in range(panels):
                column = half * hidden + step * block + p * LANES
                owner, panel = column // columns, (column % columns) // LANES
                add(
                    stage.at[slot, :, pl.ds(p * LANES, LANES)],
                    packed_ref.at[owner, pl.ds(pl.multiple_of(base + panel * width, 8), width), :],
                )
        start = columns // LANES * width
    for q in range(block // rows_down):
        owner = step * (block // rows_down) + q
        for c in range(width // LANES):
            add(
                stage_d.at[slot, pl.ds(q * rows_down, rows_down), pl.ds(c * LANES, LANES)],
                packed_ref.at[owner, pl.ds(base + start + c * rows_down, rows_down), :],
            )
    return out


def packed_rows(width, hidden, owners):
    return 3 * width * hidden // owners // LANES


def ffn_kernel(out_type, layout, block, axis, count, x_ref, gy_ref, wg_ref, wu_ref, wd_ref, sent_ref, *rest):
    y_ref, gx_ref, packed_ref, kept_ref, xt, y_acc, gx_acc, stage_g, stage_u, stage_d, sems, *exchange_sems = rest[-14:]
    exchange = Exchange(axis, count, sent_ref, kept_ref, *exchange_sems)
    step = pl.program_id(0)
    steps = layout[2] // block
    width = x_ref.shape[1]
    slot = step % 2
    copies = functools.partial(copies_of, layout, block, width)

    @pl.when(step == 0)
    def _():
        exchange.start()
        xt[...] = x_ref[...].T
        y_acc[...] = jnp.zeros_like(y_acc)
        gx_acc[...] = jnp.zeros_like(gx_acc)

    @pl.when(step >= 2)
    def _():
        for copy in copies(step - 2, stage_g, stage_u, stage_d, slot, packed_ref, sems):
            copy.wait()

    x, gy = x_ref[...], gy_ref[...].reshape(x_ref.shape)
    if layout[0]:
        wg, wu = wg_ref[...].reshape(width, block), wu_ref[...].reshape(width, block)
        rows = wd_ref.shape[1] // (width // block)
        wd = jnp.concatenate(
            [wd_ref[:, pl.ds(c * rows, rows), :].reshape(block, block) for c in range(width // block)], axis=1
        )
    else:
        wg, wu, wd = wg_ref[...], wu_ref[...], wd_ref[...]
    gate, up = dot_nn(x, wg), dot_nn(x, wu)
    grad_hidden = dot_nt(gy, wd)
    sigmoid = jax.nn.sigmoid(gate)
    value = gate * sigmoid
    hidden = (value * up).astype(BF16)
    grad_up = (grad_hidden * value).astype(BF16)
    grad_gate = (grad_hidden * up * (sigmoid * (1.0 + gate * (1.0 - sigmoid)))).astype(BF16)
    y_acc[...] += dot_nn(hidden, wd)
    gx_acc[...] += dot_nt(grad_gate, wg) + dot_nt(grad_up, wu)
    stage_g[slot] = dot_nn(xt[...], grad_gate).astype(BF16).reshape(stage_g.shape[1:])
    stage_u[slot] = dot_nn(xt[...], grad_up).astype(BF16).reshape(stage_u.shape[1:])
    stage_d[slot] = dot_tn(hidden, gy).astype(BF16)
    for copy in copies(step, stage_g, stage_u, stage_d, slot, packed_ref, sems):
        copy.start()

    @pl.when(step == steps - 1)
    def _():
        exchange.wait()
        y_ref[...] = y_acc[...].astype(out_type).reshape(y_ref.shape)
        gx_ref[...] = gx_acc[...].astype(out_type)
        for back in (1, 0):
            if steps > back:
                for copy in copies(steps - 1 - back, stage_g, stage_u, stage_d, (steps - 1 - back) % 2, packed_ref, sems):
                    copy.wait()


BLOCK = 256


def ffn_both(x, gy, w_gu, w_down, hidden, expert, owners, out_type, sent, axis, count, collective_id, parts=1, held=()):
    rows, width = x.shape
    block = BLOCK
    steps = hidden // block
    by_rows = expert is None
    if by_rows:
        own, own_down, panels = width // owners, hidden // owners, width // block
        ahead = 2 * steps * own // (panels * own_down)
        gate = pl.BlockSpec((owners, own, block), lambda f: (0, f, 0))
        up = pl.BlockSpec((owners, own, block), lambda f: (0, steps + f, 0))
        down = pl.BlockSpec((block // own_down, panels * own_down, block), lambda f: (f, ahead, 0))
        stage = (2, owners, own, block)
    else:
        gate = pl.BlockSpec((None, width, block), lambda f: (expert, 0, f))
        up = pl.BlockSpec((None, width, block), lambda f: (expert, 0, steps + f))
        down = pl.BlockSpec((None, block, width), lambda f: (expert, f, 0))
        stage = (2, width, block)
    if by_rows:
        grads = whole((rows, width))
        y_block, y_shape = whole((rows, width)), (rows, width)
    else:
        y_shape = (gy.shape[0], parts * (rows // gy.shape[0]), width)
        y_block = pl.BlockSpec(
            (gy.shape[0], rows // gy.shape[0], width), lambda f: (0, expert, 0), pipeline_mode=pl.Buffered(1)
        )
        grads = pl.BlockSpec(
            (gy.shape[0], rows // gy.shape[0], width), lambda f: (0, expert, 0), pipeline_mode=pl.Buffered(1)
        )
    out_rows = whole((rows, width))
    pack_rows = packed_rows(width, hidden, owners)
    layout = (by_rows, owners, hidden, (expert or 0) * pack_rows)
    hbm = pl.BlockSpec(memory_space=pl.ANY)
    sent = sent.reshape(count, -1, width)
    copies = 2 * (block // LANES) + block // (hidden // owners) * (width // LANES)
    y, gx, pack, kept = call(
        functools.partial(ffn_kernel, out_type, layout, block, axis, count), (steps,),
        [whole((rows, width)), grads, gate, up, down, hbm] + [hbm] * len(held),
        [y_block, out_rows, hbm, hbm],
        [shape_of(y_shape, out_type), shape_of((rows, width), out_type),
         shape_of((owners, parts * pack_rows, LANES), BF16), shape_of(sent.shape, BF16)],
        scratch=[pltpu.VMEM((width, rows), BF16), pltpu.VMEM((rows, width), F32), pltpu.VMEM((rows, width), F32),
                 pltpu.VMEM(stage, BF16), pltpu.VMEM(stage, BF16), pltpu.VMEM((2, block, width), BF16),
                 pltpu.SemaphoreType.DMA((2, copies))] + Exchange.scratch(count),
        flops=18 * rows * width * hidden, moved=12 * width * hidden + 16 * rows * width, trans=rows * hidden,
        aliases={6: 0, 7: 2} if held else None, collective_id=collective_id,
    )(x, gy, w_gu, w_gu, w_down, sent, *held)
    return y, gx, pack, kept.reshape(-1, width)


def to_panels(array):
    rows, columns = array.shape
    return jnp.transpose(array.reshape(rows, columns // BLOCK, BLOCK), (1, 0, 2)).reshape(-1, BLOCK)


def attention_weights_kernel(per, normed_ref, mixed_ref, gq_ref, gk_ref, gv_ref, ga_ref, gains_ref, out_ref, xt):
    step = pl.program_id(0)
    owners, rows = out_ref.shape[0], out_ref.shape[1] // (out_ref.shape[1] // (normed_ref.shape[1] // out_ref.shape[0]))
    panels = out_ref.shape[1] // rows

    @pl.when(step == 0)
    def _():
        xt[...] = normed_ref[...].T

    @pl.when(step == 3 * per)
    def _():
        xt[...] = mixed_ref[...].T

    for index, grad_ref in enumerate((gq_ref, gk_ref, gv_ref, ga_ref)):

        @pl.when((step >= index * per) & (step < (index + 1) * per))
        def _():
            product = dot_nn(xt[...], grad_ref[...]).astype(BF16)
            for p in range(panels):
                out_ref[:, pl.ds(p * rows, rows), :] = product[:, p * LANES : (p + 1) * LANES].reshape(owners, rows, LANES)

    @pl.when(step >= 4 * per)
    def _():
        out_ref[...] = jnp.zeros_like(out_ref)

    @pl.when(step == 4 * per)
    def _():
        out_ref[:, pl.ds(0, gains_ref.shape[1]), :] = gains_ref[...]


def attention_weights(normed, mixed, grads, grad_attn, gains, owners, pieces):
    tokens, width = normed.shape
    rows = width // owners
    block = BLOCK
    panels, per = block // LANES, width // block
    steps = 4 * per + 1
    while steps * panels * rows % (16 * pieces):
        steps += 1

    def columns(index):
        return pl.BlockSpec((tokens, block), lambda i: (0, jnp.clip(i - index * per, 0, per - 1)))

    return call(
        functools.partial(attention_weights_kernel, per), (steps,),
        [whole((tokens, width)), whole((tokens, width))] + [columns(index) for index in range(4)] + [whole(gains.shape)],
        pl.BlockSpec((owners, panels * rows, LANES), lambda i: (0, i, 0)),
        shape_of((owners, steps * panels * rows, LANES), BF16),
        scratch=[pltpu.VMEM((width, tokens), BF16)],
        flops=8 * tokens * width * width, moved=16 * tokens * width,
    )(normed, mixed, *grads, grad_attn, gains)


GROUP = ("dp", "shard")


def local(
    tokens,
    lengths,
    routes,
    route_gates,
    cotangent,
    norm_gains,
    w_qkv,
    w_out,
    w_shared_gu,
    w_shared_down,
    w_expert_gu,
    w_expert_down,
):
    tok_count, width = tokens.shape
    seq_count = lengths.shape[0]
    length = tok_count // seq_count
    local_experts = w_expert_gu.shape[0]
    owners = lax.axis_size("expert")
    experts = local_experts * owners
    top = routes.shape[1]
    capacity = tok_count * top * 9 // (8 * experts)
    head_dim = width // HEADS
    hidden = w_expert_down.shape[1]

    gains = lax.all_gather(norm_gains, GROUP, axis=1, tiled=True).astype(F32)
    attention_weight = lax.all_gather(jnp.concatenate([w_qkv, w_out], axis=1), GROUP, axis=0, tiled=True)
    shared_weight = lax.all_gather(
        jnp.concatenate([to_panels(w_shared_gu), to_panels(w_shared_down)], axis=0)[None], GROUP, axis=0, tiled=True
    )
    gain_one, gain_two = gains[0:1], gains[1:2]

    live_bool = lax.iota(jnp.int32, tok_count) % length < jnp.repeat(lengths, length)
    live = live_bool.astype(F32)[:, None]
    live_row = live_bool.astype(jnp.int32)[None, :]

    group = lax.axis_size("dp") * lax.axis_size("shard")
    shared_hidden = w_shared_down.shape[0] * group

    table_t, table = slots_of(routes.T, live_row, experts, local_experts, capacity)
    gates_t = route_gates.T
    grad_b = jnp.where(live_bool[:, None], cotangent, 0).astype(BF16)

    def exchange(rows):
        return lax.all_to_all(
            rows.reshape(owners, -1, width), "expert", split_axis=0, concat_axis=0, tiled=True
        ).reshape(rows.shape)

    send_grad = dispatch(table_t, gates_t, grad_b, experts, capacity, True, 0, 0)
    received_grad = exchange(send_grad).reshape(owners, local_experts * capacity, width)

    cosine, sine = rotary_tables(length, head_dim)
    normed_one = norm_one(tokens, gain_one)
    queries, keys, values, mixed, lse = attend_forward(normed_one, attention_weight, cosine, sine, length, head_dim)
    first_sum, normed_two = norm_two(mixed, tokens, attention_weight, gain_two)

    send_rows = []
    for j in range(local_experts):
        send_rows.append(dispatch(table_t, gates_t, normed_two, owners, capacity, False, j * owners, top))
    shared_out, grad_shared, shared_pack, received = ffn_both(
        normed_two, grad_b, shared_weight, shared_weight, shared_hidden, None, group, F32,
        send_rows[0], "expert", owners, 3,
    )
    waiting = send_rows[1:]
    back_rows, base, held = [], grad_shared, ()
    for j in range(local_experts):
        y, gx, pack, arrived = ffn_both(
            received, received_grad, w_expert_gu, w_expert_down, hidden, j, group, BF16,
            waiting.pop(0), "expert", owners, 4 + j, local_experts, held,
        )
        held = (y, pack)
        waiting.append(gx)
        if j < local_experts - 1:
            received = arrived
        else:
            back_rows.append(arrived)
    for j, sent in enumerate(waiting):
        base, arrived = add_part(
            top, table, base, back_rows[j], j, sent, "expert", owners, 4 + local_experts + j
        )
        back_rows.append(arrived)
    y, base = lax.optimization_barrier((y, base))
    grad_first, grad_attn, grad_mixed, grad_gain_two = norm_two_back(
        top, table, live, cotangent, first_sum, base, gain_two, attention_weight, back_rows[-1], local_experts - 1
    )

    grads = attend_backward(queries, keys, values, mixed, grad_mixed, lse, cosine, sine, length, head_dim)
    own = width // group
    grad_gains = grad_gain_two.reshape(group, 1, own)
    grad_gains = jnp.pad(grad_gains, ((0, 0), (0, 15), (0, LANES - own))).astype(BF16)
    attention_pack = attention_weights(normed_one, mixed, grads, grad_attn, grad_gains, group, owners)

    def spread(pack):
        return lax.psum_scatter(pack, GROUP, scatter_dimension=0, tiled=True)[0]

    shared_share = spread(shared_pack)
    expert_share = spread(pack)
    input_grad, attention_share, shared_share = settle(
        grads, attention_weight, tokens, grad_first, gain_one, attention_pack, shared_share,
        (lax.axis_size("dp"), lax.axis_size("shard"), owners),
    )
    returned = exchange(y)
    layer_out, expert_gu, expert_down, qkv_grad, out_grad, shared_gu, shared_down, gain_rows = combine(
        table, route_gates, live, first_sum, shared_out, returned.reshape(-1, width), attention_share, shared_share,
        expert_share, local_experts, "expert", owners, own, shared_hidden, hidden,
    )
    grad_gain_one = jnp.sum(w_qkv.astype(F32) * qkv_grad, axis=1) / norm_gains[0].astype(F32)
    grad_gains = jnp.stack([grad_gain_one, gain_rows[0, :own]])
    return layer_out, input_grad, grad_gains, qkv_grad, out_grad, shared_gu, shared_down, expert_gu, expert_down


def solution(mesh):
    rows = P(("dp", "expert", "shard"), None)
    split = P(GROUP, None)
    in_specs = (
        rows,
        P(("dp", "expert", "shard")),
        rows,
        rows,
        rows,
        P(None, GROUP),
        split,
        split,
        split,
        split,
        P("expert", None, None),
        P("expert", None, None),
    )
    out_specs = (
        rows,
        rows,
        P(None, GROUP),
        split,
        split,
        split,
        split,
        P("expert", None, GROUP),
        P("expert", GROUP, None),
    )

    return jax.shard_map(local, mesh=mesh, in_specs=in_specs, out_specs=out_specs, check_vma=False)
```

```python
import functools
import math

import jax
import jax.numpy as jnp
from jax import lax
from jax.experimental import pallas as pl
from jax.experimental.pallas import tpu as pltpu
from jax.sharding import PartitionSpec as P


HEADS = 12
LANES = 128
EPSILON = 1e-05
VMEM_BYTES = 60 * 1024 * 1024
BF16 = jnp.bfloat16
F32 = jnp.float32


def call(kernel, grid, in_specs, out_specs, out_shape, scratch=(), flops=0, moved=0, trans=0, collective_id=None, aliases=None):
    return pl.pallas_call(
        kernel,
        grid_spec=pltpu.PrefetchScalarGridSpec(
            num_scalar_prefetch=0,
            grid=grid,
            in_specs=in_specs,
            out_specs=out_specs,
            scratch_shapes=list(scratch),
        ),
        out_shape=out_shape,
        input_output_aliases=aliases or {},
        compiler_params=pltpu.CompilerParams(
            dimension_semantics=("arbitrary",) * len(grid), vmem_limit_bytes=VMEM_BYTES, collective_id=collective_id,
            has_side_effects=collective_id is not None,
        ),
        cost_estimate=pl.CostEstimate(flops=flops, bytes_accessed=moved, transcendentals=trans),
    )


def shape_of(shape, dtype):
    return jax.ShapeDtypeStruct(shape, dtype)


def whole(shape):
    return pl.BlockSpec(shape, lambda *_: (0,) * len(shape), pipeline_mode=pl.Buffered(1))


def dot_nn(left, right):
    return lax.dot_general(left, right, (((1,), (0,)), ((), ())), preferred_element_type=F32)


def dot_nt(left, right):
    return lax.dot_general(left, right, (((1,), (1,)), ((), ())), preferred_element_type=F32)


def dot_tn(left, right):
    return lax.dot_general(left, right, (((0,), (0,)), ((), ())), preferred_element_type=F32)


def rotary_tables(length, head_dim):
    half_dim = head_dim // 2
    position = lax.iota(F32, length)[:, None]
    frequency = jnp.exp(lax.iota(F32, half_dim) * (-2.0 * math.log(10000.0) / head_dim))
    angle_table = position * frequency[None, :]
    cosine, sine = jnp.cos(angle_table), jnp.sin(angle_table)
    repeats = LANES // head_dim
    return (
        jnp.tile(jnp.concatenate([cosine, cosine], axis=1), (1, repeats)),
        jnp.tile(jnp.concatenate([-sine, sine], axis=1), (1, repeats)),
    )


def turn(values, cosine, signed_sine, head_dim):
    lane = lax.broadcasted_iota(jnp.int32, values.shape, 1)
    half = head_dim // 2
    other = jnp.where(
        lane % head_dim < half,
        pltpu.roll(values, LANES - half, 1),
        pltpu.roll(values, half, 1),
    )
    return values * cosine + other * signed_sine


def attend_forward_kernel(
    head_dim, block, x_ref, wq_ref, wk_ref, wv_ref, cos_ref, sin_ref, q_ref, k_ref, v_ref, o_ref, lse_ref, lse_tile
):
    length = x_ref.shape[0]
    heads = LANES // head_dim
    x = x_ref[...]
    cosine, sine = cos_ref[...], sin_ref[...]
    scale = 1.0 / math.sqrt(head_dim)
    q_ref[...] = (turn(dot_nn(x, wq_ref[...]), cosine, sine, head_dim) * scale).astype(BF16)
    k_ref[...] = turn(dot_nn(x, wk_ref[...]), cosine, sine, head_dim).astype(BF16)
    v_ref[...] = dot_nn(x, wv_ref[...]).astype(BF16)
    lane = lax.broadcasted_iota(jnp.int32, (1, LANES), 1)
    own_lane = lax.broadcasted_iota(jnp.int32, (block, LANES), 1) // head_dim
    below = lax.broadcasted_iota(jnp.int32, (block, block), 0) >= lax.broadcasted_iota(
        jnp.int32, (block, block), 1
    )
    for first in range(0, length, block):
        rows = pl.ds(first, block)
        mixed = None
        logs = None
        for head in range(heads):
            select = (lane // head_dim == head).astype(F32).astype(BF16)
            queries = q_ref[rows, :] * select
            near = jnp.where(below, dot_nt(queries, k_ref[rows, :]), -1e30)
            peak = jnp.max(near, axis=1, keepdims=True)
            if first:
                far = dot_nt(queries, k_ref[pl.ds(0, first), :])
                peak = jnp.maximum(peak, jnp.max(far, axis=1, keepdims=True))
            near = jnp.exp(near - peak)
            total = jnp.sum(near, axis=1, keepdims=True)
            part = dot_nn(near.astype(BF16), v_ref[rows, :])
            if first:
                far = jnp.exp(far - peak)
                total = total + jnp.sum(far, axis=1, keepdims=True)
                part = part + dot_nn(far.astype(BF16), v_ref[pl.ds(0, first), :])
            part = part * (1.0 / total)
            log_total = jnp.broadcast_to(peak + jnp.log(total), (block, LANES))
            mixed = part if head == 0 else jnp.where(own_lane == head, part, mixed)
            logs = log_total if head == 0 else jnp.where(own_lane == head, log_total, logs)
        o_ref[rows, :] = mixed.astype(BF16)
        lse_tile[rows, :] = logs
    turned = lse_tile[...].T
    for head in range(heads):
        lse_ref[pl.ds(head * 8, 8), :] = turned[head * head_dim : head * head_dim + 8, :]


def attend_forward(normed, w_qkv, cosine, sine, length, head_dim):
    tokens, width = normed.shape
    seqs, pairs, heads = tokens // length, width // LANES, LANES // head_dim
    block = min(256, length)
    rows = pl.BlockSpec((length, LANES), lambda s, p: (s, p))

    def weight(part):
        return pl.BlockSpec((width, LANES), lambda s, p: (0, part * pairs + p))

    table = whole((length, LANES))
    return call(
        functools.partial(attend_forward_kernel, head_dim, block),
        (seqs, pairs),
        [pl.BlockSpec((length, width), lambda s, p: (s, 0)), weight(0), weight(1), weight(2), table, table],
        [rows, rows, rows, rows, pl.BlockSpec((8 * heads, length), lambda s, p: (s * pairs + p, 0))],
        [shape_of((tokens, width), BF16)] * 4 + [shape_of((seqs * pairs * 8 * heads, length), F32)],
        scratch=[pltpu.VMEM((length, LANES), F32)],
        flops=6 * tokens * width * width + 4 * tokens * length * width,
        moved=16 * tokens * width,
        trans=tokens * length * width // head_dim // 2,
    )(normed, w_qkv, w_qkv, w_qkv, cosine, sine)


def attend_backward_kernel(
    head_dim, block, q_ref, k_ref, v_ref, o_ref, g_ref, lse_ref, cos_ref, sin_ref, gq_ref, gk_ref, gv_ref, gq_acc
):
    length = q_ref.shape[0]
    heads = LANES // head_dim
    scale = 1.0 / math.sqrt(head_dim)
    product = (g_ref[...].astype(F32) * o_ref[...].astype(F32)).T
    inner = [
        jnp.sum(product[head * head_dim : (head + 1) * head_dim, :], axis=0, keepdims=True)
        for head in range(heads)
    ]
    gq_acc[...] = jnp.zeros_like(gq_acc)
    lane = lax.broadcasted_iota(jnp.int32, (1, LANES), 1)
    own_lane = lax.broadcasted_iota(jnp.int32, (block, LANES), 1) // head_dim
    above = lax.broadcasted_iota(jnp.int32, (block, block), 1) >= lax.broadcasted_iota(
        jnp.int32, (block, block), 0
    )
    for first in range(0, length, block):
        rows = pl.ds(first, block)
        keys_grad = None
        values_grad = None
        for head in range(heads):
            select = (lane // head_dim == head).astype(F32).astype(BF16)
            keys = k_ref[rows, :] * select
            values = v_ref[rows, :] * select
            log_total = lse_ref[pl.ds(head * 8, 1), :]
            pieces = [(first, block, True)]
            if first + block < length:
                pieces.append((first + block, length - first - block, False))
            keys_part = None
            values_part = None
            for start, count, diagonal in pieces:
                span = pl.ds(start, count)
                queries, grads = q_ref[span, :], g_ref[span, :]
                scores = dot_nt(keys, queries)
                probs = jnp.exp(scores - log_total[:, start : start + count])
                if diagonal:
                    probs = jnp.where(above, probs, 0.0)
                grad_probs = dot_nt(values, grads)
                grad_scores = (probs * (grad_probs - inner[head][:, start : start + count])).astype(BF16)
                piece_values = dot_nn(probs.astype(BF16), grads)
                piece_keys = dot_nn(grad_scores, queries)
                values_part = piece_values if values_part is None else values_part + piece_values
                keys_part = piece_keys if keys_part is None else keys_part + piece_keys
                gq_acc[span, :] += dot_tn(grad_scores, keys)
            keys_grad = keys_part if head == 0 else jnp.where(own_lane == head, keys_part, keys_grad)
            values_grad = values_part if head == 0 else jnp.where(own_lane == head, values_part, values_grad)
        gk_ref[rows, :] = turn(keys_grad, cos_ref[rows, :], -sin_ref[rows, :], head_dim).astype(BF16)
        gv_ref[rows, :] = values_grad.astype(BF16)
    gq_ref[...] = turn(gq_acc[...] * scale, cos_ref[...], -sin_ref[...], head_dim).astype(BF16)


def attend_backward(queries, keys, values, mixed, grad_mixed, lse, cosine, sine, length, head_dim):
    tokens, width = queries.shape
    seqs, pairs, heads = tokens // length, width // LANES, LANES // head_dim
    block = min(256, length)
    rows = pl.BlockSpec((length, LANES), lambda s, p: (s, p))
    table = whole((length, LANES))
    return call(
        functools.partial(attend_backward_kernel, head_dim, block),
        (seqs, pairs),
        [rows] * 5 + [pl.BlockSpec((8 * heads, length), lambda s, p: (s * pairs + p, 0)), table, table],
        [rows] * 3,
        [shape_of((tokens, width), BF16)] * 3,
        scratch=[pltpu.VMEM((length, LANES), F32)],
        flops=10 * tokens * length * width,
        moved=16 * tokens * width,
        trans=tokens * length * width // head_dim // 2,
    )(queries, keys, values, mixed, grad_mixed, lse, cosine, sine)


def square(width, part):
    return pl.BlockSpec((width, width), lambda i: (0, part), pipeline_mode=pl.Buffered(1))


def norm_one_kernel(x_ref, gain_ref, out_ref):
    x = x_ref[...].astype(F32)
    scale = lax.rsqrt(jnp.mean(x * x, axis=1, keepdims=True) + EPSILON)
    out_ref[...] = (x * scale * gain_ref[...]).astype(BF16)


def norm_one(tokens, gain):
    rows, width = tokens.shape
    block = min(256, rows)
    blocked = pl.BlockSpec((block, width), lambda i: (i, 0))
    return call(
        norm_one_kernel, (rows // block,), [blocked, whole((1, width))], blocked, shape_of((rows, width), BF16),
        flops=5 * rows * width, moved=4 * rows * width,
    )(tokens, gain)


def norm_two_kernel(mixed_ref, tokens_ref, weight_ref, gain_ref, sum_ref, normed_ref):
    first_sum = tokens_ref[...].astype(F32) + dot_nn(mixed_ref[...], weight_ref[...])
    sum_ref[...] = first_sum
    scale = lax.rsqrt(jnp.mean(first_sum * first_sum, axis=1, keepdims=True) + EPSILON)
    normed_ref[...] = (first_sum * scale * gain_ref[...]).astype(BF16)


def norm_two(mixed, tokens, weight, gain):
    rows, width = tokens.shape
    block = min(256, rows)
    blocked = pl.BlockSpec((block, width), lambda i: (i, 0))
    return call(
        norm_two_kernel, (rows // block,), [blocked, blocked, square(width, 3), whole((1, width))],
        [blocked, blocked], [shape_of((rows, width), F32), shape_of((rows, width), BF16)],
        flops=2 * rows * width * width, moved=10 * rows * width,
    )(mixed, tokens, weight, gain)


def slots_kernel(experts, parts, capacity, routes_ref, live_ref, rows_ref, columns_ref):
    top, tokens = routes_ref.shape
    live = live_ref[...]
    number = lax.broadcasted_iota(jnp.int32, (experts, tokens), 0)
    hits = [
        jnp.where((routes_ref[pl.ds(k, 1), :] == number) & (live > 0), 1.0, 0.0) for k in range(top)
    ]
    earlier = jnp.where(
        lax.broadcasted_iota(jnp.int32, (tokens, tokens), 0)
        <= lax.broadcasted_iota(jnp.int32, (tokens, tokens), 1),
        1.0,
        0.0,
    ).astype(BF16)
    ranks = dot_nn(jnp.concatenate(hits, axis=0).astype(BF16), earlier)
    before = jnp.zeros((experts, 1), F32)
    expert = lax.broadcasted_iota(jnp.int32, (experts, tokens), 0)
    start = ((expert % parts) * (experts // parts) + expert // parts) * capacity
    found = []
    for k in range(top):
        rank = ranks[k * experts : (k + 1) * experts, :] + before - 1.0
        for first in (number * capacity, start):
            slot = jnp.sum(hits[k] * (first.astype(F32) + rank), axis=0, keepdims=True).astype(jnp.int32)
            found.append(jnp.where(live > 0, slot, experts * capacity))
        before = before + jnp.sum(hits[k], axis=1, keepdims=True)
    table = jnp.concatenate(found[0::2] + found[1::2] + [jnp.zeros((8 - 2 * top, tokens), jnp.int32)], axis=0)
    rows_ref[...] = table
    columns_ref[...] = table.T


def slots_of(routes_t, live_row, experts, parts, capacity):
    top, tokens = routes_t.shape
    return call(
        functools.partial(slots_kernel, experts, parts, capacity), (1,),
        [whole((top, tokens)), whole((1, tokens))], [whole((8, tokens)), whole((tokens, 8))],
        [shape_of((8, tokens), jnp.int32), shape_of((tokens, 8), jnp.int32)],
        flops=2 * top * experts * tokens * tokens, moved=16 * tokens,
    )(routes_t, live_row)


def dispatch_kernel(gated, first, base, dest_ref, gates_ref, x_ref, out_ref):
    top, tokens = gates_ref.shape
    capacity = out_ref.shape[0]
    slot = lax.broadcasted_iota(jnp.int32, (capacity, tokens), 0) + (first + pl.program_id(0)) * capacity
    hits = [slot == dest_ref[pl.ds(base + k, 1), :] for k in range(top)]
    chosen = functools.reduce(jnp.logical_or, hits)
    rows = dot_nn(jnp.where(chosen, 1.0, 0.0).astype(BF16), x_ref[...])
    if gated:
        weights = jnp.zeros((capacity, tokens), F32)
        for k in range(top):
            weights = jnp.where(hits[k], gates_ref[pl.ds(k, 1), :], weights)
        rows = rows * jnp.sum(weights, axis=1, keepdims=True)
    out_ref[...] = rows.astype(BF16)


def dispatch(dest_t, gates_t, x, experts, capacity, gated, first, base):
    top, tokens = gates_t.shape
    width = x.shape[1]
    return call(
        functools.partial(dispatch_kernel, gated, first, base), (experts,),
        [whole(dest_t.shape), whole((top, tokens)), whole((tokens, width))],
        pl.BlockSpec((capacity, width), lambda e: (e, 0)),
        shape_of((experts * capacity, width), BF16),
        flops=2 * experts * capacity * tokens * width, moved=2 * (experts * capacity + tokens) * width,
    )(dest_t, gates_t, x)


def unpack(source, start, rows, panels, target):
    for p in range(panels):
        target[:, pl.ds(p * LANES, LANES)] = source[pl.ds(start + p * rows, rows), :].astype(F32)


def combine_kernel(dest_ref, gates_ref, live_ref, sum_ref, shared_ref, y_ref, out_ref):
    block, top = gates_ref.shape
    total = sum_ref[...] + shared_ref[...]
    dest = dest_ref[...]
    gates = gates_ref[...]
    slot = slot_numbers(block, y_ref.shape[0], 0)
    for k in range(top):
        hit = jnp.where(slot == dest[:, k : k + 1], 1.0, 0.0).astype(BF16)
        total = total + dot_nn(hit, y_ref[...]) * gates[:, k : k + 1]
    out_ref[...] = (live_ref[...] * total).astype(BF16)


def combine(dest, gates, live, first_sum, shared_out, returned):
    rows, width = first_sum.shape
    top = gates.shape[1]
    block = min(256, rows)
    blocked = pl.BlockSpec((block, width), lambda i: (i, 0))
    slots = returned.shape[0]
    return call(
        combine_kernel, (rows // block,),
        [pl.BlockSpec((block, dest.shape[1]), lambda i: (i, 0)), pl.BlockSpec((block, top), lambda i: (i, 0)),
         pl.BlockSpec((block, 1), lambda i: (i, 0)), blocked, blocked, whole(returned.shape)],
        blocked, shape_of((rows, width), BF16),
        flops=4 * rows * slots * width, moved=10 * rows * width + 2 * slots * width,
    )(dest, gates, live, first_sum, shared_out, returned)


def unpack(source, start, rows, panels, target):
    for p in range(panels):
        target[:, pl.ds(p * LANES, LANES)] = source[pl.ds(start + p * rows, rows), :].astype(F32)


def lay_out_kernel(parts, own, gu_panels, shared_ref, pack_ref, egu_ref, ed_ref, sgu_ref, sd_ref):
    step = pl.program_id(0)
    width = ed_ref.shape[2]
    packed = pack_ref.shape[0] // parts
    e_panels, e_rows = egu_ref.shape[2] // LANES, egu_ref.shape[1]
    for e in range(parts):
        for p in range(e_panels):
            rows = pl.ds(pl.multiple_of(e * packed + p * width + step * e_rows, 16), e_rows)
            egu_ref[e, :, pl.ds(p * LANES, LANES)] = pack_ref[rows, :].astype(F32)

    @pl.when(step == 0)
    def _():
        for e in range(parts):
            unpack(pack_ref, e * packed + e_panels * width, ed_ref.shape[1], width // LANES, ed_ref.at[e])

    @pl.when(step == pl.num_programs(0) - 1)
    def _():
        unpack(shared_ref, 0, own, gu_panels, sgu_ref)
        unpack(shared_ref, gu_panels * own, sd_ref.shape[0], width // LANES, sd_ref)


def lay_out(shared, pack, parts, own, width, shared_hidden, hidden):
    group, steps = width // own, 4
    columns = 2 * hidden // group
    outs = [
        (parts, width, columns), (parts, hidden // group, width), (own, 2 * shared_hidden), (shared_hidden // group, width)
    ]
    return call(
        functools.partial(lay_out_kernel, parts, own, 2 * shared_hidden // LANES), (steps,),
        [whole(shared.shape), whole(pack.shape)],
        [pl.BlockSpec((parts, width // steps, columns), lambda i: (0, i, 0))] + [whole(shape) for shape in outs[1:]],
        [shape_of(shape, F32) for shape in outs],
        flops=shared.size + pack.size, moved=6 * (shared.size + pack.size),
    )(shared, pack)


def lay_out_attention_kernel(own, x_ref, qkv_ref, wo_ref, gain_ref):
    panels = wo_ref.shape[1] // LANES
    unpack(x_ref, 0, own, 3 * panels, qkv_ref)
    unpack(x_ref, 3 * panels * own, own, panels, wo_ref)
    gain_ref[...] = x_ref[pl.ds(4 * panels * own, gain_ref.shape[0]), :].astype(F32)


def lay_out_attention(x, own, width):
    outs = [(own, 3 * width), (own, width), (8, LANES)]
    return call(
        functools.partial(lay_out_attention_kernel, own), (1,), [whole(x.shape)], [whole(shape) for shape in outs],
        [shape_of(shape, F32) for shape in outs], flops=x.size, moved=6 * x.size,
    )(x)


def slot_numbers(block, slots, part):
    return lax.broadcasted_iota(jnp.int32, (block, slots), 1) + part * slots


def gathered(top, dest_ref, y_ref, part):
    block = dest_ref.shape[0]
    dest = dest_ref[:, top : 2 * top]
    slot = slot_numbers(block, y_ref.shape[0], part)
    hit = functools.reduce(jnp.logical_or, [slot == dest[:, k : k + 1] for k in range(top)])
    return dot_nn(jnp.where(hit, 1.0, 0.0).astype(BF16), y_ref[...])


class Exchange:
    def __init__(self, axis, count, sent_ref, kept_ref, own_sem, send_sem, recv_sem):
        self.axis, self.count = axis, count
        me = lax.axis_index(axis)
        self.peers = [lax.rem(me + ahead, count) for ahead in range(1, count)]
        self.me, self.sent_ref, self.kept_ref = me, sent_ref, kept_ref
        self.own_sem, self.send_sem, self.recv_sem = own_sem, send_sem, recv_sem

    def copies(self):
        out = [pltpu.make_async_copy(self.sent_ref.at[self.me], self.kept_ref.at[self.me], self.own_sem)]
        for index, peer in enumerate(self.peers):
            out.append(
                pltpu.make_async_remote_copy(
                    src_ref=self.sent_ref.at[peer], dst_ref=self.kept_ref.at[self.me],
                    send_sem=self.send_sem.at[index], recv_sem=self.recv_sem.at[index],
                    device_id={self.axis: peer}, device_id_type=pl.DeviceIdType.MESH,
                )
            )
        return out

    def start(self):
        barrier = pltpu.get_barrier_semaphore()
        for peer in self.peers:
            pl.semaphore_signal(barrier, inc=1, device_id={self.axis: peer}, device_id_type=pl.DeviceIdType.MESH)
        pl.semaphore_wait(barrier, self.count - 1)
        for copy in self.copies():
            copy.start()

    def wait(self):
        for copy in self.copies():
            copy.wait()

    @staticmethod
    def scratch(count):
        sems = pltpu.SemaphoreType.DMA((count - 1,))
        return [pltpu.SemaphoreType.DMA, sems, sems]


def add_part_kernel(part, top, axis, count, dest_ref, base_ref, y_ref, sent_ref, out_ref, kept_ref, *sems):
    exchange = Exchange(axis, count, sent_ref, kept_ref, *sems)

    @pl.when(pl.program_id(0) == 0)
    def _():
        exchange.start()

    out_ref[...] = base_ref[...] + gathered(top, dest_ref, y_ref, part)

    @pl.when(pl.program_id(0) == pl.num_programs(0) - 1)
    def _():
        exchange.wait()


def add_part(top, dest, base, rows_of, part, sent, axis, count, collective_id):
    rows, width = base.shape
    block = min(256, rows)
    blocked = pl.BlockSpec((block, width), lambda i: (i, 0))
    hbm = pl.BlockSpec(memory_space=pl.ANY)
    sent = sent.reshape(count, -1, width)
    out, kept = call(
        functools.partial(add_part_kernel, part, top, axis, count), (rows // block,),
        [pl.BlockSpec((block, dest.shape[1]), lambda i: (i, 0)), blocked, whole(rows_of.shape), hbm],
        [blocked, hbm], [shape_of((rows, width), F32), shape_of(sent.shape, BF16)],
        scratch=Exchange.scratch(count),
        flops=2 * rows * rows_of.shape[0] * width, moved=8 * rows * width, collective_id=collective_id,
    )(dest, base, rows_of, sent)
    return out, kept.reshape(-1, width)


def norm_two_back_kernel(part, top, dest_ref, live_ref, cot_ref, sum_ref, base_ref, gain_ref, weight_ref, y_ref,
                         first_ref, attn_ref, mixed_ref, gain_grad_ref):
    grad_normed = base_ref[...] + gathered(top, dest_ref, y_ref, part)
    first_sum = sum_ref[...]
    scale = lax.rsqrt(jnp.mean(first_sum * first_sum, axis=1, keepdims=True) + EPSILON)
    weighted = grad_normed * gain_ref[...]
    inner = jnp.mean(first_sum * weighted, axis=1, keepdims=True)
    grad_first = (
        cot_ref[...].astype(F32) * live_ref[...] + scale * weighted - first_sum * (scale * scale * scale * inner)
    )
    first_ref[...] = grad_first
    grad_attn = grad_first.astype(BF16)
    attn_ref[...] = grad_attn
    mixed_ref[...] = dot_nt(grad_attn, weight_ref[...]).astype(BF16)

    @pl.when(pl.program_id(0) == 0)
    def _():
        gain_grad_ref[...] = jnp.zeros_like(gain_grad_ref)

    gain_grad_ref[...] += jnp.sum(grad_normed * first_sum * scale, axis=0, keepdims=True)


def norm_two_back(top, dest, live, cotangent, first_sum, base, gain, weights, rows_of, part):
    rows, width = first_sum.shape
    block = min(256, rows)
    blocked = pl.BlockSpec((block, width), lambda i: (i, 0))
    return call(
        functools.partial(norm_two_back_kernel, part, top), (rows // block,),
        [pl.BlockSpec((block, dest.shape[1]), lambda i: (i, 0)), pl.BlockSpec((block, 1), lambda i: (i, 0)), blocked, blocked,
         blocked, whole((1, width)), square(width, 3), whole(rows_of.shape)],
        [blocked, blocked, blocked, pl.BlockSpec((1, width), lambda i: (0, 0))],
        [shape_of((rows, width), F32), shape_of((rows, width), BF16), shape_of((rows, width), BF16),
         shape_of((1, width), F32)],
        flops=2 * rows * (rows_of.shape[0] + width) * width, moved=18 * rows * width,
    )(dest, live, cotangent, first_sum, base, gain, weights, rows_of)


def line_copy(axis, ahead, source, target, send_sem, recv_sem):
    return pltpu.make_async_remote_copy(
        src_ref=source, dst_ref=target, send_sem=send_sem, recv_sem=recv_sem,
        device_id={axis: lax.axis_index(axis) + ahead}, device_id_type=pl.DeviceIdType.MESH,
    )


class LineSum:
    def __init__(self, axis, count, x_ref, buffers, send_sem, recv_sem, turn, turns):
        self.axis, self.count, self.x_ref, self.buffers = axis, count, x_ref, buffers
        self.send_sem, self.recv_sem = send_sem, recv_sem
        self.rows, self.turn, self.turns = buffers.shape[3], turn, turns

    def own(self, piece):
        first = (piece * self.turns + self.turn) * self.rows
        return self.x_ref[pl.ds(pl.multiple_of(first, 16), self.rows), :].astype(F32)

    def copy(self, way, piece):
        return line_copy(
            self.axis, 1 - 2 * way, self.buffers.at[way, 1, piece], self.buffers.at[way, 0, piece],
            self.send_sem.at[way, piece], self.recv_sem.at[way, piece],
        )

    def each(self, body):
        me = lax.axis_index(self.axis)
        for k in range(self.count - 1):
            for way, piece in ((0, self.count - 1 - k), (1, k)):
                before = me > 0 if way == 0 else me < self.count - 1
                sends = me < piece if way == 0 else me > piece
                body(way, piece, before, sends)

    def start(self):
        def body(way, piece, before, sends):
            @pl.when(sends & jnp.logical_not(before))
            def _():
                self.buffers[way, 1, piece] = self.own(piece).astype(BF16)
                self.copy(way, piece).start()

        self.each(body)

    def relay(self):
        def body(way, piece, before, sends):
            @pl.when(sends & before)
            def _():
                self.copy(way, piece).wait_recv()
                self.buffers[way, 1, piece] = (self.own(piece) + self.buffers[way, 0, piece].astype(F32)).astype(BF16)
                self.copy(way, piece).start()

        self.each(body)

    def finish(self, total_ref):
        me = lax.axis_index(self.axis)
        total_ref[...] = self.own(me)
        for way, before in ((0, me > 0), (1, me < self.count - 1)):

            @pl.when(before)
            def _():
                self.copy(way, me).wait_recv()
                total_ref[...] += self.buffers[way, 0, me].astype(F32)

        def body(way, piece, before, sends):
            @pl.when(sends)
            def _():
                self.copy(way, piece).wait_send()

        self.each(body)


class LineGather:
    def __init__(self, axis, count, out_ref, send_sem, recv_sem, turn, turns):
        self.axis, self.count, self.out_ref = axis, count, out_ref
        self.send_sem, self.recv_sem = send_sem, recv_sem
        self.rows, self.turn, self.turns = out_ref.shape[0] // count // turns, turn, turns

    def place(self, piece):
        first = (piece * self.turns + self.turn) * self.rows
        return self.out_ref.at[pl.ds(pl.multiple_of(first, 16), self.rows), :]

    def copy(self, way, piece):
        return line_copy(
            self.axis, 1 - 2 * way, self.place(piece), self.place(piece),
            self.send_sem.at[way, piece], self.recv_sem.at[way, piece],
        )

    def start(self, value):
        me = lax.axis_index(self.axis)
        self.place(me)[...] = value
        for way, more in ((0, me < self.count - 1), (1, me > 0)):

            @pl.when(more)
            def _():
                self.copy(way, me).start()

    def relay(self, k):
        me = lax.axis_index(self.axis)
        for way, piece, there, more in (
            (0, me - k, me >= k, me < self.count - 1),
            (1, me + k, me + k < self.count, me > 0),
        ):

            @pl.when(there)
            def _():
                self.copy(way, piece).wait_recv()

            @pl.when(there & more)
            def _():
                self.copy(way, piece).start()

    def finish(self):
        me = lax.axis_index(self.axis)
        for k in range(self.count):
            for way, piece, sent in (
                (0, me - k, (me >= k) & (me < self.count - 1)),
                (1, me + k, (me + k < self.count) & (me > 0)),
            ):

                @pl.when(sent)
                def _():
                    self.copy(way, piece).wait_send()


def greet_neighbours(barrier, axis, count):
    me = lax.axis_index(axis)
    for ahead, there in ((1, me < count - 1), (-1, me > 0)):

        @pl.when(there)
        def _():
            pl.semaphore_signal(barrier, inc=1, device_id={axis: me + ahead}, device_id_type=pl.DeviceIdType.MESH)

    return (me < count - 1).astype(jnp.int32) + (me > 0).astype(jnp.int32)


def settle_kernel(sizes, gq_ref, gk_ref, gv_ref, wq_ref, wk_ref, wv_ref, tokens_ref, first_ref, gain_ref, pack_ref,
                  x_ref, out_ref, share_ref, all_ref, own, landed, chosen, arrived, sem, pair_send, pair_recv, send_sem,
                  recv_sem, x_buffers, x_total, x_all, x_send, x_recv, g_send, g_recv):
    dp_size, shard_size, count = sizes
    spread = shard_size // 2
    halves = dp_size * spread
    dp, shard = lax.axis_index("dp"), lax.axis_index("shard")
    side = shard % 2
    place = dp * spread + shard // 2
    step = pl.program_id(0)
    last = pl.num_programs(0) - 1

    def target(piece, bit):
        return {"dp": piece // spread, "shard": (piece % spread) * 2 + bit}

    turns = x_buffers.shape[0]
    lines = [
        LineSum("expert", count, x_ref, x_buffers.at[t], x_send.at[t], x_recv.at[t], t, turns) for t in range(turns)
    ]
    gathers = [LineGather("expert", count, x_all, g_send.at[t], g_recv.at[t], t, turns) for t in range(turns)]

    def pair_copy():
        return pltpu.make_async_remote_copy(
            src_ref=pack_ref.at[:, 1 - side], dst_ref=landed, send_sem=pair_send, recv_sem=pair_recv,
            device_id=target(place, 1 - side), device_id_type=pl.DeviceIdType.MESH,
        )

    def own_copy():
        return pltpu.make_async_copy(pack_ref.at[:, side], own, sem)

    def send(index):
        return pltpu.make_async_remote_copy(
            src_ref=chosen.at[index], dst_ref=arrived.at[index], send_sem=send_sem.at[index], recv_sem=recv_sem.at[index],
            device_id=target(lax.rem(place + index + 1, halves), side), device_id_type=pl.DeviceIdType.MESH,
        )

    @pl.when(step == 0)
    def _():
        barrier = pltpu.get_barrier_semaphore()
        pl.semaphore_signal(barrier, inc=1, device_id=target(place, 1 - side), device_id_type=pl.DeviceIdType.MESH)
        for index in range(halves - 1):
            pl.semaphore_signal(
                barrier, inc=1, device_id=target(lax.rem(place + index + 1, halves), side),
                device_id_type=pl.DeviceIdType.MESH,
            )
        neighbours = greet_neighbours(barrier, "expert", count)
        pl.semaphore_wait(barrier, halves + neighbours)
        pair_copy().start()
        own_copy().start()
        lines[0].start()

    @pl.when(step == 1)
    def _():
        own_copy().wait()
        pair_copy().wait()
        for index in range(halves - 1):
            piece = lax.rem(place + index + 1, halves)
            chosen[index] = (own[piece].astype(F32) + landed[piece].astype(F32)).astype(BF16)
            send(index).start()

    grad_normed = (
        dot_nt(gq_ref[...], wq_ref[...]) + dot_nt(gk_ref[...], wk_ref[...]) + dot_nt(gv_ref[...], wv_ref[...])
    )
    source = tokens_ref[...].astype(F32)
    scale = lax.rsqrt(jnp.mean(source * source, axis=1, keepdims=True) + EPSILON)
    weighted = grad_normed * gain_ref[...]
    inner = jnp.mean(source * weighted, axis=1, keepdims=True)
    out_ref[...] = first_ref[...] + scale * weighted - source * (scale * scale * scale * inner)

    @pl.when(step == last)
    def _():
        for t in range(turns):
            if t:
                lines[t].start()
            lines[t].relay()
            if t:
                gathers[t - 1].relay(1)
            lines[t].finish(x_total)
            gathers[t].start(x_total[...].astype(BF16))
        total = own[place].astype(F32) + landed[place].astype(F32)
        for index in range(halves - 1):
            send(index).wait()
            total = total + arrived[index].astype(F32)
        share_ref[...] = total.astype(BF16)
        for k in range(1, count):
            for t in range(turns):
                if k > 1 or t == turns - 1:
                    gathers[t].relay(k)
        for gather in gathers:
            gather.finish()
        all_ref[...] = x_all[...]


def settle(grads, w_qkv, tokens, grad_first, gain, pack, x, sizes):
    rows, width = tokens.shape
    block = min(256, rows)
    blocked = pl.BlockSpec((block, width), lambda i: (i, 0))
    halves, count = sizes[0] * sizes[1] // 2, pack.shape[1]
    piece = (count, LANES)
    turns = 2 if x.shape[0] // sizes[2] % 32 == 0 else 1
    x_piece = (x.shape[0] // sizes[2] // turns, LANES)
    return call(
        functools.partial(settle_kernel, sizes), (rows // block,),
        [blocked] * 3 + [square(width, 0), square(width, 1), square(width, 2), blocked, blocked, whole((1, width)),
                         pl.BlockSpec(memory_space=pl.ANY), whole(x.shape)],
        [blocked, whole(piece), whole(x.shape)],
        [shape_of((rows, width), F32), shape_of(piece, BF16), shape_of(x.shape, BF16)],
        scratch=[pltpu.VMEM((halves,) + piece, BF16), pltpu.VMEM((halves,) + piece, BF16),
                 pltpu.VMEM((halves - 1,) + piece, BF16), pltpu.VMEM((halves - 1,) + piece, BF16),
                 pltpu.SemaphoreType.DMA, pltpu.SemaphoreType.DMA, pltpu.SemaphoreType.DMA,
                 pltpu.SemaphoreType.DMA((halves - 1,)), pltpu.SemaphoreType.DMA((halves - 1,)),
                 pltpu.VMEM((turns, 2, 2, sizes[2]) + x_piece, BF16), pltpu.VMEM(x_piece, F32), pltpu.VMEM(x.shape, BF16)]
        + [pltpu.SemaphoreType.DMA((turns, 2, sizes[2]))] * 4,
        flops=6 * rows * width * width, moved=22 * rows * width, collective_id=1,
    )(*grads, w_qkv, w_qkv, w_qkv, tokens, grad_first, gain, pack.reshape((halves, 2) + piece), x)


def copies_of(layout, block, width, step, stage_g, stage_u, stage_d, slot, packed_ref, sems):
    by_rows, owners, hidden, base = layout
    panels = block // LANES
    rows_down = hidden // owners
    out = []

    def add(source, target):
        out.append(pltpu.make_async_copy(source, target, sems.at[slot, len(out)]))

    if by_rows:
        rows = width // owners
        for half, stage in enumerate((stage_g, stage_u)):
            for p in range(panels):
                panel = half * (hidden // LANES) + step * panels + p
                add(
                    stage.at[slot, :, :, pl.ds(p * LANES, LANES)],
                    packed_ref.at[:, pl.ds(pl.multiple_of(base + panel * rows, 8), rows), :],
                )
        start = 2 * hidden // LANES * rows
    else:
        columns = 2 * hidden // owners
        for half, stage in enumerate((stage_g, stage_u)):
            for p in range(panels):
                column = half * hidden + step * block + p * LANES
                owner, panel = column // columns, (column % columns) // LANES
                add(
                    stage.at[slot, :, pl.ds(p * LANES, LANES)],
                    packed_ref.at[owner, pl.ds(pl.multiple_of(base + panel * width, 8), width), :],
                )
        start = columns // LANES * width
    for q in range(block // rows_down):
        owner = step * (block // rows_down) + q
        for c in range(width // LANES):
            add(
                stage_d.at[slot, pl.ds(q * rows_down, rows_down), pl.ds(c * LANES, LANES)],
                packed_ref.at[owner, pl.ds(base + start + c * rows_down, rows_down), :],
            )
    return out


def packed_rows(width, hidden, owners):
    return 3 * width * hidden // owners // LANES


def ffn_kernel(out_type, layout, block, axis, count, x_ref, gy_ref, wg_ref, wu_ref, wd_ref, sent_ref, *rest):
    y_ref, gx_ref, packed_ref, kept_ref, xt, y_acc, gx_acc, stage_g, stage_u, stage_d, sems, *exchange_sems = rest[-14:]
    exchange = Exchange(axis, count, sent_ref, kept_ref, *exchange_sems)
    step = pl.program_id(0)
    steps = layout[2] // block
    width = x_ref.shape[1]
    slot = step % 2
    copies = functools.partial(copies_of, layout, block, width)

    @pl.when(step == 0)
    def _():
        exchange.start()
        xt[...] = x_ref[...].T
        y_acc[...] = jnp.zeros_like(y_acc)
        gx_acc[...] = jnp.zeros_like(gx_acc)

    @pl.when(step >= 2)
    def _():
        for copy in copies(step - 2, stage_g, stage_u, stage_d, slot, packed_ref, sems):
            copy.wait()

    x, gy = x_ref[...], gy_ref[...].reshape(x_ref.shape)
    if layout[0]:
        wg, wu = wg_ref[...].reshape(width, block), wu_ref[...].reshape(width, block)
        rows = wd_ref.shape[1] // (width // block)
        wd = jnp.concatenate(
            [wd_ref[:, pl.ds(c * rows, rows), :].reshape(block, block) for c in range(width // block)], axis=1
        )
    else:
        wg, wu, wd = wg_ref[...], wu_ref[...], wd_ref[...]
    gate, up = dot_nn(x, wg), dot_nn(x, wu)
    grad_hidden = dot_nt(gy, wd)
    sigmoid = jax.nn.sigmoid(gate)
    value = gate * sigmoid
    hidden = (value * up).astype(BF16)
    grad_up = (grad_hidden * value).astype(BF16)
    grad_gate = (grad_hidden * up * (sigmoid * (1.0 + gate * (1.0 - sigmoid)))).astype(BF16)
    y_acc[...] += dot_nn(hidden, wd)
    gx_acc[...] += dot_nt(grad_gate, wg) + dot_nt(grad_up, wu)
    stage_g[slot] = dot_nn(xt[...], grad_gate).astype(BF16).reshape(stage_g.shape[1:])
    stage_u[slot] = dot_nn(xt[...], grad_up).astype(BF16).reshape(stage_u.shape[1:])
    stage_d[slot] = dot_tn(hidden, gy).astype(BF16)
    for copy in copies(step, stage_g, stage_u, stage_d, slot, packed_ref, sems):
        copy.start()

    @pl.when(step == steps - 1)
    def _():
        exchange.wait()
        y_ref[...] = y_acc[...].astype(out_type).reshape(y_ref.shape)
        gx_ref[...] = gx_acc[...].astype(out_type)
        for back in (1, 0):
            if steps > back:
                for copy in copies(steps - 1 - back, stage_g, stage_u, stage_d, (steps - 1 - back) % 2, packed_ref, sems):
                    copy.wait()


BLOCK = 256


def ffn_both(x, gy, w_gu, w_down, hidden, expert, owners, out_type, sent, axis, count, collective_id, parts=1, held=()):
    rows, width = x.shape
    block = BLOCK
    steps = hidden // block
    by_rows = expert is None
    if by_rows:
        own, own_down, panels = width // owners, hidden // owners, width // block
        ahead = 2 * steps * own // (panels * own_down)
        gate = pl.BlockSpec((owners, own, block), lambda f: (0, f, 0))
        up = pl.BlockSpec((owners, own, block), lambda f: (0, steps + f, 0))
        down = pl.BlockSpec((block // own_down, panels * own_down, block), lambda f: (f, ahead, 0))
        stage = (2, owners, own, block)
    else:
        gate = pl.BlockSpec((None, width, block), lambda f: (expert, 0, f))
        up = pl.BlockSpec((None, width, block), lambda f: (expert, 0, steps + f))
        down = pl.BlockSpec((None, block, width), lambda f: (expert, f, 0))
        stage = (2, width, block)
    if by_rows:
        grads = whole((rows, width))
        y_block, y_shape = whole((rows, width)), (rows, width)
    else:
        y_shape = (gy.shape[0], parts * (rows // gy.shape[0]), width)
        y_block = pl.BlockSpec(
            (gy.shape[0], rows // gy.shape[0], width), lambda f: (0, expert, 0), pipeline_mode=pl.Buffered(1)
        )
        grads = pl.BlockSpec(
            (gy.shape[0], rows // gy.shape[0], width), lambda f: (0, expert, 0), pipeline_mode=pl.Buffered(1)
        )
    out_rows = whole((rows, width))
    pack_rows = packed_rows(width, hidden, owners)
    layout = (by_rows, owners, hidden, (expert or 0) * pack_rows)
    hbm = pl.BlockSpec(memory_space=pl.ANY)
    sent = sent.reshape(count, -1, width)
    copies = 2 * (block // LANES) + block // (hidden // owners) * (width // LANES)
    y, gx, pack, kept = call(
        functools.partial(ffn_kernel, out_type, layout, block, axis, count), (steps,),
        [whole((rows, width)), grads, gate, up, down, hbm] + [hbm] * len(held),
        [y_block, out_rows, hbm, hbm],
        [shape_of(y_shape, out_type), shape_of((rows, width), out_type),
         shape_of((owners, parts * pack_rows, LANES), BF16), shape_of(sent.shape, BF16)],
        scratch=[pltpu.VMEM((width, rows), BF16), pltpu.VMEM((rows, width), F32), pltpu.VMEM((rows, width), F32),
                 pltpu.VMEM(stage, BF16), pltpu.VMEM(stage, BF16), pltpu.VMEM((2, block, width), BF16),
                 pltpu.SemaphoreType.DMA((2, copies))] + Exchange.scratch(count),
        flops=18 * rows * width * hidden, moved=12 * width * hidden + 16 * rows * width, trans=rows * hidden,
        aliases={6: 0, 7: 2} if held else None, collective_id=collective_id,
    )(x, gy, w_gu, w_gu, w_down, sent, *held)
    return y, gx, pack, kept.reshape(-1, width)


def to_panels(array):
    rows, columns = array.shape
    return jnp.transpose(array.reshape(rows, columns // BLOCK, BLOCK), (1, 0, 2)).reshape(-1, BLOCK)


def attention_weights_kernel(per, normed_ref, mixed_ref, gq_ref, gk_ref, gv_ref, ga_ref, gains_ref, out_ref, xt):
    step = pl.program_id(0)
    owners, rows = out_ref.shape[0], out_ref.shape[1] // (out_ref.shape[1] // (normed_ref.shape[1] // out_ref.shape[0]))
    panels = out_ref.shape[1] // rows

    @pl.when(step == 0)
    def _():
        xt[...] = normed_ref[...].T

    @pl.when(step == 3 * per)
    def _():
        xt[...] = mixed_ref[...].T

    for index, grad_ref in enumerate((gq_ref, gk_ref, gv_ref, ga_ref)):

        @pl.when((step >= index * per) & (step < (index + 1) * per))
        def _():
            product = dot_nn(xt[...], grad_ref[...]).astype(BF16)
            for p in range(panels):
                out_ref[:, pl.ds(p * rows, rows), :] = product[:, p * LANES : (p + 1) * LANES].reshape(owners, rows, LANES)

    @pl.when(step >= 4 * per)
    def _():
        out_ref[...] = jnp.zeros_like(out_ref)

    @pl.when(step == 4 * per)
    def _():
        out_ref[:, pl.ds(0, gains_ref.shape[1]), :] = gains_ref[...]


def attention_weights(normed, mixed, grads, grad_attn, gains, owners, pieces):
    tokens, width = normed.shape
    rows = width // owners
    block = BLOCK
    panels, per = block // LANES, width // block
    steps = 4 * per + 1
    while steps * panels * rows % (16 * pieces):
        steps += 1

    def columns(index):
        return pl.BlockSpec((tokens, block), lambda i: (0, jnp.clip(i - index * per, 0, per - 1)))

    return call(
        functools.partial(attention_weights_kernel, per), (steps,),
        [whole((tokens, width)), whole((tokens, width))] + [columns(index) for index in range(4)] + [whole(gains.shape)],
        pl.BlockSpec((owners, panels * rows, LANES), lambda i: (0, i, 0)),
        shape_of((owners, steps * panels * rows, LANES), BF16),
        scratch=[pltpu.VMEM((width, tokens), BF16)],
        flops=8 * tokens * width * width, moved=16 * tokens * width,
    )(normed, mixed, *grads, grad_attn, gains)


GROUP = ("dp", "shard")


def local(
    tokens,
    lengths,
    routes,
    route_gates,
    cotangent,
    norm_gains,
    w_qkv,
    w_out,
    w_shared_gu,
    w_shared_down,
    w_expert_gu,
    w_expert_down,
):
    tok_count, width = tokens.shape
    seq_count = lengths.shape[0]
    length = tok_count // seq_count
    local_experts = w_expert_gu.shape[0]
    owners = lax.axis_size("expert")
    experts = local_experts * owners
    top = routes.shape[1]
    capacity = tok_count * top * 9 // (8 * experts)
    head_dim = width // HEADS
    hidden = w_expert_down.shape[1]

    gains = lax.all_gather(norm_gains, GROUP, axis=1, tiled=True).astype(F32)
    attention_weight = lax.all_gather(jnp.concatenate([w_qkv, w_out], axis=1), GROUP, axis=0, tiled=True)
    shared_weight = lax.all_gather(
        jnp.concatenate([to_panels(w_shared_gu), to_panels(w_shared_down)], axis=0)[None], GROUP, axis=0, tiled=True
    )
    gain_one, gain_two = gains[0:1], gains[1:2]

    live_bool = lax.iota(jnp.int32, tok_count) % length < jnp.repeat(lengths, length)
    live = live_bool.astype(F32)[:, None]
    live_row = live_bool.astype(jnp.int32)[None, :]

    group = lax.axis_size("dp") * lax.axis_size("shard")
    shared_hidden = w_shared_down.shape[0] * group

    table_t, table = slots_of(routes.T, live_row, experts, local_experts, capacity)
    gates_t = route_gates.T
    grad_b = jnp.where(live_bool[:, None], cotangent, 0).astype(BF16)

    def exchange(rows):
        return lax.all_to_all(
            rows.reshape(owners, -1, width), "expert", split_axis=0, concat_axis=0, tiled=True
        ).reshape(rows.shape)

    send_grad = dispatch(table_t, gates_t, grad_b, experts, capacity, True, 0, 0)
    received_grad = exchange(send_grad).reshape(owners, local_experts * capacity, width)

    cosine, sine = rotary_tables(length, head_dim)
    normed_one = norm_one(tokens, gain_one)
    queries, keys, values, mixed, lse = attend_forward(normed_one, attention_weight, cosine, sine, length, head_dim)
    first_sum, normed_two = norm_two(mixed, tokens, attention_weight, gain_two)

    send_rows = []
    for j in range(local_experts):
        send_rows.append(dispatch(table_t, gates_t, normed_two, owners, capacity, False, j * owners, top))
    shared_out, grad_shared, shared_pack, received = ffn_both(
        normed_two, grad_b, shared_weight, shared_weight, shared_hidden, None, group, F32,
        send_rows[0], "expert", owners, 3,
    )
    waiting = send_rows[1:]
    back_rows, base, held = [], grad_shared, ()
    for j in range(local_experts):
        y, gx, pack, arrived = ffn_both(
            received, received_grad, w_expert_gu, w_expert_down, hidden, j, group, BF16,
            waiting.pop(0), "expert", owners, 4 + j, local_experts, held,
        )
        held = (y, pack)
        waiting.append(gx)
        if j < local_experts - 1:
            received = arrived
        else:
            back_rows.append(arrived)
    for j, sent in enumerate(waiting):
        base, arrived = add_part(
            top, table, base, back_rows[j], j, sent, "expert", owners, 4 + local_experts + j
        )
        back_rows.append(arrived)
    y, base = lax.optimization_barrier((y, base))
    grad_first, grad_attn, grad_mixed, grad_gain_two = norm_two_back(
        top, table, live, cotangent, first_sum, base, gain_two, attention_weight, back_rows[-1], local_experts - 1
    )

    grads = attend_backward(queries, keys, values, mixed, grad_mixed, lse, cosine, sine, length, head_dim)
    own = width // group
    grad_gains = grad_gain_two.reshape(group, 1, own)
    grad_gains = jnp.pad(grad_gains, ((0, 0), (0, 15), (0, LANES - own))).astype(BF16)
    attention_pack = attention_weights(normed_one, mixed, grads, grad_attn, grad_gains, group, owners)

    def spread(pack):
        return lax.psum_scatter(pack, GROUP, scatter_dimension=0, tiled=True)[0]

    shared_share = spread(shared_pack)
    expert_share = spread(pack)
    input_grad, attention_share, shared_share = settle(
        grads, attention_weight, tokens, grad_first, gain_one, attention_pack, shared_share,
        (lax.axis_size("dp"), lax.axis_size("shard"), owners),
    )
    returned = exchange(y)
    pieces = lax.all_to_all(
        attention_share.reshape(owners, -1, LANES), "expert", split_axis=0, concat_axis=0, tiled=True
    )
    piece = jnp.sum(pieces.astype(F32), axis=0).astype(BF16)
    attention_share = lax.all_to_all(
        jnp.broadcast_to(piece[None], pieces.shape), "expert", split_axis=0, concat_axis=0, tiled=True
    ).reshape(attention_share.shape)
    layer_out = combine(table, route_gates, live, first_sum, shared_out, returned.reshape(-1, width))
    expert_gu, expert_down, shared_gu, shared_down = lay_out(
        shared_share, expert_share, local_experts, own, width, shared_hidden, hidden
    )
    qkv_grad, out_grad, gain_rows = lay_out_attention(attention_share, own, width)
    grad_gain_one = jnp.sum(w_qkv.astype(F32) * qkv_grad, axis=1) / norm_gains[0].astype(F32)
    grad_gains = jnp.stack([grad_gain_one, gain_rows[0, :own]])
    return layer_out, input_grad, grad_gains, qkv_grad, out_grad, shared_gu, shared_down, expert_gu, expert_down


def solution(mesh):
    rows = P(("dp", "expert", "shard"), None)
    split = P(GROUP, None)
    in_specs = (
        rows,
        P(("dp", "expert", "shard")),
        rows,
        rows,
        rows,
        P(None, GROUP),
        split,
        split,
        split,
        split,
        P("expert", None, None),
        P("expert", None, None),
    )
    out_specs = (
        rows,
        rows,
        P(None, GROUP),
        split,
        split,
        split,
        split,
        P("expert", None, GROUP),
        P("expert", GROUP, None),
    )

    return jax.shard_map(local, mesh=mesh, in_specs=in_specs, out_specs=out_specs, check_vma=False)
```

```python
import functools
import math

import jax
import jax.numpy as jnp
from jax import lax
from jax.experimental import pallas as pl
from jax.experimental.pallas import tpu as pltpu
from jax.sharding import PartitionSpec as P


HEADS = 12
LANES = 128
EPSILON = 1e-05
VMEM_BYTES = 60 * 1024 * 1024
BF16 = jnp.bfloat16
F32 = jnp.float32


def call(kernel, grid, in_specs, out_specs, out_shape, scratch=(), flops=0, moved=0, trans=0, collective_id=None, aliases=None):
    return pl.pallas_call(
        kernel,
        grid_spec=pltpu.PrefetchScalarGridSpec(
            num_scalar_prefetch=0,
            grid=grid,
            in_specs=in_specs,
            out_specs=out_specs,
            scratch_shapes=list(scratch),
        ),
        out_shape=out_shape,
        input_output_aliases=aliases or {},
        compiler_params=pltpu.CompilerParams(
            dimension_semantics=("arbitrary",) * len(grid), vmem_limit_bytes=VMEM_BYTES, collective_id=collective_id,
            has_side_effects=collective_id is not None,
        ),
        cost_estimate=pl.CostEstimate(flops=flops, bytes_accessed=moved, transcendentals=trans),
    )


def shape_of(shape, dtype):
    return jax.ShapeDtypeStruct(shape, dtype)


def whole(shape):
    return pl.BlockSpec(shape, lambda *_: (0,) * len(shape), pipeline_mode=pl.Buffered(1))


def dot_nn(left, right):
    return lax.dot_general(left, right, (((1,), (0,)), ((), ())), preferred_element_type=F32)


def dot_nt(left, right):
    return lax.dot_general(left, right, (((1,), (1,)), ((), ())), preferred_element_type=F32)


def dot_tn(left, right):
    return lax.dot_general(left, right, (((0,), (0,)), ((), ())), preferred_element_type=F32)


def rotary_tables(length, head_dim):
    half_dim = head_dim // 2
    position = lax.iota(F32, length)[:, None]
    frequency = jnp.exp(lax.iota(F32, half_dim) * (-2.0 * math.log(10000.0) / head_dim))
    angle_table = position * frequency[None, :]
    cosine, sine = jnp.cos(angle_table), jnp.sin(angle_table)
    repeats = LANES // head_dim
    return (
        jnp.tile(jnp.concatenate([cosine, cosine], axis=1), (1, repeats)),
        jnp.tile(jnp.concatenate([-sine, sine], axis=1), (1, repeats)),
    )


def turn(values, cosine, signed_sine, head_dim):
    lane = lax.broadcasted_iota(jnp.int32, values.shape, 1)
    half = head_dim // 2
    other = jnp.where(
        lane % head_dim < half,
        pltpu.roll(values, LANES - half, 1),
        pltpu.roll(values, half, 1),
    )
    return values * cosine + other * signed_sine


def attend_forward_kernel(
    head_dim, block, x_ref, wq_ref, wk_ref, wv_ref, cos_ref, sin_ref, q_ref, k_ref, v_ref, o_ref, lse_ref, lse_tile
):
    length = x_ref.shape[0]
    heads = LANES // head_dim
    x = x_ref[...]
    cosine, sine = cos_ref[...], sin_ref[...]
    scale = 1.0 / math.sqrt(head_dim)
    q_ref[...] = (turn(dot_nn(x, wq_ref[...]), cosine, sine, head_dim) * scale).astype(BF16)
    k_ref[...] = turn(dot_nn(x, wk_ref[...]), cosine, sine, head_dim).astype(BF16)
    v_ref[...] = dot_nn(x, wv_ref[...]).astype(BF16)
    lane = lax.broadcasted_iota(jnp.int32, (1, LANES), 1)
    own_lane = lax.broadcasted_iota(jnp.int32, (block, LANES), 1) // head_dim
    below = lax.broadcasted_iota(jnp.int32, (block, block), 0) >= lax.broadcasted_iota(
        jnp.int32, (block, block), 1
    )
    for first in range(0, length, block):
        rows = pl.ds(first, block)
        mixed = None
        logs = None
        for head in range(heads):
            select = (lane // head_dim == head).astype(F32).astype(BF16)
            queries = q_ref[rows, :] * select
            near = jnp.where(below, dot_nt(queries, k_ref[rows, :]), -1e30)
            peak = jnp.max(near, axis=1, keepdims=True)
            if first:
                far = dot_nt(queries, k_ref[pl.ds(0, first), :])
                peak = jnp.maximum(peak, jnp.max(far, axis=1, keepdims=True))
            near = jnp.exp(near - peak)
            total = jnp.sum(near, axis=1, keepdims=True)
            part = dot_nn(near.astype(BF16), v_ref[rows, :])
            if first:
                far = jnp.exp(far - peak)
                total = total + jnp.sum(far, axis=1, keepdims=True)
                part = part + dot_nn(far.astype(BF16), v_ref[pl.ds(0, first), :])
            part = part * (1.0 / total)
            log_total = jnp.broadcast_to(peak + jnp.log(total), (block, LANES))
            mixed = part if head == 0 else jnp.where(own_lane == head, part, mixed)
            logs = log_total if head == 0 else jnp.where(own_lane == head, log_total, logs)
        o_ref[rows, :] = mixed.astype(BF16)
        lse_tile[rows, :] = logs
    turned = lse_tile[...].T
    for head in range(heads):
        lse_ref[pl.ds(head * 8, 8), :] = turned[head * head_dim : head * head_dim + 8, :]


def attend_forward(normed, w_qkv, cosine, sine, length, head_dim):
    tokens, width = normed.shape
    seqs, pairs, heads = tokens // length, width // LANES, LANES // head_dim
    block = min(256, length)
    rows = pl.BlockSpec((length, LANES), lambda s, p: (s, p))

    def weight(part):
        return pl.BlockSpec((width, LANES), lambda s, p: (0, part * pairs + p))

    table = whole((length, LANES))
    return call(
        functools.partial(attend_forward_kernel, head_dim, block),
        (seqs, pairs),
        [pl.BlockSpec((length, width), lambda s, p: (s, 0)), weight(0), weight(1), weight(2), table, table],
        [rows, rows, rows, rows, pl.BlockSpec((8 * heads, length), lambda s, p: (s * pairs + p, 0))],
        [shape_of((tokens, width), BF16)] * 4 + [shape_of((seqs * pairs * 8 * heads, length), F32)],
        scratch=[pltpu.VMEM((length, LANES), F32)],
        flops=6 * tokens * width * width + 4 * tokens * length * width,
        moved=16 * tokens * width,
        trans=tokens * length * width // head_dim // 2,
    )(normed, w_qkv, w_qkv, w_qkv, cosine, sine)


def attend_backward_kernel(
    head_dim, block, q_ref, k_ref, v_ref, o_ref, g_ref, lse_ref, cos_ref, sin_ref, gq_ref, gk_ref, gv_ref, gq_acc
):
    length = q_ref.shape[0]
    heads = LANES // head_dim
    scale = 1.0 / math.sqrt(head_dim)
    product = (g_ref[...].astype(F32) * o_ref[...].astype(F32)).T
    inner = [
        jnp.sum(product[head * head_dim : (head + 1) * head_dim, :], axis=0, keepdims=True)
        for head in range(heads)
    ]
    gq_acc[...] = jnp.zeros_like(gq_acc)
    lane = lax.broadcasted_iota(jnp.int32, (1, LANES), 1)
    own_lane = lax.broadcasted_iota(jnp.int32, (block, LANES), 1) // head_dim
    above = lax.broadcasted_iota(jnp.int32, (block, block), 1) >= lax.broadcasted_iota(
        jnp.int32, (block, block), 0
    )
    for first in range(0, length, block):
        rows = pl.ds(first, block)
        keys_grad = None
        values_grad = None
        for head in range(heads):
            select = (lane // head_dim == head).astype(F32).astype(BF16)
            keys = k_ref[rows, :] * select
            values = v_ref[rows, :] * select
            log_total = lse_ref[pl.ds(head * 8, 1), :]
            pieces = [(first, block, True)]
            if first + block < length:
                pieces.append((first + block, length - first - block, False))
            keys_part = None
            values_part = None
            for start, count, diagonal in pieces:
                span = pl.ds(start, count)
                queries, grads = q_ref[span, :], g_ref[span, :]
                scores = dot_nt(keys, queries)
                probs = jnp.exp(scores - log_total[:, start : start + count])
                if diagonal:
                    probs = jnp.where(above, probs, 0.0)
                grad_probs = dot_nt(values, grads)
                grad_scores = (probs * (grad_probs - inner[head][:, start : start + count])).astype(BF16)
                piece_values = dot_nn(probs.astype(BF16), grads)
                piece_keys = dot_nn(grad_scores, queries)
                values_part = piece_values if values_part is None else values_part + piece_values
                keys_part = piece_keys if keys_part is None else keys_part + piece_keys
                gq_acc[span, :] += dot_tn(grad_scores, keys)
            keys_grad = keys_part if head == 0 else jnp.where(own_lane == head, keys_part, keys_grad)
            values_grad = values_part if head == 0 else jnp.where(own_lane == head, values_part, values_grad)
        gk_ref[rows, :] = turn(keys_grad, cos_ref[rows, :], -sin_ref[rows, :], head_dim).astype(BF16)
        gv_ref[rows, :] = values_grad.astype(BF16)
    gq_ref[...] = turn(gq_acc[...] * scale, cos_ref[...], -sin_ref[...], head_dim).astype(BF16)


def attend_backward(queries, keys, values, mixed, grad_mixed, lse, cosine, sine, length, head_dim):
    tokens, width = queries.shape
    seqs, pairs, heads = tokens // length, width // LANES, LANES // head_dim
    block = min(256, length)
    rows = pl.BlockSpec((length, LANES), lambda s, p: (s, p))
    table = whole((length, LANES))
    return call(
        functools.partial(attend_backward_kernel, head_dim, block),
        (seqs, pairs),
        [rows] * 5 + [pl.BlockSpec((8 * heads, length), lambda s, p: (s * pairs + p, 0)), table, table],
        [rows] * 3,
        [shape_of((tokens, width), BF16)] * 3,
        scratch=[pltpu.VMEM((length, LANES), F32)],
        flops=10 * tokens * length * width,
        moved=16 * tokens * width,
        trans=tokens * length * width // head_dim // 2,
    )(queries, keys, values, mixed, grad_mixed, lse, cosine, sine)


def square(width, part):
    return pl.BlockSpec((width, width), lambda i: (0, part), pipeline_mode=pl.Buffered(1))


def norm_one_kernel(x_ref, gain_ref, out_ref):
    x = x_ref[...].astype(F32)
    scale = lax.rsqrt(jnp.mean(x * x, axis=1, keepdims=True) + EPSILON)
    out_ref[...] = (x * scale * gain_ref[...]).astype(BF16)


def norm_one(tokens, gain):
    rows, width = tokens.shape
    block = min(256, rows)
    blocked = pl.BlockSpec((block, width), lambda i: (i, 0))
    return call(
        norm_one_kernel, (rows // block,), [blocked, whole((1, width))], blocked, shape_of((rows, width), BF16),
        flops=5 * rows * width, moved=4 * rows * width,
    )(tokens, gain)


def norm_two_kernel(mixed_ref, tokens_ref, weight_ref, gain_ref, sum_ref, normed_ref):
    first_sum = tokens_ref[...].astype(F32) + dot_nn(mixed_ref[...], weight_ref[...])
    sum_ref[...] = first_sum
    scale = lax.rsqrt(jnp.mean(first_sum * first_sum, axis=1, keepdims=True) + EPSILON)
    normed_ref[...] = (first_sum * scale * gain_ref[...]).astype(BF16)


def norm_two(mixed, tokens, weight, gain):
    rows, width = tokens.shape
    block = min(256, rows)
    blocked = pl.BlockSpec((block, width), lambda i: (i, 0))
    return call(
        norm_two_kernel, (rows // block,), [blocked, blocked, square(width, 3), whole((1, width))],
        [blocked, blocked], [shape_of((rows, width), F32), shape_of((rows, width), BF16)],
        flops=2 * rows * width * width, moved=10 * rows * width,
    )(mixed, tokens, weight, gain)


def slots_kernel(experts, parts, capacity, routes_ref, live_ref, rows_ref, columns_ref):
    top, tokens = routes_ref.shape
    live = live_ref[...]
    number = lax.broadcasted_iota(jnp.int32, (experts, tokens), 0)
    hits = [
        jnp.where((routes_ref[pl.ds(k, 1), :] == number) & (live > 0), 1.0, 0.0) for k in range(top)
    ]
    earlier = jnp.where(
        lax.broadcasted_iota(jnp.int32, (tokens, tokens), 0)
        <= lax.broadcasted_iota(jnp.int32, (tokens, tokens), 1),
        1.0,
        0.0,
    ).astype(BF16)
    ranks = dot_nn(jnp.concatenate(hits, axis=0).astype(BF16), earlier)
    before = jnp.zeros((experts, 1), F32)
    expert = lax.broadcasted_iota(jnp.int32, (experts, tokens), 0)
    start = ((expert % parts) * (experts // parts) + expert // parts) * capacity
    found = []
    for k in range(top):
        rank = ranks[k * experts : (k + 1) * experts, :] + before - 1.0
        for first in (number * capacity, start):
            slot = jnp.sum(hits[k] * (first.astype(F32) + rank), axis=0, keepdims=True).astype(jnp.int32)
            found.append(jnp.where(live > 0, slot, experts * capacity))
        before = before + jnp.sum(hits[k], axis=1, keepdims=True)
    table = jnp.concatenate(found[0::2] + found[1::2] + [jnp.zeros((8 - 2 * top, tokens), jnp.int32)], axis=0)
    rows_ref[...] = table
    columns_ref[...] = table.T


def slots_of(routes_t, live_row, experts, parts, capacity):
    top, tokens = routes_t.shape
    return call(
        functools.partial(slots_kernel, experts, parts, capacity), (1,),
        [whole((top, tokens)), whole((1, tokens))], [whole((8, tokens)), whole((tokens, 8))],
        [shape_of((8, tokens), jnp.int32), shape_of((tokens, 8), jnp.int32)],
        flops=2 * top * experts * tokens * tokens, moved=16 * tokens,
    )(routes_t, live_row)


def dispatch_kernel(gated, first, base, dest_ref, gates_ref, x_ref, out_ref):
    top, tokens = gates_ref.shape
    capacity = out_ref.shape[0]
    slot = lax.broadcasted_iota(jnp.int32, (capacity, tokens), 0) + (first + pl.program_id(0)) * capacity
    hits = [slot == dest_ref[pl.ds(base + k, 1), :] for k in range(top)]
    chosen = functools.reduce(jnp.logical_or, hits)
    rows = dot_nn(jnp.where(chosen, 1.0, 0.0).astype(BF16), x_ref[...])
    if gated:
        weights = jnp.zeros((capacity, tokens), F32)
        for k in range(top):
            weights = jnp.where(hits[k], gates_ref[pl.ds(k, 1), :], weights)
        rows = rows * jnp.sum(weights, axis=1, keepdims=True)
    out_ref[...] = rows.astype(BF16)


def dispatch(dest_t, gates_t, x, experts, capacity, gated, first, base):
    top, tokens = gates_t.shape
    width = x.shape[1]
    return call(
        functools.partial(dispatch_kernel, gated, first, base), (experts,),
        [whole(dest_t.shape), whole((top, tokens)), whole((tokens, width))],
        pl.BlockSpec((capacity, width), lambda e: (e, 0)),
        shape_of((experts * capacity, width), BF16),
        flops=2 * experts * capacity * tokens * width, moved=2 * (experts * capacity + tokens) * width,
    )(dest_t, gates_t, x)


def unpack(source, start, rows, panels, target):
    for p in range(panels):
        target[:, pl.ds(p * LANES, LANES)] = source[pl.ds(start + p * rows, rows), :].astype(F32)


def combine_kernel(dest_ref, gates_ref, live_ref, sum_ref, shared_ref, y_ref, out_ref):
    block, top = gates_ref.shape
    total = sum_ref[...] + shared_ref[...]
    dest = dest_ref[...]
    gates = gates_ref[...]
    slot = slot_numbers(block, y_ref.shape[0], 0)
    for k in range(top):
        hit = jnp.where(slot == dest[:, k : k + 1], 1.0, 0.0).astype(BF16)
        total = total + dot_nn(hit, y_ref[...]) * gates[:, k : k + 1]
    out_ref[...] = (live_ref[...] * total).astype(BF16)


def combine(dest, gates, live, first_sum, shared_out, returned):
    rows, width = first_sum.shape
    top = gates.shape[1]
    block = min(256, rows)
    blocked = pl.BlockSpec((block, width), lambda i: (i, 0))
    slots = returned.shape[0]
    return call(
        combine_kernel, (rows // block,),
        [pl.BlockSpec((block, dest.shape[1]), lambda i: (i, 0)), pl.BlockSpec((block, top), lambda i: (i, 0)),
         pl.BlockSpec((block, 1), lambda i: (i, 0)), blocked, blocked, whole(returned.shape)],
        blocked, shape_of((rows, width), BF16),
        flops=4 * rows * slots * width, moved=10 * rows * width + 2 * slots * width,
    )(dest, gates, live, first_sum, shared_out, returned)


def unpack(source, start, rows, panels, target):
    for p in range(panels):
        target[:, pl.ds(p * LANES, LANES)] = source[pl.ds(start + p * rows, rows), :].astype(F32)


def lay_out_kernel(parts, pack_ref, egu_ref, ed_ref):
    step = pl.program_id(0)
    width = ed_ref.shape[2]
    packed = pack_ref.shape[0] // parts
    e_panels, e_rows = egu_ref.shape[2] // LANES, egu_ref.shape[1]
    for e in range(parts):
        for p in range(e_panels):
            rows = pl.ds(pl.multiple_of(e * packed + p * width + step * e_rows, 16), e_rows)
            egu_ref[e, :, pl.ds(p * LANES, LANES)] = pack_ref[rows, :].astype(F32)

    @pl.when(step == 0)
    def _():
        for e in range(parts):
            unpack(pack_ref, e * packed + e_panels * width, ed_ref.shape[1], width // LANES, ed_ref.at[e])


def lay_out(pack, parts, own, width, hidden):
    group, steps = width // own, 4
    columns = 2 * hidden // group
    outs = [(parts, width, columns), (parts, hidden // group, width)]
    return call(
        functools.partial(lay_out_kernel, parts), (steps,), [whole(pack.shape)],
        [pl.BlockSpec((parts, width // steps, columns), lambda i: (0, i, 0)), whole(outs[1])],
        [shape_of(shape, F32) for shape in outs],
        flops=pack.size, moved=6 * pack.size,
    )(pack)


def lay_out_shared_kernel(own, gu_panels, x_ref, sgu_ref, sd_ref):
    unpack(x_ref, 0, own, gu_panels, sgu_ref)
    unpack(x_ref, gu_panels * own, sd_ref.shape[0], sd_ref.shape[1] // LANES, sd_ref)


def lay_out_shared(x, own, width, hidden):
    outs = [(own, 2 * hidden), (hidden // (width // own), width)]
    return call(
        functools.partial(lay_out_shared_kernel, own, 2 * hidden // LANES), (1,), [whole(x.shape)],
        [whole(shape) for shape in outs], [shape_of(shape, F32) for shape in outs], flops=x.size, moved=6 * x.size,
    )(x)


def lay_out_attention_kernel(own, x_ref, qkv_ref, wo_ref, gain_ref):
    panels = wo_ref.shape[1] // LANES
    unpack(x_ref, 0, own, 3 * panels, qkv_ref)
    unpack(x_ref, 3 * panels * own, own, panels, wo_ref)
    gain_ref[...] = x_ref[pl.ds(4 * panels * own, gain_ref.shape[0]), :].astype(F32)


def lay_out_attention(x, own, width):
    outs = [(own, 3 * width), (own, width), (8, LANES)]
    return call(
        functools.partial(lay_out_attention_kernel, own), (1,), [whole(x.shape)], [whole(shape) for shape in outs],
        [shape_of(shape, F32) for shape in outs], flops=x.size, moved=6 * x.size,
    )(x)


def slot_numbers(block, slots, part):
    return lax.broadcasted_iota(jnp.int32, (block, slots), 1) + part * slots


def gathered(top, dest_ref, y_ref, part):
    block = dest_ref.shape[0]
    dest = dest_ref[:, top : 2 * top]
    slot = slot_numbers(block, y_ref.shape[0], part)
    hit = functools.reduce(jnp.logical_or, [slot == dest[:, k : k + 1] for k in range(top)])
    return dot_nn(jnp.where(hit, 1.0, 0.0).astype(BF16), y_ref[...])


class Exchange:
    def __init__(self, axis, count, sent_ref, kept_ref, own_sem, send_sem, recv_sem):
        self.axis, self.count = axis, count
        me = lax.axis_index(axis)
        self.peers = [lax.rem(me + ahead, count) for ahead in range(1, count)]
        self.me, self.sent_ref, self.kept_ref = me, sent_ref, kept_ref
        self.own_sem, self.send_sem, self.recv_sem = own_sem, send_sem, recv_sem

    def copies(self):
        out = [pltpu.make_async_copy(self.sent_ref.at[self.me], self.kept_ref.at[self.me], self.own_sem)]
        for index, peer in enumerate(self.peers):
            out.append(
                pltpu.make_async_remote_copy(
                    src_ref=self.sent_ref.at[peer], dst_ref=self.kept_ref.at[self.me],
                    send_sem=self.send_sem.at[index], recv_sem=self.recv_sem.at[index],
                    device_id={self.axis: peer}, device_id_type=pl.DeviceIdType.MESH,
                )
            )
        return out

    def start(self):
        barrier = pltpu.get_barrier_semaphore()
        for peer in self.peers:
            pl.semaphore_signal(barrier, inc=1, device_id={self.axis: peer}, device_id_type=pl.DeviceIdType.MESH)
        pl.semaphore_wait(barrier, self.count - 1)
        for copy in self.copies():
            copy.start()

    def wait(self):
        for copy in self.copies():
            copy.wait()

    @staticmethod
    def scratch(count):
        sems = pltpu.SemaphoreType.DMA((count - 1,))
        return [pltpu.SemaphoreType.DMA, sems, sems]


def add_part_kernel(part, top, axis, count, dest_ref, base_ref, y_ref, sent_ref, out_ref, kept_ref, *sems):
    exchange = Exchange(axis, count, sent_ref, kept_ref, *sems)

    @pl.when(pl.program_id(0) == 0)
    def _():
        exchange.start()

    out_ref[...] = base_ref[...] + gathered(top, dest_ref, y_ref, part)

    @pl.when(pl.program_id(0) == pl.num_programs(0) - 1)
    def _():
        exchange.wait()


def add_part(top, dest, base, rows_of, part, sent, axis, count, collective_id):
    rows, width = base.shape
    block = min(256, rows)
    blocked = pl.BlockSpec((block, width), lambda i: (i, 0))
    hbm = pl.BlockSpec(memory_space=pl.ANY)
    sent = sent.reshape(count, -1, width)
    out, kept = call(
        functools.partial(add_part_kernel, part, top, axis, count), (rows // block,),
        [pl.BlockSpec((block, dest.shape[1]), lambda i: (i, 0)), blocked, whole(rows_of.shape), hbm],
        [blocked, hbm], [shape_of((rows, width), F32), shape_of(sent.shape, BF16)],
        scratch=Exchange.scratch(count),
        flops=2 * rows * rows_of.shape[0] * width, moved=8 * rows * width, collective_id=collective_id,
    )(dest, base, rows_of, sent)
    return out, kept.reshape(-1, width)


def norm_two_back_kernel(part, top, dest_ref, live_ref, cot_ref, sum_ref, base_ref, gain_ref, weight_ref, y_ref,
                         first_ref, attn_ref, mixed_ref, gain_grad_ref):
    grad_normed = base_ref[...] + gathered(top, dest_ref, y_ref, part)
    first_sum = sum_ref[...]
    scale = lax.rsqrt(jnp.mean(first_sum * first_sum, axis=1, keepdims=True) + EPSILON)
    weighted = grad_normed * gain_ref[...]
    inner = jnp.mean(first_sum * weighted, axis=1, keepdims=True)
    grad_first = (
        cot_ref[...].astype(F32) * live_ref[...] + scale * weighted - first_sum * (scale * scale * scale * inner)
    )
    first_ref[...] = grad_first
    grad_attn = grad_first.astype(BF16)
    attn_ref[...] = grad_attn
    mixed_ref[...] = dot_nt(grad_attn, weight_ref[...]).astype(BF16)

    @pl.when(pl.program_id(0) == 0)
    def _():
        gain_grad_ref[...] = jnp.zeros_like(gain_grad_ref)

    gain_grad_ref[...] += jnp.sum(grad_normed * first_sum * scale, axis=0, keepdims=True)


def norm_two_back(top, dest, live, cotangent, first_sum, base, gain, weights, rows_of, part):
    rows, width = first_sum.shape
    block = min(256, rows)
    blocked = pl.BlockSpec((block, width), lambda i: (i, 0))
    return call(
        functools.partial(norm_two_back_kernel, part, top), (rows // block,),
        [pl.BlockSpec((block, dest.shape[1]), lambda i: (i, 0)), pl.BlockSpec((block, 1), lambda i: (i, 0)), blocked, blocked,
         blocked, whole((1, width)), square(width, 3), whole(rows_of.shape)],
        [blocked, blocked, blocked, pl.BlockSpec((1, width), lambda i: (0, 0))],
        [shape_of((rows, width), F32), shape_of((rows, width), BF16), shape_of((rows, width), BF16),
         shape_of((1, width), F32)],
        flops=2 * rows * (rows_of.shape[0] + width) * width, moved=18 * rows * width,
    )(dest, live, cotangent, first_sum, base, gain, weights, rows_of)


def settle_kernel(sizes, gq_ref, gk_ref, gv_ref, wq_ref, wk_ref, wv_ref, tokens_ref, first_ref, gain_ref, pack_ref,
                  out_ref, share_ref, own, landed, chosen, arrived, sem, pair_send, pair_recv, send_sem, recv_sem):
    dp_size, shard_size = sizes
    spread = shard_size // 2
    halves = dp_size * spread
    dp, shard = lax.axis_index("dp"), lax.axis_index("shard")
    side = shard % 2
    place = dp * spread + shard // 2
    step = pl.program_id(0)
    last = pl.num_programs(0) - 1

    def target(piece, bit):
        return {"dp": piece // spread, "shard": (piece % spread) * 2 + bit}

    def pair_copy():
        return pltpu.make_async_remote_copy(
            src_ref=pack_ref.at[:, 1 - side], dst_ref=landed, send_sem=pair_send, recv_sem=pair_recv,
            device_id=target(place, 1 - side), device_id_type=pl.DeviceIdType.MESH,
        )

    def own_copy():
        return pltpu.make_async_copy(pack_ref.at[:, side], own, sem)

    def send(index):
        return pltpu.make_async_remote_copy(
            src_ref=chosen.at[index], dst_ref=arrived.at[index], send_sem=send_sem.at[index], recv_sem=recv_sem.at[index],
            device_id=target(lax.rem(place + index + 1, halves), side), device_id_type=pl.DeviceIdType.MESH,
        )

    @pl.when(step == 0)
    def _():
        barrier = pltpu.get_barrier_semaphore()
        pl.semaphore_signal(barrier, inc=1, device_id=target(place, 1 - side), device_id_type=pl.DeviceIdType.MESH)
        for index in range(halves - 1):
            pl.semaphore_signal(
                barrier, inc=1, device_id=target(lax.rem(place + index + 1, halves), side),
                device_id_type=pl.DeviceIdType.MESH,
            )
        pl.semaphore_wait(barrier, halves)
        pair_copy().start()
        own_copy().start()

    @pl.when(step == 1)
    def _():
        own_copy().wait()
        pair_copy().wait()
        for index in range(halves - 1):
            piece = lax.rem(place + index + 1, halves)
            chosen[index] = (own[piece].astype(F32) + landed[piece].astype(F32)).astype(BF16)
            send(index).start()

    grad_normed = (
        dot_nt(gq_ref[...], wq_ref[...]) + dot_nt(gk_ref[...], wk_ref[...]) + dot_nt(gv_ref[...], wv_ref[...])
    )
    source = tokens_ref[...].astype(F32)
    scale = lax.rsqrt(jnp.mean(source * source, axis=1, keepdims=True) + EPSILON)
    weighted = grad_normed * gain_ref[...]
    inner = jnp.mean(source * weighted, axis=1, keepdims=True)
    out_ref[...] = first_ref[...] + scale * weighted - source * (scale * scale * scale * inner)

    @pl.when(step == last)
    def _():
        total = own[place].astype(F32) + landed[place].astype(F32)
        for index in range(halves - 1):
            send(index).wait()
            total = total + arrived[index].astype(F32)
        share_ref[...] = total.astype(BF16)


def settle(grads, w_qkv, tokens, grad_first, gain, pack, sizes):
    rows, width = tokens.shape
    block = min(256, rows)
    blocked = pl.BlockSpec((block, width), lambda i: (i, 0))
    halves, count = sizes[0] * sizes[1] // 2, pack.shape[1]
    piece = (count, LANES)
    return call(
        functools.partial(settle_kernel, sizes), (rows // block,),
        [blocked] * 3 + [square(width, 0), square(width, 1), square(width, 2), blocked, blocked, whole((1, width)),
                         pl.BlockSpec(memory_space=pl.ANY)],
        [blocked, whole(piece)], [shape_of((rows, width), F32), shape_of(piece, BF16)],
        scratch=[pltpu.VMEM((halves,) + piece, BF16), pltpu.VMEM((halves,) + piece, BF16),
                 pltpu.VMEM((halves - 1,) + piece, BF16), pltpu.VMEM((halves - 1,) + piece, BF16),
                 pltpu.SemaphoreType.DMA, pltpu.SemaphoreType.DMA, pltpu.SemaphoreType.DMA,
                 pltpu.SemaphoreType.DMA((halves - 1,)), pltpu.SemaphoreType.DMA((halves - 1,))],
        flops=6 * rows * width * width, moved=22 * rows * width, collective_id=1,
    )(*grads, w_qkv, w_qkv, w_qkv, tokens, grad_first, gain, pack.reshape((halves, 2) + piece))


def copies_of(layout, block, width, step, stage_g, stage_u, stage_d, slot, packed_ref, sems):
    by_rows, owners, hidden, base = layout
    panels = block // LANES
    rows_down = hidden // owners
    out = []

    def add(source, target):
        out.append(pltpu.make_async_copy(source, target, sems.at[slot, len(out)]))

    if by_rows:
        rows = width // owners
        for half, stage in enumerate((stage_g, stage_u)):
            for p in range(panels):
                panel = half * (hidden // LANES) + step * panels + p
                add(
                    stage.at[slot, :, :, pl.ds(p * LANES, LANES)],
                    packed_ref.at[:, pl.ds(pl.multiple_of(base + panel * rows, 8), rows), :],
                )
        start = 2 * hidden // LANES * rows
    else:
        columns = 2 * hidden // owners
        for half, stage in enumerate((stage_g, stage_u)):
            for p in range(panels):
                column = half * hidden + step * block + p * LANES
                owner, panel = column // columns, (column % columns) // LANES
                add(
                    stage.at[slot, :, pl.ds(p * LANES, LANES)],
                    packed_ref.at[owner, pl.ds(pl.multiple_of(base + panel * width, 8), width), :],
                )
        start = columns // LANES * width
    for q in range(block // rows_down):
        owner = step * (block // rows_down) + q
        for c in range(width // LANES):
            add(
                stage_d.at[slot, pl.ds(q * rows_down, rows_down), pl.ds(c * LANES, LANES)],
                packed_ref.at[owner, pl.ds(base + start + c * rows_down, rows_down), :],
            )
    return out


def packed_rows(width, hidden, owners):
    return 3 * width * hidden // owners // LANES


def ffn_kernel(out_type, layout, block, axis, count, x_ref, gy_ref, wg_ref, wu_ref, wd_ref, sent_ref, *rest):
    y_ref, gx_ref, packed_ref, kept_ref, xt, y_acc, gx_acc, stage_g, stage_u, stage_d, sems, *exchange_sems = rest[-14:]
    exchange = Exchange(axis, count, sent_ref, kept_ref, *exchange_sems)
    step = pl.program_id(0)
    steps = layout[2] // block
    width = x_ref.shape[1]
    slot = step % 2
    copies = functools.partial(copies_of, layout, block, width)

    @pl.when(step == 0)
    def _():
        exchange.start()
        xt[...] = x_ref[...].T
        y_acc[...] = jnp.zeros_like(y_acc)
        gx_acc[...] = jnp.zeros_like(gx_acc)

    @pl.when(step >= 2)
    def _():
        for copy in copies(step - 2, stage_g, stage_u, stage_d, slot, packed_ref, sems):
            copy.wait()

    x, gy = x_ref[...], gy_ref[...].reshape(x_ref.shape)
    if layout[0]:
        wg, wu = wg_ref[...].reshape(width, block), wu_ref[...].reshape(width, block)
        rows = wd_ref.shape[1] // (width // block)
        wd = jnp.concatenate(
            [wd_ref[:, pl.ds(c * rows, rows), :].reshape(block, block) for c in range(width // block)], axis=1
        )
    else:
        wg, wu, wd = wg_ref[...], wu_ref[...], wd_ref[...]
    gate, up = dot_nn(x, wg), dot_nn(x, wu)
    grad_hidden = dot_nt(gy, wd)
    sigmoid = jax.nn.sigmoid(gate)
    value = gate * sigmoid
    hidden = (value * up).astype(BF16)
    grad_up = (grad_hidden * value).astype(BF16)
    grad_gate = (grad_hidden * up * (sigmoid * (1.0 + gate * (1.0 - sigmoid)))).astype(BF16)
    y_acc[...] += dot_nn(hidden, wd)
    gx_acc[...] += dot_nt(grad_gate, wg) + dot_nt(grad_up, wu)
    stage_g[slot] = dot_nn(xt[...], grad_gate).astype(BF16).reshape(stage_g.shape[1:])
    stage_u[slot] = dot_nn(xt[...], grad_up).astype(BF16).reshape(stage_u.shape[1:])
    stage_d[slot] = dot_tn(hidden, gy).astype(BF16)
    for copy in copies(step, stage_g, stage_u, stage_d, slot, packed_ref, sems):
        copy.start()

    @pl.when(step == steps - 1)
    def _():
        exchange.wait()
        y_ref[...] = y_acc[...].astype(out_type).reshape(y_ref.shape)
        gx_ref[...] = gx_acc[...].astype(out_type)
        for back in (1, 0):
            if steps > back:
                for copy in copies(steps - 1 - back, stage_g, stage_u, stage_d, (steps - 1 - back) % 2, packed_ref, sems):
                    copy.wait()


BLOCK = 256


def ffn_both(x, gy, w_gu, w_down, hidden, expert, owners, out_type, sent, axis, count, collective_id, parts=1, held=()):
    rows, width = x.shape
    block = BLOCK
    steps = hidden // block
    by_rows = expert is None
    if by_rows:
        own, own_down, panels = width // owners, hidden // owners, width // block
        ahead = 2 * steps * own // (panels * own_down)
        gate = pl.BlockSpec((owners, own, block), lambda f: (0, f, 0))
        up = pl.BlockSpec((owners, own, block), lambda f: (0, steps + f, 0))
        down = pl.BlockSpec((block // own_down, panels * own_down, block), lambda f: (f, ahead, 0))
        stage = (2, owners, own, block)
    else:
        gate = pl.BlockSpec((None, width, block), lambda f: (expert, 0, f))
        up = pl.BlockSpec((None, width, block), lambda f: (expert, 0, steps + f))
        down = pl.BlockSpec((None, block, width), lambda f: (expert, f, 0))
        stage = (2, width, block)
    if by_rows:
        grads = whole((rows, width))
        y_block, y_shape = whole((rows, width)), (rows, width)
    else:
        y_shape = (gy.shape[0], parts * (rows // gy.shape[0]), width)
        y_block = pl.BlockSpec(
            (gy.shape[0], rows // gy.shape[0], width), lambda f: (0, expert, 0), pipeline_mode=pl.Buffered(1)
        )
        grads = pl.BlockSpec(
            (gy.shape[0], rows // gy.shape[0], width), lambda f: (0, expert, 0), pipeline_mode=pl.Buffered(1)
        )
    out_rows = whole((rows, width))
    pack_rows = packed_rows(width, hidden, owners)
    layout = (by_rows, owners, hidden, (expert or 0) * pack_rows)
    hbm = pl.BlockSpec(memory_space=pl.ANY)
    sent = sent.reshape(count, -1, width)
    copies = 2 * (block // LANES) + block // (hidden // owners) * (width // LANES)
    y, gx, pack, kept = call(
        functools.partial(ffn_kernel, out_type, layout, block, axis, count), (steps,),
        [whole((rows, width)), grads, gate, up, down, hbm] + [hbm] * len(held),
        [y_block, out_rows, hbm, hbm],
        [shape_of(y_shape, out_type), shape_of((rows, width), out_type),
         shape_of((owners, parts * pack_rows, LANES), BF16), shape_of(sent.shape, BF16)],
        scratch=[pltpu.VMEM((width, rows), BF16), pltpu.VMEM((rows, width), F32), pltpu.VMEM((rows, width), F32),
                 pltpu.VMEM(stage, BF16), pltpu.VMEM(stage, BF16), pltpu.VMEM((2, block, width), BF16),
                 pltpu.SemaphoreType.DMA((2, copies))] + Exchange.scratch(count),
        flops=18 * rows * width * hidden, moved=12 * width * hidden + 16 * rows * width, trans=rows * hidden,
        aliases={6: 0, 7: 2} if held else None, collective_id=collective_id,
    )(x, gy, w_gu, w_gu, w_down, sent, *held)
    return y, gx, pack, kept.reshape(-1, width)


def to_panels(array):
    rows, columns = array.shape
    return jnp.transpose(array.reshape(rows, columns // BLOCK, BLOCK), (1, 0, 2)).reshape(-1, BLOCK)


def attention_weights_kernel(per, normed_ref, mixed_ref, gq_ref, gk_ref, gv_ref, ga_ref, gains_ref, out_ref, xt):
    step = pl.program_id(0)
    owners, rows = out_ref.shape[0], out_ref.shape[1] // (out_ref.shape[1] // (normed_ref.shape[1] // out_ref.shape[0]))
    panels = out_ref.shape[1] // rows

    @pl.when(step == 0)
    def _():
        xt[...] = normed_ref[...].T

    @pl.when(step == 3 * per)
    def _():
        xt[...] = mixed_ref[...].T

    for index, grad_ref in enumerate((gq_ref, gk_ref, gv_ref, ga_ref)):

        @pl.when((step >= index * per) & (step < (index + 1) * per))
        def _():
            product = dot_nn(xt[...], grad_ref[...]).astype(BF16)
            for p in range(panels):
                out_ref[:, pl.ds(p * rows, rows), :] = product[:, p * LANES : (p + 1) * LANES].reshape(owners, rows, LANES)

    @pl.when(step >= 4 * per)
    def _():
        out_ref[...] = jnp.zeros_like(out_ref)

    @pl.when(step == 4 * per)
    def _():
        out_ref[:, pl.ds(0, gains_ref.shape[1]), :] = gains_ref[...]


def attention_weights(normed, mixed, grads, grad_attn, gains, owners, pieces):
    tokens, width = normed.shape
    rows = width // owners
    block = BLOCK
    panels, per = block // LANES, width // block
    steps = 4 * per + 1
    while steps * panels * rows % (16 * pieces):
        steps += 1

    def columns(index):
        return pl.BlockSpec((tokens, block), lambda i: (0, jnp.clip(i - index * per, 0, per - 1)))

    return call(
        functools.partial(attention_weights_kernel, per), (steps,),
        [whole((tokens, width)), whole((tokens, width))] + [columns(index) for index in range(4)] + [whole(gains.shape)],
        pl.BlockSpec((owners, panels * rows, LANES), lambda i: (0, i, 0)),
        shape_of((owners, steps * panels * rows, LANES), BF16),
        scratch=[pltpu.VMEM((width, tokens), BF16)],
        flops=8 * tokens * width * width, moved=16 * tokens * width,
    )(normed, mixed, *grads, grad_attn, gains)


GROUP = ("dp", "shard")


def local(
    tokens,
    lengths,
    routes,
    route_gates,
    cotangent,
    norm_gains,
    w_qkv,
    w_out,
    w_shared_gu,
    w_shared_down,
    w_expert_gu,
    w_expert_down,
):
    tok_count, width = tokens.shape
    seq_count = lengths.shape[0]
    length = tok_count // seq_count
    local_experts = w_expert_gu.shape[0]
    owners = lax.axis_size("expert")
    experts = local_experts * owners
    top = routes.shape[1]
    capacity = tok_count * top * 9 // (8 * experts)
    head_dim = width // HEADS
    hidden = w_expert_down.shape[1]

    gains = lax.all_gather(norm_gains, GROUP, axis=1, tiled=True).astype(F32)
    attention_weight = lax.all_gather(jnp.concatenate([w_qkv, w_out], axis=1), GROUP, axis=0, tiled=True)
    shared_weight = lax.all_gather(
        jnp.concatenate([to_panels(w_shared_gu), to_panels(w_shared_down)], axis=0)[None], GROUP, axis=0, tiled=True
    )
    gain_one, gain_two = gains[0:1], gains[1:2]

    live_bool = lax.iota(jnp.int32, tok_count) % length < jnp.repeat(lengths, length)
    live = live_bool.astype(F32)[:, None]
    live_row = live_bool.astype(jnp.int32)[None, :]

    group = lax.axis_size("dp") * lax.axis_size("shard")
    shared_hidden = w_shared_down.shape[0] * group

    table_t, table = slots_of(routes.T, live_row, experts, local_experts, capacity)
    gates_t = route_gates.T
    grad_b = jnp.where(live_bool[:, None], cotangent, 0).astype(BF16)

    def exchange(rows):
        return lax.all_to_all(
            rows.reshape(owners, -1, width), "expert", split_axis=0, concat_axis=0, tiled=True
        ).reshape(rows.shape)

    send_grad = dispatch(table_t, gates_t, cotangent, experts, capacity, True, 0, 0)
    received_grad = exchange(send_grad).reshape(owners, local_experts * capacity, width)

    cosine, sine = rotary_tables(length, head_dim)
    normed_one = norm_one(tokens, gain_one)
    queries, keys, values, mixed, lse = attend_forward(normed_one, attention_weight, cosine, sine, length, head_dim)
    first_sum, normed_two = norm_two(mixed, tokens, attention_weight, gain_two)

    send_rows = []
    for j in range(local_experts):
        send_rows.append(dispatch(table_t, gates_t, normed_two, owners, capacity, False, j * owners, top))
    shared_out, grad_shared, shared_pack, received = ffn_both(
        normed_two, grad_b, shared_weight, shared_weight, shared_hidden, None, group, F32,
        send_rows[0], "expert", owners, 3,
    )
    waiting = send_rows[1:]
    back_rows, base, held = [], grad_shared, ()
    for j in range(local_experts):
        y, gx, pack, arrived = ffn_both(
            received, received_grad, w_expert_gu, w_expert_down, hidden, j, group, BF16,
            waiting.pop(0), "expert", owners, 4 + j, local_experts, held,
        )
        held = (y, pack)
        waiting.append(gx)
        if j < local_experts - 1:
            received = arrived
        else:
            back_rows.append(arrived)
    for j, sent in enumerate(waiting):
        base, arrived = add_part(
            top, table, base, back_rows[j], j, sent, "expert", owners, 4 + local_experts + j
        )
        back_rows.append(arrived)
    y, base = lax.optimization_barrier((y, base))
    grad_first, grad_attn, grad_mixed, grad_gain_two = norm_two_back(
        top, table, live, cotangent, first_sum, base, gain_two, attention_weight, back_rows[-1], local_experts - 1
    )

    grads = attend_backward(queries, keys, values, mixed, grad_mixed, lse, cosine, sine, length, head_dim)
    own = width // group
    grad_gains = grad_gain_two.reshape(group, 1, own)
    grad_gains = jnp.pad(grad_gains, ((0, 0), (0, 15), (0, LANES - own))).astype(BF16)
    attention_pack = attention_weights(normed_one, mixed, grads, grad_attn, grad_gains, group, owners)

    def spread(pack):
        return lax.psum_scatter(pack, GROUP, scatter_dimension=0, tiled=True)[0]

    shared_share = spread(shared_pack)
    expert_share = spread(pack)
    input_grad, attention_share = settle(
        grads, attention_weight, tokens, grad_first, gain_one, attention_pack,
        (lax.axis_size("dp"), lax.axis_size("shard")),
    )
    shared_share = lax.psum(shared_share, "expert")
    returned = exchange(y)
    pieces = lax.all_to_all(
        attention_share.reshape(owners, -1, LANES), "expert", split_axis=0, concat_axis=0, tiled=True
    )
    piece = jnp.sum(pieces.astype(F32), axis=0).astype(BF16)
    attention_share = lax.all_to_all(
        jnp.broadcast_to(piece[None], pieces.shape), "expert", split_axis=0, concat_axis=0, tiled=True
    ).reshape(attention_share.shape)
    layer_out = combine(table, route_gates, live, first_sum, shared_out, returned.reshape(-1, width))
    expert_gu, expert_down = lay_out(expert_share, local_experts, own, width, hidden)
    shared_gu, shared_down = lay_out_shared(shared_share, own, width, shared_hidden)
    qkv_grad, out_grad, gain_rows = lay_out_attention(attention_share, own, width)
    grad_gain_one = jnp.sum(w_qkv.astype(F32) * qkv_grad, axis=1) / norm_gains[0].astype(F32)
    grad_gains = jnp.stack([grad_gain_one, gain_rows[0, :own]])
    return layer_out, input_grad, grad_gains, qkv_grad, out_grad, shared_gu, shared_down, expert_gu, expert_down


def solution(mesh):
    rows = P(("dp", "expert", "shard"), None)
    split = P(GROUP, None)
    in_specs = (
        rows,
        P(("dp", "expert", "shard")),
        rows,
        rows,
        rows,
        P(None, GROUP),
        split,
        split,
        split,
        split,
        P("expert", None, None),
        P("expert", None, None),
    )
    out_specs = (
        rows,
        rows,
        P(None, GROUP),
        split,
        split,
        split,
        split,
        P("expert", None, GROUP),
        P("expert", GROUP, None),
    )

    return jax.shard_map(local, mesh=mesh, in_specs=in_specs, out_specs=out_specs, check_vma=False)
```

```python
import functools
import math

import jax
import jax.numpy as jnp
from jax import lax
from jax.experimental import pallas as pl
from jax.experimental.pallas import tpu as pltpu
from jax.sharding import PartitionSpec as P


HEADS = 12
LANES = 128
EPSILON = 1e-05
VMEM_BYTES = 60 * 1024 * 1024
BF16 = jnp.bfloat16
F32 = jnp.float32


def call(kernel, grid, in_specs, out_specs, out_shape, scratch=(), flops=0, moved=0, trans=0, collective_id=None, aliases=None):
    return pl.pallas_call(
        kernel,
        grid_spec=pltpu.PrefetchScalarGridSpec(
            num_scalar_prefetch=0,
            grid=grid,
            in_specs=in_specs,
            out_specs=out_specs,
            scratch_shapes=list(scratch),
        ),
        out_shape=out_shape,
        input_output_aliases=aliases or {},
        compiler_params=pltpu.CompilerParams(
            dimension_semantics=("arbitrary",) * len(grid), vmem_limit_bytes=VMEM_BYTES, collective_id=collective_id,
            has_side_effects=collective_id is not None,
        ),
        cost_estimate=pl.CostEstimate(flops=flops, bytes_accessed=moved, transcendentals=trans),
    )


def shape_of(shape, dtype):
    return jax.ShapeDtypeStruct(shape, dtype)


def whole(shape):
    return pl.BlockSpec(shape, lambda *_: (0,) * len(shape), pipeline_mode=pl.Buffered(1))


def dot_nn(left, right):
    return lax.dot_general(left, right, (((1,), (0,)), ((), ())), preferred_element_type=F32)


def dot_nt(left, right):
    return lax.dot_general(left, right, (((1,), (1,)), ((), ())), preferred_element_type=F32)


def dot_tn(left, right):
    return lax.dot_general(left, right, (((0,), (0,)), ((), ())), preferred_element_type=F32)


def rotary_tables(length, head_dim):
    half_dim = head_dim // 2
    position = lax.iota(F32, length)[:, None]
    frequency = jnp.exp(lax.iota(F32, half_dim) * (-2.0 * math.log(10000.0) / head_dim))
    angle_table = position * frequency[None, :]
    cosine, sine = jnp.cos(angle_table), jnp.sin(angle_table)
    repeats = LANES // head_dim
    return (
        jnp.tile(jnp.concatenate([cosine, cosine], axis=1), (1, repeats)),
        jnp.tile(jnp.concatenate([-sine, sine], axis=1), (1, repeats)),
    )


def turn(values, cosine, signed_sine, head_dim):
    lane = lax.broadcasted_iota(jnp.int32, values.shape, 1)
    half = head_dim // 2
    other = jnp.where(
        lane % head_dim < half,
        pltpu.roll(values, LANES - half, 1),
        pltpu.roll(values, half, 1),
    )
    return values * cosine + other * signed_sine


def attend_forward_kernel(
    head_dim, block, x_ref, wq_ref, wk_ref, wv_ref, cos_ref, sin_ref, q_ref, k_ref, v_ref, o_ref, lse_ref, lse_tile
):
    length = x_ref.shape[0]
    heads = LANES // head_dim
    x = x_ref[...]
    cosine, sine = cos_ref[...], sin_ref[...]
    scale = 1.0 / math.sqrt(head_dim)
    q_ref[...] = (turn(dot_nn(x, wq_ref[...]), cosine, sine, head_dim) * scale).astype(BF16)
    k_ref[...] = turn(dot_nn(x, wk_ref[...]), cosine, sine, head_dim).astype(BF16)
    v_ref[...] = dot_nn(x, wv_ref[...]).astype(BF16)
    lane = lax.broadcasted_iota(jnp.int32, (1, LANES), 1)
    own_lane = lax.broadcasted_iota(jnp.int32, (block, LANES), 1) // head_dim
    below = lax.broadcasted_iota(jnp.int32, (block, block), 0) >= lax.broadcasted_iota(
        jnp.int32, (block, block), 1
    )
    for first in range(0, length, block):
        rows = pl.ds(first, block)
        mixed = None
        logs = None
        for head in range(heads):
            select = (lane // head_dim == head).astype(F32).astype(BF16)
            queries = q_ref[rows, :] * select
            near = jnp.where(below, dot_nt(queries, k_ref[rows, :]), -1e30)
            peak = jnp.max(near, axis=1, keepdims=True)
            if first:
                far = dot_nt(queries, k_ref[pl.ds(0, first), :])
                peak = jnp.maximum(peak, jnp.max(far, axis=1, keepdims=True))
            near = jnp.exp(near - peak)
            total = jnp.sum(near, axis=1, keepdims=True)
            part = dot_nn(near.astype(BF16), v_ref[rows, :])
            if first:
                far = jnp.exp(far - peak)
                total = total + jnp.sum(far, axis=1, keepdims=True)
                part = part + dot_nn(far.astype(BF16), v_ref[pl.ds(0, first), :])
            part = part * (1.0 / total)
            log_total = jnp.broadcast_to(peak + jnp.log(total), (block, LANES))
            mixed = part if head == 0 else jnp.where(own_lane == head, part, mixed)
            logs = log_total if head == 0 else jnp.where(own_lane == head, log_total, logs)
        o_ref[rows, :] = mixed.astype(BF16)
        lse_tile[rows, :] = logs
    turned = lse_tile[...].T
    for head in range(heads):
        lse_ref[pl.ds(head * 8, 8), :] = turned[head * head_dim : head * head_dim + 8, :]


def attend_forward(normed, w_qkv, cosine, sine, length, head_dim):
    tokens, width = normed.shape
    seqs, pairs, heads = tokens // length, width // LANES, LANES // head_dim
    block = min(256, length)
    rows = pl.BlockSpec((length, LANES), lambda s, p: (s, p))

    def weight(part):
        return pl.BlockSpec((width, LANES), lambda s, p: (0, part * pairs + p))

    table = whole((length, LANES))
    return call(
        functools.partial(attend_forward_kernel, head_dim, block),
        (seqs, pairs),
        [pl.BlockSpec((length, width), lambda s, p: (s, 0)), weight(0), weight(1), weight(2), table, table],
        [rows, rows, rows, rows, pl.BlockSpec((8 * heads, length), lambda s, p: (s * pairs + p, 0))],
        [shape_of((tokens, width), BF16)] * 4 + [shape_of((seqs * pairs * 8 * heads, length), F32)],
        scratch=[pltpu.VMEM((length, LANES), F32)],
        flops=6 * tokens * width * width + 4 * tokens * length * width,
        moved=16 * tokens * width,
        trans=tokens * length * width // head_dim // 2,
    )(normed, w_qkv, w_qkv, w_qkv, cosine, sine)


def attend_backward_kernel(
    head_dim, block, q_ref, k_ref, v_ref, o_ref, g_ref, lse_ref, cos_ref, sin_ref, gq_ref, gk_ref, gv_ref, gq_acc
):
    length = q_ref.shape[0]
    heads = LANES // head_dim
    scale = 1.0 / math.sqrt(head_dim)
    product = (g_ref[...].astype(F32) * o_ref[...].astype(F32)).T
    inner = [
        jnp.sum(product[head * head_dim : (head + 1) * head_dim, :], axis=0, keepdims=True)
        for head in range(heads)
    ]
    gq_acc[...] = jnp.zeros_like(gq_acc)
    lane = lax.broadcasted_iota(jnp.int32, (1, LANES), 1)
    own_lane = lax.broadcasted_iota(jnp.int32, (block, LANES), 1) // head_dim
    above = lax.broadcasted_iota(jnp.int32, (block, block), 1) >= lax.broadcasted_iota(
        jnp.int32, (block, block), 0
    )
    for first in range(0, length, block):
        rows = pl.ds(first, block)
        keys_grad = None
        values_grad = None
        for head in range(heads):
            select = (lane // head_dim == head).astype(F32).astype(BF16)
            keys = k_ref[rows, :] * select
            values = v_ref[rows, :] * select
            log_total = lse_ref[pl.ds(head * 8, 1), :]
            pieces = [(first, block, True)]
            if first + block < length:
                pieces.append((first + block, length - first - block, False))
            keys_part = None
            values_part = None
            for start, count, diagonal in pieces:
                span = pl.ds(start, count)
                queries, grads = q_ref[span, :], g_ref[span, :]
                scores = dot_nt(keys, queries)
                probs = jnp.exp(scores - log_total[:, start : start + count])
                if diagonal:
                    probs = jnp.where(above, probs, 0.0)
                grad_probs = dot_nt(values, grads)
                grad_scores = (probs * (grad_probs - inner[head][:, start : start + count])).astype(BF16)
                piece_values = dot_nn(probs.astype(BF16), grads)
                piece_keys = dot_nn(grad_scores, queries)
                values_part = piece_values if values_part is None else values_part + piece_values
                keys_part = piece_keys if keys_part is None else keys_part + piece_keys
                gq_acc[span, :] += dot_tn(grad_scores, keys)
            keys_grad = keys_part if head == 0 else jnp.where(own_lane == head, keys_part, keys_grad)
            values_grad = values_part if head == 0 else jnp.where(own_lane == head, values_part, values_grad)
        gk_ref[rows, :] = turn(keys_grad, cos_ref[rows, :], -sin_ref[rows, :], head_dim).astype(BF16)
        gv_ref[rows, :] = values_grad.astype(BF16)
    gq_ref[...] = turn(gq_acc[...] * scale, cos_ref[...], -sin_ref[...], head_dim).astype(BF16)


def attend_backward(queries, keys, values, mixed, grad_mixed, lse, cosine, sine, length, head_dim):
    tokens, width = queries.shape
    seqs, pairs, heads = tokens // length, width // LANES, LANES // head_dim
    block = min(256, length)
    rows = pl.BlockSpec((length, LANES), lambda s, p: (s, p))
    table = whole((length, LANES))
    return call(
        functools.partial(attend_backward_kernel, head_dim, block),
        (seqs, pairs),
        [rows] * 5 + [pl.BlockSpec((8 * heads, length), lambda s, p: (s * pairs + p, 0)), table, table],
        [rows] * 3,
        [shape_of((tokens, width), BF16)] * 3,
        scratch=[pltpu.VMEM((length, LANES), F32)],
        flops=10 * tokens * length * width,
        moved=16 * tokens * width,
        trans=tokens * length * width // head_dim // 2,
    )(queries, keys, values, mixed, grad_mixed, lse, cosine, sine)


def square(width, part):
    return pl.BlockSpec((width, width), lambda i: (0, part), pipeline_mode=pl.Buffered(1))


def norm_one_kernel(x_ref, gain_ref, out_ref):
    x = x_ref[...].astype(F32)
    scale = lax.rsqrt(jnp.mean(x * x, axis=1, keepdims=True) + EPSILON)
    out_ref[...] = (x * scale * gain_ref[...]).astype(BF16)


def norm_one(tokens, gain):
    rows, width = tokens.shape
    block = min(256, rows)
    blocked = pl.BlockSpec((block, width), lambda i: (i, 0))
    return call(
        norm_one_kernel, (rows // block,), [blocked, whole((1, width))], blocked, shape_of((rows, width), BF16),
        flops=5 * rows * width, moved=4 * rows * width,
    )(tokens, gain)


def norm_two_kernel(mixed_ref, tokens_ref, weight_ref, gain_ref, sum_ref, normed_ref):
    first_sum = tokens_ref[...].astype(F32) + dot_nn(mixed_ref[...], weight_ref[...])
    sum_ref[...] = first_sum
    scale = lax.rsqrt(jnp.mean(first_sum * first_sum, axis=1, keepdims=True) + EPSILON)
    normed_ref[...] = (first_sum * scale * gain_ref[...]).astype(BF16)


def norm_two(mixed, tokens, weight, gain):
    rows, width = tokens.shape
    block = min(256, rows)
    blocked = pl.BlockSpec((block, width), lambda i: (i, 0))
    return call(
        norm_two_kernel, (rows // block,), [blocked, blocked, square(width, 3), whole((1, width))],
        [blocked, blocked], [shape_of((rows, width), F32), shape_of((rows, width), BF16)],
        flops=2 * rows * width * width, moved=10 * rows * width,
    )(mixed, tokens, weight, gain)


def slots_kernel(experts, parts, capacity, routes_ref, live_ref, rows_ref, columns_ref):
    top, tokens = routes_ref.shape
    live = live_ref[...]
    number = lax.broadcasted_iota(jnp.int32, (experts, tokens), 0)
    hits = [
        jnp.where((routes_ref[pl.ds(k, 1), :] == number) & (live > 0), 1.0, 0.0) for k in range(top)
    ]
    earlier = jnp.where(
        lax.broadcasted_iota(jnp.int32, (tokens, tokens), 0)
        <= lax.broadcasted_iota(jnp.int32, (tokens, tokens), 1),
        1.0,
        0.0,
    ).astype(BF16)
    ranks = dot_nn(jnp.concatenate(hits, axis=0).astype(BF16), earlier)
    before = jnp.zeros((experts, 1), F32)
    expert = lax.broadcasted_iota(jnp.int32, (experts, tokens), 0)
    start = ((expert % parts) * (experts // parts) + expert // parts) * capacity
    found = []
    for k in range(top):
        rank = ranks[k * experts : (k + 1) * experts, :] + before - 1.0
        for first in (number * capacity, start):
            slot = jnp.sum(hits[k] * (first.astype(F32) + rank), axis=0, keepdims=True).astype(jnp.int32)
            found.append(jnp.where(live > 0, slot, experts * capacity))
        before = before + jnp.sum(hits[k], axis=1, keepdims=True)
    table = jnp.concatenate(found[0::2] + found[1::2] + [jnp.zeros((8 - 2 * top, tokens), jnp.int32)], axis=0)
    rows_ref[...] = table
    columns_ref[...] = table.T


def slots_of(routes_t, live_row, experts, parts, capacity):
    top, tokens = routes_t.shape
    return call(
        functools.partial(slots_kernel, experts, parts, capacity), (1,),
        [whole((top, tokens)), whole((1, tokens))], [whole((8, tokens)), whole((tokens, 8))],
        [shape_of((8, tokens), jnp.int32), shape_of((tokens, 8), jnp.int32)],
        flops=2 * top * experts * tokens * tokens, moved=16 * tokens,
    )(routes_t, live_row)


def dispatch_kernel(gated, first, base, dest_ref, gates_ref, x_ref, out_ref):
    top, tokens = gates_ref.shape
    capacity = out_ref.shape[0]
    slot = lax.broadcasted_iota(jnp.int32, (capacity, tokens), 0) + (first + pl.program_id(0)) * capacity
    hits = [slot == dest_ref[pl.ds(base + k, 1), :] for k in range(top)]
    chosen = functools.reduce(jnp.logical_or, hits)
    rows = dot_nn(jnp.where(chosen, 1.0, 0.0).astype(BF16), x_ref[...])
    if gated:
        weights = jnp.zeros((capacity, tokens), F32)
        for k in range(top):
            weights = jnp.where(hits[k], gates_ref[pl.ds(k, 1), :], weights)
        rows = rows * jnp.sum(weights, axis=1, keepdims=True)
    out_ref[...] = rows.astype(BF16)


def dispatch(dest_t, gates_t, x, experts, capacity, gated, first, base):
    top, tokens = gates_t.shape
    width = x.shape[1]
    return call(
        functools.partial(dispatch_kernel, gated, first, base), (experts,),
        [whole(dest_t.shape), whole((top, tokens)), whole((tokens, width))],
        pl.BlockSpec((capacity, width), lambda e: (e, 0)),
        shape_of((experts * capacity, width), BF16),
        flops=2 * experts * capacity * tokens * width, moved=2 * (experts * capacity + tokens) * width,
    )(dest_t, gates_t, x)


def unpack(source, start, rows, panels, target):
    for p in range(panels):
        target[:, pl.ds(p * LANES, LANES)] = source[pl.ds(start + p * rows, rows), :].astype(F32)


def combine_kernel(dest_ref, gates_ref, live_ref, sum_ref, shared_ref, y_ref, out_ref):
    block, top = gates_ref.shape
    total = sum_ref[...] + shared_ref[...]
    dest = dest_ref[...]
    gates = gates_ref[...]
    slot = slot_numbers(block, y_ref.shape[0], 0)
    for k in range(top):
        hit = jnp.where(slot == dest[:, k : k + 1], 1.0, 0.0).astype(BF16)
        total = total + dot_nn(hit, y_ref[...]) * gates[:, k : k + 1]
    out_ref[...] = (live_ref[...] * total).astype(BF16)


def combine(dest, gates, live, first_sum, shared_out, returned):
    rows, width = first_sum.shape
    top = gates.shape[1]
    block = min(256, rows)
    blocked = pl.BlockSpec((block, width), lambda i: (i, 0))
    slots = returned.shape[0]
    return call(
        combine_kernel, (rows // block,),
        [pl.BlockSpec((block, dest.shape[1]), lambda i: (i, 0)), pl.BlockSpec((block, top), lambda i: (i, 0)),
         pl.BlockSpec((block, 1), lambda i: (i, 0)), blocked, blocked, whole(returned.shape)],
        blocked, shape_of((rows, width), BF16),
        flops=4 * rows * slots * width, moved=10 * rows * width + 2 * slots * width,
    )(dest, gates, live, first_sum, shared_out, returned)


def unpack(source, start, rows, panels, target):
    for p in range(panels):
        target[:, pl.ds(p * LANES, LANES)] = source[pl.ds(start + p * rows, rows), :].astype(F32)


def lay_out_kernel(parts, own, gu_panels, shared_ref, pack_ref, egu_ref, ed_ref, sgu_ref, sd_ref):
    step = pl.program_id(0)
    width = ed_ref.shape[2]
    packed = pack_ref.shape[0] // parts
    e_panels, e_rows = egu_ref.shape[2] // LANES, egu_ref.shape[1]
    for e in range(parts):
        for p in range(e_panels):
            rows = pl.ds(pl.multiple_of(e * packed + p * width + step * e_rows, 16), e_rows)
            egu_ref[e, :, pl.ds(p * LANES, LANES)] = pack_ref[rows, :].astype(F32)

    @pl.when(step == 0)
    def _():
        for e in range(parts):
            unpack(pack_ref, e * packed + e_panels * width, ed_ref.shape[1], width // LANES, ed_ref.at[e])

    @pl.when(step == pl.num_programs(0) - 1)
    def _():
        unpack(shared_ref, 0, own, gu_panels, sgu_ref)
        unpack(shared_ref, gu_panels * own, sd_ref.shape[0], width // LANES, sd_ref)


def lay_out(shared, pack, parts, own, width, shared_hidden, hidden):
    group, steps = width // own, 4
    columns = 2 * hidden // group
    outs = [
        (parts, width, columns), (parts, hidden // group, width), (own, 2 * shared_hidden), (shared_hidden // group, width)
    ]
    return call(
        functools.partial(lay_out_kernel, parts, own, 2 * shared_hidden // LANES), (steps,),
        [whole(shared.shape), whole(pack.shape)],
        [pl.BlockSpec((parts, width // steps, columns), lambda i: (0, i, 0))] + [whole(shape) for shape in outs[1:]],
        [shape_of(shape, F32) for shape in outs],
        flops=shared.size + pack.size, moved=6 * (shared.size + pack.size),
    )(shared, pack)


def lay_out_attention_kernel(own, x_ref, qkv_ref, wo_ref, gain_ref):
    panels = wo_ref.shape[1] // LANES
    unpack(x_ref, 0, own, 3 * panels, qkv_ref)
    unpack(x_ref, 3 * panels * own, own, panels, wo_ref)
    gain_ref[...] = x_ref[pl.ds(4 * panels * own, gain_ref.shape[0]), :].astype(F32)


def lay_out_attention(x, own, width):
    outs = [(own, 3 * width), (own, width), (8, LANES)]
    return call(
        functools.partial(lay_out_attention_kernel, own), (1,), [whole(x.shape)], [whole(shape) for shape in outs],
        [shape_of(shape, F32) for shape in outs], flops=x.size, moved=6 * x.size,
    )(x)


def slot_numbers(block, slots, part):
    return lax.broadcasted_iota(jnp.int32, (block, slots), 1) + part * slots


def gathered(top, dest_ref, y_ref, part):
    block = dest_ref.shape[0]
    dest = dest_ref[:, top : 2 * top]
    slot = slot_numbers(block, y_ref.shape[0], part)
    hit = functools.reduce(jnp.logical_or, [slot == dest[:, k : k + 1] for k in range(top)])
    return dot_nn(jnp.where(hit, 1.0, 0.0).astype(BF16), y_ref[...])


class Exchange:
    def __init__(self, axis, count, sent_ref, kept_ref, own_sem, send_sem, recv_sem):
        self.axis, self.count = axis, count
        me = lax.axis_index(axis)
        self.peers = [lax.rem(me + ahead, count) for ahead in range(1, count)]
        self.me, self.sent_ref, self.kept_ref = me, sent_ref, kept_ref
        self.own_sem, self.send_sem, self.recv_sem = own_sem, send_sem, recv_sem

    def copies(self):
        out = [pltpu.make_async_copy(self.sent_ref.at[self.me], self.kept_ref.at[self.me], self.own_sem)]
        for index, peer in enumerate(self.peers):
            out.append(
                pltpu.make_async_remote_copy(
                    src_ref=self.sent_ref.at[peer], dst_ref=self.kept_ref.at[self.me],
                    send_sem=self.send_sem.at[index], recv_sem=self.recv_sem.at[index],
                    device_id={self.axis: peer}, device_id_type=pl.DeviceIdType.MESH,
                )
            )
        return out

    def start(self):
        barrier = pltpu.get_barrier_semaphore()
        for peer in self.peers:
            pl.semaphore_signal(barrier, inc=1, device_id={self.axis: peer}, device_id_type=pl.DeviceIdType.MESH)
        pl.semaphore_wait(barrier, self.count - 1)
        for copy in self.copies():
            copy.start()

    def wait(self):
        for copy in self.copies():
            copy.wait()

    @staticmethod
    def scratch(count):
        sems = pltpu.SemaphoreType.DMA((count - 1,))
        return [pltpu.SemaphoreType.DMA, sems, sems]


def add_part_kernel(part, top, axis, count, dest_ref, base_ref, y_ref, sent_ref, out_ref, kept_ref, *sems):
    exchange = Exchange(axis, count, sent_ref, kept_ref, *sems)

    @pl.when(pl.program_id(0) == 0)
    def _():
        exchange.start()

    out_ref[...] = base_ref[...] + gathered(top, dest_ref, y_ref, part)

    @pl.when(pl.program_id(0) == pl.num_programs(0) - 1)
    def _():
        exchange.wait()


def add_part(top, dest, base, rows_of, part, sent, axis, count, collective_id):
    rows, width = base.shape
    block = min(256, rows)
    blocked = pl.BlockSpec((block, width), lambda i: (i, 0))
    hbm = pl.BlockSpec(memory_space=pl.ANY)
    sent = sent.reshape(count, -1, width)
    out, kept = call(
        functools.partial(add_part_kernel, part, top, axis, count), (rows // block,),
        [pl.BlockSpec((block, dest.shape[1]), lambda i: (i, 0)), blocked, whole(rows_of.shape), hbm],
        [blocked, hbm], [shape_of((rows, width), F32), shape_of(sent.shape, BF16)],
        scratch=Exchange.scratch(count),
        flops=2 * rows * rows_of.shape[0] * width, moved=8 * rows * width, collective_id=collective_id,
    )(dest, base, rows_of, sent)
    return out, kept.reshape(-1, width)


def norm_two_back_kernel(part, top, dest_ref, live_ref, cot_ref, sum_ref, base_ref, gain_ref, weight_ref, y_ref,
                         first_ref, attn_ref, mixed_ref, gain_grad_ref):
    grad_normed = base_ref[...] + gathered(top, dest_ref, y_ref, part)
    first_sum = sum_ref[...]
    scale = lax.rsqrt(jnp.mean(first_sum * first_sum, axis=1, keepdims=True) + EPSILON)
    weighted = grad_normed * gain_ref[...]
    inner = jnp.mean(first_sum * weighted, axis=1, keepdims=True)
    grad_first = (
        cot_ref[...].astype(F32) * live_ref[...] + scale * weighted - first_sum * (scale * scale * scale * inner)
    )
    first_ref[...] = grad_first
    grad_attn = grad_first.astype(BF16)
    attn_ref[...] = grad_attn
    mixed_ref[...] = dot_nt(grad_attn, weight_ref[...]).astype(BF16)

    @pl.when(pl.program_id(0) == 0)
    def _():
        gain_grad_ref[...] = jnp.zeros_like(gain_grad_ref)

    gain_grad_ref[...] += jnp.sum(grad_normed * first_sum * scale, axis=0, keepdims=True)


def norm_two_back(top, dest, live, cotangent, first_sum, base, gain, weights, rows_of, part):
    rows, width = first_sum.shape
    block = min(256, rows)
    blocked = pl.BlockSpec((block, width), lambda i: (i, 0))
    return call(
        functools.partial(norm_two_back_kernel, part, top), (rows // block,),
        [pl.BlockSpec((block, dest.shape[1]), lambda i: (i, 0)), pl.BlockSpec((block, 1), lambda i: (i, 0)), blocked, blocked,
         blocked, whole((1, width)), square(width, 3), whole(rows_of.shape)],
        [blocked, blocked, blocked, pl.BlockSpec((1, width), lambda i: (0, 0))],
        [shape_of((rows, width), F32), shape_of((rows, width), BF16), shape_of((rows, width), BF16),
         shape_of((1, width), F32)],
        flops=2 * rows * (rows_of.shape[0] + width) * width, moved=18 * rows * width,
    )(dest, live, cotangent, first_sum, base, gain, weights, rows_of)


def line_copy(axis, ahead, source, target, send_sem, recv_sem):
    return pltpu.make_async_remote_copy(
        src_ref=source, dst_ref=target, send_sem=send_sem, recv_sem=recv_sem,
        device_id={axis: lax.axis_index(axis) + ahead}, device_id_type=pl.DeviceIdType.MESH,
    )


class LineSum:
    def __init__(self, axis, count, x_ref, buffers, send_sem, recv_sem, turn, turns):
        self.axis, self.count, self.x_ref, self.buffers = axis, count, x_ref, buffers
        self.send_sem, self.recv_sem = send_sem, recv_sem
        self.rows, self.turn, self.turns = buffers.shape[3], turn, turns

    def own(self, piece):
        first = (piece * self.turns + self.turn) * self.rows
        return self.x_ref[pl.ds(pl.multiple_of(first, 16), self.rows), :].astype(F32)

    def copy(self, way, piece):
        return line_copy(
            self.axis, 1 - 2 * way, self.buffers.at[way, 1, piece], self.buffers.at[way, 0, piece],
            self.send_sem.at[way, piece], self.recv_sem.at[way, piece],
        )

    def each(self, body):
        me = lax.axis_index(self.axis)
        for k in range(self.count - 1):
            for way, piece in ((0, self.count - 1 - k), (1, k)):
                before = me > 0 if way == 0 else me < self.count - 1
                sends = me < piece if way == 0 else me > piece
                body(way, piece, before, sends)

    def start(self):
        def body(way, piece, before, sends):
            @pl.when(sends & jnp.logical_not(before))
            def _():
                self.buffers[way, 1, piece] = self.own(piece).astype(BF16)
                self.copy(way, piece).start()

        self.each(body)

    def relay(self):
        def body(way, piece, before, sends):
            @pl.when(sends & before)
            def _():
                self.copy(way, piece).wait_recv()
                self.buffers[way, 1, piece] = (self.own(piece) + self.buffers[way, 0, piece].astype(F32)).astype(BF16)
                self.copy(way, piece).start()

        self.each(body)

    def finish(self, total_ref):
        me = lax.axis_index(self.axis)
        total_ref[...] = self.own(me)
        for way, before in ((0, me > 0), (1, me < self.count - 1)):

            @pl.when(before)
            def _():
                self.copy(way, me).wait_recv()
                total_ref[...] += self.buffers[way, 0, me].astype(F32)

        def body(way, piece, before, sends):
            @pl.when(sends)
            def _():
                self.copy(way, piece).wait_send()

        self.each(body)


class LineGather:
    def __init__(self, axis, count, out_ref, send_sem, recv_sem, turn, turns):
        self.axis, self.count, self.out_ref = axis, count, out_ref
        self.send_sem, self.recv_sem = send_sem, recv_sem
        self.rows, self.turn, self.turns = out_ref.shape[0] // count // turns, turn, turns

    def place(self, piece):
        first = (piece * self.turns + self.turn) * self.rows
        return self.out_ref.at[pl.ds(pl.multiple_of(first, 16), self.rows), :]

    def copy(self, way, piece):
        return line_copy(
            self.axis, 1 - 2 * way, self.place(piece), self.place(piece),
            self.send_sem.at[way, piece], self.recv_sem.at[way, piece],
        )

    def start(self, value):
        me = lax.axis_index(self.axis)
        self.place(me)[...] = value
        for way, more in ((0, me < self.count - 1), (1, me > 0)):

            @pl.when(more)
            def _():
                self.copy(way, me).start()

    def relay(self, k):
        me = lax.axis_index(self.axis)
        for way, piece, there, more in (
            (0, me - k, me >= k, me < self.count - 1),
            (1, me + k, me + k < self.count, me > 0),
        ):

            @pl.when(there)
            def _():
                self.copy(way, piece).wait_recv()

            @pl.when(there & more)
            def _():
                self.copy(way, piece).start()

    def finish(self):
        me = lax.axis_index(self.axis)
        for k in range(self.count):
            for way, piece, sent in (
                (0, me - k, (me >= k) & (me < self.count - 1)),
                (1, me + k, (me + k < self.count) & (me > 0)),
            ):

                @pl.when(sent)
                def _():
                    self.copy(way, piece).wait_send()


def greet_neighbours(barrier, axis, count):
    me = lax.axis_index(axis)
    for ahead, there in ((1, me < count - 1), (-1, me > 0)):

        @pl.when(there)
        def _():
            pl.semaphore_signal(barrier, inc=1, device_id={axis: me + ahead}, device_id_type=pl.DeviceIdType.MESH)

    return (me < count - 1).astype(jnp.int32) + (me > 0).astype(jnp.int32)


def settle_kernel(sizes, gq_ref, gk_ref, gv_ref, wq_ref, wk_ref, wv_ref, tokens_ref, first_ref, gain_ref, pack_ref,
                  x_ref, out_ref, share_ref, all_ref, own, landed, chosen, arrived, sem, pair_send, pair_recv, send_sem,
                  recv_sem, x_buffers, x_total, x_all, x_send, x_recv, g_send, g_recv):
    dp_size, shard_size, count = sizes
    spread = shard_size // 2
    halves = dp_size * spread
    dp, shard = lax.axis_index("dp"), lax.axis_index("shard")
    side = shard % 2
    place = dp * spread + shard // 2
    step = pl.program_id(0)
    last = pl.num_programs(0) - 1

    def target(piece, bit):
        return {"dp": piece // spread, "shard": (piece % spread) * 2 + bit}

    turns = x_buffers.shape[0]
    lines = [
        LineSum("expert", count, x_ref, x_buffers.at[t], x_send.at[t], x_recv.at[t], t, turns) for t in range(turns)
    ]
    gathers = [LineGather("expert", count, x_all, g_send.at[t], g_recv.at[t], t, turns) for t in range(turns)]

    def pair_copy():
        return pltpu.make_async_remote_copy(
            src_ref=pack_ref.at[:, 1 - side], dst_ref=landed, send_sem=pair_send, recv_sem=pair_recv,
            device_id=target(place, 1 - side), device_id_type=pl.DeviceIdType.MESH,
        )

    def own_copy():
        return pltpu.make_async_copy(pack_ref.at[:, side], own, sem)

    def send(index):
        return pltpu.make_async_remote_copy(
            src_ref=chosen.at[index], dst_ref=arrived.at[index], send_sem=send_sem.at[index], recv_sem=recv_sem.at[index],
            device_id=target(lax.rem(place + index + 1, halves), side), device_id_type=pl.DeviceIdType.MESH,
        )

    @pl.when(step == 0)
    def _():
        barrier = pltpu.get_barrier_semaphore()
        pl.semaphore_signal(barrier, inc=1, device_id=target(place, 1 - side), device_id_type=pl.DeviceIdType.MESH)
        for index in range(halves - 1):
            pl.semaphore_signal(
                barrier, inc=1, device_id=target(lax.rem(place + index + 1, halves), side),
                device_id_type=pl.DeviceIdType.MESH,
            )
        neighbours = greet_neighbours(barrier, "expert", count)
        pl.semaphore_wait(barrier, halves + neighbours)
        pair_copy().start()
        own_copy().start()
        lines[0].start()

    @pl.when(step == 1)
    def _():
        own_copy().wait()
        pair_copy().wait()
        for index in range(halves - 1):
            piece = lax.rem(place + index + 1, halves)
            chosen[index] = (own[piece].astype(F32) + landed[piece].astype(F32)).astype(BF16)
            send(index).start()

    grad_normed = (
        dot_nt(gq_ref[...], wq_ref[...]) + dot_nt(gk_ref[...], wk_ref[...]) + dot_nt(gv_ref[...], wv_ref[...])
    )
    source = tokens_ref[...].astype(F32)
    scale = lax.rsqrt(jnp.mean(source * source, axis=1, keepdims=True) + EPSILON)
    weighted = grad_normed * gain_ref[...]
    inner = jnp.mean(source * weighted, axis=1, keepdims=True)
    out_ref[...] = first_ref[...] + scale * weighted - source * (scale * scale * scale * inner)

    @pl.when(step == last)
    def _():
        for t in range(turns):
            if t:
                lines[t].start()
            lines[t].relay()
            if t:
                gathers[t - 1].relay(1)
            lines[t].finish(x_total)
            gathers[t].start(x_total[...].astype(BF16))
        for k in range(1, count):
            for t in range(turns):
                if k > 1 or t == turns - 1:
                    gathers[t].relay(k)
        total = own[place].astype(F32) + landed[place].astype(F32)
        for index in range(halves - 1):
            send(index).wait()
            total = total + arrived[index].astype(F32)
        share_ref[...] = total.astype(BF16)
        for gather in gathers:
            gather.finish()
        all_ref[...] = x_all[...]


def settle(grads, w_qkv, tokens, grad_first, gain, pack, x, sizes):
    rows, width = tokens.shape
    block = min(256, rows)
    blocked = pl.BlockSpec((block, width), lambda i: (i, 0))
    halves, count = sizes[0] * sizes[1] // 2, pack.shape[1]
    piece = (count, LANES)
    turns = 2 if x.shape[0] // sizes[2] % 32 == 0 else 1
    x_piece = (x.shape[0] // sizes[2] // turns, LANES)
    return call(
        functools.partial(settle_kernel, sizes), (rows // block,),
        [blocked] * 3 + [square(width, 0), square(width, 1), square(width, 2), blocked, blocked, whole((1, width)),
                         pl.BlockSpec(memory_space=pl.ANY), whole(x.shape)],
        [blocked, whole(piece), whole(x.shape)],
        [shape_of((rows, width), F32), shape_of(piece, BF16), shape_of(x.shape, BF16)],
        scratch=[pltpu.VMEM((halves,) + piece, BF16), pltpu.VMEM((halves,) + piece, BF16),
                 pltpu.VMEM((halves - 1,) + piece, BF16), pltpu.VMEM((halves - 1,) + piece, BF16),
                 pltpu.SemaphoreType.DMA, pltpu.SemaphoreType.DMA, pltpu.SemaphoreType.DMA,
                 pltpu.SemaphoreType.DMA((halves - 1,)), pltpu.SemaphoreType.DMA((halves - 1,)),
                 pltpu.VMEM((turns, 2, 2, sizes[2]) + x_piece, BF16), pltpu.VMEM(x_piece, F32), pltpu.VMEM(x.shape, BF16)]
        + [pltpu.SemaphoreType.DMA((turns, 2, sizes[2]))] * 4,
        flops=6 * rows * width * width, moved=22 * rows * width, collective_id=1,
    )(*grads, w_qkv, w_qkv, w_qkv, tokens, grad_first, gain, pack.reshape((halves, 2) + piece), x)


def copies_of(layout, block, width, step, stage_g, stage_u, stage_d, slot, packed_ref, sems):
    by_rows, owners, hidden, base = layout
    panels = block // LANES
    rows_down = hidden // owners
    out = []

    def add(source, target):
        out.append(pltpu.make_async_copy(source, target, sems.at[slot, len(out)]))

    if by_rows:
        rows = width // owners
        for half, stage in enumerate((stage_g, stage_u)):
            for p in range(panels):
                panel = half * (hidden // LANES) + step * panels + p
                add(
                    stage.at[slot, :, :, pl.ds(p * LANES, LANES)],
                    packed_ref.at[:, pl.ds(pl.multiple_of(base + panel * rows, 8), rows), :],
                )
        start = 2 * hidden // LANES * rows
    else:
        columns = 2 * hidden // owners
        for half, stage in enumerate((stage_g, stage_u)):
            for p in range(panels):
                column = half * hidden + step * block + p * LANES
                owner, panel = column // columns, (column % columns) // LANES
                add(
                    stage.at[slot, :, pl.ds(p * LANES, LANES)],
                    packed_ref.at[owner, pl.ds(pl.multiple_of(base + panel * width, 8), width), :],
                )
        start = columns // LANES * width
    for q in range(block // rows_down):
        owner = step * (block // rows_down) + q
        for c in range(width // LANES):
            add(
                stage_d.at[slot, pl.ds(q * rows_down, rows_down), pl.ds(c * LANES, LANES)],
                packed_ref.at[owner, pl.ds(base + start + c * rows_down, rows_down), :],
            )
    return out


def packed_rows(width, hidden, owners):
    return 3 * width * hidden // owners // LANES


def ffn_kernel(out_type, layout, block, first, axis, count, x_ref, gy_ref, wg_ref, wu_ref, wd_ref, sent_ref, *rest):
    (y_ref, gx_ref, packed_ref, kept_ref, x_own, gy_own, xt, y_acc, gx_acc, stage_g, stage_u, stage_d, sems, load_sems,
     *exchange_sems) = rest[-17:]
    exchange = Exchange(axis, count, sent_ref, kept_ref, *exchange_sems)
    step = pl.program_id(0)
    steps = layout[2] // block
    width = x_ref.shape[1]
    slot = step % 2
    copies = functools.partial(copies_of, layout, block, width)

    @pl.when(step == 0)
    def _():
        exchange.start()
        gy_source = gy_ref if first is None else gy_ref.at[:, pl.ds(first, gy_own.shape[1]), :]
        loads = [
            pltpu.make_async_copy(x_ref, x_own, load_sems.at[0]),
            pltpu.make_async_copy(gy_source, gy_own, load_sems.at[1]),
        ]
        for load in loads:
            load.start()
        for load in loads:
            load.wait()
        xt[...] = x_own[...].T
        y_acc[...] = jnp.zeros_like(y_acc)
        gx_acc[...] = jnp.zeros_like(gx_acc)

    @pl.when(step >= 2)
    def _():
        for copy in copies(step - 2, stage_g, stage_u, stage_d, slot, packed_ref, sems):
            copy.wait()

    x, gy = x_own[...], gy_own[...].reshape(x_ref.shape)
    if layout[0]:
        wg, wu = wg_ref[...].reshape(width, block), wu_ref[...].reshape(width, block)
        rows = wd_ref.shape[1] // (width // block)
        wd = jnp.concatenate(
            [wd_ref[:, pl.ds(c * rows, rows), :].reshape(block, block) for c in range(width // block)], axis=1
        )
    else:
        wg, wu, wd = wg_ref[...], wu_ref[...], wd_ref[...]
    gate, up = dot_nn(x, wg), dot_nn(x, wu)
    grad_hidden = dot_nt(gy, wd)
    sigmoid = jax.nn.sigmoid(gate)
    value = gate * sigmoid
    hidden = (value * up).astype(BF16)
    grad_up = (grad_hidden * value).astype(BF16)
    grad_gate = (grad_hidden * up * (sigmoid * (1.0 + gate * (1.0 - sigmoid)))).astype(BF16)
    y_acc[...] += dot_nn(hidden, wd)
    gx_acc[...] += dot_nt(grad_gate, wg) + dot_nt(grad_up, wu)
    stage_g[slot] = dot_nn(xt[...], grad_gate).astype(BF16).reshape(stage_g.shape[1:])
    stage_u[slot] = dot_nn(xt[...], grad_up).astype(BF16).reshape(stage_u.shape[1:])
    stage_d[slot] = dot_tn(hidden, gy).astype(BF16)
    for copy in copies(step, stage_g, stage_u, stage_d, slot, packed_ref, sems):
        copy.start()

    @pl.when(step == steps - 1)
    def _():
        exchange.wait()
        y_ref[...] = y_acc[...].astype(out_type).reshape(y_ref.shape)
        gx_ref[...] = gx_acc[...].astype(out_type)
        for back in (1, 0):
            if steps > back:
                for copy in copies(steps - 1 - back, stage_g, stage_u, stage_d, (steps - 1 - back) % 2, packed_ref, sems):
                    copy.wait()


BLOCK = 256


def ffn_both(x, gy, w_gu, w_down, hidden, expert, owners, out_type, sent, axis, count, collective_id, parts=1, held=()):
    rows, width = x.shape
    block = BLOCK
    steps = hidden // block
    by_rows = expert is None
    if by_rows:
        own, own_down, panels = width // owners, hidden // owners, width // block
        ahead = 2 * steps * own // (panels * own_down)
        gate = pl.BlockSpec((owners, own, block), lambda f: (0, f, 0))
        up = pl.BlockSpec((owners, own, block), lambda f: (0, steps + f, 0))
        down = pl.BlockSpec((block // own_down, panels * own_down, block), lambda f: (f, ahead, 0))
        stage = (2, owners, own, block)
    else:
        gate = pl.BlockSpec((None, width, block), lambda f: (expert, 0, f))
        up = pl.BlockSpec((None, width, block), lambda f: (expert, 0, steps + f))
        down = pl.BlockSpec((None, block, width), lambda f: (expert, f, 0))
        stage = (2, width, block)
    if by_rows:
        first, gy_shape = None, (rows, width)
        y_block, y_shape = whole((rows, width)), (rows, width)
    else:
        y_shape = (gy.shape[0], parts * (rows // gy.shape[0]), width)
        y_block = pl.BlockSpec(
            (gy.shape[0], rows // gy.shape[0], width), lambda f: (0, expert, 0), pipeline_mode=pl.Buffered(1)
        )
        first, gy_shape = expert * (rows // gy.shape[0]), (gy.shape[0], rows // gy.shape[0], width)
    out_rows = whole((rows, width))
    pack_rows = packed_rows(width, hidden, owners)
    layout = (by_rows, owners, hidden, (expert or 0) * pack_rows)
    hbm = pl.BlockSpec(memory_space=pl.ANY)
    sent = sent.reshape(count, -1, width)
    copies = 2 * (block // LANES) + block // (hidden // owners) * (width // LANES)
    y, gx, pack, kept = call(
        functools.partial(ffn_kernel, out_type, layout, block, first, axis, count), (steps,),
        [hbm, hbm, gate, up, down, hbm] + [hbm] * len(held),
        [y_block, out_rows, hbm, hbm],
        [shape_of(y_shape, out_type), shape_of((rows, width), out_type),
         shape_of((owners, parts * pack_rows, LANES), BF16), shape_of(sent.shape, BF16)],
        scratch=[pltpu.VMEM((rows, width), BF16), pltpu.VMEM(gy_shape, BF16),
                 pltpu.VMEM((width, rows), BF16), pltpu.VMEM((rows, width), F32), pltpu.VMEM((rows, width), F32),
                 pltpu.VMEM(stage, BF16), pltpu.VMEM(stage, BF16), pltpu.VMEM((2, block, width), BF16),
                 pltpu.SemaphoreType.DMA((2, copies)), pltpu.SemaphoreType.DMA((2,))] + Exchange.scratch(count),
        flops=18 * rows * width * hidden, moved=12 * width * hidden + 16 * rows * width, trans=rows * hidden,
        aliases={6: 0, 7: 2} if held else None, collective_id=collective_id,
    )(x, gy, w_gu, w_gu, w_down, sent, *held)
    return y, gx, pack, kept.reshape(-1, width)


def to_panels(array):
    rows, columns = array.shape
    return jnp.transpose(array.reshape(rows, columns // BLOCK, BLOCK), (1, 0, 2)).reshape(-1, BLOCK)


def attention_weights_kernel(per, normed_ref, mixed_ref, gq_ref, gk_ref, gv_ref, ga_ref, gains_ref, out_ref, xt):
    step = pl.program_id(0)
    owners, rows = out_ref.shape[0], out_ref.shape[1] // (out_ref.shape[1] // (normed_ref.shape[1] // out_ref.shape[0]))
    panels = out_ref.shape[1] // rows

    @pl.when(step == 0)
    def _():
        xt[...] = normed_ref[...].T

    @pl.when(step == 3 * per)
    def _():
        xt[...] = mixed_ref[...].T

    for index, grad_ref in enumerate((gq_ref, gk_ref, gv_ref, ga_ref)):

        @pl.when((step >= index * per) & (step < (index + 1) * per))
        def _():
            product = dot_nn(xt[...], grad_ref[...]).astype(BF16)
            for p in range(panels):
                out_ref[:, pl.ds(p * rows, rows), :] = product[:, p * LANES : (p + 1) * LANES].reshape(owners, rows, LANES)

    @pl.when(step >= 4 * per)
    def _():
        out_ref[...] = jnp.zeros_like(out_ref)

    @pl.when(step == 4 * per)
    def _():
        out_ref[:, pl.ds(0, gains_ref.shape[1]), :] = gains_ref[...]


def attention_weights(normed, mixed, grads, grad_attn, gains, owners, pieces):
    tokens, width = normed.shape
    rows = width // owners
    block = BLOCK
    panels, per = block // LANES, width // block
    steps = 4 * per + 1
    while steps * panels * rows % (16 * pieces):
        steps += 1

    def columns(index):
        return pl.BlockSpec((tokens, block), lambda i: (0, jnp.clip(i - index * per, 0, per - 1)))

    return call(
        functools.partial(attention_weights_kernel, per), (steps,),
        [whole((tokens, width)), whole((tokens, width))] + [columns(index) for index in range(4)] + [whole(gains.shape)],
        pl.BlockSpec((owners, panels * rows, LANES), lambda i: (0, i, 0)),
        shape_of((owners, steps * panels * rows, LANES), BF16),
        scratch=[pltpu.VMEM((width, tokens), BF16)],
        flops=8 * tokens * width * width, moved=16 * tokens * width,
    )(normed, mixed, *grads, grad_attn, gains)


GROUP = ("dp", "shard")


def local(
    tokens,
    lengths,
    routes,
    route_gates,
    cotangent,
    norm_gains,
    w_qkv,
    w_out,
    w_shared_gu,
    w_shared_down,
    w_expert_gu,
    w_expert_down,
):
    tok_count, width = tokens.shape
    seq_count = lengths.shape[0]
    length = tok_count // seq_count
    local_experts = w_expert_gu.shape[0]
    owners = lax.axis_size("expert")
    experts = local_experts * owners
    top = routes.shape[1]
    capacity = tok_count * top * 9 // (8 * experts)
    head_dim = width // HEADS
    hidden = w_expert_down.shape[1]

    gains = lax.all_gather(norm_gains, GROUP, axis=1, tiled=True).astype(F32)
    attention_weight = lax.all_gather(jnp.concatenate([w_qkv, w_out], axis=1), GROUP, axis=0, tiled=True)
    shared_weight = lax.all_gather(
        jnp.concatenate([to_panels(w_shared_gu), to_panels(w_shared_down)], axis=0)[None], GROUP, axis=0, tiled=True
    )
    gain_one, gain_two = gains[0:1], gains[1:2]

    live_bool = lax.iota(jnp.int32, tok_count) % length < jnp.repeat(lengths, length)
    live = live_bool.astype(F32)[:, None]
    live_row = live_bool.astype(jnp.int32)[None, :]

    group = lax.axis_size("dp") * lax.axis_size("shard")
    shared_hidden = w_shared_down.shape[0] * group

    table_t, table = slots_of(routes.T, live_row, experts, local_experts, capacity)
    gates_t = route_gates.T
    grad_b = jnp.where(live_bool[:, None], cotangent, 0).astype(BF16)

    def exchange(rows):
        return lax.all_to_all(
            rows.reshape(owners, -1, width), "expert", split_axis=0, concat_axis=0, tiled=True
        ).reshape(rows.shape)

    send_grad = dispatch(table_t, gates_t, cotangent, experts, capacity, True, 0, 0)
    received_grad = exchange(send_grad).reshape(owners, local_experts * capacity, width)

    cosine, sine = rotary_tables(length, head_dim)
    normed_one = norm_one(tokens, gain_one)
    queries, keys, values, mixed, lse = attend_forward(normed_one, attention_weight, cosine, sine, length, head_dim)
    first_sum, normed_two = norm_two(mixed, tokens, attention_weight, gain_two)

    send_rows = []
    for j in range(local_experts):
        send_rows.append(dispatch(table_t, gates_t, normed_two, owners, capacity, False, j * owners, top))
    shared_out, grad_shared, shared_pack, received = ffn_both(
        normed_two, grad_b, shared_weight, shared_weight, shared_hidden, None, group, F32,
        send_rows[0], "expert", owners, 3,
    )
    waiting = send_rows[1:]
    back_rows, base, held = [], grad_shared, ()
    for j in range(local_experts):
        y, gx, pack, arrived = ffn_both(
            received, received_grad, w_expert_gu, w_expert_down, hidden, j, group, BF16,
            waiting.pop(0), "expert", owners, 4 + j, local_experts, held,
        )
        held = (y, pack)
        waiting.append(gx)
        if j < local_experts - 1:
            received = arrived
        else:
            back_rows.append(arrived)
    for j, sent in enumerate(waiting):
        base, arrived = add_part(
            top, table, base, back_rows[j], j, sent, "expert", owners, 4 + local_experts + j
        )
        back_rows.append(arrived)
    y, base = lax.optimization_barrier((y, base))
    grad_first, grad_attn, grad_mixed, grad_gain_two = norm_two_back(
        top, table, live, cotangent, first_sum, base, gain_two, attention_weight, back_rows[-1], local_experts - 1
    )

    grads = attend_backward(queries, keys, values, mixed, grad_mixed, lse, cosine, sine, length, head_dim)
    own = width // group
    grad_gains = grad_gain_two.reshape(group, 1, own)
    grad_gains = jnp.pad(grad_gains, ((0, 0), (0, 15), (0, LANES - own))).astype(BF16)
    attention_pack = attention_weights(normed_one, mixed, grads, grad_attn, grad_gains, group, owners)

    def spread(pack):
        return lax.psum_scatter(pack, GROUP, scatter_dimension=0, tiled=True)[0]

    shared_share = spread(shared_pack)
    expert_share = spread(pack)
    input_grad, attention_share, shared_share = settle(
        grads, attention_weight, tokens, grad_first, gain_one, attention_pack, shared_share,
        (lax.axis_size("dp"), lax.axis_size("shard"), owners),
    )
    returned = exchange(y)
    pieces = lax.all_to_all(
        attention_share.reshape(owners, -1, LANES), "expert", split_axis=0, concat_axis=0, tiled=True
    )
    piece = jnp.sum(pieces.astype(F32), axis=0).astype(BF16)
    attention_share = lax.all_to_all(
        jnp.broadcast_to(piece[None], pieces.shape), "expert", split_axis=0, concat_axis=0, tiled=True
    ).reshape(attention_share.shape)
    layer_out = combine(table, route_gates, live, first_sum, shared_out, returned.reshape(-1, width))
    expert_gu, expert_down, shared_gu, shared_down = lay_out(
        shared_share, expert_share, local_experts, own, width, shared_hidden, hidden
    )
    qkv_grad, out_grad, gain_rows = lay_out_attention(attention_share, own, width)
    grad_gain_one = jnp.sum(w_qkv.astype(F32) * qkv_grad, axis=1) / norm_gains[0].astype(F32)
    grad_gains = jnp.stack([grad_gain_one, gain_rows[0, :own]])
    return layer_out, input_grad, grad_gains, qkv_grad, out_grad, shared_gu, shared_down, expert_gu, expert_down


def solution(mesh):
    rows = P(("dp", "expert", "shard"), None)
    split = P(GROUP, None)
    in_specs = (
        rows,
        P(("dp", "expert", "shard")),
        rows,
        rows,
        rows,
        P(None, GROUP),
        split,
        split,
        split,
        split,
        P("expert", None, None),
        P("expert", None, None),
    )
    out_specs = (
        rows,
        rows,
        P(None, GROUP),
        split,
        split,
        split,
        split,
        P("expert", None, GROUP),
        P("expert", GROUP, None),
    )

    return jax.shard_map(local, mesh=mesh, in_specs=in_specs, out_specs=out_specs, check_vma=False)
```

```python
import functools
import math

import jax
import jax.numpy as jnp
from jax import lax
from jax.experimental import pallas as pl
from jax.experimental.pallas import tpu as pltpu
from jax.sharding import PartitionSpec as P


HEADS = 12
LANES = 128
EPSILON = 1e-05
VMEM_BYTES = 60 * 1024 * 1024
BF16 = jnp.bfloat16
F32 = jnp.float32


def call(kernel, grid, in_specs, out_specs, out_shape, scratch=(), flops=0, moved=0, trans=0, collective_id=None, aliases=None):
    return pl.pallas_call(
        kernel,
        grid_spec=pltpu.PrefetchScalarGridSpec(
            num_scalar_prefetch=0,
            grid=grid,
            in_specs=in_specs,
            out_specs=out_specs,
            scratch_shapes=list(scratch),
        ),
        out_shape=out_shape,
        input_output_aliases=aliases or {},
        compiler_params=pltpu.CompilerParams(
            dimension_semantics=("arbitrary",) * len(grid), vmem_limit_bytes=VMEM_BYTES, collective_id=collective_id,
            has_side_effects=collective_id is not None,
        ),
        cost_estimate=pl.CostEstimate(flops=flops, bytes_accessed=moved, transcendentals=trans),
    )


def shape_of(shape, dtype):
    return jax.ShapeDtypeStruct(shape, dtype)


def whole(shape):
    return pl.BlockSpec(shape, lambda *_: (0,) * len(shape), pipeline_mode=pl.Buffered(1))


def dot_nn(left, right):
    return lax.dot_general(left, right, (((1,), (0,)), ((), ())), preferred_element_type=F32)


def dot_nt(left, right):
    return lax.dot_general(left, right, (((1,), (1,)), ((), ())), preferred_element_type=F32)


def dot_tn(left, right):
    return lax.dot_general(left, right, (((0,), (0,)), ((), ())), preferred_element_type=F32)


def rotary_tables(length, head_dim):
    half_dim = head_dim // 2
    position = lax.iota(F32, length)[:, None]
    frequency = jnp.exp(lax.iota(F32, half_dim) * (-2.0 * math.log(10000.0) / head_dim))
    angle_table = position * frequency[None, :]
    cosine, sine = jnp.cos(angle_table), jnp.sin(angle_table)
    repeats = LANES // head_dim
    return (
        jnp.tile(jnp.concatenate([cosine, cosine], axis=1), (1, repeats)),
        jnp.tile(jnp.concatenate([-sine, sine], axis=1), (1, repeats)),
    )


def turn(values, cosine, signed_sine, head_dim):
    lane = lax.broadcasted_iota(jnp.int32, values.shape, 1)
    half = head_dim // 2
    other = jnp.where(
        lane % head_dim < half,
        pltpu.roll(values, LANES - half, 1),
        pltpu.roll(values, half, 1),
    )
    return values * cosine + other * signed_sine


def attend_forward_kernel(
    head_dim, block, x_ref, wq_ref, wk_ref, wv_ref, cos_ref, sin_ref, q_ref, k_ref, v_ref, o_ref, lse_ref, lse_tile
):
    length = x_ref.shape[0]
    heads = LANES // head_dim
    x = x_ref[...]
    cosine, sine = cos_ref[...], sin_ref[...]
    scale = 1.0 / math.sqrt(head_dim)
    q_ref[...] = (turn(dot_nn(x, wq_ref[...]), cosine, sine, head_dim) * scale).astype(BF16)
    k_ref[...] = turn(dot_nn(x, wk_ref[...]), cosine, sine, head_dim).astype(BF16)
    v_ref[...] = dot_nn(x, wv_ref[...]).astype(BF16)
    lane = lax.broadcasted_iota(jnp.int32, (1, LANES), 1)
    own_lane = lax.broadcasted_iota(jnp.int32, (block, LANES), 1) // head_dim
    below = lax.broadcasted_iota(jnp.int32, (block, block), 0) >= lax.broadcasted_iota(
        jnp.int32, (block, block), 1
    )
    for first in range(0, length, block):
        rows = pl.ds(first, block)
        mixed = None
        logs = None
        for head in range(heads):
            select = (lane // head_dim == head).astype(F32).astype(BF16)
            queries = q_ref[rows, :] * select
            near = jnp.where(below, dot_nt(queries, k_ref[rows, :]), -1e30)
            peak = jnp.max(near, axis=1, keepdims=True)
            if first:
                far = dot_nt(queries, k_ref[pl.ds(0, first), :])
                peak = jnp.maximum(peak, jnp.max(far, axis=1, keepdims=True))
            near = jnp.exp(near - peak)
            total = jnp.sum(near, axis=1, keepdims=True)
            part = dot_nn(near.astype(BF16), v_ref[rows, :])
            if first:
                far = jnp.exp(far - peak)
                total = total + jnp.sum(far, axis=1, keepdims=True)
                part = part + dot_nn(far.astype(BF16), v_ref[pl.ds(0, first), :])
            part = part * (1.0 / total)
            log_total = jnp.broadcast_to(peak + jnp.log(total), (block, LANES))
            mixed = part if head == 0 else jnp.where(own_lane == head, part, mixed)
            logs = log_total if head == 0 else jnp.where(own_lane == head, log_total, logs)
        o_ref[rows, :] = mixed.astype(BF16)
        lse_tile[rows, :] = logs
    turned = lse_tile[...].T
    for head in range(heads):
        lse_ref[pl.ds(head * 8, 8), :] = turned[head * head_dim : head * head_dim + 8, :]


def attend_forward(normed, w_qkv, cosine, sine, length, head_dim):
    tokens, width = normed.shape
    seqs, pairs, heads = tokens // length, width // LANES, LANES // head_dim
    block = min(256, length)
    rows = pl.BlockSpec((length, LANES), lambda s, p: (s, p))

    def weight(part):
        return pl.BlockSpec((width, LANES), lambda s, p: (0, part * pairs + p))

    table = whole((length, LANES))
    return call(
        functools.partial(attend_forward_kernel, head_dim, block),
        (seqs, pairs),
        [pl.BlockSpec((length, width), lambda s, p: (s, 0)), weight(0), weight(1), weight(2), table, table],
        [rows, rows, rows, rows, pl.BlockSpec((8 * heads, length), lambda s, p: (s * pairs + p, 0))],
        [shape_of((tokens, width), BF16)] * 4 + [shape_of((seqs * pairs * 8 * heads, length), F32)],
        scratch=[pltpu.VMEM((length, LANES), F32)],
        flops=6 * tokens * width * width + 4 * tokens * length * width,
        moved=16 * tokens * width,
        trans=tokens * length * width // head_dim // 2,
    )(normed, w_qkv, w_qkv, w_qkv, cosine, sine)


def attend_backward_kernel(
    head_dim, block, q_ref, k_ref, v_ref, o_ref, g_ref, lse_ref, cos_ref, sin_ref, gq_ref, gk_ref, gv_ref, gq_acc
):
    length = q_ref.shape[0]
    heads = LANES // head_dim
    scale = 1.0 / math.sqrt(head_dim)
    product = (g_ref[...].astype(F32) * o_ref[...].astype(F32)).T
    inner = [
        jnp.sum(product[head * head_dim : (head + 1) * head_dim, :], axis=0, keepdims=True)
        for head in range(heads)
    ]
    gq_acc[...] = jnp.zeros_like(gq_acc)
    lane = lax.broadcasted_iota(jnp.int32, (1, LANES), 1)
    own_lane = lax.broadcasted_iota(jnp.int32, (block, LANES), 1) // head_dim
    above = lax.broadcasted_iota(jnp.int32, (block, block), 1) >= lax.broadcasted_iota(
        jnp.int32, (block, block), 0
    )
    for first in range(0, length, block):
        rows = pl.ds(first, block)
        keys_grad = None
        values_grad = None
        for head in range(heads):
            select = (lane // head_dim == head).astype(F32).astype(BF16)
            keys = k_ref[rows, :] * select
            values = v_ref[rows, :] * select
            log_total = lse_ref[pl.ds(head * 8, 1), :]
            pieces = [(first, block, True)]
            if first + block < length:
                pieces.append((first + block, length - first - block, False))
            keys_part = None
            values_part = None
            for start, count, diagonal in pieces:
                span = pl.ds(start, count)
                queries, grads = q_ref[span, :], g_ref[span, :]
                scores = dot_nt(keys, queries)
                probs = jnp.exp(scores - log_total[:, start : start + count])
                if diagonal:
                    probs = jnp.where(above, probs, 0.0)
                grad_probs = dot_nt(values, grads)
                grad_scores = (probs * (grad_probs - inner[head][:, start : start + count])).astype(BF16)
                piece_values = dot_nn(probs.astype(BF16), grads)
                piece_keys = dot_nn(grad_scores, queries)
                values_part = piece_values if values_part is None else values_part + piece_values
                keys_part = piece_keys if keys_part is None else keys_part + piece_keys
                gq_acc[span, :] += dot_tn(grad_scores, keys)
            keys_grad = keys_part if head == 0 else jnp.where(own_lane == head, keys_part, keys_grad)
            values_grad = values_part if head == 0 else jnp.where(own_lane == head, values_part, values_grad)
        gk_ref[rows, :] = turn(keys_grad, cos_ref[rows, :], -sin_ref[rows, :], head_dim).astype(BF16)
        gv_ref[rows, :] = values_grad.astype(BF16)
    gq_ref[...] = turn(gq_acc[...] * scale, cos_ref[...], -sin_ref[...], head_dim).astype(BF16)


def attend_backward(queries, keys, values, mixed, grad_mixed, lse, cosine, sine, length, head_dim):
    tokens, width = queries.shape
    seqs, pairs, heads = tokens // length, width // LANES, LANES // head_dim
    block = min(256, length)
    rows = pl.BlockSpec((length, LANES), lambda s, p: (s, p))
    table = whole((length, LANES))
    return call(
        functools.partial(attend_backward_kernel, head_dim, block),
        (seqs, pairs),
        [rows] * 5 + [pl.BlockSpec((8 * heads, length), lambda s, p: (s * pairs + p, 0)), table, table],
        [rows] * 3,
        [shape_of((tokens, width), BF16)] * 3,
        scratch=[pltpu.VMEM((length, LANES), F32)],
        flops=10 * tokens * length * width,
        moved=16 * tokens * width,
        trans=tokens * length * width // head_dim // 2,
    )(queries, keys, values, mixed, grad_mixed, lse, cosine, sine)


def square(width, part):
    return pl.BlockSpec((width, width), lambda i: (0, part), pipeline_mode=pl.Buffered(1))


def norm_one_kernel(x_ref, gain_ref, out_ref):
    x = x_ref[...].astype(F32)
    scale = lax.rsqrt(jnp.mean(x * x, axis=1, keepdims=True) + EPSILON)
    out_ref[...] = (x * scale * gain_ref[...]).astype(BF16)


def norm_one(tokens, gain):
    rows, width = tokens.shape
    block = min(256, rows)
    blocked = pl.BlockSpec((block, width), lambda i: (i, 0))
    return call(
        norm_one_kernel, (rows // block,), [blocked, whole((1, width))], blocked, shape_of((rows, width), BF16),
        flops=5 * rows * width, moved=4 * rows * width,
    )(tokens, gain)


def norm_two_kernel(mixed_ref, tokens_ref, weight_ref, gain_ref, sum_ref, normed_ref):
    first_sum = tokens_ref[...].astype(F32) + dot_nn(mixed_ref[...], weight_ref[...])
    sum_ref[...] = first_sum
    scale = lax.rsqrt(jnp.mean(first_sum * first_sum, axis=1, keepdims=True) + EPSILON)
    normed_ref[...] = (first_sum * scale * gain_ref[...]).astype(BF16)


def norm_two(mixed, tokens, weight, gain):
    rows, width = tokens.shape
    block = min(256, rows)
    blocked = pl.BlockSpec((block, width), lambda i: (i, 0))
    return call(
        norm_two_kernel, (rows // block,), [blocked, blocked, square(width, 3), whole((1, width))],
        [blocked, blocked], [shape_of((rows, width), F32), shape_of((rows, width), BF16)],
        flops=2 * rows * width * width, moved=10 * rows * width,
    )(mixed, tokens, weight, gain)


def slots_kernel(experts, parts, capacity, routes_ref, live_ref, rows_ref, columns_ref):
    top, tokens = routes_ref.shape
    live = live_ref[...]
    number = lax.broadcasted_iota(jnp.int32, (experts, tokens), 0)
    hits = [
        jnp.where((routes_ref[pl.ds(k, 1), :] == number) & (live > 0), 1.0, 0.0) for k in range(top)
    ]
    earlier = jnp.where(
        lax.broadcasted_iota(jnp.int32, (tokens, tokens), 0)
        <= lax.broadcasted_iota(jnp.int32, (tokens, tokens), 1),
        1.0,
        0.0,
    ).astype(BF16)
    ranks = dot_nn(jnp.concatenate(hits, axis=0).astype(BF16), earlier)
    before = jnp.zeros((experts, 1), F32)
    expert = lax.broadcasted_iota(jnp.int32, (experts, tokens), 0)
    start = ((expert % parts) * (experts // parts) + expert // parts) * capacity
    found = []
    for k in range(top):
        rank = ranks[k * experts : (k + 1) * experts, :] + before - 1.0
        for first in (number * capacity, start):
            slot = jnp.sum(hits[k] * (first.astype(F32) + rank), axis=0, keepdims=True).astype(jnp.int32)
            found.append(jnp.where(live > 0, slot, experts * capacity))
        before = before + jnp.sum(hits[k], axis=1, keepdims=True)
    table = jnp.concatenate(found[0::2] + found[1::2] + [jnp.zeros((8 - 2 * top, tokens), jnp.int32)], axis=0)
    rows_ref[...] = table
    columns_ref[...] = table.T


def slots_of(routes_t, live_row, experts, parts, capacity):
    top, tokens = routes_t.shape
    return call(
        functools.partial(slots_kernel, experts, parts, capacity), (1,),
        [whole((top, tokens)), whole((1, tokens))], [whole((8, tokens)), whole((tokens, 8))],
        [shape_of((8, tokens), jnp.int32), shape_of((tokens, 8), jnp.int32)],
        flops=2 * top * experts * tokens * tokens, moved=16 * tokens,
    )(routes_t, live_row)


def dispatch_kernel(gated, first, base, dest_ref, gates_ref, x_ref, out_ref):
    top, tokens = gates_ref.shape
    capacity = out_ref.shape[0]
    slot = lax.broadcasted_iota(jnp.int32, (capacity, tokens), 0) + (first + pl.program_id(0)) * capacity
    hits = [slot == dest_ref[pl.ds(base + k, 1), :] for k in range(top)]
    chosen = functools.reduce(jnp.logical_or, hits)
    rows = dot_nn(jnp.where(chosen, 1.0, 0.0).astype(BF16), x_ref[...])
    if gated:
        weights = jnp.zeros((capacity, tokens), F32)
        for k in range(top):
            weights = jnp.where(hits[k], gates_ref[pl.ds(k, 1), :], weights)
        rows = rows * jnp.sum(weights, axis=1, keepdims=True)
    out_ref[...] = rows.astype(BF16)


def dispatch(dest_t, gates_t, x, experts, capacity, gated, first, base):
    top, tokens = gates_t.shape
    width = x.shape[1]
    return call(
        functools.partial(dispatch_kernel, gated, first, base), (experts,),
        [whole(dest_t.shape), whole((top, tokens)), whole((tokens, width))],
        pl.BlockSpec((capacity, width), lambda e: (e, 0)),
        shape_of((experts * capacity, width), BF16),
        flops=2 * experts * capacity * tokens * width, moved=2 * (experts * capacity + tokens) * width,
    )(dest_t, gates_t, x)


def unpack(source, start, rows, panels, target):
    for p in range(panels):
        target[:, pl.ds(p * LANES, LANES)] = source[pl.ds(start + p * rows, rows), :].astype(F32)


def combine_kernel(dest_ref, gates_ref, live_ref, sum_ref, shared_ref, y_ref, out_ref):
    block, top = gates_ref.shape
    total = sum_ref[...] + shared_ref[...]
    dest = dest_ref[...]
    gates = gates_ref[...]
    slot = slot_numbers(block, y_ref.shape[0], 0)
    for k in range(top):
        hit = jnp.where(slot == dest[:, k : k + 1], 1.0, 0.0).astype(BF16)
        total = total + dot_nn(hit, y_ref[...]) * gates[:, k : k + 1]
    out_ref[...] = (live_ref[...] * total).astype(BF16)


def combine(dest, gates, live, first_sum, shared_out, returned):
    rows, width = first_sum.shape
    top = gates.shape[1]
    block = min(256, rows)
    blocked = pl.BlockSpec((block, width), lambda i: (i, 0))
    slots = returned.shape[0]
    return call(
        combine_kernel, (rows // block,),
        [pl.BlockSpec((block, dest.shape[1]), lambda i: (i, 0)), pl.BlockSpec((block, top), lambda i: (i, 0)),
         pl.BlockSpec((block, 1), lambda i: (i, 0)), blocked, blocked, whole(returned.shape)],
        blocked, shape_of((rows, width), BF16),
        flops=4 * rows * slots * width, moved=10 * rows * width + 2 * slots * width,
    )(dest, gates, live, first_sum, shared_out, returned)


def unpack(source, start, rows, panels, target):
    for p in range(panels):
        target[:, pl.ds(p * LANES, LANES)] = source[pl.ds(start + p * rows, rows), :].astype(F32)


def gather_kernel(axis, count, many, *refs):
    pieces, outs, landed, sems = refs[:many], refs[many : 2 * many], refs[2 * many : 3 * many], refs[3 * many :]
    barrier = pltpu.get_barrier_semaphore()
    pl.semaphore_wait(barrier, greet_neighbours(barrier, axis, count))
    gathers = [
        LineGather(axis, count, landed[i], sems[2 * i], sems[2 * i + 1], 0, 1) for i in range(many)
    ]
    for gather, piece in zip(gathers, pieces):
        gather.start(piece[...])
    for k in range(1, count):
        for gather in gathers:
            gather.relay(k)
    for gather, out, rows in zip(gathers, outs, landed):
        gather.finish()
        out[...] = rows[...]


def gather_over(pieces, axis, count, collective_id):
    shapes = [(count * piece.shape[0], LANES) for piece in pieces]
    vmem = pl.BlockSpec(memory_space=pltpu.VMEM)
    size = sum(shape[0] for shape in shapes) * LANES
    return pl.pallas_call(
        functools.partial(gather_kernel, axis, count, len(pieces)),
        out_shape=[shape_of(shape, BF16) for shape in shapes],
        in_specs=[vmem] * len(pieces),
        out_specs=[vmem] * len(pieces),
        scratch_shapes=[pltpu.VMEM(shape, BF16) for shape in shapes]
        + [pltpu.SemaphoreType.DMA((2, count))] * (2 * len(pieces)),
        compiler_params=pltpu.CompilerParams(collective_id=collective_id, has_side_effects=True),
        cost_estimate=pl.CostEstimate(flops=size, bytes_accessed=40 * size, transcendentals=0),
    )(*pieces)


def lay_out_kernel(parts, pack_ref, egu_ref, ed_ref):
    step = pl.program_id(0)
    width = ed_ref.shape[2]
    packed = pack_ref.shape[0] // parts
    e_panels, e_rows = egu_ref.shape[2] // LANES, egu_ref.shape[1]
    for e in range(parts):
        for p in range(e_panels):
            rows = pl.ds(pl.multiple_of(e * packed + p * width + step * e_rows, 16), e_rows)
            egu_ref[e, :, pl.ds(p * LANES, LANES)] = pack_ref[rows, :].astype(F32)

    @pl.when(step == 0)
    def _():
        for e in range(parts):
            unpack(pack_ref, e * packed + e_panels * width, ed_ref.shape[1], width // LANES, ed_ref.at[e])


def lay_out(pack, parts, own, width, hidden):
    group, steps = width // own, 4
    columns = 2 * hidden // group
    outs = [(parts, width, columns), (parts, hidden // group, width)]
    return call(
        functools.partial(lay_out_kernel, parts), (steps,), [whole(pack.shape)],
        [pl.BlockSpec((parts, width // steps, columns), lambda i: (0, i, 0)), whole(outs[1])],
        [shape_of(shape, F32) for shape in outs],
        flops=pack.size, moved=6 * pack.size,
    )(pack)


def lay_out_last_kernel(own, gu_panels, x_ref, shared_ref, qkv_ref, wo_ref, gain_ref, sgu_ref, sd_ref):
    panels = wo_ref.shape[1] // LANES
    unpack(x_ref, 0, own, 3 * panels, qkv_ref)
    unpack(x_ref, 3 * panels * own, own, panels, wo_ref)
    gain_ref[...] = x_ref[pl.ds(4 * panels * own, gain_ref.shape[0]), :].astype(F32)
    unpack(shared_ref, 0, own, gu_panels, sgu_ref)
    unpack(shared_ref, gu_panels * own, sd_ref.shape[0], panels, sd_ref)


def lay_out_last(x, shared, own, width, hidden):
    outs = [(own, 3 * width), (own, width), (8, LANES), (own, 2 * hidden), (hidden // (width // own), width)]
    return call(
        functools.partial(lay_out_last_kernel, own, 2 * hidden // LANES), (1,), [whole(x.shape), whole(shared.shape)],
        [whole(shape) for shape in outs], [shape_of(shape, F32) for shape in outs],
        flops=x.size, moved=6 * (x.size + shared.size),
    )(x, shared)


def slot_numbers(block, slots, part):
    return lax.broadcasted_iota(jnp.int32, (block, slots), 1) + part * slots


def gathered(top, dest_ref, y_ref, part):
    block = dest_ref.shape[0]
    dest = dest_ref[:, top : 2 * top]
    slot = slot_numbers(block, y_ref.shape[0], part)
    hit = functools.reduce(jnp.logical_or, [slot == dest[:, k : k + 1] for k in range(top)])
    return dot_nn(jnp.where(hit, 1.0, 0.0).astype(BF16), y_ref[...])


class Exchange:
    def __init__(self, axis, count, sent_ref, kept_ref, own_sem, send_sem, recv_sem):
        self.axis, self.count = axis, count
        me = lax.axis_index(axis)
        self.peers = [lax.rem(me + ahead, count) for ahead in range(1, count)]
        self.me, self.sent_ref, self.kept_ref = me, sent_ref, kept_ref
        self.own_sem, self.send_sem, self.recv_sem = own_sem, send_sem, recv_sem

    def copies(self):
        out = [pltpu.make_async_copy(self.sent_ref.at[self.me], self.kept_ref.at[self.me], self.own_sem)]
        for index, peer in enumerate(self.peers):
            out.append(
                pltpu.make_async_remote_copy(
                    src_ref=self.sent_ref.at[peer], dst_ref=self.kept_ref.at[self.me],
                    send_sem=self.send_sem.at[index], recv_sem=self.recv_sem.at[index],
                    device_id={self.axis: peer}, device_id_type=pl.DeviceIdType.MESH,
                )
            )
        return out

    def start(self):
        barrier = pltpu.get_barrier_semaphore()
        for peer in self.peers:
            pl.semaphore_signal(barrier, inc=1, device_id={self.axis: peer}, device_id_type=pl.DeviceIdType.MESH)
        pl.semaphore_wait(barrier, self.count - 1)
        for copy in self.copies():
            copy.start()

    def wait(self):
        for copy in self.copies():
            copy.wait()

    @staticmethod
    def scratch(count):
        sems = pltpu.SemaphoreType.DMA((count - 1,))
        return [pltpu.SemaphoreType.DMA, sems, sems]


def add_part_kernel(part, top, axis, count, dest_ref, base_ref, y_ref, sent_ref, out_ref, kept_ref, *sems):
    exchange = Exchange(axis, count, sent_ref, kept_ref, *sems)

    @pl.when(pl.program_id(0) == 0)
    def _():
        exchange.start()

    out_ref[...] = base_ref[...] + gathered(top, dest_ref, y_ref, part)

    @pl.when(pl.program_id(0) == pl.num_programs(0) - 1)
    def _():
        exchange.wait()


def add_part(top, dest, base, rows_of, part, sent, axis, count, collective_id):
    rows, width = base.shape
    block = min(256, rows)
    blocked = pl.BlockSpec((block, width), lambda i: (i, 0))
    hbm = pl.BlockSpec(memory_space=pl.ANY)
    sent = sent.reshape(count, -1, width)
    out, kept = call(
        functools.partial(add_part_kernel, part, top, axis, count), (rows // block,),
        [pl.BlockSpec((block, dest.shape[1]), lambda i: (i, 0)), blocked, whole(rows_of.shape), hbm],
        [blocked, hbm], [shape_of((rows, width), F32), shape_of(sent.shape, BF16)],
        scratch=Exchange.scratch(count),
        flops=2 * rows * rows_of.shape[0] * width, moved=8 * rows * width, collective_id=collective_id,
    )(dest, base, rows_of, sent)
    return out, kept.reshape(-1, width)


def norm_two_back_kernel(part, top, dest_ref, live_ref, cot_ref, sum_ref, base_ref, gain_ref, weight_ref, y_ref,
                         first_ref, attn_ref, mixed_ref, gain_grad_ref):
    grad_normed = base_ref[...] + gathered(top, dest_ref, y_ref, part)
    first_sum = sum_ref[...]
    scale = lax.rsqrt(jnp.mean(first_sum * first_sum, axis=1, keepdims=True) + EPSILON)
    weighted = grad_normed * gain_ref[...]
    inner = jnp.mean(first_sum * weighted, axis=1, keepdims=True)
    grad_first = (
        cot_ref[...].astype(F32) * live_ref[...] + scale * weighted - first_sum * (scale * scale * scale * inner)
    )
    first_ref[...] = grad_first
    grad_attn = grad_first.astype(BF16)
    attn_ref[...] = grad_attn
    mixed_ref[...] = dot_nt(grad_attn, weight_ref[...]).astype(BF16)

    @pl.when(pl.program_id(0) == 0)
    def _():
        gain_grad_ref[...] = jnp.zeros_like(gain_grad_ref)

    gain_grad_ref[...] += jnp.sum(grad_normed * first_sum * scale, axis=0, keepdims=True)


def norm_two_back(top, dest, live, cotangent, first_sum, base, gain, weights, rows_of, part):
    rows, width = first_sum.shape
    block = min(256, rows)
    blocked = pl.BlockSpec((block, width), lambda i: (i, 0))
    return call(
        functools.partial(norm_two_back_kernel, part, top), (rows // block,),
        [pl.BlockSpec((block, dest.shape[1]), lambda i: (i, 0)), pl.BlockSpec((block, 1), lambda i: (i, 0)), blocked, blocked,
         blocked, whole((1, width)), square(width, 3), whole(rows_of.shape)],
        [blocked, blocked, blocked, pl.BlockSpec((1, width), lambda i: (0, 0))],
        [shape_of((rows, width), F32), shape_of((rows, width), BF16), shape_of((rows, width), BF16),
         shape_of((1, width), F32)],
        flops=2 * rows * (rows_of.shape[0] + width) * width, moved=18 * rows * width,
    )(dest, live, cotangent, first_sum, base, gain, weights, rows_of)


def line_copy(axis, ahead, source, target, send_sem, recv_sem):
    return pltpu.make_async_remote_copy(
        src_ref=source, dst_ref=target, send_sem=send_sem, recv_sem=recv_sem,
        device_id={axis: lax.axis_index(axis) + ahead}, device_id_type=pl.DeviceIdType.MESH,
    )


class LineSum:
    def __init__(self, axis, count, x_ref, buffers, send_sem, recv_sem, turn, turns):
        self.axis, self.count, self.x_ref, self.buffers = axis, count, x_ref, buffers
        self.send_sem, self.recv_sem = send_sem, recv_sem
        self.rows, self.turn, self.turns = buffers.shape[3], turn, turns

    def own(self, piece):
        first = (piece * self.turns + self.turn) * self.rows
        return self.x_ref[pl.ds(pl.multiple_of(first, 16), self.rows), :].astype(F32)

    def copy(self, way, piece):
        return line_copy(
            self.axis, 1 - 2 * way, self.buffers.at[way, 1, piece], self.buffers.at[way, 0, piece],
            self.send_sem.at[way, piece], self.recv_sem.at[way, piece],
        )

    def each(self, body):
        me = lax.axis_index(self.axis)
        for k in range(self.count - 1):
            for way, piece in ((0, self.count - 1 - k), (1, k)):
                before = me > 0 if way == 0 else me < self.count - 1
                sends = me < piece if way == 0 else me > piece
                body(way, piece, before, sends)

    def start(self):
        def body(way, piece, before, sends):
            @pl.when(sends & jnp.logical_not(before))
            def _():
                self.buffers[way, 1, piece] = self.own(piece).astype(BF16)
                self.copy(way, piece).start()

        self.each(body)

    def relay(self):
        def body(way, piece, before, sends):
            @pl.when(sends & before)
            def _():
                self.copy(way, piece).wait_recv()
                self.buffers[way, 1, piece] = (self.own(piece) + self.buffers[way, 0, piece].astype(F32)).astype(BF16)
                self.copy(way, piece).start()

        self.each(body)

    def finish(self, total_ref):
        me = lax.axis_index(self.axis)
        total_ref[...] = self.own(me)
        for way, before in ((0, me > 0), (1, me < self.count - 1)):

            @pl.when(before)
            def _():
                self.copy(way, me).wait_recv()
                total_ref[...] += self.buffers[way, 0, me].astype(F32)

        def body(way, piece, before, sends):
            @pl.when(sends)
            def _():
                self.copy(way, piece).wait_send()

        self.each(body)


class LineGather:
    def __init__(self, axis, count, out_ref, send_sem, recv_sem, turn, turns):
        self.axis, self.count, self.out_ref = axis, count, out_ref
        self.send_sem, self.recv_sem = send_sem, recv_sem
        self.rows, self.turn, self.turns = out_ref.shape[0] // count // turns, turn, turns

    def place(self, piece):
        first = (piece * self.turns + self.turn) * self.rows
        return self.out_ref.at[pl.ds(pl.multiple_of(first, 16), self.rows), :]

    def copy(self, way, piece):
        return line_copy(
            self.axis, 1 - 2 * way, self.place(piece), self.place(piece),
            self.send_sem.at[way, piece], self.recv_sem.at[way, piece],
        )

    def start(self, value):
        me = lax.axis_index(self.axis)
        self.place(me)[...] = value
        for way, more in ((0, me < self.count - 1), (1, me > 0)):

            @pl.when(more)
            def _():
                self.copy(way, me).start()

    def relay(self, k):
        me = lax.axis_index(self.axis)
        for way, piece, there, more in (
            (0, me - k, me >= k, me < self.count - 1),
            (1, me + k, me + k < self.count, me > 0),
        ):

            @pl.when(there)
            def _():
                self.copy(way, piece).wait_recv()

            @pl.when(there & more)
            def _():
                self.copy(way, piece).start()

    def finish(self):
        me = lax.axis_index(self.axis)
        for k in range(self.count):
            for way, piece, sent in (
                (0, me - k, (me >= k) & (me < self.count - 1)),
                (1, me + k, (me + k < self.count) & (me > 0)),
            ):

                @pl.when(sent)
                def _():
                    self.copy(way, piece).wait_send()


def greet_neighbours(barrier, axis, count):
    me = lax.axis_index(axis)
    for ahead, there in ((1, me < count - 1), (-1, me > 0)):

        @pl.when(there)
        def _():
            pl.semaphore_signal(barrier, inc=1, device_id={axis: me + ahead}, device_id_type=pl.DeviceIdType.MESH)

    return (me < count - 1).astype(jnp.int32) + (me > 0).astype(jnp.int32)


def settle_kernel(sizes, gq_ref, gk_ref, gv_ref, wq_ref, wk_ref, wv_ref, tokens_ref, first_ref, gain_ref, pack_ref,
                  x_ref, out_ref, share_ref, piece_ref, own, landed, chosen, arrived, sem, pair_send, pair_recv, send_sem,
                  recv_sem, x_buffers, x_total, x_send, x_recv):
    dp_size, shard_size, count = sizes
    spread = shard_size // 2
    halves = dp_size * spread
    dp, shard = lax.axis_index("dp"), lax.axis_index("shard")
    side = shard % 2
    place = dp * spread + shard // 2
    step = pl.program_id(0)
    last = pl.num_programs(0) - 1

    def target(piece, bit):
        return {"dp": piece // spread, "shard": (piece % spread) * 2 + bit}

    line = LineSum("expert", count, x_ref, x_buffers, x_send, x_recv, 0, 1)

    def pair_copy():
        return pltpu.make_async_remote_copy(
            src_ref=pack_ref.at[:, 1 - side], dst_ref=landed, send_sem=pair_send, recv_sem=pair_recv,
            device_id=target(place, 1 - side), device_id_type=pl.DeviceIdType.MESH,
        )

    def own_copy():
        return pltpu.make_async_copy(pack_ref.at[:, side], own, sem)

    def send(index):
        return pltpu.make_async_remote_copy(
            src_ref=chosen.at[index], dst_ref=arrived.at[index], send_sem=send_sem.at[index], recv_sem=recv_sem.at[index],
            device_id=target(lax.rem(place + index + 1, halves), side), device_id_type=pl.DeviceIdType.MESH,
        )

    @pl.when(step == 0)
    def _():
        barrier = pltpu.get_barrier_semaphore()
        pl.semaphore_signal(barrier, inc=1, device_id=target(place, 1 - side), device_id_type=pl.DeviceIdType.MESH)
        for index in range(halves - 1):
            pl.semaphore_signal(
                barrier, inc=1, device_id=target(lax.rem(place + index + 1, halves), side),
                device_id_type=pl.DeviceIdType.MESH,
            )
        neighbours = greet_neighbours(barrier, "expert", count)
        pl.semaphore_wait(barrier, halves + neighbours)
        pair_copy().start()
        own_copy().start()
        line.start()

    @pl.when(step == 1)
    def _():
        own_copy().wait()
        pair_copy().wait()
        for index in range(halves - 1):
            piece = lax.rem(place + index + 1, halves)
            chosen[index] = (own[piece].astype(F32) + landed[piece].astype(F32)).astype(BF16)
            send(index).start()

    grad_normed = (
        dot_nt(gq_ref[...], wq_ref[...]) + dot_nt(gk_ref[...], wk_ref[...]) + dot_nt(gv_ref[...], wv_ref[...])
    )
    source = tokens_ref[...].astype(F32)
    scale = lax.rsqrt(jnp.mean(source * source, axis=1, keepdims=True) + EPSILON)
    weighted = grad_normed * gain_ref[...]
    inner = jnp.mean(source * weighted, axis=1, keepdims=True)
    out_ref[...] = first_ref[...] + scale * weighted - source * (scale * scale * scale * inner)

    @pl.when(step == last)
    def _():
        line.relay()
        total = own[place].astype(F32) + landed[place].astype(F32)
        for index in range(halves - 1):
            send(index).wait()
            total = total + arrived[index].astype(F32)
        share_ref[...] = total.astype(BF16)
        line.finish(x_total)
        piece_ref[...] = x_total[...].astype(BF16)


def settle(grads, w_qkv, tokens, grad_first, gain, pack, x, sizes):
    rows, width = tokens.shape
    block = min(256, rows)
    blocked = pl.BlockSpec((block, width), lambda i: (i, 0))
    halves, count = sizes[0] * sizes[1] // 2, pack.shape[1]
    piece = (count, LANES)
    x_piece = (x.shape[0] // sizes[2], LANES)
    return call(
        functools.partial(settle_kernel, sizes), (rows // block,),
        [blocked] * 3 + [square(width, 0), square(width, 1), square(width, 2), blocked, blocked, whole((1, width)),
                         pl.BlockSpec(memory_space=pl.ANY), whole(x.shape)],
        [blocked, whole(piece), whole(x_piece)],
        [shape_of((rows, width), F32), shape_of(piece, BF16), shape_of(x_piece, BF16)],
        scratch=[pltpu.VMEM((halves,) + piece, BF16), pltpu.VMEM((halves,) + piece, BF16),
                 pltpu.VMEM((halves - 1,) + piece, BF16), pltpu.VMEM((halves - 1,) + piece, BF16),
                 pltpu.SemaphoreType.DMA, pltpu.SemaphoreType.DMA, pltpu.SemaphoreType.DMA,
                 pltpu.SemaphoreType.DMA((halves - 1,)), pltpu.SemaphoreType.DMA((halves - 1,)),
                 pltpu.VMEM((2, 2, sizes[2]) + x_piece, BF16), pltpu.VMEM(x_piece, F32)]
        + [pltpu.SemaphoreType.DMA((2, sizes[2]))] * 2,
        flops=6 * rows * width * width, moved=22 * rows * width, collective_id=1,
    )(*grads, w_qkv, w_qkv, w_qkv, tokens, grad_first, gain, pack.reshape((halves, 2) + piece), x)


def copies_of(layout, block, width, step, stage_g, stage_u, stage_d, slot, packed_ref, sems):
    by_rows, owners, hidden, base = layout
    panels = block // LANES
    rows_down = hidden // owners
    out = []

    def add(source, target):
        out.append(pltpu.make_async_copy(source, target, sems.at[slot, len(out)]))

    if by_rows:
        rows = width // owners
        for half, stage in enumerate((stage_g, stage_u)):
            for p in range(panels):
                panel = half * (hidden // LANES) + step * panels + p
                add(
                    stage.at[slot, :, :, pl.ds(p * LANES, LANES)],
                    packed_ref.at[:, pl.ds(pl.multiple_of(base + panel * rows, 8), rows), :],
                )
        start = 2 * hidden // LANES * rows
    else:
        columns = 2 * hidden // owners
        for half, stage in enumerate((stage_g, stage_u)):
            for p in range(panels):
                column = half * hidden + step * block + p * LANES
                owner, panel = column // columns, (column % columns) // LANES
                add(
                    stage.at[slot, :, pl.ds(p * LANES, LANES)],
                    packed_ref.at[owner, pl.ds(pl.multiple_of(base + panel * width, 8), width), :],
                )
        start = columns // LANES * width
    for q in range(block // rows_down):
        owner = step * (block // rows_down) + q
        for c in range(width // LANES):
            add(
                stage_d.at[slot, pl.ds(q * rows_down, rows_down), pl.ds(c * LANES, LANES)],
                packed_ref.at[owner, pl.ds(base + start + c * rows_down, rows_down), :],
            )
    return out


def packed_rows(width, hidden, owners):
    return 3 * width * hidden // owners // LANES


def ffn_kernel(out_type, layout, block, axis, count, x_ref, gy_ref, wg_ref, wu_ref, wd_ref, sent_ref, *rest):
    y_ref, gx_ref, packed_ref, kept_ref, xt, y_acc, gx_acc, stage_g, stage_u, stage_d, sems, *exchange_sems = rest[-14:]
    exchange = Exchange(axis, count, sent_ref, kept_ref, *exchange_sems)
    step = pl.program_id(0)
    steps = layout[2] // block
    width = x_ref.shape[1]
    slot = step % 2
    copies = functools.partial(copies_of, layout, block, width)

    @pl.when(step == 0)
    def _():
        exchange.start()
        xt[...] = x_ref[...].T
        y_acc[...] = jnp.zeros_like(y_acc)
        gx_acc[...] = jnp.zeros_like(gx_acc)

    @pl.when(step >= 2)
    def _():
        for copy in copies(step - 2, stage_g, stage_u, stage_d, slot, packed_ref, sems):
            copy.wait()

    x, gy = x_ref[...], gy_ref[...].reshape(x_ref.shape)
    if layout[0]:
        wg, wu = wg_ref[...].reshape(width, block), wu_ref[...].reshape(width, block)
        rows = wd_ref.shape[1] // (width // block)
        wd = jnp.concatenate(
            [wd_ref[:, pl.ds(c * rows, rows), :].reshape(block, block) for c in range(width // block)], axis=1
        )
    else:
        wg, wu, wd = wg_ref[...], wu_ref[...], wd_ref[...]
    gate, up = dot_nn(x, wg), dot_nn(x, wu)
    grad_hidden = dot_nt(gy, wd)
    sigmoid = jax.nn.sigmoid(gate)
    value = gate * sigmoid
    hidden = (value * up).astype(BF16)
    grad_up = (grad_hidden * value).astype(BF16)
    grad_gate = (grad_hidden * up * (sigmoid * (1.0 + gate * (1.0 - sigmoid)))).astype(BF16)
    y_acc[...] += dot_nn(hidden, wd)
    gx_acc[...] += dot_nt(grad_gate, wg) + dot_nt(grad_up, wu)
    stage_g[slot] = dot_nn(xt[...], grad_gate).astype(BF16).reshape(stage_g.shape[1:])
    stage_u[slot] = dot_nn(xt[...], grad_up).astype(BF16).reshape(stage_u.shape[1:])
    stage_d[slot] = dot_tn(hidden, gy).astype(BF16)
    for copy in copies(step, stage_g, stage_u, stage_d, slot, packed_ref, sems):
        copy.start()

    @pl.when(step == steps - 1)
    def _():
        exchange.wait()
        y_ref[...] = y_acc[...].astype(out_type).reshape(y_ref.shape)
        gx_ref[...] = gx_acc[...].astype(out_type)
        for back in (1, 0):
            if steps > back:
                for copy in copies(steps - 1 - back, stage_g, stage_u, stage_d, (steps - 1 - back) % 2, packed_ref, sems):
                    copy.wait()


BLOCK = 256


def ffn_both(x, gy, w_gu, w_down, hidden, expert, owners, out_type, sent, axis, count, collective_id, parts=1, held=()):
    rows, width = x.shape
    block = BLOCK
    steps = hidden // block
    by_rows = expert is None
    if by_rows:
        own, own_down, panels = width // owners, hidden // owners, width // block
        ahead = 2 * steps * own // (panels * own_down)
        gate = pl.BlockSpec((owners, own, block), lambda f: (0, f, 0))
        up = pl.BlockSpec((owners, own, block), lambda f: (0, steps + f, 0))
        down = pl.BlockSpec((block // own_down, panels * own_down, block), lambda f: (f, ahead, 0))
        stage = (2, owners, own, block)
    else:
        gate = pl.BlockSpec((None, width, block), lambda f: (expert, 0, f))
        up = pl.BlockSpec((None, width, block), lambda f: (expert, 0, steps + f))
        down = pl.BlockSpec((None, block, width), lambda f: (expert, f, 0))
        stage = (2, width, block)
    if by_rows:
        grads = whole((rows, width))
        y_block, y_shape = whole((rows, width)), (rows, width)
    else:
        y_shape = (gy.shape[0], parts * (rows // gy.shape[0]), width)
        y_block = pl.BlockSpec(
            (gy.shape[0], rows // gy.shape[0], width), lambda f: (0, expert, 0), pipeline_mode=pl.Buffered(1)
        )
        grads = pl.BlockSpec(
            (gy.shape[0], rows // gy.shape[0], width), lambda f: (0, expert, 0), pipeline_mode=pl.Buffered(1)
        )
    out_rows = whole((rows, width))
    pack_rows = packed_rows(width, hidden, owners)
    layout = (by_rows, owners, hidden, (expert or 0) * pack_rows)
    hbm = pl.BlockSpec(memory_space=pl.ANY)
    sent = sent.reshape(count, -1, width)
    copies = 2 * (block // LANES) + block // (hidden // owners) * (width // LANES)
    y, gx, pack, kept = call(
        functools.partial(ffn_kernel, out_type, layout, block, axis, count), (steps,),
        [whole((rows, width)), grads, gate, up, down, hbm] + [hbm] * len(held),
        [y_block, out_rows, hbm, hbm],
        [shape_of(y_shape, out_type), shape_of((rows, width), out_type),
         shape_of((owners, parts * pack_rows, LANES), BF16), shape_of(sent.shape, BF16)],
        scratch=[pltpu.VMEM((width, rows), BF16), pltpu.VMEM((rows, width), F32), pltpu.VMEM((rows, width), F32),
                 pltpu.VMEM(stage, BF16), pltpu.VMEM(stage, BF16), pltpu.VMEM((2, block, width), BF16),
                 pltpu.SemaphoreType.DMA((2, copies))] + Exchange.scratch(count),
        flops=18 * rows * width * hidden, moved=12 * width * hidden + 16 * rows * width, trans=rows * hidden,
        aliases={6: 0, 7: 2} if held else None, collective_id=collective_id,
    )(x, gy, w_gu, w_gu, w_down, sent, *held)
    return y, gx, pack, kept.reshape(-1, width)


def to_panels(array):
    rows, columns = array.shape
    return jnp.transpose(array.reshape(rows, columns // BLOCK, BLOCK), (1, 0, 2)).reshape(-1, BLOCK)


def attention_weights_kernel(per, normed_ref, mixed_ref, gq_ref, gk_ref, gv_ref, ga_ref, gains_ref, out_ref, xt):
    step = pl.program_id(0)
    owners, rows = out_ref.shape[0], out_ref.shape[1] // (out_ref.shape[1] // (normed_ref.shape[1] // out_ref.shape[0]))
    panels = out_ref.shape[1] // rows

    @pl.when(step == 0)
    def _():
        xt[...] = normed_ref[...].T

    @pl.when(step == 3 * per)
    def _():
        xt[...] = mixed_ref[...].T

    for index, grad_ref in enumerate((gq_ref, gk_ref, gv_ref, ga_ref)):

        @pl.when((step >= index * per) & (step < (index + 1) * per))
        def _():
            product = dot_nn(xt[...], grad_ref[...]).astype(BF16)
            for p in range(panels):
                out_ref[:, pl.ds(p * rows, rows), :] = product[:, p * LANES : (p + 1) * LANES].reshape(owners, rows, LANES)

    @pl.when(step >= 4 * per)
    def _():
        out_ref[...] = jnp.zeros_like(out_ref)

    @pl.when(step == 4 * per)
    def _():
        out_ref[:, pl.ds(0, gains_ref.shape[1]), :] = gains_ref[...]


def attention_weights(normed, mixed, grads, grad_attn, gains, owners, pieces):
    tokens, width = normed.shape
    rows = width // owners
    block = BLOCK
    panels, per = block // LANES, width // block
    steps = 4 * per + 1
    while steps * panels * rows % (16 * pieces):
        steps += 1

    def columns(index):
        return pl.BlockSpec((tokens, block), lambda i: (0, jnp.clip(i - index * per, 0, per - 1)))

    return call(
        functools.partial(attention_weights_kernel, per), (steps,),
        [whole((tokens, width)), whole((tokens, width))] + [columns(index) for index in range(4)] + [whole(gains.shape)],
        pl.BlockSpec((owners, panels * rows, LANES), lambda i: (0, i, 0)),
        shape_of((owners, steps * panels * rows, LANES), BF16),
        scratch=[pltpu.VMEM((width, tokens), BF16)],
        flops=8 * tokens * width * width, moved=16 * tokens * width,
    )(normed, mixed, *grads, grad_attn, gains)


GROUP = ("dp", "shard")


def local(
    tokens,
    lengths,
    routes,
    route_gates,
    cotangent,
    norm_gains,
    w_qkv,
    w_out,
    w_shared_gu,
    w_shared_down,
    w_expert_gu,
    w_expert_down,
):
    tok_count, width = tokens.shape
    seq_count = lengths.shape[0]
    length = tok_count // seq_count
    local_experts = w_expert_gu.shape[0]
    owners = lax.axis_size("expert")
    experts = local_experts * owners
    top = routes.shape[1]
    capacity = tok_count * top * 9 // (8 * experts)
    head_dim = width // HEADS
    hidden = w_expert_down.shape[1]

    gains = lax.all_gather(norm_gains, GROUP, axis=1, tiled=True).astype(F32)
    attention_weight = lax.all_gather(jnp.concatenate([w_qkv, w_out], axis=1), GROUP, axis=0, tiled=True)
    shared_weight = lax.all_gather(
        jnp.concatenate([to_panels(w_shared_gu), to_panels(w_shared_down)], axis=0)[None], GROUP, axis=0, tiled=True
    )
    gain_one, gain_two = gains[0:1], gains[1:2]

    live_bool = lax.iota(jnp.int32, tok_count) % length < jnp.repeat(lengths, length)
    live = live_bool.astype(F32)[:, None]
    live_row = live_bool.astype(jnp.int32)[None, :]

    group = lax.axis_size("dp") * lax.axis_size("shard")
    shared_hidden = w_shared_down.shape[0] * group

    table_t, table = slots_of(routes.T, live_row, experts, local_experts, capacity)
    gates_t = route_gates.T
    grad_b = jnp.where(live_bool[:, None], cotangent, 0).astype(BF16)

    def exchange(rows):
        return lax.all_to_all(
            rows.reshape(owners, -1, width), "expert", split_axis=0, concat_axis=0, tiled=True
        ).reshape(rows.shape)

    send_grad = dispatch(table_t, gates_t, cotangent, experts, capacity, True, 0, 0)
    received_grad = exchange(send_grad).reshape(owners, local_experts * capacity, width)

    cosine, sine = rotary_tables(length, head_dim)
    normed_one = norm_one(tokens, gain_one)
    queries, keys, values, mixed, lse = attend_forward(normed_one, attention_weight, cosine, sine, length, head_dim)
    first_sum, normed_two = norm_two(mixed, tokens, attention_weight, gain_two)

    send_rows = []
    for j in range(local_experts):
        send_rows.append(dispatch(table_t, gates_t, normed_two, owners, capacity, False, j * owners, top))
    shared_out, grad_shared, shared_pack, received = ffn_both(
        normed_two, grad_b, shared_weight, shared_weight, shared_hidden, None, group, F32,
        send_rows[0], "expert", owners, 3,
    )
    waiting = send_rows[1:]
    back_rows, base, held = [], grad_shared, ()
    for j in range(local_experts):
        y, gx, pack, arrived = ffn_both(
            received, received_grad, w_expert_gu, w_expert_down, hidden, j, group, BF16,
            waiting.pop(0), "expert", owners, 4 + j, local_experts, held,
        )
        held = (y, pack)
        waiting.append(gx)
        if j < local_experts - 1:
            received = arrived
        else:
            back_rows.append(arrived)
    for j, sent in enumerate(waiting):
        base, arrived = add_part(
            top, table, base, back_rows[j], j, sent, "expert", owners, 4 + local_experts + j
        )
        back_rows.append(arrived)
    y, base = lax.optimization_barrier((y, base))
    grad_first, grad_attn, grad_mixed, grad_gain_two = norm_two_back(
        top, table, live, cotangent, first_sum, base, gain_two, attention_weight, back_rows[-1], local_experts - 1
    )

    grads = attend_backward(queries, keys, values, mixed, grad_mixed, lse, cosine, sine, length, head_dim)
    own = width // group
    grad_gains = grad_gain_two.reshape(group, 1, own)
    grad_gains = jnp.pad(grad_gains, ((0, 0), (0, 15), (0, LANES - own))).astype(BF16)
    attention_pack = attention_weights(normed_one, mixed, grads, grad_attn, grad_gains, group, owners)

    def spread(pack):
        return lax.psum_scatter(pack, GROUP, scatter_dimension=0, tiled=True)[0]

    shared_share = spread(shared_pack)
    expert_share = spread(pack)
    input_grad, attention_share, shared_piece = settle(
        grads, attention_weight, tokens, grad_first, gain_one, attention_pack, shared_share,
        (lax.axis_size("dp"), lax.axis_size("shard"), owners),
    )
    returned = exchange(y)
    pieces = lax.all_to_all(
        attention_share.reshape(owners, -1, LANES), "expert", split_axis=0, concat_axis=0, tiled=True
    )
    piece = jnp.sum(pieces.astype(F32), axis=0).astype(BF16)
    layer_out = combine(table, route_gates, live, first_sum, shared_out, returned.reshape(-1, width))
    expert_gu, expert_down = lay_out(expert_share, local_experts, own, width, hidden)
    attention_share, shared_share = gather_over([piece, shared_piece], "expert", owners, 2)
    qkv_grad, out_grad, gain_rows, shared_gu, shared_down = lay_out_last(
        attention_share, shared_share, own, width, shared_hidden
    )
    grad_gain_one = jnp.sum(w_qkv.astype(F32) * qkv_grad, axis=1) / norm_gains[0].astype(F32)
    grad_gains = jnp.stack([grad_gain_one, gain_rows[0, :own]])
    return layer_out, input_grad, grad_gains, qkv_grad, out_grad, shared_gu, shared_down, expert_gu, expert_down


def solution(mesh):
    rows = P(("dp", "expert", "shard"), None)
    split = P(GROUP, None)
    in_specs = (
        rows,
        P(("dp", "expert", "shard")),
        rows,
        rows,
        rows,
        P(None, GROUP),
        split,
        split,
        split,
        split,
        P("expert", None, None),
        P("expert", None, None),
    )
    out_specs = (
        rows,
        rows,
        P(None, GROUP),
        split,
        split,
        split,
        split,
        P("expert", None, GROUP),
        P("expert", GROUP, None),
    )

    return jax.shard_map(local, mesh=mesh, in_specs=in_specs, out_specs=out_specs, check_vma=False)
```

```python
import functools
import math

import jax
import jax.numpy as jnp
from jax import lax
from jax.experimental import pallas as pl
from jax.experimental.pallas import tpu as pltpu
from jax.sharding import PartitionSpec as P


HEADS = 12
LANES = 128
EPSILON = 1e-05
VMEM_BYTES = 60 * 1024 * 1024
BF16 = jnp.bfloat16
F32 = jnp.float32


def call(kernel, grid, in_specs, out_specs, out_shape, scratch=(), flops=0, moved=0, trans=0, collective_id=None, aliases=None):
    return pl.pallas_call(
        kernel,
        grid_spec=pltpu.PrefetchScalarGridSpec(
            num_scalar_prefetch=0,
            grid=grid,
            in_specs=in_specs,
            out_specs=out_specs,
            scratch_shapes=list(scratch),
        ),
        out_shape=out_shape,
        input_output_aliases=aliases or {},
        compiler_params=pltpu.CompilerParams(
            dimension_semantics=("arbitrary",) * len(grid), vmem_limit_bytes=VMEM_BYTES, collective_id=collective_id,
            has_side_effects=collective_id is not None,
        ),
        cost_estimate=pl.CostEstimate(flops=flops, bytes_accessed=moved, transcendentals=trans),
    )


def shape_of(shape, dtype):
    return jax.ShapeDtypeStruct(shape, dtype)


def whole(shape):
    return pl.BlockSpec(shape, lambda *_: (0,) * len(shape), pipeline_mode=pl.Buffered(1))


def dot_nn(left, right):
    return lax.dot_general(left, right, (((1,), (0,)), ((), ())), preferred_element_type=F32)


def dot_nt(left, right):
    return lax.dot_general(left, right, (((1,), (1,)), ((), ())), preferred_element_type=F32)


def dot_tn(left, right):
    return lax.dot_general(left, right, (((0,), (0,)), ((), ())), preferred_element_type=F32)


def rotary_tables(length, head_dim):
    half_dim = head_dim // 2
    position = lax.iota(F32, length)[:, None]
    frequency = jnp.exp(lax.iota(F32, half_dim) * (-2.0 * math.log(10000.0) / head_dim))
    angle_table = position * frequency[None, :]
    cosine, sine = jnp.cos(angle_table), jnp.sin(angle_table)
    repeats = LANES // head_dim
    return (
        jnp.tile(jnp.concatenate([cosine, cosine], axis=1), (1, repeats)),
        jnp.tile(jnp.concatenate([-sine, sine], axis=1), (1, repeats)),
    )


def turn(values, cosine, signed_sine, head_dim):
    lane = lax.broadcasted_iota(jnp.int32, values.shape, 1)
    half = head_dim // 2
    other = jnp.where(
        lane % head_dim < half,
        pltpu.roll(values, LANES - half, 1),
        pltpu.roll(values, half, 1),
    )
    return values * cosine + other * signed_sine


def attend_forward_kernel(
    head_dim, block, x_ref, wq_ref, wk_ref, wv_ref, cos_ref, sin_ref, q_ref, k_ref, v_ref, o_ref, lse_ref, lse_tile
):
    length = x_ref.shape[0]
    heads = LANES // head_dim
    x = x_ref[...]
    cosine, sine = cos_ref[...], sin_ref[...]
    scale = 1.0 / math.sqrt(head_dim)
    q_ref[...] = (turn(dot_nn(x, wq_ref[...]), cosine, sine, head_dim) * scale).astype(BF16)
    k_ref[...] = turn(dot_nn(x, wk_ref[...]), cosine, sine, head_dim).astype(BF16)
    v_ref[...] = dot_nn(x, wv_ref[...]).astype(BF16)
    lane = lax.broadcasted_iota(jnp.int32, (1, LANES), 1)
    own_lane = lax.broadcasted_iota(jnp.int32, (block, LANES), 1) // head_dim
    below = lax.broadcasted_iota(jnp.int32, (block, block), 0) >= lax.broadcasted_iota(
        jnp.int32, (block, block), 1
    )
    for first in range(0, length, block):
        rows = pl.ds(first, block)
        mixed = None
        logs = None
        for head in range(heads):
            select = (lane // head_dim == head).astype(F32).astype(BF16)
            queries = q_ref[rows, :] * select
            near = jnp.where(below, dot_nt(queries, k_ref[rows, :]), -1e30)
            peak = jnp.max(near, axis=1, keepdims=True)
            if first:
                far = dot_nt(queries, k_ref[pl.ds(0, first), :])
                peak = jnp.maximum(peak, jnp.max(far, axis=1, keepdims=True))
            near = jnp.exp(near - peak)
            total = jnp.sum(near, axis=1, keepdims=True)
            part = dot_nn(near.astype(BF16), v_ref[rows, :])
            if first:
                far = jnp.exp(far - peak)
                total = total + jnp.sum(far, axis=1, keepdims=True)
                part = part + dot_nn(far.astype(BF16), v_ref[pl.ds(0, first), :])
            part = part * (1.0 / total)
            log_total = jnp.broadcast_to(peak + jnp.log(total), (block, LANES))
            mixed = part if head == 0 else jnp.where(own_lane == head, part, mixed)
            logs = log_total if head == 0 else jnp.where(own_lane == head, log_total, logs)
        o_ref[rows, :] = mixed.astype(BF16)
        lse_tile[rows, :] = logs
    turned = lse_tile[...].T
    for head in range(heads):
        lse_ref[pl.ds(head * 8, 8), :] = turned[head * head_dim : head * head_dim + 8, :]


def attend_forward(normed, w_qkv, cosine, sine, length, head_dim):
    tokens, width = normed.shape
    seqs, pairs, heads = tokens // length, width // LANES, LANES // head_dim
    block = min(256, length)
    rows = pl.BlockSpec((length, LANES), lambda s, p: (s, p))

    def weight(part):
        return pl.BlockSpec((width, LANES), lambda s, p: (0, part * pairs + p))

    table = whole((length, LANES))
    return call(
        functools.partial(attend_forward_kernel, head_dim, block),
        (seqs, pairs),
        [pl.BlockSpec((length, width), lambda s, p: (s, 0)), weight(0), weight(1), weight(2), table, table],
        [rows, rows, rows, rows, pl.BlockSpec((8 * heads, length), lambda s, p: (s * pairs + p, 0))],
        [shape_of((tokens, width), BF16)] * 4 + [shape_of((seqs * pairs * 8 * heads, length), F32)],
        scratch=[pltpu.VMEM((length, LANES), F32)],
        flops=6 * tokens * width * width + 4 * tokens * length * width,
        moved=16 * tokens * width,
        trans=tokens * length * width // head_dim // 2,
    )(normed, w_qkv, w_qkv, w_qkv, cosine, sine)


def attend_backward_kernel(
    head_dim, block, q_ref, k_ref, v_ref, o_ref, g_ref, lse_ref, cos_ref, sin_ref, gq_ref, gk_ref, gv_ref, gq_acc
):
    length = q_ref.shape[0]
    heads = LANES // head_dim
    scale = 1.0 / math.sqrt(head_dim)
    product = (g_ref[...].astype(F32) * o_ref[...].astype(F32)).T
    inner = [
        jnp.sum(product[head * head_dim : (head + 1) * head_dim, :], axis=0, keepdims=True)
        for head in range(heads)
    ]
    gq_acc[...] = jnp.zeros_like(gq_acc)
    lane = lax.broadcasted_iota(jnp.int32, (1, LANES), 1)
    own_lane = lax.broadcasted_iota(jnp.int32, (block, LANES), 1) // head_dim
    above = lax.broadcasted_iota(jnp.int32, (block, block), 1) >= lax.broadcasted_iota(
        jnp.int32, (block, block), 0
    )
    for first in range(0, length, block):
        rows = pl.ds(first, block)
        keys_grad = None
        values_grad = None
        for head in range(heads):
            select = (lane // head_dim == head).astype(F32).astype(BF16)
            keys = k_ref[rows, :] * select
            values = v_ref[rows, :] * select
            log_total = lse_ref[pl.ds(head * 8, 1), :]
            pieces = [(first, block, True)]
            if first + block < length:
                pieces.append((first + block, length - first - block, False))
            keys_part = None
            values_part = None
            for start, count, diagonal in pieces:
                span = pl.ds(start, count)
                queries, grads = q_ref[span, :], g_ref[span, :]
                scores = dot_nt(keys, queries)
                probs = jnp.exp(scores - log_total[:, start : start + count])
                if diagonal:
                    probs = jnp.where(above, probs, 0.0)
                grad_probs = dot_nt(values, grads)
                grad_scores = (probs * (grad_probs - inner[head][:, start : start + count])).astype(BF16)
                piece_values = dot_nn(probs.astype(BF16), grads)
                piece_keys = dot_nn(grad_scores, queries)
                values_part = piece_values if values_part is None else values_part + piece_values
                keys_part = piece_keys if keys_part is None else keys_part + piece_keys
                gq_acc[span, :] += dot_tn(grad_scores, keys)
            keys_grad = keys_part if head == 0 else jnp.where(own_lane == head, keys_part, keys_grad)
            values_grad = values_part if head == 0 else jnp.where(own_lane == head, values_part, values_grad)
        gk_ref[rows, :] = turn(keys_grad, cos_ref[rows, :], -sin_ref[rows, :], head_dim).astype(BF16)
        gv_ref[rows, :] = values_grad.astype(BF16)
    gq_ref[...] = turn(gq_acc[...] * scale, cos_ref[...], -sin_ref[...], head_dim).astype(BF16)


def attend_backward(queries, keys, values, mixed, grad_mixed, lse, cosine, sine, length, head_dim):
    tokens, width = queries.shape
    seqs, pairs, heads = tokens // length, width // LANES, LANES // head_dim
    block = min(256, length)
    rows = pl.BlockSpec((length, LANES), lambda s, p: (s, p))
    table = whole((length, LANES))
    return call(
        functools.partial(attend_backward_kernel, head_dim, block),
        (seqs, pairs),
        [rows] * 5 + [pl.BlockSpec((8 * heads, length), lambda s, p: (s * pairs + p, 0)), table, table],
        [rows] * 3,
        [shape_of((tokens, width), BF16)] * 3,
        scratch=[pltpu.VMEM((length, LANES), F32)],
        flops=10 * tokens * length * width,
        moved=16 * tokens * width,
        trans=tokens * length * width // head_dim // 2,
    )(queries, keys, values, mixed, grad_mixed, lse, cosine, sine)


def square(width, part):
    return pl.BlockSpec((width, width), lambda i: (0, part), pipeline_mode=pl.Buffered(1))


def norm_one_kernel(x_ref, gain_ref, out_ref):
    x = x_ref[...].astype(F32)
    scale = lax.rsqrt(jnp.mean(x * x, axis=1, keepdims=True) + EPSILON)
    out_ref[...] = (x * scale * gain_ref[...]).astype(BF16)


def norm_one(tokens, gain):
    rows, width = tokens.shape
    block = min(256, rows)
    blocked = pl.BlockSpec((block, width), lambda i: (i, 0))
    return call(
        norm_one_kernel, (rows // block,), [blocked, whole((1, width))], blocked, shape_of((rows, width), BF16),
        flops=5 * rows * width, moved=4 * rows * width,
    )(tokens, gain)


def norm_two_kernel(mixed_ref, tokens_ref, weight_ref, gain_ref, sum_ref, normed_ref):
    first_sum = tokens_ref[...].astype(F32) + dot_nn(mixed_ref[...], weight_ref[...])
    sum_ref[...] = first_sum
    scale = lax.rsqrt(jnp.mean(first_sum * first_sum, axis=1, keepdims=True) + EPSILON)
    normed_ref[...] = (first_sum * scale * gain_ref[...]).astype(BF16)


def norm_two(mixed, tokens, weight, gain):
    rows, width = tokens.shape
    block = min(256, rows)
    blocked = pl.BlockSpec((block, width), lambda i: (i, 0))
    return call(
        norm_two_kernel, (rows // block,), [blocked, blocked, square(width, 3), whole((1, width))],
        [blocked, blocked], [shape_of((rows, width), F32), shape_of((rows, width), BF16)],
        flops=2 * rows * width * width, moved=10 * rows * width,
    )(mixed, tokens, weight, gain)


def slots_kernel(experts, parts, capacity, routes_ref, live_ref, rows_ref, columns_ref):
    top, tokens = routes_ref.shape
    live = live_ref[...]
    number = lax.broadcasted_iota(jnp.int32, (experts, tokens), 0)
    hits = [
        jnp.where((routes_ref[pl.ds(k, 1), :] == number) & (live > 0), 1.0, 0.0) for k in range(top)
    ]
    earlier = jnp.where(
        lax.broadcasted_iota(jnp.int32, (tokens, tokens), 0)
        <= lax.broadcasted_iota(jnp.int32, (tokens, tokens), 1),
        1.0,
        0.0,
    ).astype(BF16)
    ranks = dot_nn(jnp.concatenate(hits, axis=0).astype(BF16), earlier)
    before = jnp.zeros((experts, 1), F32)
    expert = lax.broadcasted_iota(jnp.int32, (experts, tokens), 0)
    start = ((expert % parts) * (experts // parts) + expert // parts) * capacity
    found = []
    for k in range(top):
        rank = ranks[k * experts : (k + 1) * experts, :] + before - 1.0
        for first in (number * capacity, start):
            slot = jnp.sum(hits[k] * (first.astype(F32) + rank), axis=0, keepdims=True).astype(jnp.int32)
            found.append(jnp.where(live > 0, slot, experts * capacity))
        before = before + jnp.sum(hits[k], axis=1, keepdims=True)
    table = jnp.concatenate(found[0::2] + found[1::2] + [jnp.zeros((8 - 2 * top, tokens), jnp.int32)], axis=0)
    rows_ref[...] = table
    columns_ref[...] = table.T


def slots_of(routes_t, live_row, experts, parts, capacity):
    top, tokens = routes_t.shape
    return call(
        functools.partial(slots_kernel, experts, parts, capacity), (1,),
        [whole((top, tokens)), whole((1, tokens))], [whole((8, tokens)), whole((tokens, 8))],
        [shape_of((8, tokens), jnp.int32), shape_of((tokens, 8), jnp.int32)],
        flops=2 * top * experts * tokens * tokens, moved=16 * tokens,
    )(routes_t, live_row)


def dispatch_kernel(gated, first, base, dest_ref, gates_ref, x_ref, out_ref):
    top, tokens = gates_ref.shape
    capacity = out_ref.shape[0]
    slot = lax.broadcasted_iota(jnp.int32, (capacity, tokens), 0) + (first + pl.program_id(0)) * capacity
    hits = [slot == dest_ref[pl.ds(base + k, 1), :] for k in range(top)]
    chosen = functools.reduce(jnp.logical_or, hits)
    rows = dot_nn(jnp.where(chosen, 1.0, 0.0).astype(BF16), x_ref[...])
    if gated:
        weights = jnp.zeros((capacity, tokens), F32)
        for k in range(top):
            weights = jnp.where(hits[k], gates_ref[pl.ds(k, 1), :], weights)
        rows = rows * jnp.sum(weights, axis=1, keepdims=True)
    out_ref[...] = rows.astype(BF16)


def dispatch(dest_t, gates_t, x, experts, capacity, gated, first, base):
    top, tokens = gates_t.shape
    width = x.shape[1]
    return call(
        functools.partial(dispatch_kernel, gated, first, base), (experts,),
        [whole(dest_t.shape), whole((top, tokens)), whole((tokens, width))],
        pl.BlockSpec((capacity, width), lambda e: (e, 0)),
        shape_of((experts * capacity, width), BF16),
        flops=2 * experts * capacity * tokens * width, moved=2 * (experts * capacity + tokens) * width,
    )(dest_t, gates_t, x)


def unpack(source, start, rows, panels, target):
    for p in range(panels):
        target[:, pl.ds(p * LANES, LANES)] = source[pl.ds(start + p * rows, rows), :].astype(F32)


def combine_kernel(dest_ref, gates_ref, live_ref, sum_ref, shared_ref, y_ref, out_ref):
    block, top = gates_ref.shape
    total = sum_ref[...] + shared_ref[...]
    dest = dest_ref[...]
    gates = gates_ref[...]
    slot = slot_numbers(block, y_ref.shape[0], 0)
    for k in range(top):
        hit = jnp.where(slot == dest[:, k : k + 1], 1.0, 0.0).astype(BF16)
        total = total + dot_nn(hit, y_ref[...]) * gates[:, k : k + 1]
    out_ref[...] = (live_ref[...] * total).astype(BF16)


def combine(dest, gates, live, first_sum, shared_out, returned):
    rows, width = first_sum.shape
    top = gates.shape[1]
    block = min(256, rows)
    blocked = pl.BlockSpec((block, width), lambda i: (i, 0))
    slots = returned.shape[0]
    return call(
        combine_kernel, (rows // block,),
        [pl.BlockSpec((block, dest.shape[1]), lambda i: (i, 0)), pl.BlockSpec((block, top), lambda i: (i, 0)),
         pl.BlockSpec((block, 1), lambda i: (i, 0)), blocked, blocked, whole(returned.shape)],
        blocked, shape_of((rows, width), BF16),
        flops=4 * rows * slots * width, moved=10 * rows * width + 2 * slots * width,
    )(dest, gates, live, first_sum, shared_out, returned)


def unpack(source, start, rows, panels, target):
    for p in range(panels):
        target[:, pl.ds(p * LANES, LANES)] = source[pl.ds(start + p * rows, rows), :].astype(F32)


def gather_kernel(axis, count, many, *refs):
    pieces, outs, landed, sems = refs[:many], refs[many : 2 * many], refs[2 * many : 3 * many], refs[3 * many :]
    barrier = pltpu.get_barrier_semaphore()
    pl.semaphore_wait(barrier, greet_neighbours(barrier, axis, count))
    gathers = [
        LineGather(axis, count, landed[i], sems[2 * i], sems[2 * i + 1], 0, 1) for i in range(many)
    ]
    for gather, piece in zip(gathers, pieces):
        gather.start(piece[...])
    for k in range(1, count):
        for gather in gathers:
            gather.relay(k)
    for gather, out, rows in zip(gathers, outs, landed):
        gather.finish()
        out[...] = rows[...]


def gather_over(pieces, axis, count, collective_id):
    shapes = [(count * piece.shape[0], LANES) for piece in pieces]
    vmem = pl.BlockSpec(memory_space=pltpu.VMEM)
    size = sum(shape[0] for shape in shapes) * LANES
    return pl.pallas_call(
        functools.partial(gather_kernel, axis, count, len(pieces)),
        out_shape=[shape_of(shape, BF16) for shape in shapes],
        in_specs=[vmem] * len(pieces),
        out_specs=[vmem] * len(pieces),
        scratch_shapes=[pltpu.VMEM(shape, BF16) for shape in shapes]
        + [pltpu.SemaphoreType.DMA((2, count))] * (2 * len(pieces)),
        compiler_params=pltpu.CompilerParams(collective_id=collective_id, has_side_effects=True),
        cost_estimate=pl.CostEstimate(flops=size, bytes_accessed=40 * size, transcendentals=0),
    )(*pieces)


def lay_out_kernel(parts, pack_ref, egu_ref, ed_ref):
    step = pl.program_id(0)
    width = ed_ref.shape[2]
    packed = pack_ref.shape[0] // parts
    e_panels, e_rows = egu_ref.shape[2] // LANES, egu_ref.shape[1]
    for e in range(parts):
        for p in range(e_panels):
            rows = pl.ds(pl.multiple_of(e * packed + p * width + step * e_rows, 16), e_rows)
            egu_ref[e, :, pl.ds(p * LANES, LANES)] = pack_ref[rows, :].astype(F32)

    @pl.when(step == 0)
    def _():
        for e in range(parts):
            unpack(pack_ref, e * packed + e_panels * width, ed_ref.shape[1], width // LANES, ed_ref.at[e])


def lay_out(pack, parts, own, width, hidden):
    group, steps = width // own, 4
    columns = 2 * hidden // group
    outs = [(parts, width, columns), (parts, hidden // group, width)]
    return call(
        functools.partial(lay_out_kernel, parts), (steps,), [whole(pack.shape)],
        [pl.BlockSpec((parts, width // steps, columns), lambda i: (0, i, 0)), whole(outs[1])],
        [shape_of(shape, F32) for shape in outs],
        flops=pack.size, moved=6 * pack.size,
    )(pack)


def lay_out_last_kernel(own, gu_panels, x_ref, shared_ref, qkv_ref, wo_ref, gain_ref, sgu_ref, sd_ref):
    panels = wo_ref.shape[1] // LANES
    unpack(x_ref, 0, own, 3 * panels, qkv_ref)
    unpack(x_ref, 3 * panels * own, own, panels, wo_ref)
    gain_ref[...] = x_ref[pl.ds(4 * panels * own, gain_ref.shape[0]), :].astype(F32)
    unpack(shared_ref, 0, own, gu_panels, sgu_ref)
    unpack(shared_ref, gu_panels * own, sd_ref.shape[0], panels, sd_ref)


def lay_out_last(x, shared, own, width, hidden):
    outs = [(own, 3 * width), (own, width), (8, LANES), (own, 2 * hidden), (hidden // (width // own), width)]
    return call(
        functools.partial(lay_out_last_kernel, own, 2 * hidden // LANES), (1,), [whole(x.shape), whole(shared.shape)],
        [whole(shape) for shape in outs], [shape_of(shape, F32) for shape in outs],
        flops=x.size, moved=6 * (x.size + shared.size),
    )(x, shared)


def slot_numbers(block, slots, part):
    return lax.broadcasted_iota(jnp.int32, (block, slots), 1) + part * slots


def gathered(top, dest_ref, y_ref, part):
    block = dest_ref.shape[0]
    dest = dest_ref[:, top : 2 * top]
    slot = slot_numbers(block, y_ref.shape[0], part)
    hit = functools.reduce(jnp.logical_or, [slot == dest[:, k : k + 1] for k in range(top)])
    return dot_nn(jnp.where(hit, 1.0, 0.0).astype(BF16), y_ref[...])


class Exchange:
    def __init__(self, axis, count, sent_ref, kept_ref, own_sem, send_sem, recv_sem):
        self.axis, self.count = axis, count
        me = lax.axis_index(axis)
        self.peers = [lax.rem(me + ahead, count) for ahead in range(1, count)]
        self.me, self.sent_ref, self.kept_ref = me, sent_ref, kept_ref
        self.own_sem, self.send_sem, self.recv_sem = own_sem, send_sem, recv_sem

    def copies(self):
        out = [pltpu.make_async_copy(self.sent_ref.at[self.me], self.kept_ref.at[self.me], self.own_sem)]
        for index, peer in enumerate(self.peers):
            out.append(
                pltpu.make_async_remote_copy(
                    src_ref=self.sent_ref.at[peer], dst_ref=self.kept_ref.at[self.me],
                    send_sem=self.send_sem.at[index], recv_sem=self.recv_sem.at[index],
                    device_id={self.axis: peer}, device_id_type=pl.DeviceIdType.MESH,
                )
            )
        return out

    def start(self):
        barrier = pltpu.get_barrier_semaphore()
        for peer in self.peers:
            pl.semaphore_signal(barrier, inc=1, device_id={self.axis: peer}, device_id_type=pl.DeviceIdType.MESH)
        pl.semaphore_wait(barrier, self.count - 1)
        for copy in self.copies():
            copy.start()

    def wait(self):
        for copy in self.copies():
            copy.wait()

    @staticmethod
    def scratch(count):
        sems = pltpu.SemaphoreType.DMA((count - 1,))
        return [pltpu.SemaphoreType.DMA, sems, sems]


def add_part_kernel(part, top, axis, count, dest_ref, base_ref, y_ref, sent_ref, out_ref, kept_ref, *sems):
    exchange = Exchange(axis, count, sent_ref, kept_ref, *sems)

    @pl.when(pl.program_id(0) == 0)
    def _():
        exchange.start()

    out_ref[...] = base_ref[...] + gathered(top, dest_ref, y_ref, part)

    @pl.when(pl.program_id(0) == pl.num_programs(0) - 1)
    def _():
        exchange.wait()


def add_part(top, dest, base, rows_of, part, sent, axis, count, collective_id):
    rows, width = base.shape
    block = min(256, rows)
    blocked = pl.BlockSpec((block, width), lambda i: (i, 0))
    hbm = pl.BlockSpec(memory_space=pl.ANY)
    sent = sent.reshape(count, -1, width)
    out, kept = call(
        functools.partial(add_part_kernel, part, top, axis, count), (rows // block,),
        [pl.BlockSpec((block, dest.shape[1]), lambda i: (i, 0)), blocked, whole(rows_of.shape), hbm],
        [blocked, hbm], [shape_of((rows, width), F32), shape_of(sent.shape, BF16)],
        scratch=Exchange.scratch(count),
        flops=2 * rows * rows_of.shape[0] * width, moved=8 * rows * width, collective_id=collective_id,
    )(dest, base, rows_of, sent)
    return out, kept.reshape(-1, width)


def norm_two_back_kernel(part, top, dest_ref, live_ref, cot_ref, sum_ref, base_ref, gain_ref, weight_ref, y_ref,
                         first_ref, attn_ref, mixed_ref, gain_grad_ref):
    grad_normed = base_ref[...] + gathered(top, dest_ref, y_ref, part)
    first_sum = sum_ref[...]
    scale = lax.rsqrt(jnp.mean(first_sum * first_sum, axis=1, keepdims=True) + EPSILON)
    weighted = grad_normed * gain_ref[...]
    inner = jnp.mean(first_sum * weighted, axis=1, keepdims=True)
    grad_first = (
        cot_ref[...].astype(F32) * live_ref[...] + scale * weighted - first_sum * (scale * scale * scale * inner)
    )
    first_ref[...] = grad_first
    grad_attn = grad_first.astype(BF16)
    attn_ref[...] = grad_attn
    mixed_ref[...] = dot_nt(grad_attn, weight_ref[...]).astype(BF16)

    @pl.when(pl.program_id(0) == 0)
    def _():
        gain_grad_ref[...] = jnp.zeros_like(gain_grad_ref)

    gain_grad_ref[...] += jnp.sum(grad_normed * first_sum * scale, axis=0, keepdims=True)


def norm_two_back(top, dest, live, cotangent, first_sum, base, gain, weights, rows_of, part):
    rows, width = first_sum.shape
    block = min(256, rows)
    blocked = pl.BlockSpec((block, width), lambda i: (i, 0))
    return call(
        functools.partial(norm_two_back_kernel, part, top), (rows // block,),
        [pl.BlockSpec((block, dest.shape[1]), lambda i: (i, 0)), pl.BlockSpec((block, 1), lambda i: (i, 0)), blocked, blocked,
         blocked, whole((1, width)), square(width, 3), whole(rows_of.shape)],
        [blocked, blocked, blocked, pl.BlockSpec((1, width), lambda i: (0, 0))],
        [shape_of((rows, width), F32), shape_of((rows, width), BF16), shape_of((rows, width), BF16),
         shape_of((1, width), F32)],
        flops=2 * rows * (rows_of.shape[0] + width) * width, moved=18 * rows * width,
    )(dest, live, cotangent, first_sum, base, gain, weights, rows_of)


def line_copy(axis, ahead, source, target, send_sem, recv_sem):
    return pltpu.make_async_remote_copy(
        src_ref=source, dst_ref=target, send_sem=send_sem, recv_sem=recv_sem,
        device_id={axis: lax.axis_index(axis) + ahead}, device_id_type=pl.DeviceIdType.MESH,
    )


class LineSum:
    def __init__(self, axis, count, x_ref, buffers, send_sem, recv_sem, turn, turns):
        self.axis, self.count, self.x_ref, self.buffers = axis, count, x_ref, buffers
        self.send_sem, self.recv_sem = send_sem, recv_sem
        self.rows, self.turn, self.turns = buffers.shape[3], turn, turns

    def own(self, piece):
        first = (piece * self.turns + self.turn) * self.rows
        return self.x_ref[pl.ds(pl.multiple_of(first, 16), self.rows), :].astype(F32)

    def copy(self, way, piece):
        return line_copy(
            self.axis, 1 - 2 * way, self.buffers.at[way, 1, piece], self.buffers.at[way, 0, piece],
            self.send_sem.at[way, piece], self.recv_sem.at[way, piece],
        )

    def each(self, body):
        me = lax.axis_index(self.axis)
        for k in range(self.count - 1):
            for way, piece in ((0, self.count - 1 - k), (1, k)):
                before = me > 0 if way == 0 else me < self.count - 1
                sends = me < piece if way == 0 else me > piece
                body(way, piece, before, sends)

    def start(self):
        def body(way, piece, before, sends):
            @pl.when(sends & jnp.logical_not(before))
            def _():
                self.buffers[way, 1, piece] = self.own(piece).astype(BF16)
                self.copy(way, piece).start()

        self.each(body)

    def relay(self):
        def body(way, piece, before, sends):
            @pl.when(sends & before)
            def _():
                self.copy(way, piece).wait_recv()
                self.buffers[way, 1, piece] = (self.own(piece) + self.buffers[way, 0, piece].astype(F32)).astype(BF16)
                self.copy(way, piece).start()

        self.each(body)

    def finish(self, total_ref):
        me = lax.axis_index(self.axis)
        total_ref[...] = self.own(me)
        for way, before in ((0, me > 0), (1, me < self.count - 1)):

            @pl.when(before)
            def _():
                self.copy(way, me).wait_recv()
                total_ref[...] += self.buffers[way, 0, me].astype(F32)

        def body(way, piece, before, sends):
            @pl.when(sends)
            def _():
                self.copy(way, piece).wait_send()

        self.each(body)


class LineGather:
    def __init__(self, axis, count, out_ref, send_sem, recv_sem, turn, turns):
        self.axis, self.count, self.out_ref = axis, count, out_ref
        self.send_sem, self.recv_sem = send_sem, recv_sem
        self.rows, self.turn, self.turns = out_ref.shape[0] // count // turns, turn, turns

    def place(self, piece):
        first = (piece * self.turns + self.turn) * self.rows
        return self.out_ref.at[pl.ds(pl.multiple_of(first, 16), self.rows), :]

    def copy(self, way, piece):
        return line_copy(
            self.axis, 1 - 2 * way, self.place(piece), self.place(piece),
            self.send_sem.at[way, piece], self.recv_sem.at[way, piece],
        )

    def start(self, value):
        me = lax.axis_index(self.axis)
        self.place(me)[...] = value
        for way, more in ((0, me < self.count - 1), (1, me > 0)):

            @pl.when(more)
            def _():
                self.copy(way, me).start()

    def relay(self, k):
        me = lax.axis_index(self.axis)
        for way, piece, there, more in (
            (0, me - k, me >= k, me < self.count - 1),
            (1, me + k, me + k < self.count, me > 0),
        ):

            @pl.when(there)
            def _():
                self.copy(way, piece).wait_recv()

            @pl.when(there & more)
            def _():
                self.copy(way, piece).start()

    def finish(self):
        me = lax.axis_index(self.axis)
        for k in range(self.count):
            for way, piece, sent in (
                (0, me - k, (me >= k) & (me < self.count - 1)),
                (1, me + k, (me + k < self.count) & (me > 0)),
            ):

                @pl.when(sent)
                def _():
                    self.copy(way, piece).wait_send()


def greet_neighbours(barrier, axis, count):
    me = lax.axis_index(axis)
    for ahead, there in ((1, me < count - 1), (-1, me > 0)):

        @pl.when(there)
        def _():
            pl.semaphore_signal(barrier, inc=1, device_id={axis: me + ahead}, device_id_type=pl.DeviceIdType.MESH)

    return (me < count - 1).astype(jnp.int32) + (me > 0).astype(jnp.int32)


def settle_kernel(sizes, gq_ref, gk_ref, gv_ref, wq_ref, wk_ref, wv_ref, tokens_ref, first_ref, gain_ref, pack_ref,
                  x_ref, out_ref, share_ref, piece_ref, own, landed, chosen, arrived, sem, pair_send, pair_recv, send_sem,
                  recv_sem, x_buffers, x_total, x_send, x_recv):
    dp_size, shard_size, count = sizes
    spread = shard_size // 2
    halves = dp_size * spread
    dp, shard = lax.axis_index("dp"), lax.axis_index("shard")
    side = shard % 2
    place = dp * spread + shard // 2
    step = pl.program_id(0)
    last = pl.num_programs(0) - 1

    def target(piece, bit):
        return {"dp": piece // spread, "shard": (piece % spread) * 2 + bit}

    line = LineSum("expert", count, x_ref, x_buffers, x_send, x_recv, 0, 1)

    def pair_copy():
        return pltpu.make_async_remote_copy(
            src_ref=pack_ref.at[:, 1 - side], dst_ref=landed, send_sem=pair_send, recv_sem=pair_recv,
            device_id=target(place, 1 - side), device_id_type=pl.DeviceIdType.MESH,
        )

    def own_copy():
        return pltpu.make_async_copy(pack_ref.at[:, side], own, sem)

    def send(index):
        return pltpu.make_async_remote_copy(
            src_ref=chosen.at[index], dst_ref=arrived.at[index], send_sem=send_sem.at[index], recv_sem=recv_sem.at[index],
            device_id=target(lax.rem(place + index + 1, halves), side), device_id_type=pl.DeviceIdType.MESH,
        )

    @pl.when(step == 0)
    def _():
        barrier = pltpu.get_barrier_semaphore()
        pl.semaphore_signal(barrier, inc=1, device_id=target(place, 1 - side), device_id_type=pl.DeviceIdType.MESH)
        for index in range(halves - 1):
            pl.semaphore_signal(
                barrier, inc=1, device_id=target(lax.rem(place + index + 1, halves), side),
                device_id_type=pl.DeviceIdType.MESH,
            )
        neighbours = greet_neighbours(barrier, "expert", count)
        pl.semaphore_wait(barrier, halves + neighbours)
        pair_copy().start()
        own_copy().start()
        line.start()

    @pl.when(step == 1)
    def _():
        own_copy().wait()
        pair_copy().wait()
        for index in range(halves - 1):
            piece = lax.rem(place + index + 1, halves)
            chosen[index] = (own[piece].astype(F32) + landed[piece].astype(F32)).astype(BF16)
            send(index).start()

    grad_normed = (
        dot_nt(gq_ref[...], wq_ref[...]) + dot_nt(gk_ref[...], wk_ref[...]) + dot_nt(gv_ref[...], wv_ref[...])
    )
    source = tokens_ref[...].astype(F32)
    scale = lax.rsqrt(jnp.mean(source * source, axis=1, keepdims=True) + EPSILON)
    weighted = grad_normed * gain_ref[...]
    inner = jnp.mean(source * weighted, axis=1, keepdims=True)
    out_ref[...] = first_ref[...] + scale * weighted - source * (scale * scale * scale * inner)

    @pl.when(step == last)
    def _():
        line.relay()
        total = own[place].astype(F32) + landed[place].astype(F32)
        for index in range(halves - 1):
            send(index).wait()
            total = total + arrived[index].astype(F32)
        share_ref[...] = total.astype(BF16)
        line.finish(x_total)
        piece_ref[...] = x_total[...].astype(BF16)


def settle(grads, w_qkv, tokens, grad_first, gain, pack, x, sizes):
    rows, width = tokens.shape
    block = min(256, rows)
    blocked = pl.BlockSpec((block, width), lambda i: (i, 0))
    halves, count = sizes[0] * sizes[1] // 2, pack.shape[1]
    piece = (count, LANES)
    x_piece = (x.shape[0] // sizes[2], LANES)
    return call(
        functools.partial(settle_kernel, sizes), (rows // block,),
        [blocked] * 3 + [square(width, 0), square(width, 1), square(width, 2), blocked, blocked, whole((1, width)),
                         pl.BlockSpec(memory_space=pl.ANY), whole(x.shape)],
        [blocked, whole(piece), whole(x_piece)],
        [shape_of((rows, width), F32), shape_of(piece, BF16), shape_of(x_piece, BF16)],
        scratch=[pltpu.VMEM((halves,) + piece, BF16), pltpu.VMEM((halves,) + piece, BF16),
                 pltpu.VMEM((halves - 1,) + piece, BF16), pltpu.VMEM((halves - 1,) + piece, BF16),
                 pltpu.SemaphoreType.DMA, pltpu.SemaphoreType.DMA, pltpu.SemaphoreType.DMA,
                 pltpu.SemaphoreType.DMA((halves - 1,)), pltpu.SemaphoreType.DMA((halves - 1,)),
                 pltpu.VMEM((2, 2, sizes[2]) + x_piece, BF16), pltpu.VMEM(x_piece, F32)]
        + [pltpu.SemaphoreType.DMA((2, sizes[2]))] * 2,
        flops=6 * rows * width * width, moved=22 * rows * width, collective_id=1,
    )(*grads, w_qkv, w_qkv, w_qkv, tokens, grad_first, gain, pack.reshape((halves, 2) + piece), x)


def copies_of(layout, block, width, step, stage_g, stage_u, stage_d, slot, packed_ref, sems):
    by_rows, owners, hidden, base = layout
    panels = block // LANES
    rows_down = hidden // owners
    out = []

    def add(source, target):
        out.append(pltpu.make_async_copy(source, target, sems.at[slot, len(out)]))

    if by_rows:
        rows = width // owners
        for half, stage in enumerate((stage_g, stage_u)):
            for p in range(panels):
                panel = half * (hidden // LANES) + step * panels + p
                add(
                    stage.at[slot, :, :, pl.ds(p * LANES, LANES)],
                    packed_ref.at[:, pl.ds(pl.multiple_of(base + panel * rows, 8), rows), :],
                )
        start = 2 * hidden // LANES * rows
    else:
        columns = 2 * hidden // owners
        for half, stage in enumerate((stage_g, stage_u)):
            for p in range(panels):
                column = half * hidden + step * block + p * LANES
                owner, panel = column // columns, (column % columns) // LANES
                add(
                    stage.at[slot, :, pl.ds(p * LANES, LANES)],
                    packed_ref.at[owner, pl.ds(pl.multiple_of(base + panel * width, 8), width), :],
                )
        start = columns // LANES * width
    for q in range(block // rows_down):
        owner = step * (block // rows_down) + q
        for c in range(width // LANES):
            add(
                stage_d.at[slot, pl.ds(q * rows_down, rows_down), pl.ds(c * LANES, LANES)],
                packed_ref.at[owner, pl.ds(base + start + c * rows_down, rows_down), :],
            )
    return out


def packed_rows(width, hidden, owners):
    return 3 * width * hidden // owners // LANES


def ffn_kernel(out_type, layout, block, first, axis, count, x_ref, gy_ref, wg_ref, wu_ref, wd_ref, sent_ref, *rest):
    (y_ref, gx_ref, packed_ref, kept_ref, x_own, gy_own, xt, y_acc, gx_acc, stage_g, stage_u, stage_d, sems, load_sems,
     *exchange_sems) = rest[-17:]
    exchange = Exchange(axis, count, sent_ref, kept_ref, *exchange_sems)
    step = pl.program_id(0)
    steps = layout[2] // block
    width = x_ref.shape[1]
    slot = step % 2
    copies = functools.partial(copies_of, layout, block, width)

    @pl.when(step == 0)
    def _():
        exchange.start()
        gy_source = gy_ref if first is None else gy_ref.at[:, pl.ds(first, gy_own.shape[1]), :]
        loads = [
            pltpu.make_async_copy(x_ref, x_own, load_sems.at[0]),
            pltpu.make_async_copy(gy_source, gy_own, load_sems.at[1]),
        ]
        for load in loads:
            load.start()
        for load in loads:
            load.wait()
        xt[...] = x_own[...].T
        y_acc[...] = jnp.zeros_like(y_acc)
        gx_acc[...] = jnp.zeros_like(gx_acc)

    @pl.when(step >= 2)
    def _():
        for copy in copies(step - 2, stage_g, stage_u, stage_d, slot, packed_ref, sems):
            copy.wait()

    x, gy = x_own[...], gy_own[...].reshape(x_ref.shape)
    if layout[0]:
        wg, wu = wg_ref[...].reshape(width, block), wu_ref[...].reshape(width, block)
        rows = wd_ref.shape[1] // (width // block)
        wd = jnp.concatenate(
            [wd_ref[:, pl.ds(c * rows, rows), :].reshape(block, block) for c in range(width // block)], axis=1
        )
    else:
        wg, wu, wd = wg_ref[...], wu_ref[...], wd_ref[...]
    gate, up = dot_nn(x, wg), dot_nn(x, wu)
    grad_hidden = dot_nt(gy, wd)
    sigmoid = jax.nn.sigmoid(gate)
    value = gate * sigmoid
    hidden = (value * up).astype(BF16)
    grad_up = (grad_hidden * value).astype(BF16)
    grad_gate = (grad_hidden * up * (sigmoid * (1.0 + gate * (1.0 - sigmoid)))).astype(BF16)
    y_acc[...] += dot_nn(hidden, wd)
    gx_acc[...] += dot_nt(grad_gate, wg) + dot_nt(grad_up, wu)
    stage_g[slot] = dot_nn(xt[...], grad_gate).astype(BF16).reshape(stage_g.shape[1:])
    stage_u[slot] = dot_nn(xt[...], grad_up).astype(BF16).reshape(stage_u.shape[1:])
    stage_d[slot] = dot_tn(hidden, gy).astype(BF16)
    for copy in copies(step, stage_g, stage_u, stage_d, slot, packed_ref, sems):
        copy.start()

    @pl.when(step == steps - 1)
    def _():
        exchange.wait()
        y_ref[...] = y_acc[...].astype(out_type).reshape(y_ref.shape)
        gx_ref[...] = gx_acc[...].astype(out_type)
        for back in (1, 0):
            if steps > back:
                for copy in copies(steps - 1 - back, stage_g, stage_u, stage_d, (steps - 1 - back) % 2, packed_ref, sems):
                    copy.wait()


BLOCK = 256


def ffn_both(x, gy, w_gu, w_down, hidden, expert, owners, out_type, sent, axis, count, collective_id, parts=1, held=()):
    rows, width = x.shape
    block = BLOCK
    steps = hidden // block
    by_rows = expert is None
    if by_rows:
        own, own_down, panels = width // owners, hidden // owners, width // block
        ahead = 2 * steps * own // (panels * own_down)
        gate = pl.BlockSpec((owners, own, block), lambda f: (0, f, 0))
        up = pl.BlockSpec((owners, own, block), lambda f: (0, steps + f, 0))
        down = pl.BlockSpec((block // own_down, panels * own_down, block), lambda f: (f, ahead, 0))
        stage = (2, owners, own, block)
    else:
        gate = pl.BlockSpec((None, width, block), lambda f: (expert, 0, f))
        up = pl.BlockSpec((None, width, block), lambda f: (expert, 0, steps + f))
        down = pl.BlockSpec((None, block, width), lambda f: (expert, f, 0))
        stage = (2, width, block)
    if by_rows:
        first, gy_shape = None, (rows, width)
        y_block, y_shape = whole((rows, width)), (rows, width)
    else:
        y_shape = (gy.shape[0], parts * (rows // gy.shape[0]), width)
        y_block = pl.BlockSpec(
            (gy.shape[0], rows // gy.shape[0], width), lambda f: (0, expert, 0), pipeline_mode=pl.Buffered(1)
        )
        first, gy_shape = expert * (rows // gy.shape[0]), (gy.shape[0], rows // gy.shape[0], width)
    out_rows = whole((rows, width))
    pack_rows = packed_rows(width, hidden, owners)
    layout = (by_rows, owners, hidden, (expert or 0) * pack_rows)
    hbm = pl.BlockSpec(memory_space=pl.ANY)
    sent = sent.reshape(count, -1, width)
    copies = 2 * (block // LANES) + block // (hidden // owners) * (width // LANES)
    y, gx, pack, kept = call(
        functools.partial(ffn_kernel, out_type, layout, block, first, axis, count), (steps,),
        [hbm, hbm, gate, up, down, hbm] + [hbm] * len(held),
        [y_block, out_rows, hbm, hbm],
        [shape_of(y_shape, out_type), shape_of((rows, width), out_type),
         shape_of((owners, parts * pack_rows, LANES), BF16), shape_of(sent.shape, BF16)],
        scratch=[pltpu.VMEM((rows, width), BF16), pltpu.VMEM(gy_shape, BF16),
                 pltpu.VMEM((width, rows), BF16), pltpu.VMEM((rows, width), F32), pltpu.VMEM((rows, width), F32),
                 pltpu.VMEM(stage, BF16), pltpu.VMEM(stage, BF16), pltpu.VMEM((2, block, width), BF16),
                 pltpu.SemaphoreType.DMA((2, copies)), pltpu.SemaphoreType.DMA((2,))] + Exchange.scratch(count),
        flops=18 * rows * width * hidden, moved=12 * width * hidden + 16 * rows * width, trans=rows * hidden,
        aliases={6: 0, 7: 2} if held else None, collective_id=collective_id,
    )(x, gy, w_gu, w_gu, w_down, sent, *held)
    return y, gx, pack, kept.reshape(-1, width)


def to_panels(array):
    rows, columns = array.shape
    return jnp.transpose(array.reshape(rows, columns // BLOCK, BLOCK), (1, 0, 2)).reshape(-1, BLOCK)


def attention_weights_kernel(per, normed_ref, mixed_ref, gq_ref, gk_ref, gv_ref, ga_ref, gains_ref, out_ref, xt):
    step = pl.program_id(0)
    owners, rows = out_ref.shape[0], out_ref.shape[1] // (out_ref.shape[1] // (normed_ref.shape[1] // out_ref.shape[0]))
    panels = out_ref.shape[1] // rows

    @pl.when(step == 0)
    def _():
        xt[...] = normed_ref[...].T

    @pl.when(step == 3 * per)
    def _():
        xt[...] = mixed_ref[...].T

    for index, grad_ref in enumerate((gq_ref, gk_ref, gv_ref, ga_ref)):

        @pl.when((step >= index * per) & (step < (index + 1) * per))
        def _():
            product = dot_nn(xt[...], grad_ref[...]).astype(BF16)
            for p in range(panels):
                out_ref[:, pl.ds(p * rows, rows), :] = product[:, p * LANES : (p + 1) * LANES].reshape(owners, rows, LANES)

    @pl.when(step >= 4 * per)
    def _():
        out_ref[...] = jnp.zeros_like(out_ref)

    @pl.when(step == 4 * per)
    def _():
        out_ref[:, pl.ds(0, gains_ref.shape[1]), :] = gains_ref[...]


def attention_weights(normed, mixed, grads, grad_attn, gains, owners, pieces):
    tokens, width = normed.shape
    rows = width // owners
    block = BLOCK
    panels, per = block // LANES, width // block
    steps = 4 * per + 1
    while steps * panels * rows % (16 * pieces):
        steps += 1

    def columns(index):
        return pl.BlockSpec((tokens, block), lambda i: (0, jnp.clip(i - index * per, 0, per - 1)))

    return call(
        functools.partial(attention_weights_kernel, per), (steps,),
        [whole((tokens, width)), whole((tokens, width))] + [columns(index) for index in range(4)] + [whole(gains.shape)],
        pl.BlockSpec((owners, panels * rows, LANES), lambda i: (0, i, 0)),
        shape_of((owners, steps * panels * rows, LANES), BF16),
        scratch=[pltpu.VMEM((width, tokens), BF16)],
        flops=8 * tokens * width * width, moved=16 * tokens * width,
    )(normed, mixed, *grads, grad_attn, gains)


GROUP = ("dp", "shard")


def local(
    tokens,
    lengths,
    routes,
    route_gates,
    cotangent,
    norm_gains,
    w_qkv,
    w_out,
    w_shared_gu,
    w_shared_down,
    w_expert_gu,
    w_expert_down,
):
    tok_count, width = tokens.shape
    seq_count = lengths.shape[0]
    length = tok_count // seq_count
    local_experts = w_expert_gu.shape[0]
    owners = lax.axis_size("expert")
    experts = local_experts * owners
    top = routes.shape[1]
    capacity = tok_count * top * 9 // (8 * experts)
    head_dim = width // HEADS
    hidden = w_expert_down.shape[1]

    gains = lax.all_gather(norm_gains, GROUP, axis=1, tiled=True).astype(F32)
    attention_weight = lax.all_gather(jnp.concatenate([w_qkv, w_out], axis=1), GROUP, axis=0, tiled=True)
    shared_weight = lax.all_gather(
        jnp.concatenate([to_panels(w_shared_gu), to_panels(w_shared_down)], axis=0)[None], GROUP, axis=0, tiled=True
    )
    gain_one, gain_two = gains[0:1], gains[1:2]

    live_bool = lax.iota(jnp.int32, tok_count) % length < jnp.repeat(lengths, length)
    live = live_bool.astype(F32)[:, None]
    live_row = live_bool.astype(jnp.int32)[None, :]

    group = lax.axis_size("dp") * lax.axis_size("shard")
    shared_hidden = w_shared_down.shape[0] * group

    table_t, table = slots_of(routes.T, live_row, experts, local_experts, capacity)
    gates_t = route_gates.T
    grad_b = jnp.where(live_bool[:, None], cotangent, 0).astype(BF16)

    def exchange(rows):
        return lax.all_to_all(
            rows.reshape(owners, -1, width), "expert", split_axis=0, concat_axis=0, tiled=True
        ).reshape(rows.shape)

    send_grad = dispatch(table_t, gates_t, cotangent, experts, capacity, True, 0, 0)
    received_grad = exchange(send_grad).reshape(owners, local_experts * capacity, width)

    cosine, sine = rotary_tables(length, head_dim)
    normed_one = norm_one(tokens, gain_one)
    queries, keys, values, mixed, lse = attend_forward(normed_one, attention_weight, cosine, sine, length, head_dim)
    first_sum, normed_two = norm_two(mixed, tokens, attention_weight, gain_two)

    send_rows = []
    for j in range(local_experts):
        send_rows.append(dispatch(table_t, gates_t, normed_two, owners, capacity, False, j * owners, top))
    shared_out, grad_shared, shared_pack, received = ffn_both(
        normed_two, grad_b, shared_weight, shared_weight, shared_hidden, None, group, F32,
        send_rows[0], "expert", owners, 3,
    )
    waiting = send_rows[1:]
    back_rows, base, held = [], grad_shared, ()
    for j in range(local_experts):
        y, gx, pack, arrived = ffn_both(
            received, received_grad, w_expert_gu, w_expert_down, hidden, j, group, BF16,
            waiting.pop(0), "expert", owners, 4 + j, local_experts, held,
        )
        held = (y, pack)
        waiting.append(gx)
        if j < local_experts - 1:
            received = arrived
        else:
            back_rows.append(arrived)
    for j, sent in enumerate(waiting):
        base, arrived = add_part(
            top, table, base, back_rows[j], j, sent, "expert", owners, 4 + local_experts + j
        )
        back_rows.append(arrived)
    y, base = lax.optimization_barrier((y, base))
    grad_first, grad_attn, grad_mixed, grad_gain_two = norm_two_back(
        top, table, live, cotangent, first_sum, base, gain_two, attention_weight, back_rows[-1], local_experts - 1
    )

    grads = attend_backward(queries, keys, values, mixed, grad_mixed, lse, cosine, sine, length, head_dim)
    own = width // group
    grad_gains = grad_gain_two.reshape(group, 1, own)
    grad_gains = jnp.pad(grad_gains, ((0, 0), (0, 15), (0, LANES - own))).astype(BF16)
    attention_pack = attention_weights(normed_one, mixed, grads, grad_attn, grad_gains, group, owners)

    def spread(pack):
        return lax.psum_scatter(pack, GROUP, scatter_dimension=0, tiled=True)[0]

    shared_share = spread(shared_pack)
    expert_share = spread(pack)
    input_grad, attention_share, shared_piece = settle(
        grads, attention_weight, tokens, grad_first, gain_one, attention_pack, shared_share,
        (lax.axis_size("dp"), lax.axis_size("shard"), owners),
    )
    returned = exchange(y)
    pieces = lax.all_to_all(
        attention_share.reshape(owners, -1, LANES), "expert", split_axis=0, concat_axis=0, tiled=True
    )
    piece = jnp.sum(pieces.astype(F32), axis=0).astype(BF16)
    layer_out = combine(table, route_gates, live, first_sum, shared_out, returned.reshape(-1, width))
    expert_gu, expert_down = lay_out(expert_share, local_experts, own, width, hidden)
    attention_share, shared_share = gather_over([piece, shared_piece], "expert", owners, 2)
    qkv_grad, out_grad, gain_rows, shared_gu, shared_down = lay_out_last(
        attention_share, shared_share, own, width, shared_hidden
    )
    grad_gain_one = jnp.sum(w_qkv.astype(F32) * qkv_grad, axis=1) / norm_gains[0].astype(F32)
    grad_gains = jnp.stack([grad_gain_one, gain_rows[0, :own]])
    return layer_out, input_grad, grad_gains, qkv_grad, out_grad, shared_gu, shared_down, expert_gu, expert_down


def solution(mesh):
    rows = P(("dp", "expert", "shard"), None)
    split = P(GROUP, None)
    in_specs = (
        rows,
        P(("dp", "expert", "shard")),
        rows,
        rows,
        rows,
        P(None, GROUP),
        split,
        split,
        split,
        split,
        P("expert", None, None),
        P("expert", None, None),
    )
    out_specs = (
        rows,
        rows,
        P(None, GROUP),
        split,
        split,
        split,
        split,
        P("expert", None, GROUP),
        P("expert", GROUP, None),
    )

    return jax.shard_map(local, mesh=mesh, in_specs=in_specs, out_specs=out_specs, check_vma=False)
```
